32 devices in a mesh: grp: 2 (over y), gx: 4 (over z), gy: 2 (over x), gz: 2 (over core).
Axes of the slice: x: 2, y: 2, z: 4, core: 2. Of those that a mesh axis runs over, the one named last changes fastest.
Arguments:
- position: float32 [64, 16, 4, 256], P(None, ('grp', 'gx'), 'gy', 'gz'), parts along dimension 1, may hold values from -6 to 6
- momentum: float32 [64, 16, 4, 256], P(None, ('grp', 'gx'), 'gy', 'gz'), parts along dimension 1, may hold values from -6 to 6
- noise: bfloat16 [3, 64, 16, 4, 256], P(None, None, ('grp', 'gx'), 'gy', 'gz'), parts along dimension 2, may hold values from -6 to 6
- filter_in: bfloat16 [64, 64, 3, 3, 3], P('gx', 'gy'), may hold values from -0.15625 to 0.15625
- filter_out: bfloat16 [64, 64, 3, 3, 3], P('gx', 'gy'), may hold values from -0.15625 to 0.15625
- bias: float32 [64], replicated, may hold values from -4 to 4
Outputs:
- final_position: float32 [64, 16, 4, 256], P(None, ('grp', 'gx'), 'gy', 'gz'), parts along dimension 1
- final_momentum: float32 [64, 16, 4, 256], P(None, ('grp', 'gx'), 'gy', 'gz'), parts along dimension 1
The draws below stay inside these ranges and needn't reach their ends.
There are 2 independent parts, one for each index of `grp`. The reference program is written for one: setup_inputs(seed, part) draws one part's arguments, and reference() takes and returns one part's arrays. A program takes and returns all parts, laid end to end along the dimension named above; an argument that names none is the same for every part. Nothing has to cross between parts.
All inputs are finite; a program needn't handle non-finite values.
Results may differ from the reference program's by a relative error of at most 0.0013.
Values may be sent and summed in bfloat16 or wider, within the bound.
A program may use at most 64 MiB of HBM per device.

```python
import jax
import jax.numpy as jnp
from jax import lax

C = 64
STEPS = 3
NX = 8
NY = 4
NZ = 256


def block_scale(own_key, shape, pieces, smallest, top_value):
    def one(axis_at, parts):
        steps = jax.random.uniform(jax.random.fold_in(jax.random.fold_in(own_key, 6), axis_at), (parts,), jnp.float32, smallest / len(pieces), top_value / len(pieces))
        return jnp.repeat(jnp.exp(steps), shape[axis_at] // parts).reshape((-1,) + (1,) * (len(shape) - axis_at - 1))

    loudness = one(*pieces[0])
    for cut in pieces[1:]:
        loudness = loudness * one(*cut)
    return loudness


def scatter_about(key, dims, scale, most, pieces=(), kind=jnp.bfloat16):
    drawn = jax.random.normal(key, dims, jnp.float32) * scale
    if len(pieces) > 0:
        drawn = block_scale(key, dims, pieces, -0.22, 0.18) * drawn
    return jnp.clip(drawn, min=-most, max=most).astype(kind)


def setup_inputs(seed: int = 0, part: int = 0) -> dict:
    streams_of = jax.random.split(jax.random.key(seed), 7)
    part_splits = jax.random.split(jax.random.fold_in(streams_of[6], part), 7)
    position = scatter_about(part_splits[0], (C, NX, NY, NZ), 1.0, 6.0, ((1, 4), (2, 2), (3, 2)), jnp.float32)
    momentum = scatter_about(part_splits[1], (C, NX, NY, NZ), 1.0, 6.0, ((1, 4), (2, 2), (3, 2)), jnp.float32)
    noise = scatter_about(part_splits[2], (STEPS, C, NX, NY, NZ), 1.0, 6.0, ((2, 4), (3, 2), (4, 2)))
    filter_in = scatter_about(streams_of[3], (C, C, 3, 3, 3), (27 * C) ** -0.5, 0.15625, ((0, 4), (1, 2)))
    filter_out = scatter_about(streams_of[4], (C, C, 3, 3, 3), (27 * C) ** -0.5, 0.15625, ((0, 4), (1, 2)))
    bias = scatter_about(streams_of[5], (C,), 1.0, 4.0, (), jnp.float32)
    return {"position": position, "momentum": momentum, "noise": noise, "filter_in": filter_in, "filter_out": filter_out, "bias": bias}


def convolve(field, filters):
    padded = jnp.pad(field, ((0, 0), (1, 1), (1, 1), (1, 1)), mode='wrap')
    return lax.conv_general_dilated(padded[None], filters, (1, 1, 1), 'VALID', dimension_numbers=('NCDHW', 'OIDHW', 'NCDHW'), preferred_element_type=jnp.float32)[0]

def adjoint(filters):
    return jnp.transpose(jnp.flip(filters, (2, 3, 4)), (1, 0, 2, 3, 4))

def reference(position, momentum, noise, filter_in, filter_out, bias):
    back_in = adjoint(filter_in)
    back_out = adjoint(filter_out)
    bias_col = bias[:, None, None, None]

    def gradient(field):
        rounded = field.astype(jnp.bfloat16)
        pre = convolve(rounded, filter_in) + bias_col
        active = jnp.tanh(pre)
        output = convolve(active.astype(jnp.bfloat16), filter_out)
        back = convolve(output.astype(jnp.bfloat16), back_out)
        hidden = (back * (1.0 - active * active)).astype(jnp.bfloat16)
        return convolve(hidden, back_in) + field
    step = 0.25
    decay = jnp.exp(jnp.float32(-0.25))
    kick = jnp.sqrt(1.0 - decay * decay)
    field = position
    moment = momentum
    force = gradient(field)
    for index in range(STEPS):
        moment = moment - 0.5 * step * force
        field = field + 0.5 * step * moment
        moment = decay * moment + kick * noise[index].astype(jnp.float32)
        field = field + 0.5 * step * moment
        force = gradient(field)
        moment = moment - 0.5 * step * force
    return (field, moment)
```

```python
import functools

import jax
import jax.numpy as jnp
import numpy as np
from jax import lax
from jax.experimental import pallas as pl
from jax.experimental.pallas import tpu as pltpu
from jax.sharding import PartitionSpec as P

EDGE = 16
MESH = pl.DeviceIdType.MESH


def kernel(steps, sizes, pos_ref, mom_ref, noise_ref, w_ref, bias_ref,
           q_out, p_out, a1, a2, b1, b2, eq, eh, t_ref, q_ref, p_ref, send, recv, *gather):
    nx, ny, nz = sizes
    c = pos_ref.shape[0]
    inside = len(gather) > 0
    if inside:
        wg, wf, wsend, wrecv = gather
    x, z, lanes = q_ref.shape
    y = lanes // c
    full = eq.shape[1]
    wrap = ny == 2
    slots = eq.shape[2] // c
    own = slice(EDGE, EDGE + z)
    mine = slice(lanes, 2 * lanes)

    ix, iy, iz = lax.axis_index("gx"), lax.axis_index("gy"), lax.axis_index("gz")
    up = {"gx": lax.rem(ix + 1, nx), "gy": lax.rem(iy + 1, ny), "gz": lax.rem(iz + 1, nz)}
    down = {
        "gx": lax.rem(ix + nx - 1, nx),
        "gy": lax.rem(iy + ny - 1, ny),
        "gz": lax.rem(iz + nz - 1, nz),
    }

    def at_side(**which):
        return {axis: which[axis][axis] for axis in which}

    def early(buf):
        core = slice(2, 2 + x)
        low, high = slice(0, EDGE), slice(z + EDGE, full)
        block = buf.at[core, own, mine]
        edges = (
            (up, buf.at[core, z : z + EDGE, mine], low),
            (down, buf.at[core, EDGE : 2 * EDGE, mine], high),
        )
        out = []
        for side, source, rows in edges:
            out.append((at_side(gz=side), source, buf.at[core, rows, mine], True))
        for beside, part in others:
            out.append((at_side(gy=beside), block, buf.at[core, own, part], True))
            for side, source, rows in edges:
                target = buf.at[core, rows, part]
                out.append((at_side(gy=beside, gz=side), source, target, True))
        out.append(
            (at_side(gx=down), buf.at[2:4, own, mine], buf.at[2 + x : 4 + x, own, mine], False)
        )
        out.append((at_side(gx=up), buf.at[x : 2 + x, own, mine], buf.at[0:2, own, mine], False))
        return out

    def late(buf):
        low, high = slice(0, EDGE), slice(z + EDGE, full)
        from_low = (up, slice(x, 2 + x), slice(0, 2))
        from_high = (down, slice(2, 4), slice(2 + x, 4 + x))
        plan = []
        for _, part in others:
            plan.append((from_low, slice(0, full), part))
            plan += [(from_high, low, part), (from_high, high, part)]
        for side in (from_low, from_high):
            plan += [(side, low, mine), (side, high, mine)]
        return [
            (at_side(gx=side), buf.at[source, rows, part], buf.at[target, rows, part])
            for (side, source, target), rows, part in plan
        ]

    def forward(buf):
        planes = slice(2 + x, 4 + x)
        return [
            (at_side(gy=beside), buf.at[planes, own, mine], buf.at[planes, own, part])
            for beside, part in others
        ]

    others = [(up, slice(0, lanes))]
    if not wrap:
        others.append((down, slice(2 * lanes, 3 * lanes)))

    def remote(source, target, sems, number, device):
        return pltpu.make_async_remote_copy(
            src_ref=source,
            dst_ref=target,
            send_sem=sems[0].at[number],
            recv_sem=sems[1].at[number],
            device_id=device,
            device_id_type=MESH,
        )

    peers = []
    if inside:
        for dx in range(nx):
            for dy in range(ny):
                if dx or dy:
                    peers.append({"gx": lax.rem(ix + dx, nx), "gy": lax.rem(iy + dy, ny)})
    barrier = pltpu.get_barrier_semaphore()
    greeted = peers + [device for device, _, _, _ in early(eq)]
    for device in greeted:
        pl.semaphore_signal(barrier, inc=1, device_id=device, device_id_type=MESH)
    pl.semaphore_wait(barrier, len(greeted))

    if inside:
        copies = []
        for number, device in enumerate(peers):
            copy = remote(w_ref, wg.at[iy, ix], (wsend, wrecv), number, device)
            copy.start()
            copies.append(copy)
        wg[iy, ix] = w_ref[...]
        for copy in copies:
            copy.wait()
        ci = c // ny
        for which in range(2):
            for at in range(27):
                columns = []
                for j in range(ny):
                    pieces = [wg[j, i, which, :, at * ci : (at + 1) * ci] for i in range(nx)]
                    columns.append(jnp.concatenate(pieces, axis=0))
                wf[which, at // 3, at % 3] = jnp.concatenate(columns, axis=1)
        filters = wf
    else:
        filters = w_ref

    def exchange(buf, bank):
        sems = (send.at[bank], recv.at[bank])
        first, own_x = [], []
        number = 0
        for device, source, target, passed in early(buf):
            copy = remote(source, target, sems, number, device)
            number += 1
            copy.start()
            (first if passed else own_x).append(copy)
        for copy in first:
            copy.wait_recv()
        second = []
        for device, source, target in late(buf):
            copy = remote(source, target, sems, number, device)
            number += 1
            copy.start()
            second.append(copy)
        own_x[0].wait_recv()
        for device, source, target in forward(buf):
            copy = remote(source, target, sems, number, device)
            number += 1
            copy.start()
            second.append(copy)
        for copy in own_x[1:] + second:
            copy.wait_recv()
        for copy in first + own_x + second:
            copy.wait_send()

    def slot(at):
        return at % slots

    def unfold(tap, carry):
        blank = jnp.zeros((c, c), jnp.bfloat16)

        def rows(out, which, at, flip, cols, pick):
            line = [blank] * cols
            for col, b in pick:
                line[col] = filters[which, at, 2 - b if flip else b]
            return jnp.concatenate(line, axis=1)

        back = 8 - tap
        for yo in range(y + 2):
            a1[tap, yo * c : (yo + 1) * c, :] = rows(
                a1, 0, tap, False, slots, [(slot(yo + b), b) for b in range(3)]
            )
        for yo in range(y):
            a2[tap, yo * c : (yo + 1) * c, :] = rows(
                a2, 1, tap, False, y + 2, [(yo + b, b) for b in range(3)]
            )
        for s in range(slots):
            pick = [(yo, b) for yo in range(y + 2) for b in range(3) if slot(yo + b) == s]
            b2[tap, s * c : (s + 1) * c, :] = rows(b2, 1, back, True, y + 2, pick)
        for yi in range(y + 2):
            pick = [(yo, yi - yo) for yo in range(y) if 0 <= yi - yo <= 2]
            b1[tap, yi * c : (yi + 1) * c, :] = rows(b1, 0, back, True, y, pick)
        return carry

    lax.fori_loop(0, 9, unfold, 0)

    def load(ref2d, at):
        span = [ref2d[:, (at * y + j) * z : (at * y + j + 1) * z] for j in range(y)]
        return jnp.concatenate(span, axis=0).astype(jnp.float32).T

    for at in range(x):
        q_ref[at] = load(pos_ref, at)
        p_ref[at] = load(mom_ref, at)

    def conv(source, weights, out_x, transposed):
        width = source.shape[2]
        total = None
        for tz in range(3):
            part = None
            for tx in range(3):
                left = source[tx : tx + out_x].reshape(out_x * full, width)
                term = lax.dot_general(
                    left,
                    weights[tx * 3 + tz],
                    (((1,), (1 if transposed else 0,)), ((), ())),
                    preferred_element_type=jnp.float32,
                )
                part = term if part is None else part + term
            if tz != 1:
                part = pltpu.roll(part, 1 if tz == 0 else out_x * full - 1, 0)
            total = part if total is None else total + part
        return total.reshape(out_x, full, total.shape[-1])

    step = 0.25
    decay = jnp.exp(jnp.float32(-0.25))
    kick = jnp.sqrt(1.0 - decay * decay)

    def body(k, carry):
        eq[2 : 2 + x, own, mine] = q_ref[...].astype(jnp.bfloat16)
        exchange(eq, 0)
        t_ref[...] = jnp.tanh(conv(eq, a1, x + 2, True) + bias_ref[...][None])
        h2 = conv(t_ref[...].astype(jnp.bfloat16), a2, x, True)
        eh[2 : 2 + x, own, mine] = h2[:, own].astype(jnp.bfloat16)
        exchange(eh, 1)
        gu = conv(eh, b2, x + 2, False)
        t = t_ref[...]
        gh = (gu * (1.0 - t * t)).astype(jnp.bfloat16)
        force = conv(gh, b1, x, False)[:, own] + q_ref[...]
        half = 0.5 * step

        @pl.when(k > 0)
        def _():
            p_ref[...] = p_ref[...] - half * force

        @pl.when(k < steps)
        def _():
            p = p_ref[...] - half * force
            q = q_ref[...] + half * p
            now = noise_ref.at[k]
            drawn = jnp.stack([load(now, at) for at in range(x)])
            p = decay * p + kick * drawn
            q_ref[...] = q + half * p
            p_ref[...] = p

        return carry

    lax.fori_loop(0, steps + 1, body, 0)

    for ref, out in ((q_ref, q_out), (p_ref, p_out)):
        for at in range(x):
            flat = ref[at].T
            for j in range(y):
                out[:, (at * y + j) * z : (at * y + j + 1) * z] = flat[j * c : (j + 1) * c]


LANES = 128
ROWS = 8


def ring_place(r, nx):
    row, step = r // nx, r % nx
    return step + (row % 2) * (nx - 1 - 2 * step), row


def ring_kernel(steps, sizes, pos_ref, mom_ref, noise_ref, fin_ref, fout_ref, bias_ref,
                q_out, p_out, own_w, all_w, mats, turned, edges, msg0, got0, msgd, gotd,
                stage, lhs, t_ref, base, extra, dq, dp, qb, halo, back_q, got_q, back_p, got_p,
                send, recv):
    nx, ny, nz = sizes
    ring = nx * ny
    x, zb = msg0.shape[1] - 1, msg0.shape[2]
    lane = LANES
    z = ring * zb
    taps, co, ci = fin_ref.shape
    c = ny * ci
    y = lane // c
    xx, yy = x * nx, y * ny
    per = lane // ci
    tiles = own_w.shape[0] // 2
    wide = yy * c
    reach = 4
    rows = zb * xx

    ix, iy, iz = lax.axis_index("gx"), lax.axis_index("gy"), lax.axis_index("gz")
    me = iy * nx + ix + (iy % 2) * (nx - 1 - 2 * ix)

    def device(r, core):
        gx, gy = ring_place(r, nx)
        return {"gx": gx, "gy": gy, "gz": core}

    barrier = pltpu.get_barrier_semaphore()
    everyone = 0
    for dx in range(nx):
        for dy in range(ny):
            for dz in range(nz):
                if dx or dy or dz:
                    everyone += 1
                    pl.semaphore_signal(
                        barrier,
                        inc=1,
                        device_id={"gx": (ix + dx) % nx, "gy": (iy + dy) % ny, "gz": (iz + dz) % nz},
                        device_id_type=MESH,
                    )

    def remote(source, target, number, where):
        copy = pltpu.make_async_remote_copy(
            src_ref=source,
            dst_ref=target,
            send_sem=send.at[number],
            recv_sem=recv.at[number],
            device_id=where,
            device_id_type=MESH,
        )
        copy.start()
        return copy

    sent = []
    used = [0]

    def start(source, target, where):
        copy = remote(source, target, used[0], where)
        used[0] += 1
        sent.append(copy)
        return copy

    def to_ring(source, target):
        out = []
        for j in range(1, ring):
            r = (me + j) % ring
            out.append(start(source(r), target, device(r, iz)))
        return out

    def arrive(copies):
        for copy in copies:
            copy.wait_recv()

    for which, ref in enumerate((fin_ref, fout_ref)):
        for tile in range(tiles):
            parts = [ref[t].astype(jnp.float32) for t in range(tile * per, min(taps, (tile + 1) * per))]
            parts += [jnp.zeros((co, ci), jnp.float32)] * (per - len(parts))
            own_w[which * tiles + tile] = jnp.concatenate(parts, axis=1).astype(jnp.bfloat16)
    first, second = (2 * tiles + 3) // 4, 0
    second = tiles - first

    def turn(ref, at):
        parts = [ref[pl.ds(at * y + j, c, stride=x * y), :] for j in range(y)]
        return jnp.concatenate(parts, axis=0).T

    for at in range(x):
        turned[at] = turn(pos_ref, at)

    pl.semaphore_wait(barrier, everyone)

    head = pl.ds(iz * first, first)
    tail = pl.ds(2 * first + iz * second, second)
    filters_a = to_ring(lambda r: own_w.at[head], all_w.at[me, head])
    low = start(turned.at[:, z - ROWS : z], edges.at[0], {"gz": (iz + 1) % nz})
    high = start(turned.at[:, 0:ROWS], edges.at[1], {"gz": (iz + nz - 1) % nz})
    all_w[me, head] = own_w[head]
    all_w[me, tail] = own_w[tail]

    upper = lax.broadcasted_iota(jnp.int32, (ROWS, lane), 0) < reach
    arrive([low, high])
    for r in range(ring):
        around = []
        for at in range(x):
            block = turned[at, r * zb : (r + 1) * zb]
            msg0[r, at] = block.astype(jnp.bfloat16)
            before = turned[at, r * zb - ROWS : r * zb] if r else edges[0, at]
            after = turned[at, (r + 1) * zb : (r + 1) * zb + ROWS] if r < ring - 1 else edges[1, at]
            around.append(jnp.where(upper, after, before))
        msg0[r, x] = jnp.concatenate(around, axis=0).astype(jnp.bfloat16)
    fields = to_ring(lambda r: msg0.at[r], got0.at[me])
    got0[me] = msg0[me]
    filters_b = to_ring(lambda r: own_w.at[tail], all_w.at[me, tail])

    half = 0.125
    decay = float(np.exp(np.float32(-0.25)))
    kick = float(np.sqrt(np.float32(1.0) - np.exp(np.float32(-0.25)) ** 2))
    push = half * (1.0 + decay)
    q = pos_ref[...]
    known = q.astype(jnp.bfloat16).astype(jnp.float32)
    p = mom_ref[...] - half * q
    total = x * y * c
    drifts = []
    for k in range(steps):
        noise = noise_ref[k * total : (k + 1) * total].astype(jnp.float32)
        q = q + push * p + (half * kick) * noise
        drift = (q - known).astype(jnp.bfloat16).astype(jnp.float32)
        known = known + drift
        last = k == steps - 1
        p = decay * p + kick * noise - (half if last else 2 * half) * q
        q_out[...] = drift
        for at in range(x):
            flat = turn(q_out, at).astype(jnp.bfloat16)
            for r in range(ring):
                msgd[k, r, at] = flat[r * zb : (r + 1) * zb]
        drifts.append(to_ring(lambda r: msgd.at[k, r], gotd.at[k, me]))
        gotd[k, me] = msgd[k, me]
    q_out[...] = q
    p_out[...] = p

    other = {"gz": (iz + 1) % nz}
    arrive(filters_a)
    swap_a = start(all_w.at[:, head], all_w.at[:, head], other)
    at_lane = lax.broadcasted_iota(jnp.int32, (co, lane), 1)

    def build(which):
        def place(gx, carry):
            row = pl.multiple_of(gx * co, co)
            for a in range(3):
                for cz in range(3):
                    moved = {}
                    for b in range(3):
                        t = a * 9 + b * 3 + cz
                        tile, spot = which * tiles + t // per, t % per
                        for side in range(2):
                            pieces = []
                            for gy in range(ny):
                                r = gy * nx + gx + (gy % 2) * (nx - 1 - 2 * gx)
                                piece = all_w[r, tile].astype(jnp.float32)
                                shift = (side * ny + gy - spot) % per
                                pieces.append(pltpu.roll(piece, shift * ci, 1) if shift else piece)
                            moved[b, side] = pieces
                    pairs = []
                    for b in range(yy):
                        value = jnp.zeros((co, lane), jnp.float32)
                        for side in range(y):
                            near = (b + side) % yy
                            if near > 2:
                                continue
                            for gy in range(ny):
                                spot = (side * ny + gy) * ci
                                inside = (at_lane >= spot) & (at_lane < spot + ci)
                                value = jnp.where(inside, moved[near, side][gy], value)
                        pairs.append(value.astype(jnp.bfloat16))
                    for yo in range(yy):
                        for h in range(yy // y):
                            mats[which, a * 3 + cz, pl.ds(yo * c + row, co), h * lane : (h + 1) * lane] = (
                                pairs[(h * y + 1 - yo) % yy]
                            )
            return carry

        lax.fori_loop(0, nx, place, 0)

    def scatter(target, zs, value, r, at):
        gx, gy = ring_place(r, nx)
        target[gy, pl.ds(zs * xx + gx * x + at, value.shape[0], stride=xx), :] = value

    def whole(ref, rows_from, rows_to):
        return jnp.concatenate([ref[gy, rows_from:rows_to] for gy in range(ny)], axis=1)

    arrive(fields)
    for r in range(ring):
        around = got0[r, x].astype(jnp.float32)
        for at in range(x):
            scatter(stage, 0, got0[r, at].astype(jnp.float32), r, at)
            scatter(stage, zb, around[at * ROWS : (at + 1) * ROWS], r, at)
    base[...] = whole(stage, 0, rows)
    arrive([swap_a])
    build(0)
    arrive(filters_b)
    swap_b = start(all_w.at[:, tail], all_w.at[:, tail], other)

    def spread(value):
        n = value.shape[0]
        cube = value.reshape(n // xx, xx, wide)
        for a in range(3):
            moved = cube if a == 1 else pltpu.roll(cube, (1 - a) % xx, 1)
            moved = moved.reshape(n, wide)
            lhs[a, 0, 0:n] = moved.astype(jnp.bfloat16)
            lhs[a, 1, 0 : n - 2 * xx] = moved[xx : n - xx].astype(jnp.bfloat16)

    def conv(which, n, adjoint):
        out = None
        for a in range(3):
            for cz in range(3):
                left = lhs[a, 1, 0:n] if cz == 1 else lhs[a, 0, cz * xx : cz * xx + n]
                tap = a * 3 + cz
                term = lax.dot_general(
                    left,
                    mats[which, 8 - tap if adjoint else tap],
                    (((1,), (0 if adjoint else 1,)), ((), ())),
                    preferred_element_type=jnp.float32,
                )
                out = term if out is None else out + term
        return out

    row = jnp.concatenate([bias_ref[...]] * yy, axis=1)

    def gradient(between):
        n = rows + 2 * (reach - 1) * xx
        t = jnp.tanh(conv(0, n, False) + row)
        t_ref[...] = t
        spread(t)
        between()
        n -= 2 * xx
        spread(conv(1, n, False))
        n -= 2 * xx
        gu = conv(1, n, True)
        t = t_ref[2 * xx : 2 * xx + n]
        spread(gu * (1.0 - t * t))
        n -= 2 * xx
        return conv(0, n, True)

    def take_drift(k):
        arrive(drifts[k])
        for r in range(ring):
            for at in range(x):
                scatter(extra, 0, gotd[k, r, at].astype(jnp.float32), r, at)
        base[...] = base[...] + whole(extra, 0, rows)

    def second_filters():
        arrive([swap_b])
        build(1)

    def collect(ref, r, at):
        gx, gy = ring_place(r, nx)
        return ref[gy, pl.ds(gx * x + at, zb, stride=xx), :]

    def put(ref, value):
        for gy in range(ny):
            ref[gy] = value[:, gy * lane : (gy + 1) * lane]

    turn_at = (zb + reach) * xx
    field = [whole(stage, turn_at, turn_at + reach * xx), whole(stage, 0, turn_at)]
    spread(jnp.concatenate(field, axis=0))
    g = gradient(second_filters)
    put(dp, -half * g)
    put(dq, (-half * push) * g)
    take_drift(0)

    left_r, right_r = (me + ring - 1) % ring, (me + 1) % ring
    left = device(left_r, (iz + nz - 1 + (me + ring - 1) // ring) % nz)
    right = device(right_r, (iz + (me + 1) // ring) % nz)
    edge = reach * xx
    mine = pl.ds(pl.multiple_of(me * zb, zb), zb)
    for k in range(1, steps + 1):
        q = base[...] + whole(dq, 0, rows)
        qb[k - 1] = q.astype(jnp.bfloat16)
        below = start(qb.at[k - 1, rows - edge : rows], halo.at[k - 1, 0], right)
        above = start(qb.at[k - 1, 0:edge], halo.at[k - 1, 1], left)
        if k < steps:
            take_drift(k)
        else:
            dp[...] = decay * dp[...] - half * dq[...]
            for r in range(ring):
                for at in range(x):
                    back_q[r, at] = collect(dq, r, at)
                    back_p[0, r, at] = collect(dp, r, at).astype(jnp.bfloat16)
            sent_q = to_ring(lambda r: back_q.at[r], got_q.at[:, mine])
            sent_p = to_ring(lambda r: back_p.at[0, r], got_p.at[0, :, mine])
            got_q[:, mine] = back_q[me]
            got_p[0, :, mine] = back_p[0, me]
            dp[...] = dp[...] - dp[...].astype(jnp.bfloat16).astype(jnp.float32)
        arrive([below, above])
        spread(
            jnp.concatenate(
                [halo[k - 1, 0].astype(jnp.float32), q, halo[k - 1, 1].astype(jnp.float32)], axis=0
            )
        )
        g = gradient(lambda: None)
        if k < steps:
            shift = whole(dq, 0, rows)
            now = decay * whole(dp, 0, rows) - (2 * half) * (g + shift)
            put(dp, now)
            put(dq, shift + push * now)
        else:
            put(dp, whole(dp, 0, rows) - half * g)
    for r in range(ring):
        for at in range(x):
            back_p[1, r, at] = collect(dp, r, at).astype(jnp.bfloat16)
    last_p = to_ring(lambda r: back_p.at[1, r], got_p.at[1, :, mine])
    got_p[1, :, mine] = back_p[1, me]

    def untie(value, out, at):
        flat = value.T
        for j in range(y):
            part = pl.ds(at * y + j, c, stride=x * y)
            out[part, :] = out[part, :] + flat[j * c : (j + 1) * c]

    arrive(sent_q)
    for at in range(x):
        untie(got_q[at], q_out, at)
    arrive(sent_p)
    arrive(last_p)
    for at in range(x):
        untie(got_p[0, at].astype(jnp.float32) + got_p[1, at].astype(jnp.float32), p_out, at)
    for copy in sent:
        copy.wait_send()


def fits_ring(sizes, position, filter_in):
    nx, ny, nz = sizes
    c, x, y, z = position.shape
    co, ci = filter_in.shape[:2]
    ring = nx * ny
    return (
        nz == 2 and ny == 2 and nx > 1 and y * c == LANES and x * nx == ROWS and y * ny > 2
        and z % (ring * EDGE) == 0 and z // ring == EDGE and co % EDGE == 0 and LANES % ci == 0
        and y * ny * ci == LANES
    )


def on_ring(sizes, position, momentum, noise, filter_in, filter_out, bias):
    nx, ny, nz = sizes
    c, x, y, z = position.shape
    steps = noise.shape[0]
    co, ci = filter_in.shape[:2]
    ring = nx * ny
    zb = z // ring
    xx, yy = x * nx, y * ny
    wide = yy * c
    rows = zb * xx
    lane = LANES
    tiles = -(-27 * ci // lane)
    flat = jax.ShapeDtypeStruct((c * x * y, z), jnp.float32)
    copies = (7 + steps) * (ring - 1) + 4 + 2 * steps
    vmem = pl.BlockSpec(memory_space=pltpu.VMEM)
    bf16, f32 = jnp.bfloat16, jnp.float32
    q, p = pl.pallas_call(
        functools.partial(ring_kernel, steps, sizes),
        out_shape=(flat, flat),
        in_specs=[vmem] * 6,
        out_specs=(vmem, vmem),
        scratch_shapes=[
            pltpu.VMEM((2 * tiles, co, lane), bf16),
            pltpu.VMEM((ring, 2 * tiles, co, lane), bf16),
            pltpu.VMEM((2, 9, wide, wide), bf16),
            pltpu.VMEM((x, z, lane), f32),
            pltpu.VMEM((2, x, ROWS, lane), f32),
            pltpu.VMEM((ring, x + 1, zb, lane), bf16),
            pltpu.VMEM((ring, x + 1, zb, lane), bf16),
            pltpu.VMEM((steps, ring, x, zb, lane), bf16),
            pltpu.VMEM((steps, ring, x, zb, lane), bf16),
            pltpu.VMEM((ny, rows + ROWS * xx, lane), f32),
            pltpu.VMEM((3, 2, rows + ROWS * xx, wide), bf16),
            pltpu.VMEM((rows + 6 * xx, wide), f32),
            pltpu.VMEM((rows, wide), f32),
            pltpu.VMEM((ny, rows, lane), f32),
            pltpu.VMEM((ny, rows, lane), f32),
            pltpu.VMEM((ny, rows, lane), f32),
            pltpu.VMEM((steps, rows, wide), bf16),
            pltpu.VMEM((steps, 2, 4 * xx, wide), bf16),
            pltpu.VMEM((ring, x, zb, lane), f32),
            pltpu.VMEM((x, z, lane), f32),
            pltpu.VMEM((2, ring, x, zb, lane), bf16),
            pltpu.VMEM((2, x, z, lane), bf16),
            pltpu.SemaphoreType.DMA((copies,)),
            pltpu.SemaphoreType.DMA((copies,)),
        ],
        compiler_params=pltpu.CompilerParams(
            collective_id=0, has_side_effects=True, vmem_limit_bytes=56 * 2**20
        ),
    )(
        position.reshape(-1, z),
        momentum.reshape(-1, z),
        noise.reshape(-1, z),
        filter_in.transpose(2, 3, 4, 0, 1).reshape(27, co, ci),
        filter_out.transpose(2, 3, 4, 0, 1).reshape(27, co, ci),
        bias[None],
    )
    return q.reshape(position.shape), p.reshape(momentum.shape)


def on_device(sizes, position, momentum, noise, filter_in, filter_out, bias):
    if fits_ring(sizes, position, filter_in):
        return on_ring(sizes, position, momentum, noise, filter_in, filter_out, bias)
    nx, ny, nz = sizes
    c, x, y, z = position.shape
    steps = noise.shape[0]
    assert x >= 2 and y == 2 and z % EDGE == 0 and nx > 2 and ny > 1
    both = jnp.stack([filter_in, filter_out])
    co, ci = both.shape[1], both.shape[2]
    gather = []
    if co % EDGE == 0:
        both = both.transpose(0, 1, 3, 5, 4, 2).reshape(2, co, 27 * ci)
        gather = [
            pltpu.VMEM((ny, nx, 2, co, 27 * ci), jnp.bfloat16),
            pltpu.VMEM((2, 9, 3, c, c), jnp.bfloat16),
            pltpu.SemaphoreType.DMA((nx * ny - 1,)),
            pltpu.SemaphoreType.DMA((nx * ny - 1,)),
        ]
    else:
        both = both.reshape(2 * co, ci * 27)
        both = lax.all_gather(both, ("gx", "gy"), axis=0, tiled=True)
        both = both.reshape(nx, ny, 2, co, ci, 3, 3, 3)
        both = both.transpose(2, 5, 7, 6, 0, 3, 1, 4).reshape(2, 9, 3, c, c)
    lanes = y * c
    slots = 2 * y if ny == 2 else 3 * y
    full = z + 2 * EDGE
    wide = (y + 2) * c
    flat = jax.ShapeDtypeStruct((c, x * y * z), jnp.float32)
    copies = 15 if ny == 2 else 24
    vmem = pl.BlockSpec(memory_space=pltpu.VMEM)
    q, p = pl.pallas_call(
        functools.partial(kernel, steps, sizes),
        out_shape=(flat, flat),
        in_specs=[vmem] * 5,
        out_specs=(vmem, vmem),
        scratch_shapes=[
            pltpu.VMEM((9, wide, slots * c), jnp.bfloat16),
            pltpu.VMEM((9, lanes, wide), jnp.bfloat16),
            pltpu.VMEM((9, wide, lanes), jnp.bfloat16),
            pltpu.VMEM((9, slots * c, wide), jnp.bfloat16),
            pltpu.VMEM((x + 4, full, slots * c), jnp.bfloat16),
            pltpu.VMEM((x + 4, full, slots * c), jnp.bfloat16),
            pltpu.VMEM((x + 2, full, wide), jnp.float32),
            pltpu.VMEM((x, z, lanes), jnp.float32),
            pltpu.VMEM((x, z, lanes), jnp.float32),
            pltpu.SemaphoreType.DMA((2, copies)),
            pltpu.SemaphoreType.DMA((2, copies)),
            *gather,
        ],
        compiler_params=pltpu.CompilerParams(
            collective_id=0, has_side_effects=True, vmem_limit_bytes=56 * 2**20
        ),
    )(
        position.reshape(c, -1),
        momentum.reshape(c, -1),
        noise.reshape(steps, c, -1),
        both,
        jnp.tile(bias, y + 2)[None],
    )
    return q.reshape(position.shape), p.reshape(momentum.shape)


def solution(mesh):
    field = P(None, ("grp", "gx"), "gy", "gz")
    filters = P("gx", "gy", None, None, None)
    sizes = tuple(mesh.shape[name] for name in ("gx", "gy", "gz"))
    return jax.shard_map(
        functools.partial(on_device, sizes),
        mesh=mesh,
        in_specs=(field, field, P(None, None, ("grp", "gx"), "gy", "gz"), filters, filters, P()),
        out_specs=(field, field),
        check_vma=False,
    )
```

```python
import functools

import jax
import jax.numpy as jnp
import numpy as np
from jax import lax
from jax.experimental import pallas as pl
from jax.experimental.pallas import tpu as pltpu
from jax.sharding import PartitionSpec as P

EDGE = 16
MESH = pl.DeviceIdType.MESH


def kernel(steps, sizes, pos_ref, mom_ref, noise_ref, w_ref, bias_ref,
           q_out, p_out, a1, a2, b1, b2, eq, eh, t_ref, q_ref, p_ref, send, recv, *gather):
    nx, ny, nz = sizes
    c = pos_ref.shape[0]
    inside = len(gather) > 0
    if inside:
        wg, wf, wsend, wrecv = gather
    x, z, lanes = q_ref.shape
    y = lanes // c
    full = eq.shape[1]
    wrap = ny == 2
    slots = eq.shape[2] // c
    own = slice(EDGE, EDGE + z)
    mine = slice(lanes, 2 * lanes)

    ix, iy, iz = lax.axis_index("gx"), lax.axis_index("gy"), lax.axis_index("gz")
    up = {"gx": lax.rem(ix + 1, nx), "gy": lax.rem(iy + 1, ny), "gz": lax.rem(iz + 1, nz)}
    down = {
        "gx": lax.rem(ix + nx - 1, nx),
        "gy": lax.rem(iy + ny - 1, ny),
        "gz": lax.rem(iz + nz - 1, nz),
    }

    def at_side(**which):
        return {axis: which[axis][axis] for axis in which}

    def early(buf):
        core = slice(2, 2 + x)
        low, high = slice(0, EDGE), slice(z + EDGE, full)
        block = buf.at[core, own, mine]
        edges = (
            (up, buf.at[core, z : z + EDGE, mine], low),
            (down, buf.at[core, EDGE : 2 * EDGE, mine], high),
        )
        out = []
        for side, source, rows in edges:
            out.append((at_side(gz=side), source, buf.at[core, rows, mine], True))
        for beside, part in others:
            out.append((at_side(gy=beside), block, buf.at[core, own, part], True))
            for side, source, rows in edges:
                target = buf.at[core, rows, part]
                out.append((at_side(gy=beside, gz=side), source, target, True))
        out.append(
            (at_side(gx=down), buf.at[2:4, own, mine], buf.at[2 + x : 4 + x, own, mine], False)
        )
        out.append((at_side(gx=up), buf.at[x : 2 + x, own, mine], buf.at[0:2, own, mine], False))
        return out

    def late(buf):
        low, high = slice(0, EDGE), slice(z + EDGE, full)
        from_low = (up, slice(x, 2 + x), slice(0, 2))
        from_high = (down, slice(2, 4), slice(2 + x, 4 + x))
        plan = []
        for _, part in others:
            plan.append((from_low, slice(0, full), part))
            plan += [(from_high, low, part), (from_high, high, part)]
        for side in (from_low, from_high):
            plan += [(side, low, mine), (side, high, mine)]
        return [
            (at_side(gx=side), buf.at[source, rows, part], buf.at[target, rows, part])
            for (side, source, target), rows, part in plan
        ]

    def forward(buf):
        planes = slice(2 + x, 4 + x)
        return [
            (at_side(gy=beside), buf.at[planes, own, mine], buf.at[planes, own, part])
            for beside, part in others
        ]

    others = [(up, slice(0, lanes))]
    if not wrap:
        others.append((down, slice(2 * lanes, 3 * lanes)))

    def remote(source, target, sems, number, device):
        return pltpu.make_async_remote_copy(
            src_ref=source,
            dst_ref=target,
            send_sem=sems[0].at[number],
            recv_sem=sems[1].at[number],
            device_id=device,
            device_id_type=MESH,
        )

    peers = []
    if inside:
        for dx in range(nx):
            for dy in range(ny):
                if dx or dy:
                    peers.append({"gx": lax.rem(ix + dx, nx), "gy": lax.rem(iy + dy, ny)})
    barrier = pltpu.get_barrier_semaphore()
    greeted = peers + [device for device, _, _, _ in early(eq)]
    for device in greeted:
        pl.semaphore_signal(barrier, inc=1, device_id=device, device_id_type=MESH)
    pl.semaphore_wait(barrier, len(greeted))

    if inside:
        copies = []
        for number, device in enumerate(peers):
            copy = remote(w_ref, wg.at[iy, ix], (wsend, wrecv), number, device)
            copy.start()
            copies.append(copy)
        wg[iy, ix] = w_ref[...]
        for copy in copies:
            copy.wait()
        ci = c // ny
        for which in range(2):
            for at in range(27):
                columns = []
                for j in range(ny):
                    pieces = [wg[j, i, which, :, at * ci : (at + 1) * ci] for i in range(nx)]
                    columns.append(jnp.concatenate(pieces, axis=0))
                wf[which, at // 3, at % 3] = jnp.concatenate(columns, axis=1)
        filters = wf
    else:
        filters = w_ref

    def exchange(buf, bank):
        sems = (send.at[bank], recv.at[bank])
        first, own_x = [], []
        number = 0
        for device, source, target, passed in early(buf):
            copy = remote(source, target, sems, number, device)
            number += 1
            copy.start()
            (first if passed else own_x).append(copy)
        for copy in first:
            copy.wait_recv()
        second = []
        for device, source, target in late(buf):
            copy = remote(source, target, sems, number, device)
            number += 1
            copy.start()
            second.append(copy)
        own_x[0].wait_recv()
        for device, source, target in forward(buf):
            copy = remote(source, target, sems, number, device)
            number += 1
            copy.start()
            second.append(copy)
        for copy in own_x[1:] + second:
            copy.wait_recv()
        for copy in first + own_x + second:
            copy.wait_send()

    def slot(at):
        return at % slots

    def unfold(tap, carry):
        blank = jnp.zeros((c, c), jnp.bfloat16)

        def rows(out, which, at, flip, cols, pick):
            line = [blank] * cols
            for col, b in pick:
                line[col] = filters[which, at, 2 - b if flip else b]
            return jnp.concatenate(line, axis=1)

        back = 8 - tap
        for yo in range(y + 2):
            a1[tap, yo * c : (yo + 1) * c, :] = rows(
                a1, 0, tap, False, slots, [(slot(yo + b), b) for b in range(3)]
            )
        for yo in range(y):
            a2[tap, yo * c : (yo + 1) * c, :] = rows(
                a2, 1, tap, False, y + 2, [(yo + b, b) for b in range(3)]
            )
        for s in range(slots):
            pick = [(yo, b) for yo in range(y + 2) for b in range(3) if slot(yo + b) == s]
            b2[tap, s * c : (s + 1) * c, :] = rows(b2, 1, back, True, y + 2, pick)
        for yi in range(y + 2):
            pick = [(yo, yi - yo) for yo in range(y) if 0 <= yi - yo <= 2]
            b1[tap, yi * c : (yi + 1) * c, :] = rows(b1, 0, back, True, y, pick)
        return carry

    lax.fori_loop(0, 9, unfold, 0)

    def load(ref2d, at):
        span = [ref2d[:, (at * y + j) * z : (at * y + j + 1) * z] for j in range(y)]
        return jnp.concatenate(span, axis=0).astype(jnp.float32).T

    for at in range(x):
        q_ref[at] = load(pos_ref, at)
        p_ref[at] = load(mom_ref, at)

    def conv(source, weights, out_x, transposed):
        width = source.shape[2]
        total = None
        for tz in range(3):
            part = None
            for tx in range(3):
                left = source[tx : tx + out_x].reshape(out_x * full, width)
                term = lax.dot_general(
                    left,
                    weights[tx * 3 + tz],
                    (((1,), (1 if transposed else 0,)), ((), ())),
                    preferred_element_type=jnp.float32,
                )
                part = term if part is None else part + term
            if tz != 1:
                part = pltpu.roll(part, 1 if tz == 0 else out_x * full - 1, 0)
            total = part if total is None else total + part
        return total.reshape(out_x, full, total.shape[-1])

    step = 0.25
    decay = jnp.exp(jnp.float32(-0.25))
    kick = jnp.sqrt(1.0 - decay * decay)

    def body(k, carry):
        eq[2 : 2 + x, own, mine] = q_ref[...].astype(jnp.bfloat16)
        exchange(eq, 0)
        t_ref[...] = jnp.tanh(conv(eq, a1, x + 2, True) + bias_ref[...][None])
        h2 = conv(t_ref[...].astype(jnp.bfloat16), a2, x, True)
        eh[2 : 2 + x, own, mine] = h2[:, own].astype(jnp.bfloat16)
        exchange(eh, 1)
        gu = conv(eh, b2, x + 2, False)
        t = t_ref[...]
        gh = (gu * (1.0 - t * t)).astype(jnp.bfloat16)
        force = conv(gh, b1, x, False)[:, own] + q_ref[...]
        half = 0.5 * step

        @pl.when(k > 0)
        def _():
            p_ref[...] = p_ref[...] - half * force

        @pl.when(k < steps)
        def _():
            p = p_ref[...] - half * force
            q = q_ref[...] + half * p
            now = noise_ref.at[k]
            drawn = jnp.stack([load(now, at) for at in range(x)])
            p = decay * p + kick * drawn
            q_ref[...] = q + half * p
            p_ref[...] = p

        return carry

    lax.fori_loop(0, steps + 1, body, 0)

    for ref, out in ((q_ref, q_out), (p_ref, p_out)):
        for at in range(x):
            flat = ref[at].T
            for j in range(y):
                out[:, (at * y + j) * z : (at * y + j + 1) * z] = flat[j * c : (j + 1) * c]


LANES = 128
ROWS = 8


def ring_place(r, nx):
    row, step = r // nx, r % nx
    return step + (row % 2) * (nx - 1 - 2 * step), row


def ring_kernel(steps, sizes, heights, *refs):
    accs = []
    for unit in range(2):
        for height in heights:
            low = -(-height // (2 * EDGE)) * EDGE
            for part in (low, height - low):
                accs.append(pltpu.ACC(unit)((part, 2 * LANES), jnp.float32))
    pl.run_scoped(functools.partial(ring_body, steps, sizes, refs), *accs)


def ring_body(steps, sizes, refs, *sums):
    nx, ny, nz = sizes
    count = len(sums) // 2
    accs = [
        [[sums[unit * count + 2 * place + part] for part in range(2)] for unit in range(2)]
        for place in range(count // 2)
    ]
    inputs, refs = refs[:6], refs[6:]
    (q_out, p_out, pos_ref, mom_ref, noise_ref, fin_ref, fout_ref, bias_ref, own_w, all_w, mats,
     flipped, turned, edges, msg0, got0, msgd, gotd, stage, lhs, t_ref, base, extra, dq, dp, qb,
     halo, back_q, got_q, back_p, got_p, fixed, loose, send, recv, load) = refs
    ring = nx * ny
    x, zb = msg0.shape[1] - 1, msg0.shape[2]
    lane = LANES
    z = ring * zb
    taps, co, ci = fin_ref.shape
    c = ny * ci
    y = lane // c
    xx, yy = x * nx, y * ny
    per = lane // ci
    tiles = own_w.shape[0] // 2
    wide = yy * c
    reach = 4
    rows = zb * xx

    ix, iy, iz = lax.axis_index("gx"), lax.axis_index("gy"), lax.axis_index("gz")
    me = iy * nx + ix + (iy % 2) * (nx - 1 - 2 * ix)

    def device(r, core):
        gx, gy = ring_place(r, nx)
        return {"gx": gx, "gy": gy, "gz": core}

    barrier = pltpu.get_barrier_semaphore()
    everyone = 0
    for dx in range(nx):
        for dy in range(ny):
            for dz in range(nz):
                if dx or dy or dz:
                    everyone += 1
                    pl.semaphore_signal(
                        barrier,
                        inc=1,
                        device_id={"gx": (ix + dx) % nx, "gy": (iy + dy) % ny, "gz": (iz + dz) % nz},
                        device_id_type=MESH,
                    )

    loads = []
    held = (pos_ref, mom_ref, noise_ref, fin_ref, fout_ref, bias_ref)
    for number in (3, 4, 0, 1, 2, 5):
        copy = pltpu.make_async_copy(inputs[number], held[number], load.at[number])
        copy.start()
        loads.append(copy)

    def remote(source, target, number, where):
        copy = pltpu.make_async_remote_copy(
            src_ref=source,
            dst_ref=target,
            send_sem=send.at[number],
            recv_sem=recv.at[number],
            device_id=where,
            device_id_type=MESH,
        )
        copy.start()
        return copy

    sent = []
    used = [0]

    def start(source, target, where):
        copy = remote(source, target, used[0], where)
        used[0] += 1
        sent.append(copy)
        return copy

    def to_ring(source, target):
        out = []
        for j in range(1, ring):
            r = (me + j) % ring
            out.append(start(source(r), target, device(r, iz)))
        return out

    def arrive(copies):
        for copy in copies:
            copy.wait_recv()

    loads[0].wait()
    loads[1].wait()
    for which, ref in enumerate((fin_ref, fout_ref)):
        for tile in range(tiles):
            parts = [ref[t].astype(jnp.float32) for t in range(tile * per, min(taps, (tile + 1) * per))]
            parts += [jnp.zeros((co, ci), jnp.float32)] * (per - len(parts))
            own_w[which * tiles + tile] = jnp.concatenate(parts, axis=1).astype(jnp.bfloat16)
    first, second = (2 * tiles + 3) // 4, 0
    second = tiles - first

    def turn(ref, at):
        parts = [ref[pl.ds(at * y + j, c, stride=x * y), :] for j in range(y)]
        return jnp.concatenate(parts, axis=0).T

    loads[2].wait()
    for at in range(x):
        turned[at] = turn(pos_ref, at)

    for each in sums:
        pltpu.matmul_pop(each)

    pl.semaphore_wait(barrier, everyone)

    head = pl.ds(iz * first, first)
    tail = pl.ds(2 * first + iz * second, second)
    beside = {"gy": (iy + 1) % ny}

    def to_column(part):
        out = []
        for dx in range(1, nx):
            out.append(start(own_w.at[part], all_w.at[me, part], {"gx": (ix + dx) % nx}))
        return out, [start(own_w.at[part], all_w.at[me, part], beside)]

    def pass_on(part, column, across):
        for dx in range(1, nx):
            arrive([column[dx - 1]])
            gx = (ix + nx - dx) % nx
            r = iy * nx + gx + (iy % 2) * (nx - 1 - 2 * gx)
            across.append(start(all_w.at[r, part], all_w.at[r, part], beside))

    column_a, across_a = to_column(head)
    low = start(turned.at[:, z - ROWS : z], edges.at[0], {"gz": (iz + 1) % nz})
    high = start(turned.at[:, 0:ROWS], edges.at[1], {"gz": (iz + nz - 1) % nz})
    column_b, across_b = to_column(tail)
    all_w[me, head] = own_w[head]
    all_w[me, tail] = own_w[tail]

    upper = lax.broadcasted_iota(jnp.int32, (ROWS, lane), 0) < reach
    arrive([low, high])
    for r in range(ring):
        around = []
        for at in range(x):
            block = turned[at, r * zb : (r + 1) * zb]
            msg0[r, at] = block.astype(jnp.bfloat16)
            before = turned[at, r * zb - ROWS : r * zb] if r else edges[0, at]
            after = turned[at, (r + 1) * zb : (r + 1) * zb + ROWS] if r < ring - 1 else edges[1, at]
            around.append(jnp.where(upper, after, before))
        msg0[r, x] = jnp.concatenate(around, axis=0).astype(jnp.bfloat16)
    fields = to_ring(lambda r: msg0.at[r], got0.at[me])
    got0[me] = msg0[me]

    half = 0.125
    decay = float(np.exp(np.float32(-0.25)))
    kick = float(np.sqrt(np.float32(1.0) - np.exp(np.float32(-0.25)) ** 2))
    push = half * (1.0 + decay)
    loads[3].wait()
    loads[4].wait()
    loads[5].wait()
    q = pos_ref[...]
    known = q.astype(jnp.bfloat16).astype(jnp.float32)
    p = mom_ref[...] - half * q
    total = x * y * c
    drifts = []
    for k in range(steps):
        noise = noise_ref[k * total : (k + 1) * total].astype(jnp.float32)
        q = q + push * p + (half * kick) * noise
        drift = (q - known).astype(jnp.bfloat16).astype(jnp.float32)
        known = known + drift
        last = k == steps - 1
        p = decay * p + kick * noise - (half if last else 2 * half) * q
        loose[k] = drift
        for at in range(x):
            flat = turn(loose.at[k], at).astype(jnp.bfloat16)
            for r in range(ring):
                msgd[k, r, at] = flat[r * zb : (r + 1) * zb]
        gotd[k, me] = msgd[k, me]
    fixed[0] = q
    fixed[1] = p

    def send_drift(k):
        drifts.append(to_ring(lambda r: msgd.at[k, r], gotd.at[k, me]))

    other = {"gz": (iz + 1) % nz}
    pass_on(head, column_a, across_a)
    pass_on(tail, column_b, across_b)
    arrive(across_a)
    swap_a = start(all_w.at[:, head], all_w.at[:, head], other)
    at_lane = lax.broadcasted_iota(jnp.int32, (co, lane), 1)

    def build(which):
        def place(gx, carry):
            row = pl.multiple_of(gx * co, co)
            for a in range(3):
                for cz in range(3):
                    moved = {}
                    for b in range(3):
                        t = a * 9 + b * 3 + cz
                        tile, spot = which * tiles + t // per, t % per
                        for side in range(2):
                            pieces = []
                            for gy in range(ny):
                                r = gy * nx + gx + (gy % 2) * (nx - 1 - 2 * gx)
                                piece = all_w[r, tile].astype(jnp.float32)
                                shift = (side * ny + gy - spot) % per
                                pieces.append(pltpu.roll(piece, shift * ci, 1) if shift else piece)
                            moved[b, side] = pieces
                    pairs = []
                    for b in range(yy):
                        value = jnp.zeros((co, lane), jnp.float32)
                        for side in range(y):
                            near = (b + side) % yy
                            if near > 2:
                                continue
                            for gy in range(ny):
                                spot = (side * ny + gy) * ci
                                inside = (at_lane >= spot) & (at_lane < spot + ci)
                                value = jnp.where(inside, moved[near, side][gy], value)
                        pairs.append(value.astype(jnp.bfloat16))
                    for yo in range(yy):
                        for h in range(yy // y):
                            mats[which, a * 3 + cz, pl.ds(yo * c + row, co), h * lane : (h + 1) * lane] = (
                                pairs[(h * y + 1 - yo) % yy]
                            )
            return carry

        lax.fori_loop(0, nx, place, 0)

    def turn_over(which):
        for tap in range(9):
            flipped[which, tap] = mats[which, tap].T

    def scatter(target, zs, value, r, at):
        gx, gy = ring_place(r, nx)
        target[gy, pl.ds(zs * xx + gx * x + at, value.shape[0], stride=xx), :] = value

    def whole(ref, rows_from, rows_to):
        return jnp.concatenate([ref[gy, rows_from:rows_to] for gy in range(ny)], axis=1)

    arrive([swap_a])
    build(0)
    arrive(across_b)
    swap_b = start(all_w.at[:, tail], all_w.at[:, tail], other)
    turn_over(0)
    arrive(fields)
    send_drift(0)
    for r in range(ring):
        around = got0[r, x].astype(jnp.float32)
        for at in range(x):
            scatter(stage, 0, got0[r, at].astype(jnp.float32), r, at)
            scatter(stage, zb, around[at * ROWS : (at + 1) * ROWS], r, at)
    base[...] = whole(stage, 0, rows)

    def spread(value):
        n = value.shape[0]
        cube = value.reshape(n // xx, xx, wide)
        for a in range(3):
            moved = cube if a == 1 else pltpu.roll(cube, (1 - a) % xx, 1)
            moved = moved.reshape(n, wide)
            lhs[a, 0, 0:n] = moved.astype(jnp.bfloat16)
            lhs[a, 1, 0 : n - 2 * xx] = moved[xx : n - xx].astype(jnp.bfloat16)

    def conv(place, which, adjoint, flip=False):
        source = mats if adjoint or flip else flipped
        sums = accs[place]
        low, high = sums[0][0].shape[0], sums[0][1].shape[0]
        plans = (
            [(0, True, True), (1, True, True), (2, True, True), (3, True, True), (4, True, False)],
            [(8, True, True), (7, True, True), (6, True, True), (5, True, True), (4, False, True)],
        )
        for at in range(5):
            for unit in range(2):
                tap, use_low, use_high = plans[unit][at]
                a, cz = tap // 3, tap % 3
                pltpu.matmul_push_rhs(
                    source[which, 8 - tap if adjoint else tap],
                    staging_register=at % 2,
                    mxu_index=unit,
                    transpose=flip,
                )
                copy, first_row = (1, 0) if cz == 1 else (0, cz * xx)
                fresh = at % 2
                if use_low:
                    left = lhs[a, copy, first_row : first_row + low]
                    pltpu.matmul_acc_lhs(sums[unit][0], left, load_staged_rhs=fresh)
                    fresh = None
                if use_high:
                    left = lhs[a, copy, first_row + low : first_row + low + high]
                    pltpu.matmul_acc_lhs(sums[unit][1], left, load_staged_rhs=fresh)
        halves = [pltpu.matmul_pop(sums[0][part]) + pltpu.matmul_pop(sums[1][part]) for part in range(2)]
        return jnp.concatenate(halves, axis=0)

    row = jnp.concatenate([bias_ref[...]] * yy, axis=1)

    def gradient(between, flip=False):
        t = jnp.tanh(conv(0, 0, False) + row)
        t_ref[...] = t
        spread(t)
        between()
        spread(conv(1, 1, False, flip))
        gu = conv(2, 1, True)
        t = t_ref[2 * xx : 2 * xx + gu.shape[0]]
        spread(gu * (1.0 - t * t))
        return conv(3, 0, True)

    def take_drift(k):
        arrive(drifts[k])
        for r in range(ring):
            for at in range(x):
                scatter(extra, 0, gotd[k, r, at].astype(jnp.float32), r, at)
        base[...] = base[...] + whole(extra, 0, rows)

    def second_filters():
        arrive([swap_b])
        send_drift(1)
        build(1)

    def collect(ref, r, at):
        gx, gy = ring_place(r, nx)
        return ref[gy, pl.ds(gx * x + at, zb, stride=xx), :]

    def put(ref, value):
        for gy in range(ny):
            ref[gy] = value[:, gy * lane : (gy + 1) * lane]

    turn_at = (zb + reach) * xx
    field = [whole(stage, turn_at, turn_at + reach * xx), whole(stage, 0, turn_at)]
    spread(jnp.concatenate(field, axis=0))
    g = gradient(second_filters, True)
    put(dp, -half * g)
    put(dq, (-half * push) * g)
    take_drift(0)

    left_r, right_r = (me + ring - 1) % ring, (me + 1) % ring
    left = device(left_r, (iz + nz - 1 + (me + ring - 1) // ring) % nz)
    right = device(right_r, (iz + (me + 1) // ring) % nz)
    edge = reach * xx
    mine = pl.ds(pl.multiple_of(me * zb, zb), zb)
    for k in range(1, steps + 1):
        q = base[...] + whole(dq, 0, rows)
        qb[k - 1] = q.astype(jnp.bfloat16)
        below = start(qb.at[k - 1, rows - edge : rows], halo.at[k - 1, 0], right)
        above = start(qb.at[k - 1, 0:edge], halo.at[k - 1, 1], left)
        if k == 1:
            for later in range(2, steps):
                send_drift(later)
            turn_over(1)
        if k < steps:
            take_drift(k)
        else:
            dp[...] = decay * dp[...] - half * dq[...]
            for r in range(ring):
                for at in range(x):
                    back_q[r, at] = collect(dq, r, at)
                    back_p[0, r, at] = collect(dp, r, at).astype(jnp.bfloat16)
            sent_q = to_ring(lambda r: back_q.at[r], got_q.at[:, mine])
            sent_p = to_ring(lambda r: back_p.at[0, r], got_p.at[0, :, mine])
            got_q[:, mine] = back_q[me]
            got_p[0, :, mine] = back_p[0, me]
            dp[...] = dp[...] - dp[...].astype(jnp.bfloat16).astype(jnp.float32)
        arrive([below, above])
        spread(
            jnp.concatenate(
                [halo[k - 1, 0].astype(jnp.float32), q, halo[k - 1, 1].astype(jnp.float32)], axis=0
            )
        )
        g = gradient(lambda: None)
        if k < steps:
            shift = whole(dq, 0, rows)
            now = decay * whole(dp, 0, rows) - (2 * half) * (g + shift)
            put(dp, now)
            put(dq, shift + push * now)
        else:
            put(dp, whole(dp, 0, rows) - half * g)
    for r in range(ring):
        for at in range(x):
            back_p[1, r, at] = collect(dp, r, at).astype(jnp.bfloat16)
    last_p = to_ring(lambda r: back_p.at[1, r], got_p.at[1, :, mine])
    got_p[1, :, mine] = back_p[1, me]

    def untie(value, which, out, at):
        flat = value.T
        for j in range(y):
            part = pl.ds(at * y + j, c, stride=x * y)
            out[part, :] = fixed[which, part, :] + flat[j * c : (j + 1) * c]

    arrive(sent_q)
    for at in range(x):
        untie(got_q[at], 0, q_out, at)
    arrive(sent_p)
    arrive(last_p)
    for at in range(x):
        untie(got_p[0, at].astype(jnp.float32) + got_p[1, at].astype(jnp.float32), 1, p_out, at)
    for copy in sent:
        copy.wait_send()


def fits_ring(sizes, position, filter_in):
    nx, ny, nz = sizes
    c, x, y, z = position.shape
    co, ci = filter_in.shape[:2]
    ring = nx * ny
    return (
        nz == 2 and ny == 2 and nx > 1 and y * c == LANES and x * nx == ROWS and y * ny > 2
        and z % (ring * EDGE) == 0 and z // ring == EDGE and co % EDGE == 0 and LANES % ci == 0
        and y * ny * ci == LANES
    )


def on_ring(sizes, position, momentum, noise, filter_in, filter_out, bias):
    nx, ny, nz = sizes
    c, x, y, z = position.shape
    steps = noise.shape[0]
    co, ci = filter_in.shape[:2]
    ring = nx * ny
    zb = z // ring
    xx, yy = x * nx, y * ny
    wide = yy * c
    rows = zb * xx
    lane = LANES
    tiles = -(-27 * ci // lane)
    flat = jax.ShapeDtypeStruct((c * x * y, z), jnp.float32)
    copies = (4 + steps) * (ring - 1) + 4 * nx + 4 + 2 * steps
    heights = [(zb + 2 * reach) * xx for reach in (3, 2, 1, 0)]
    vmem = pl.BlockSpec(memory_space=pltpu.VMEM)
    bf16, f32 = jnp.bfloat16, jnp.float32
    q, p = pl.pallas_call(
        functools.partial(ring_kernel, steps, sizes, heights),
        out_shape=(flat, flat),
        in_specs=[pl.BlockSpec(memory_space=pl.ANY)] * 6,
        out_specs=(vmem, vmem),
        scratch_shapes=[
            pltpu.VMEM((c * x * y, z), f32),
            pltpu.VMEM((c * x * y, z), f32),
            pltpu.VMEM((steps * c * x * y, z), bf16),
            pltpu.VMEM((27, co, ci), bf16),
            pltpu.VMEM((27, co, ci), bf16),
            pltpu.VMEM((1, c), f32),
            pltpu.VMEM((2 * tiles, co, lane), bf16),
            pltpu.VMEM((ring, 2 * tiles, co, lane), bf16),
            pltpu.VMEM((2, 9, wide, wide), bf16),
            pltpu.VMEM((2, 9, wide, wide), bf16),
            pltpu.VMEM((x, z, lane), f32),
            pltpu.VMEM((2, x, ROWS, lane), f32),
            pltpu.VMEM((ring, x + 1, zb, lane), bf16),
            pltpu.VMEM((ring, x + 1, zb, lane), bf16),
            pltpu.VMEM((steps, ring, x, zb, lane), bf16),
            pltpu.VMEM((steps, ring, x, zb, lane), bf16),
            pltpu.VMEM((ny, rows + ROWS * xx, lane), f32),
            pltpu.VMEM((3, 2, rows + ROWS * xx, wide), bf16),
            pltpu.VMEM((rows + 6 * xx, wide), f32),
            pltpu.VMEM((rows, wide), f32),
            pltpu.VMEM((ny, rows, lane), f32),
            pltpu.VMEM((ny, rows, lane), f32),
            pltpu.VMEM((ny, rows, lane), f32),
            pltpu.VMEM((steps, rows, wide), bf16),
            pltpu.VMEM((steps, 2, 4 * xx, wide), bf16),
            pltpu.VMEM((ring, x, zb, lane), f32),
            pltpu.VMEM((x, z, lane), f32),
            pltpu.VMEM((2, ring, x, zb, lane), bf16),
            pltpu.VMEM((2, x, z, lane), bf16),
            pltpu.VMEM((2, c * x * y, z), f32),
            pltpu.VMEM((steps, c * x * y, z), f32),
            pltpu.SemaphoreType.DMA((copies,)),
            pltpu.SemaphoreType.DMA((copies,)),
            pltpu.SemaphoreType.DMA((6,)),
        ],
        compiler_params=pltpu.CompilerParams(
            collective_id=0, has_side_effects=True, vmem_limit_bytes=24 * 2**20
        ),
    )(
        *(
            pltpu.with_memory_space_constraint(each, pltpu.HBM)
            for each in (
                position.reshape(-1, z),
                momentum.reshape(-1, z),
                noise.reshape(-1, z),
                filter_in.transpose(2, 3, 4, 0, 1).reshape(27, co, ci),
                filter_out.transpose(2, 3, 4, 0, 1).reshape(27, co, ci),
                bias[None],
            )
        )
    )
    return q.reshape(position.shape), p.reshape(momentum.shape)


def on_device(sizes, position, momentum, noise, filter_in, filter_out, bias):
    if fits_ring(sizes, position, filter_in):
        return on_ring(sizes, position, momentum, noise, filter_in, filter_out, bias)
    nx, ny, nz = sizes
    c, x, y, z = position.shape
    steps = noise.shape[0]
    assert x >= 2 and y == 2 and z % EDGE == 0 and nx > 2 and ny > 1
    both = jnp.stack([filter_in, filter_out])
    co, ci = both.shape[1], both.shape[2]
    gather = []
    if co % EDGE == 0:
        both = both.transpose(0, 1, 3, 5, 4, 2).reshape(2, co, 27 * ci)
        gather = [
            pltpu.VMEM((ny, nx, 2, co, 27 * ci), jnp.bfloat16),
            pltpu.VMEM((2, 9, 3, c, c), jnp.bfloat16),
            pltpu.SemaphoreType.DMA((nx * ny - 1,)),
            pltpu.SemaphoreType.DMA((nx * ny - 1,)),
        ]
    else:
        both = both.reshape(2 * co, ci * 27)
        both = lax.all_gather(both, ("gx", "gy"), axis=0, tiled=True)
        both = both.reshape(nx, ny, 2, co, ci, 3, 3, 3)
        both = both.transpose(2, 5, 7, 6, 0, 3, 1, 4).reshape(2, 9, 3, c, c)
    lanes = y * c
    slots = 2 * y if ny == 2 else 3 * y
    full = z + 2 * EDGE
    wide = (y + 2) * c
    flat = jax.ShapeDtypeStruct((c, x * y * z), jnp.float32)
    copies = 15 if ny == 2 else 24
    vmem = pl.BlockSpec(memory_space=pltpu.VMEM)
    q, p = pl.pallas_call(
        functools.partial(kernel, steps, sizes),
        out_shape=(flat, flat),
        in_specs=[vmem] * 5,
        out_specs=(vmem, vmem),
        scratch_shapes=[
            pltpu.VMEM((9, wide, slots * c), jnp.bfloat16),
            pltpu.VMEM((9, lanes, wide), jnp.bfloat16),
            pltpu.VMEM((9, wide, lanes), jnp.bfloat16),
            pltpu.VMEM((9, slots * c, wide), jnp.bfloat16),
            pltpu.VMEM((x + 4, full, slots * c), jnp.bfloat16),
            pltpu.VMEM((x + 4, full, slots * c), jnp.bfloat16),
            pltpu.VMEM((x + 2, full, wide), jnp.float32),
            pltpu.VMEM((x, z, lanes), jnp.float32),
            pltpu.VMEM((x, z, lanes), jnp.float32),
            pltpu.SemaphoreType.DMA((2, copies)),
            pltpu.SemaphoreType.DMA((2, copies)),
            *gather,
        ],
        compiler_params=pltpu.CompilerParams(
            collective_id=0, has_side_effects=True, vmem_limit_bytes=56 * 2**20
        ),
    )(
        position.reshape(c, -1),
        momentum.reshape(c, -1),
        noise.reshape(steps, c, -1),
        both,
        jnp.tile(bias, y + 2)[None],
    )
    return q.reshape(position.shape), p.reshape(momentum.shape)


def solution(mesh):
    field = P(None, ("grp", "gx"), "gy", "gz")
    filters = P("gx", "gy", None, None, None)
    sizes = tuple(mesh.shape[name] for name in ("gx", "gy", "gz"))
    return jax.shard_map(
        functools.partial(on_device, sizes),
        mesh=mesh,
        in_specs=(field, field, P(None, None, ("grp", "gx"), "gy", "gz"), filters, filters, P()),
        out_specs=(field, field),
        check_vma=False,
    )
```

```python
import functools

import jax
import jax.numpy as jnp
import numpy as np
from jax import lax
from jax.experimental import pallas as pl
from jax.experimental.pallas import tpu as pltpu
from jax.sharding import PartitionSpec as P

EDGE = 16
MESH = pl.DeviceIdType.MESH


def kernel(steps, sizes, pos_ref, mom_ref, noise_ref, w_ref, bias_ref,
           q_out, p_out, a1, a2, b1, b2, eq, eh, t_ref, q_ref, p_ref, send, recv, *gather):
    nx, ny, nz = sizes
    c = pos_ref.shape[0]
    inside = len(gather) > 0
    if inside:
        wg, wf, wsend, wrecv = gather
    x, z, lanes = q_ref.shape
    y = lanes // c
    full = eq.shape[1]
    wrap = ny == 2
    slots = eq.shape[2] // c
    own = slice(EDGE, EDGE + z)
    mine = slice(lanes, 2 * lanes)

    ix, iy, iz = lax.axis_index("gx"), lax.axis_index("gy"), lax.axis_index("gz")
    up = {"gx": lax.rem(ix + 1, nx), "gy": lax.rem(iy + 1, ny), "gz": lax.rem(iz + 1, nz)}
    down = {
        "gx": lax.rem(ix + nx - 1, nx),
        "gy": lax.rem(iy + ny - 1, ny),
        "gz": lax.rem(iz + nz - 1, nz),
    }

    def at_side(**which):
        return {axis: which[axis][axis] for axis in which}

    def early(buf):
        core = slice(2, 2 + x)
        low, high = slice(0, EDGE), slice(z + EDGE, full)
        block = buf.at[core, own, mine]
        edges = (
            (up, buf.at[core, z : z + EDGE, mine], low),
            (down, buf.at[core, EDGE : 2 * EDGE, mine], high),
        )
        out = []
        for side, source, rows in edges:
            out.append((at_side(gz=side), source, buf.at[core, rows, mine], True))
        for beside, part in others:
            out.append((at_side(gy=beside), block, buf.at[core, own, part], True))
            for side, source, rows in edges:
                target = buf.at[core, rows, part]
                out.append((at_side(gy=beside, gz=side), source, target, True))
        out.append(
            (at_side(gx=down), buf.at[2:4, own, mine], buf.at[2 + x : 4 + x, own, mine], False)
        )
        out.append((at_side(gx=up), buf.at[x : 2 + x, own, mine], buf.at[0:2, own, mine], False))
        return out

    def late(buf):
        low, high = slice(0, EDGE), slice(z + EDGE, full)
        from_low = (up, slice(x, 2 + x), slice(0, 2))
        from_high = (down, slice(2, 4), slice(2 + x, 4 + x))
        plan = []
        for _, part in others:
            plan.append((from_low, slice(0, full), part))
            plan += [(from_high, low, part), (from_high, high, part)]
        for side in (from_low, from_high):
            plan += [(side, low, mine), (side, high, mine)]
        return [
            (at_side(gx=side), buf.at[source, rows, part], buf.at[target, rows, part])
            for (side, source, target), rows, part in plan
        ]

    def forward(buf):
        planes = slice(2 + x, 4 + x)
        return [
            (at_side(gy=beside), buf.at[planes, own, mine], buf.at[planes, own, part])
            for beside, part in others
        ]

    others = [(up, slice(0, lanes))]
    if not wrap:
        others.append((down, slice(2 * lanes, 3 * lanes)))

    def remote(source, target, sems, number, device):
        return pltpu.make_async_remote_copy(
            src_ref=source,
            dst_ref=target,
            send_sem=sems[0].at[number],
            recv_sem=sems[1].at[number],
            device_id=device,
            device_id_type=MESH,
        )

    peers = []
    if inside:
        for dx in range(nx):
            for dy in range(ny):
                if dx or dy:
                    peers.append({"gx": lax.rem(ix + dx, nx), "gy": lax.rem(iy + dy, ny)})
    barrier = pltpu.get_barrier_semaphore()
    greeted = peers + [device for device, _, _, _ in early(eq)]
    for device in greeted:
        pl.semaphore_signal(barrier, inc=1, device_id=device, device_id_type=MESH)
    pl.semaphore_wait(barrier, len(greeted))

    if inside:
        copies = []
        for number, device in enumerate(peers):
            copy = remote(w_ref, wg.at[iy, ix], (wsend, wrecv), number, device)
            copy.start()
            copies.append(copy)
        wg[iy, ix] = w_ref[...]
        for copy in copies:
            copy.wait()
        ci = c // ny
        for which in range(2):
            for at in range(27):
                columns = []
                for j in range(ny):
                    pieces = [wg[j, i, which, :, at * ci : (at + 1) * ci] for i in range(nx)]
                    columns.append(jnp.concatenate(pieces, axis=0))
                wf[which, at // 3, at % 3] = jnp.concatenate(columns, axis=1)
        filters = wf
    else:
        filters = w_ref

    def exchange(buf, bank):
        sems = (send.at[bank], recv.at[bank])
        first, own_x = [], []
        number = 0
        for device, source, target, passed in early(buf):
            copy = remote(source, target, sems, number, device)
            number += 1
            copy.start()
            (first if passed else own_x).append(copy)
        for copy in first:
            copy.wait_recv()
        second = []
        for device, source, target in late(buf):
            copy = remote(source, target, sems, number, device)
            number += 1
            copy.start()
            second.append(copy)
        own_x[0].wait_recv()
        for device, source, target in forward(buf):
            copy = remote(source, target, sems, number, device)
            number += 1
            copy.start()
            second.append(copy)
        for copy in own_x[1:] + second:
            copy.wait_recv()
        for copy in first + own_x + second:
            copy.wait_send()

    def slot(at):
        return at % slots

    def unfold(tap, carry):
        blank = jnp.zeros((c, c), jnp.bfloat16)

        def rows(out, which, at, flip, cols, pick):
            line = [blank] * cols
            for col, b in pick:
                line[col] = filters[which, at, 2 - b if flip else b]
            return jnp.concatenate(line, axis=1)

        back = 8 - tap
        for yo in range(y + 2):
            a1[tap, yo * c : (yo + 1) * c, :] = rows(
                a1, 0, tap, False, slots, [(slot(yo + b), b) for b in range(3)]
            )
        for yo in range(y):
            a2[tap, yo * c : (yo + 1) * c, :] = rows(
                a2, 1, tap, False, y + 2, [(yo + b, b) for b in range(3)]
            )
        for s in range(slots):
            pick = [(yo, b) for yo in range(y + 2) for b in range(3) if slot(yo + b) == s]
            b2[tap, s * c : (s + 1) * c, :] = rows(b2, 1, back, True, y + 2, pick)
        for yi in range(y + 2):
            pick = [(yo, yi - yo) for yo in range(y) if 0 <= yi - yo <= 2]
            b1[tap, yi * c : (yi + 1) * c, :] = rows(b1, 0, back, True, y, pick)
        return carry

    lax.fori_loop(0, 9, unfold, 0)

    def load(ref2d, at):
        span = [ref2d[:, (at * y + j) * z : (at * y + j + 1) * z] for j in range(y)]
        return jnp.concatenate(span, axis=0).astype(jnp.float32).T

    for at in range(x):
        q_ref[at] = load(pos_ref, at)
        p_ref[at] = load(mom_ref, at)

    def conv(source, weights, out_x, transposed):
        width = source.shape[2]
        total = None
        for tz in range(3):
            part = None
            for tx in range(3):
                left = source[tx : tx + out_x].reshape(out_x * full, width)
                term = lax.dot_general(
                    left,
                    weights[tx * 3 + tz],
                    (((1,), (1 if transposed else 0,)), ((), ())),
                    preferred_element_type=jnp.float32,
                )
                part = term if part is None else part + term
            if tz != 1:
                part = pltpu.roll(part, 1 if tz == 0 else out_x * full - 1, 0)
            total = part if total is None else total + part
        return total.reshape(out_x, full, total.shape[-1])

    step = 0.25
    decay = jnp.exp(jnp.float32(-0.25))
    kick = jnp.sqrt(1.0 - decay * decay)

    def body(k, carry):
        eq[2 : 2 + x, own, mine] = q_ref[...].astype(jnp.bfloat16)
        exchange(eq, 0)
        t_ref[...] = jnp.tanh(conv(eq, a1, x + 2, True) + bias_ref[...][None])
        h2 = conv(t_ref[...].astype(jnp.bfloat16), a2, x, True)
        eh[2 : 2 + x, own, mine] = h2[:, own].astype(jnp.bfloat16)
        exchange(eh, 1)
        gu = conv(eh, b2, x + 2, False)
        t = t_ref[...]
        gh = (gu * (1.0 - t * t)).astype(jnp.bfloat16)
        force = conv(gh, b1, x, False)[:, own] + q_ref[...]
        half = 0.5 * step

        @pl.when(k > 0)
        def _():
            p_ref[...] = p_ref[...] - half * force

        @pl.when(k < steps)
        def _():
            p = p_ref[...] - half * force
            q = q_ref[...] + half * p
            now = noise_ref.at[k]
            drawn = jnp.stack([load(now, at) for at in range(x)])
            p = decay * p + kick * drawn
            q_ref[...] = q + half * p
            p_ref[...] = p

        return carry

    lax.fori_loop(0, steps + 1, body, 0)

    for ref, out in ((q_ref, q_out), (p_ref, p_out)):
        for at in range(x):
            flat = ref[at].T
            for j in range(y):
                out[:, (at * y + j) * z : (at * y + j + 1) * z] = flat[j * c : (j + 1) * c]


LANES = 128
ROWS = 8


def ring_place(r, nx):
    row, step = r // nx, r % nx
    return step + (row % 2) * (nx - 1 - 2 * step), row


def ring_kernel(steps, sizes, heights, *refs):
    accs = []
    for unit in range(2):
        for height in heights:
            low = -(-height // (2 * EDGE)) * EDGE
            for part in (low, height - low):
                accs.append(pltpu.ACC(unit)((part, 2 * LANES), jnp.float32))
    pl.run_scoped(functools.partial(ring_body, steps, sizes, refs), *accs)


def ring_body(steps, sizes, refs, *sums):
    nx, ny, nz = sizes
    count = len(sums) // 2
    accs = [
        [[sums[unit * count + 2 * place + part] for part in range(2)] for unit in range(2)]
        for place in range(count // 2)
    ]
    inputs, refs = refs[:6], refs[6:]
    (q_out, p_out, pos_ref, mom_ref, noise_ref, fin_ref, fout_ref, bias_ref, own_w, all_w, mats,
     flipped, turned, edges, msg0, got0, msgd, gotd, stage, lhs, t_ref, base, extra, dq, dp, qb,
     halo, back_q, got_q, back_p, got_p, fixed, loose, send, recv, load) = refs
    ring = nx * ny
    x, zb = msg0.shape[1] - 1, msg0.shape[2]
    lane = LANES
    z = ring * zb
    taps, co, ci = fin_ref.shape
    c = ny * ci
    y = lane // c
    xx, yy = x * nx, y * ny
    per = lane // ci
    tiles = own_w.shape[1]
    wide = yy * c
    reach = 4
    rows = zb * xx

    ix, iy, iz = lax.axis_index("gx"), lax.axis_index("gy"), lax.axis_index("gz")
    me = iy * nx + ix + (iy % 2) * (nx - 1 - 2 * ix)
    block = nz * me + iz
    home = block // ring == iz
    filed = block % ring

    def device(r, core):
        gx, gy = ring_place(r, nx)
        return {"gx": gx, "gy": gy, "gz": core}

    barrier = pltpu.get_barrier_semaphore()
    everyone = 0
    for dx in range(nx):
        for dy in range(ny):
            for dz in range(nz):
                if dx or dy or dz:
                    everyone += 1
                    pl.semaphore_signal(
                        barrier,
                        inc=1,
                        device_id={"gx": (ix + dx) % nx, "gy": (iy + dy) % ny, "gz": (iz + dz) % nz},
                        device_id_type=MESH,
                    )

    loads = []
    held = (pos_ref, mom_ref, noise_ref, fin_ref, fout_ref, bias_ref)
    for number in (3, 4, 0, 1, 2, 5):
        copy = pltpu.make_async_copy(inputs[number], held[number], load.at[number])
        copy.start()
        loads.append(copy)

    def copy_of(source, target, number, where):
        return pltpu.make_async_remote_copy(
            src_ref=source,
            dst_ref=target,
            send_sem=send.at[number],
            recv_sem=recv.at[number],
            device_id=where,
            device_id_type=MESH,
        )

    across = {"gy": (iy + 1) % ny}
    other = {"gz": (iz + 1) % nz}

    def start(source, target, number, where):
        copy_of(source, target, number, where).start()

    def arrive(number, like):
        copy_of(like, like, number, other).wait_recv()

    def leave(number, like):
        copy_of(like, like, number, other).wait_send()

    def start_or_keep(source, target, number, where):
        @pl.when(home)
        def _():
            pltpu.make_async_copy(source, target, recv.at[number]).start()

        @pl.when(jnp.logical_not(home))
        def _():
            start(source, target, number, where)

    def to_owners(buf, target, number):
        for j in range(1, ring + 1):
            at = (filed + j) % ring
            owner = iz * ring + at
            go = start if j < ring else start_or_keep
            go(buf.at[at], target, number, device(owner // nz, owner % nz))

    def to_sources(buf, target, number):
        for j in range(1, ring + 1):
            r = (me + j) % ring
            go = start if j < ring else start_or_keep
            go(buf.at[r], target, number, device(r, block // ring))

    def left_ring(number, buf):
        @pl.when(home)
        def _():
            leave(number, buf.at[0 : ring - 1])

        @pl.when(jnp.logical_not(home))
        def _():
            leave(number, buf)

    column_sems = [[which * (nx - 1) + dx for dx in range(nx - 1)] for which in range(2)]
    across_sem = [2 * (nx - 1), 2 * (nx - 1) + 1]
    swap_sem = [2 * nx, 2 * nx + 1]
    edge_sem, field_sem = 2 * nx + 2, 2 * nx + 3
    drift_sem = [2 * nx + 4 + k for k in range(steps)]
    halo_sem = [2 * nx + 4 + steps + k for k in range(steps)]
    q_sem, p_sem = 2 * nx + 4 + 2 * steps, [2 * nx + 5 + 2 * steps, 2 * nx + 6 + 2 * steps]

    outer = iz == nz - 1
    loads[0].wait()
    loads[1].wait()

    @pl.when(outer)
    def _():
        for which, ref in enumerate((fin_ref, fout_ref)):
            for tile in range(tiles):
                span = range(tile * per, min(taps, (tile + 1) * per))
                parts = [ref[t].astype(jnp.float32) for t in span]
                parts += [jnp.zeros((co, ci), jnp.float32)] * (per - len(parts))
                own_w[which, tile] = jnp.concatenate(parts, axis=1).astype(jnp.bfloat16)

    def turn(ref, at):
        parts = [ref[pl.ds(at * y + j, c, stride=x * y), :] for j in range(y)]
        return jnp.concatenate(parts, axis=0).T

    loads[2].wait()
    for at in range(x):
        turned[at] = turn(pos_ref, at)

    for each in sums:
        pltpu.matmul_pop(each)

    pl.semaphore_wait(barrier, everyone)

    def to_column(which):
        for dx in range(1, nx):
            there = {"gx": (ix + dx) % nx}
            start(own_w.at[which], all_w.at[which, me], column_sems[which][dx - 1], there)
        start(own_w.at[which], all_w.at[which, me], across_sem[which], across)

    def pass_on(which):
        for dx in range(1, nx):
            arrive(column_sems[which][dx - 1], own_w.at[which])
            gx = (ix + nx - dx) % nx
            r = iy * nx + gx + (iy % 2) * (nx - 1 - 2 * gx)
            start(all_w.at[which, r], all_w.at[which, r], across_sem[which], across)

    @pl.when(outer)
    def _():
        to_column(0)

    start(turned.at[:, z - ROWS : z], edges.at[0], edge_sem, {"gz": (iz + 1) % nz})
    start(turned.at[:, 0:ROWS], edges.at[1], edge_sem, {"gz": (iz + nz - 1) % nz})

    @pl.when(outer)
    def _():
        to_column(1)
        all_w[:, me] = own_w[...]

    upper = lax.broadcasted_iota(jnp.int32, (ROWS, lane), 0) < reach
    arrive(edge_sem, edges)
    for r in range(ring):
        around = []
        for at in range(x):
            msg0[r, at] = turned[at, r * zb : (r + 1) * zb].astype(jnp.bfloat16)
            before = turned[at, r * zb - ROWS : r * zb] if r else edges[0, at]
            after = turned[at, (r + 1) * zb : (r + 1) * zb + ROWS] if r < ring - 1 else edges[1, at]
            around.append(jnp.where(upper, after, before))
        msg0[r, x] = jnp.concatenate(around, axis=0).astype(jnp.bfloat16)
    to_owners(msg0, got0.at[me], field_sem)

    half = 0.125
    decay = float(np.exp(np.float32(-0.25)))
    kick = float(np.sqrt(np.float32(1.0) - np.exp(np.float32(-0.25)) ** 2))
    push = half * (1.0 + decay)
    loads[3].wait()
    loads[4].wait()
    loads[5].wait()
    q = pos_ref[...]
    known = q.astype(jnp.bfloat16).astype(jnp.float32)
    p = mom_ref[...] - half * q
    total = x * y * c
    for k in range(steps):
        noise = noise_ref[k * total : (k + 1) * total].astype(jnp.float32)
        q = q + push * p + (half * kick) * noise
        drift = (q - known).astype(jnp.bfloat16).astype(jnp.float32)
        known = known + drift
        last = k == steps - 1
        p = decay * p + kick * noise - (half if last else 2 * half) * q
        loose[k] = drift
        for at in range(x):
            flat = turn(loose.at[k], at).astype(jnp.bfloat16)
            for r in range(ring):
                msgd[k, r, at] = flat[r * zb : (r + 1) * zb]
    fixed[0] = q
    fixed[1] = p

    def send_drift(k):
        to_owners(msgd.at[k], gotd.at[k, me], drift_sem[k])

    @pl.when(outer)
    def _():
        pass_on(0)
        pass_on(1)

    send_drift(0)

    def swap(which):
        @pl.when(outer)
        def _():
            arrive(across_sem[which], all_w.at[which, 0:nx])
            start(all_w.at[which], all_w.at[which], swap_sem[which], other)

    def swapped(which):
        @pl.when(jnp.logical_not(outer))
        def _():
            arrive(swap_sem[which], all_w.at[which])

    at_lane = lax.broadcasted_iota(jnp.int32, (co, lane), 1)

    def build(which):
        def place(gx, carry):
            row = pl.multiple_of(gx * co, co)
            for a in range(3):
                for cz in range(3):
                    moved = {}
                    for b in range(3):
                        t = a * 9 + b * 3 + cz
                        tile, spot = t // per, t % per
                        for side in range(2):
                            pieces = []
                            for gy in range(ny):
                                r = gy * nx + gx + (gy % 2) * (nx - 1 - 2 * gx)
                                piece = all_w[which, r, tile].astype(jnp.float32)
                                shift = (side * ny + gy - spot) % per
                                pieces.append(pltpu.roll(piece, shift * ci, 1) if shift else piece)
                            moved[b, side] = pieces
                    pairs = []
                    for b in range(yy):
                        value = jnp.zeros((co, lane), jnp.float32)
                        for side in range(y):
                            near = (b + side) % yy
                            if near > 2:
                                continue
                            for gy in range(ny):
                                spot = (side * ny + gy) * ci
                                inside = (at_lane >= spot) & (at_lane < spot + ci)
                                value = jnp.where(inside, moved[near, side][gy], value)
                        pairs.append(value.astype(jnp.bfloat16))
                    for yo in range(yy):
                        for h in range(yy // y):
                            mats[which, a * 3 + cz, pl.ds(yo * c + row, co), h * lane : (h + 1) * lane] = (
                                pairs[(h * y + 1 - yo) % yy]
                            )
            return carry

        lax.fori_loop(0, nx, place, 0)

    def turn_over(which):
        for tap in range(9):
            flipped[which, tap] = mats[which, tap].T

    def scatter(target, zs, value, r, at):
        gx, gy = ring_place(r, nx)
        target[gy, pl.ds(zs * xx + gx * x + at, value.shape[0], stride=xx), :] = value

    def whole(ref, rows_from, rows_to):
        return jnp.concatenate([ref[gy, rows_from:rows_to] for gy in range(ny)], axis=1)

    swap(0)
    swapped(0)
    build(0)
    swap(1)
    turn_over(0)
    arrive(field_sem, got0)
    send_drift(1)
    for r in range(ring):
        around = got0[r, x].astype(jnp.float32)
        for at in range(x):
            scatter(stage, 0, got0[r, at].astype(jnp.float32), r, at)
            scatter(stage, zb, around[at * ROWS : (at + 1) * ROWS], r, at)
    base[...] = whole(stage, 0, rows)

    def spread(value):
        n = value.shape[0]
        cube = value.reshape(n // xx, xx, wide)
        for a in range(3):
            moved = cube if a == 1 else pltpu.roll(cube, (1 - a) % xx, 1)
            moved = moved.reshape(n, wide)
            lhs[a, 0, 0:n] = moved.astype(jnp.bfloat16)
            lhs[a, 1, 0 : n - 2 * xx] = moved[xx : n - xx].astype(jnp.bfloat16)

    def conv(place, which, adjoint, flip=False):
        source = mats if adjoint or flip else flipped
        sums = accs[place]
        low, high = sums[0][0].shape[0], sums[0][1].shape[0]
        plans = (
            [(0, True, True), (1, True, True), (2, True, True), (3, True, True), (4, True, False)],
            [(8, True, True), (7, True, True), (6, True, True), (5, True, True), (4, False, True)],
        )
        for at in range(5):
            for unit in range(2):
                tap, use_low, use_high = plans[unit][at]
                a, cz = tap // 3, tap % 3
                pltpu.matmul_push_rhs(
                    source[which, 8 - tap if adjoint else tap],
                    staging_register=at % 2,
                    mxu_index=unit,
                    transpose=flip,
                )
                copy, first_row = (1, 0) if cz == 1 else (0, cz * xx)
                fresh = at % 2
                if use_low:
                    left = lhs[a, copy, first_row : first_row + low]
                    pltpu.matmul_acc_lhs(sums[unit][0], left, load_staged_rhs=fresh)
                    fresh = None
                if use_high:
                    left = lhs[a, copy, first_row + low : first_row + low + high]
                    pltpu.matmul_acc_lhs(sums[unit][1], left, load_staged_rhs=fresh)
        halves = [pltpu.matmul_pop(sums[0][part]) + pltpu.matmul_pop(sums[1][part]) for part in range(2)]
        return jnp.concatenate(halves, axis=0)

    row = jnp.concatenate([bias_ref[...]] * yy, axis=1)

    def gradient(between, flip=False):
        t = jnp.tanh(conv(0, 0, False) + row)
        t_ref[...] = t
        spread(t)
        between()
        spread(conv(1, 1, False, flip))
        gu = conv(2, 1, True)
        t = t_ref[2 * xx : 2 * xx + gu.shape[0]]
        spread(gu * (1.0 - t * t))
        return conv(3, 0, True)

    def take_drift(k):
        arrive(drift_sem[k], gotd.at[k])
        for r in range(ring):
            for at in range(x):
                scatter(extra, 0, gotd[k, r, at].astype(jnp.float32), r, at)
        base[...] = base[...] + whole(extra, 0, rows)

    def second_filters():
        swapped(1)
        build(1)

    def collect(ref, r, at):
        gx, gy = ring_place(r, nx)
        return ref[gy, pl.ds(gx * x + at, zb, stride=xx), :]

    def put(ref, value):
        for gy in range(ny):
            ref[gy] = value[:, gy * lane : (gy + 1) * lane]

    turn_at = (zb + reach) * xx
    field = [whole(stage, turn_at, turn_at + reach * xx), whole(stage, 0, turn_at)]
    spread(jnp.concatenate(field, axis=0))
    g = gradient(second_filters, True)
    put(dp, -half * g)
    put(dq, (-half * push) * g)
    take_drift(0)

    left = device((me + ring - 1 + iz) % ring, 1 - iz)
    right = device((me + iz) % ring, 1 - iz)
    edge = reach * xx
    mine = pl.ds(pl.multiple_of(filed * zb, zb), zb)
    for k in range(1, steps + 1):
        q = base[...] + whole(dq, 0, rows)
        qb[k - 1] = q.astype(jnp.bfloat16)
        start(qb.at[k - 1, rows - edge : rows], halo.at[k - 1, 0], halo_sem[k - 1], right)
        start(qb.at[k - 1, 0:edge], halo.at[k - 1, 1], halo_sem[k - 1], left)
        if k == 1:
            for later in range(2, steps):
                send_drift(later)
            turn_over(1)
        if k < steps:
            take_drift(k)
        else:
            dp[...] = decay * dp[...] - half * dq[...]
            for r in range(ring):
                for at in range(x):
                    back_q[r, at] = collect(dq, r, at).astype(jnp.bfloat16)
                    back_p[0, r, at] = collect(dp, r, at).astype(jnp.bfloat16)
            to_sources(back_q, got_q.at[:, mine], q_sem)
            to_sources(back_p.at[0], got_p.at[0, :, mine], p_sem[0])
            dp[...] = dp[...] - dp[...].astype(jnp.bfloat16).astype(jnp.float32)
        arrive(halo_sem[k - 1], halo.at[k - 1])
        spread(
            jnp.concatenate(
                [halo[k - 1, 0].astype(jnp.float32), q, halo[k - 1, 1].astype(jnp.float32)], axis=0
            )
        )
        g = gradient(lambda: None)
        if k < steps:
            shift = whole(dq, 0, rows)
            now = decay * whole(dp, 0, rows) - (2 * half) * (g + shift)
            put(dp, now)
            put(dq, shift + push * now)
        else:
            put(dp, whole(dp, 0, rows) - half * g)
    for r in range(ring):
        for at in range(x):
            back_p[1, r, at] = collect(dp, r, at).astype(jnp.bfloat16)
    to_sources(back_p.at[1], got_p.at[1, :, mine], p_sem[1])

    def untie(value, which, out, at):
        flat = value.T
        for j in range(y):
            part = pl.ds(at * y + j, c, stride=x * y)
            out[part, :] = fixed[which, part, :] + flat[j * c : (j + 1) * c]

    arrive(q_sem, got_q)
    for at in range(x):
        untie(got_q[at].astype(jnp.float32), 0, q_out, at)
    arrive(p_sem[0], got_p.at[0])
    arrive(p_sem[1], got_p.at[1])
    for at in range(x):
        untie(got_p[0, at].astype(jnp.float32) + got_p[1, at].astype(jnp.float32), 1, p_out, at)

    @pl.when(outer)
    def _():
        for which in range(2):
            for number in column_sems[which]:
                leave(number, own_w.at[which])
            leave(across_sem[which], all_w.at[which, 0:nx])
            leave(swap_sem[which], all_w.at[which])

    leave(edge_sem, edges)
    left_ring(field_sem, msg0)
    for k in range(steps):
        left_ring(drift_sem[k], msgd.at[k])
        leave(halo_sem[k], halo.at[k])
    left_ring(q_sem, back_q)
    for part in range(2):
        left_ring(p_sem[part], back_p.at[part])


def fits_ring(sizes, position, filter_in):
    nx, ny, nz = sizes
    c, x, y, z = position.shape
    co, ci = filter_in.shape[:2]
    ring = nx * ny
    return (
        nz == 2 and ny == 2 and nx > 1 and y * c == LANES and x * nx == ROWS and y * ny > 2
        and z % (ring * EDGE) == 0 and z // ring == EDGE and co % EDGE == 0 and LANES % ci == 0
        and y * ny * ci == LANES
    )


def on_ring(sizes, position, momentum, noise, filter_in, filter_out, bias):
    nx, ny, nz = sizes
    c, x, y, z = position.shape
    steps = noise.shape[0]
    co, ci = filter_in.shape[:2]
    ring = nx * ny
    zb = z // ring
    xx, yy = x * nx, y * ny
    wide = yy * c
    rows = zb * xx
    lane = LANES
    tiles = -(-27 * ci // lane)
    flat = jax.ShapeDtypeStruct((c * x * y, z), jnp.float32)
    copies = 2 * nx + 7 + 2 * steps
    heights = [(zb + 2 * reach) * xx for reach in (3, 2, 1, 0)]
    vmem = pl.BlockSpec(memory_space=pltpu.VMEM)
    bf16, f32 = jnp.bfloat16, jnp.float32
    q, p = pl.pallas_call(
        functools.partial(ring_kernel, steps, sizes, heights),
        out_shape=(flat, flat),
        in_specs=[pl.BlockSpec(memory_space=pl.ANY)] * 6,
        out_specs=(vmem, vmem),
        scratch_shapes=[
            pltpu.VMEM((c * x * y, z), f32),
            pltpu.VMEM((c * x * y, z), f32),
            pltpu.VMEM((steps * c * x * y, z), bf16),
            pltpu.VMEM((27, co, ci), bf16),
            pltpu.VMEM((27, co, ci), bf16),
            pltpu.VMEM((1, c), f32),
            pltpu.VMEM((2, tiles, co, lane), bf16),
            pltpu.VMEM((2, ring, tiles, co, lane), bf16),
            pltpu.VMEM((2, 9, wide, wide), bf16),
            pltpu.VMEM((2, 9, wide, wide), bf16),
            pltpu.VMEM((x, z, lane), f32),
            pltpu.VMEM((2, x, ROWS, lane), f32),
            pltpu.VMEM((ring, x + 1, zb, lane), bf16),
            pltpu.VMEM((ring, x + 1, zb, lane), bf16),
            pltpu.VMEM((steps, ring, x, zb, lane), bf16),
            pltpu.VMEM((steps, ring, x, zb, lane), bf16),
            pltpu.VMEM((ny, rows + ROWS * xx, lane), f32),
            pltpu.VMEM((3, 2, rows + ROWS * xx, wide), bf16),
            pltpu.VMEM((rows + 6 * xx, wide), f32),
            pltpu.VMEM((rows, wide), f32),
            pltpu.VMEM((ny, rows, lane), f32),
            pltpu.VMEM((ny, rows, lane), f32),
            pltpu.VMEM((ny, rows, lane), f32),
            pltpu.VMEM((steps, rows, wide), bf16),
            pltpu.VMEM((steps, 2, 4 * xx, wide), bf16),
            pltpu.VMEM((ring, x, zb, lane), bf16),
            pltpu.VMEM((x, z, lane), bf16),
            pltpu.VMEM((2, ring, x, zb, lane), bf16),
            pltpu.VMEM((2, x, z, lane), bf16),
            pltpu.VMEM((2, c * x * y, z), f32),
            pltpu.VMEM((steps, c * x * y, z), f32),
            pltpu.SemaphoreType.DMA((copies,)),
            pltpu.SemaphoreType.DMA((copies,)),
            pltpu.SemaphoreType.DMA((6,)),
        ],
        compiler_params=pltpu.CompilerParams(
            collective_id=0, has_side_effects=True, vmem_limit_bytes=24 * 2**20
        ),
    )(
        *(
            pltpu.with_memory_space_constraint(each, pltpu.HBM)
            for each in (
                position.reshape(-1, z),
                momentum.reshape(-1, z),
                noise.reshape(-1, z),
                filter_in.transpose(2, 3, 4, 0, 1).reshape(27, co, ci),
                filter_out.transpose(2, 3, 4, 0, 1).reshape(27, co, ci),
                bias[None],
            )
        )
    )
    return q.reshape(position.shape), p.reshape(momentum.shape)


def on_device(sizes, position, momentum, noise, filter_in, filter_out, bias):
    if fits_ring(sizes, position, filter_in):
        return on_ring(sizes, position, momentum, noise, filter_in, filter_out, bias)
    nx, ny, nz = sizes
    c, x, y, z = position.shape
    steps = noise.shape[0]
    assert x >= 2 and y == 2 and z % EDGE == 0 and nx > 2 and ny > 1
    both = jnp.stack([filter_in, filter_out])
    co, ci = both.shape[1], both.shape[2]
    gather = []
    if co % EDGE == 0:
        both = both.transpose(0, 1, 3, 5, 4, 2).reshape(2, co, 27 * ci)
        gather = [
            pltpu.VMEM((ny, nx, 2, co, 27 * ci), jnp.bfloat16),
            pltpu.VMEM((2, 9, 3, c, c), jnp.bfloat16),
            pltpu.SemaphoreType.DMA((nx * ny - 1,)),
            pltpu.SemaphoreType.DMA((nx * ny - 1,)),
        ]
    else:
        both = both.reshape(2 * co, ci * 27)
        both = lax.all_gather(both, ("gx", "gy"), axis=0, tiled=True)
        both = both.reshape(nx, ny, 2, co, ci, 3, 3, 3)
        both = both.transpose(2, 5, 7, 6, 0, 3, 1, 4).reshape(2, 9, 3, c, c)
    lanes = y * c
    slots = 2 * y if ny == 2 else 3 * y
    full = z + 2 * EDGE
    wide = (y + 2) * c
    flat = jax.ShapeDtypeStruct((c, x * y * z), jnp.float32)
    copies = 15 if ny == 2 else 24
    vmem = pl.BlockSpec(memory_space=pltpu.VMEM)
    q, p = pl.pallas_call(
        functools.partial(kernel, steps, sizes),
        out_shape=(flat, flat),
        in_specs=[vmem] * 5,
        out_specs=(vmem, vmem),
        scratch_shapes=[
            pltpu.VMEM((9, wide, slots * c), jnp.bfloat16),
            pltpu.VMEM((9, lanes, wide), jnp.bfloat16),
            pltpu.VMEM((9, wide, lanes), jnp.bfloat16),
            pltpu.VMEM((9, slots * c, wide), jnp.bfloat16),
            pltpu.VMEM((x + 4, full, slots * c), jnp.bfloat16),
            pltpu.VMEM((x + 4, full, slots * c), jnp.bfloat16),
            pltpu.VMEM((x + 2, full, wide), jnp.float32),
            pltpu.VMEM((x, z, lanes), jnp.float32),
            pltpu.VMEM((x, z, lanes), jnp.float32),
            pltpu.SemaphoreType.DMA((2, copies)),
            pltpu.SemaphoreType.DMA((2, copies)),
            *gather,
        ],
        compiler_params=pltpu.CompilerParams(
            collective_id=0, has_side_effects=True, vmem_limit_bytes=56 * 2**20
        ),
    )(
        position.reshape(c, -1),
        momentum.reshape(c, -1),
        noise.reshape(steps, c, -1),
        both,
        jnp.tile(bias, y + 2)[None],
    )
    return q.reshape(position.shape), p.reshape(momentum.shape)


def solution(mesh):
    field = P(None, ("grp", "gx"), "gy", "gz")
    filters = P("gx", "gy", None, None, None)
    sizes = tuple(mesh.shape[name] for name in ("gx", "gy", "gz"))
    return jax.shard_map(
        functools.partial(on_device, sizes),
        mesh=mesh,
        in_specs=(field, field, P(None, None, ("grp", "gx"), "gy", "gz"), filters, filters, P()),
        out_specs=(field, field),
        check_vma=False,
    )
```

```python
import functools

import jax
import jax.numpy as jnp
import numpy as np
from jax import lax
from jax.experimental import pallas as pl
from jax.experimental.pallas import tpu as pltpu
from jax.sharding import PartitionSpec as P

EDGE = 16
MESH = pl.DeviceIdType.MESH


def kernel(steps, sizes, pos_ref, mom_ref, noise_ref, w_ref, bias_ref,
           q_out, p_out, a1, a2, b1, b2, eq, eh, t_ref, q_ref, p_ref, send, recv, *gather):
    nx, ny, nz = sizes
    c = pos_ref.shape[0]
    inside = len(gather) > 0
    if inside:
        wg, wf, wsend, wrecv = gather
    x, z, lanes = q_ref.shape
    y = lanes // c
    full = eq.shape[1]
    wrap = ny == 2
    slots = eq.shape[2] // c
    own = slice(EDGE, EDGE + z)
    mine = slice(lanes, 2 * lanes)

    ix, iy, iz = lax.axis_index("gx"), lax.axis_index("gy"), lax.axis_index("gz")
    up = {"gx": lax.rem(ix + 1, nx), "gy": lax.rem(iy + 1, ny), "gz": lax.rem(iz + 1, nz)}
    down = {
        "gx": lax.rem(ix + nx - 1, nx),
        "gy": lax.rem(iy + ny - 1, ny),
        "gz": lax.rem(iz + nz - 1, nz),
    }

    def at_side(**which):
        return {axis: which[axis][axis] for axis in which}

    def early(buf):
        core = slice(2, 2 + x)
        low, high = slice(0, EDGE), slice(z + EDGE, full)
        block = buf.at[core, own, mine]
        edges = (
            (up, buf.at[core, z : z + EDGE, mine], low),
            (down, buf.at[core, EDGE : 2 * EDGE, mine], high),
        )
        out = []
        for side, source, rows in edges:
            out.append((at_side(gz=side), source, buf.at[core, rows, mine], True))
        for beside, part in others:
            out.append((at_side(gy=beside), block, buf.at[core, own, part], True))
            for side, source, rows in edges:
                target = buf.at[core, rows, part]
                out.append((at_side(gy=beside, gz=side), source, target, True))
        out.append(
            (at_side(gx=down), buf.at[2:4, own, mine], buf.at[2 + x : 4 + x, own, mine], False)
        )
        out.append((at_side(gx=up), buf.at[x : 2 + x, own, mine], buf.at[0:2, own, mine], False))
        return out

    def late(buf):
        low, high = slice(0, EDGE), slice(z + EDGE, full)
        from_low = (up, slice(x, 2 + x), slice(0, 2))
        from_high = (down, slice(2, 4), slice(2 + x, 4 + x))
        plan = []
        for _, part in others:
            plan.append((from_low, slice(0, full), part))
            plan += [(from_high, low, part), (from_high, high, part)]
        for side in (from_low, from_high):
            plan += [(side, low, mine), (side, high, mine)]
        return [
            (at_side(gx=side), buf.at[source, rows, part], buf.at[target, rows, part])
            for (side, source, target), rows, part in plan
        ]

    def forward(buf):
        planes = slice(2 + x, 4 + x)
        return [
            (at_side(gy=beside), buf.at[planes, own, mine], buf.at[planes, own, part])
            for beside, part in others
        ]

    others = [(up, slice(0, lanes))]
    if not wrap:
        others.append((down, slice(2 * lanes, 3 * lanes)))

    def remote(source, target, sems, number, device):
        return pltpu.make_async_remote_copy(
            src_ref=source,
            dst_ref=target,
            send_sem=sems[0].at[number],
            recv_sem=sems[1].at[number],
            device_id=device,
            device_id_type=MESH,
        )

    peers = []
    if inside:
        for dx in range(nx):
            for dy in range(ny):
                if dx or dy:
                    peers.append({"gx": lax.rem(ix + dx, nx), "gy": lax.rem(iy + dy, ny)})
    barrier = pltpu.get_barrier_semaphore()
    greeted = peers + [device for device, _, _, _ in early(eq)]
    for device in greeted:
        pl.semaphore_signal(barrier, inc=1, device_id=device, device_id_type=MESH)
    pl.semaphore_wait(barrier, len(greeted))

    if inside:
        copies = []
        for number, device in enumerate(peers):
            copy = remote(w_ref, wg.at[iy, ix], (wsend, wrecv), number, device)
            copy.start()
            copies.append(copy)
        wg[iy, ix] = w_ref[...]
        for copy in copies:
            copy.wait()
        ci = c // ny
        for which in range(2):
            for at in range(27):
                columns = []
                for j in range(ny):
                    pieces = [wg[j, i, which, :, at * ci : (at + 1) * ci] for i in range(nx)]
                    columns.append(jnp.concatenate(pieces, axis=0))
                wf[which, at // 3, at % 3] = jnp.concatenate(columns, axis=1)
        filters = wf
    else:
        filters = w_ref

    def exchange(buf, bank):
        sems = (send.at[bank], recv.at[bank])
        first, own_x = [], []
        number = 0
        for device, source, target, passed in early(buf):
            copy = remote(source, target, sems, number, device)
            number += 1
            copy.start()
            (first if passed else own_x).append(copy)
        for copy in first:
            copy.wait_recv()
        second = []
        for device, source, target in late(buf):
            copy = remote(source, target, sems, number, device)
            number += 1
            copy.start()
            second.append(copy)
        own_x[0].wait_recv()
        for device, source, target in forward(buf):
            copy = remote(source, target, sems, number, device)
            number += 1
            copy.start()
            second.append(copy)
        for copy in own_x[1:] + second:
            copy.wait_recv()
        for copy in first + own_x + second:
            copy.wait_send()

    def slot(at):
        return at % slots

    def unfold(tap, carry):
        blank = jnp.zeros((c, c), jnp.bfloat16)

        def rows(out, which, at, flip, cols, pick):
            line = [blank] * cols
            for col, b in pick:
                line[col] = filters[which, at, 2 - b if flip else b]
            return jnp.concatenate(line, axis=1)

        back = 8 - tap
        for yo in range(y + 2):
            a1[tap, yo * c : (yo + 1) * c, :] = rows(
                a1, 0, tap, False, slots, [(slot(yo + b), b) for b in range(3)]
            )
        for yo in range(y):
            a2[tap, yo * c : (yo + 1) * c, :] = rows(
                a2, 1, tap, False, y + 2, [(yo + b, b) for b in range(3)]
            )
        for s in range(slots):
            pick = [(yo, b) for yo in range(y + 2) for b in range(3) if slot(yo + b) == s]
            b2[tap, s * c : (s + 1) * c, :] = rows(b2, 1, back, True, y + 2, pick)
        for yi in range(y + 2):
            pick = [(yo, yi - yo) for yo in range(y) if 0 <= yi - yo <= 2]
            b1[tap, yi * c : (yi + 1) * c, :] = rows(b1, 0, back, True, y, pick)
        return carry

    lax.fori_loop(0, 9, unfold, 0)

    def load(ref2d, at):
        span = [ref2d[:, (at * y + j) * z : (at * y + j + 1) * z] for j in range(y)]
        return jnp.concatenate(span, axis=0).astype(jnp.float32).T

    for at in range(x):
        q_ref[at] = load(pos_ref, at)
        p_ref[at] = load(mom_ref, at)

    def conv(source, weights, out_x, transposed):
        width = source.shape[2]
        total = None
        for tz in range(3):
            part = None
            for tx in range(3):
                left = source[tx : tx + out_x].reshape(out_x * full, width)
                term = lax.dot_general(
                    left,
                    weights[tx * 3 + tz],
                    (((1,), (1 if transposed else 0,)), ((), ())),
                    preferred_element_type=jnp.float32,
                )
                part = term if part is None else part + term
            if tz != 1:
                part = pltpu.roll(part, 1 if tz == 0 else out_x * full - 1, 0)
            total = part if total is None else total + part
        return total.reshape(out_x, full, total.shape[-1])

    step = 0.25
    decay = jnp.exp(jnp.float32(-0.25))
    kick = jnp.sqrt(1.0 - decay * decay)

    def body(k, carry):
        eq[2 : 2 + x, own, mine] = q_ref[...].astype(jnp.bfloat16)
        exchange(eq, 0)
        t_ref[...] = jnp.tanh(conv(eq, a1, x + 2, True) + bias_ref[...][None])
        h2 = conv(t_ref[...].astype(jnp.bfloat16), a2, x, True)
        eh[2 : 2 + x, own, mine] = h2[:, own].astype(jnp.bfloat16)
        exchange(eh, 1)
        gu = conv(eh, b2, x + 2, False)
        t = t_ref[...]
        gh = (gu * (1.0 - t * t)).astype(jnp.bfloat16)
        force = conv(gh, b1, x, False)[:, own] + q_ref[...]
        half = 0.5 * step

        @pl.when(k > 0)
        def _():
            p_ref[...] = p_ref[...] - half * force

        @pl.when(k < steps)
        def _():
            p = p_ref[...] - half * force
            q = q_ref[...] + half * p
            now = noise_ref.at[k]
            drawn = jnp.stack([load(now, at) for at in range(x)])
            p = decay * p + kick * drawn
            q_ref[...] = q + half * p
            p_ref[...] = p

        return carry

    lax.fori_loop(0, steps + 1, body, 0)

    for ref, out in ((q_ref, q_out), (p_ref, p_out)):
        for at in range(x):
            flat = ref[at].T
            for j in range(y):
                out[:, (at * y + j) * z : (at * y + j + 1) * z] = flat[j * c : (j + 1) * c]


LANES = 128
ROWS = 8


def ring_place(r, nx):
    row, step = r // nx, r % nx
    return step + (row % 2) * (nx - 1 - 2 * step), row


def split_rows(height):
    low = -(-height // (2 * EDGE)) * EDGE
    return low, height - low


def ring_kernel(steps, sizes, heights, *refs):
    pool = {}
    for height in heights:
        parts = split_rows(height)
        for part in parts:
            pool[part] = max(pool.get(part, 0), parts.count(part))
    order = [(unit, part, i) for unit in range(2) for part in sorted(pool) for i in range(pool[part])]
    spaces = [pltpu.ACC(unit)((part, 2 * LANES), jnp.float32) for unit, part, _ in order]
    pl.run_scoped(functools.partial(ring_body, steps, sizes, order, refs), *spaces)


def ring_body(steps, sizes, order, refs, *sums):
    nx, ny, nz = sizes
    banks = dict(zip(order, sums))
    inputs, refs = refs[:6], refs[6:]
    (q_out, p_out, pos_ref, mom_ref, noise_ref, fin_ref, fout_ref, bias_ref, own_w, all_w, mats,
     flipped, turned, turned_d, edges, msg0, got0, msgd, gotd, stage, lhs, t_ref, base, extra, dq, dp, qb,
     halo, vb, ring_v, back_q, got_q, back_p, got_p, fixed, loose, edges_d, msge, gote, send, recv,
     load) = refs
    ring = nx * ny
    x, zb = msg0.shape[1] // 2, msg0.shape[2]
    lane = LANES
    z = ring * zb
    taps, co, ci = fin_ref.shape
    c = ny * ci
    y = lane // c
    xx, yy = x * nx, y * ny
    per = lane // ci
    tiles = own_w.shape[1]
    wide = yy * c
    reach = 4
    rows = zb * xx

    ix, iy, iz = lax.axis_index("gx"), lax.axis_index("gy"), lax.axis_index("gz")
    me = iy * nx + ix + (iy % 2) * (nx - 1 - 2 * ix)
    block = nz * me + iz
    home = block // ring == iz
    filed = block % ring

    def device(r, core):
        gx, gy = ring_place(r, nx)
        return {"gx": gx, "gy": gy, "gz": core}

    barrier = pltpu.get_barrier_semaphore()
    everyone = 0
    for dx in range(nx):
        for dy in range(ny):
            for dz in range(nz):
                if dx or dy or dz:
                    everyone += 1
                    pl.semaphore_signal(
                        barrier,
                        inc=1,
                        device_id={"gx": (ix + dx) % nx, "gy": (iy + dy) % ny, "gz": (iz + dz) % nz},
                        device_id_type=MESH,
                    )

    loads = []
    held = (pos_ref, mom_ref, noise_ref, fin_ref, fout_ref, bias_ref)
    for number in (3, 4, 0, 1, 2, 5):
        copy = pltpu.make_async_copy(inputs[number], held[number], load.at[number])
        copy.start()
        loads.append(copy)

    def copy_of(source, target, number, where):
        return pltpu.make_async_remote_copy(
            src_ref=source,
            dst_ref=target,
            send_sem=send.at[number],
            recv_sem=recv.at[number],
            device_id=where,
            device_id_type=MESH,
        )

    across = {"gy": (iy + 1) % ny}
    other = {"gz": (iz + 1) % nz}

    def start(source, target, number, where):
        copy_of(source, target, number, where).start()

    def arrive(number, like):
        copy_of(like, like, number, other).wait_recv()

    def leave(number, like):
        copy_of(like, like, number, other).wait_send()

    def start_or_keep(source, target, number, where):
        @pl.when(home)
        def _():
            pltpu.make_async_copy(source, target, recv.at[number]).start()

        @pl.when(jnp.logical_not(home))
        def _():
            start(source, target, number, where)

    def to_owners(buf, target, number):
        for j in range(1, ring + 1):
            at = (filed + j) % ring
            owner = iz * ring + at
            go = start if j < ring else start_or_keep
            go(buf.at[at], target, number, device(owner // nz, owner % nz))

    def to_sources(buf, target, number):
        for j in range(1, ring + 1):
            r = (me + j) % ring
            go = start if j < ring else start_or_keep
            go(buf.at[r], target, number, device(r, block // ring))

    def left_ring(number, buf):
        @pl.when(home)
        def _():
            leave(number, buf.at[0 : ring - 1])

        @pl.when(jnp.logical_not(home))
        def _():
            leave(number, buf)

    column_sems = [[which * (nx - 1) + dx for dx in range(nx - 1)] for which in range(2)]
    across_sem = [2 * (nx - 1), 2 * (nx - 1) + 1]
    swap_sem = [2 * nx, 2 * nx + 1]
    edge_sem, field_sem = 2 * nx + 2, 2 * nx + 3
    drift_sem = [2 * nx + 4 + k for k in range(steps)]
    pairs = (steps - 1) // 2
    q_sem = 2 * nx + 4 + steps
    p_sem = [q_sem + 1, q_sem + 2]
    drift_edge_sem = q_sem + 3
    halo_sem = [q_sem + 4 + k for k in range(pairs)]
    v_sem = [q_sem + 4 + pairs + k for k in range(pairs)]

    outer = iz == nz - 1
    loads[0].wait()
    loads[1].wait()

    @pl.when(outer)
    def _():
        for which, ref in enumerate((fin_ref, fout_ref)):
            for tile in range(tiles):
                span = range(tile * per, min(taps, (tile + 1) * per))
                parts = [ref[t].astype(jnp.float32) for t in span]
                parts += [jnp.zeros((co, ci), jnp.float32)] * (per - len(parts))
                own_w[which, tile] = jnp.concatenate(parts, axis=1).astype(jnp.bfloat16)

    def turn(ref, at):
        parts = [ref[pl.ds(at * y + j, c, stride=x * y), :] for j in range(y)]
        return jnp.concatenate(parts, axis=0).T

    loads[2].wait()
    for at in range(x):
        turned[at] = turn(pos_ref, at)

    for each in sums:
        pltpu.matmul_pop(each)

    pl.semaphore_wait(barrier, everyone)

    def to_column(which):
        for dx in range(1, nx):
            there = {"gx": (ix + dx) % nx}
            start(own_w.at[which], all_w.at[which, me], column_sems[which][dx - 1], there)
        start(own_w.at[which], all_w.at[which, me], across_sem[which], across)

    def pass_on(which):
        for dx in range(1, nx):
            arrive(column_sems[which][dx - 1], own_w.at[which])
            gx = (ix + nx - dx) % nx
            r = iy * nx + gx + (iy % 2) * (nx - 1 - 2 * gx)
            start(all_w.at[which, r], all_w.at[which, r], across_sem[which], across)

    @pl.when(outer)
    def _():
        to_column(0)

    start(turned.at[:, z - ROWS : z], edges.at[0], edge_sem, {"gz": (iz + 1) % nz})
    start(turned.at[:, 0:ROWS], edges.at[1], edge_sem, {"gz": (iz + nz - 1) % nz})

    @pl.when(outer)
    def _():
        to_column(1)
        all_w[:, me] = own_w[...]

    upper = lax.broadcasted_iota(jnp.int32, (ROWS, lane), 0) < reach

    def around(ref, beyond, r, at):
        before = ref[at, r * zb - ROWS : r * zb] if r else beyond[0, at]
        after = ref[at, (r + 1) * zb : (r + 1) * zb + ROWS] if r < ring - 1 else beyond[1, at]
        return before, after

    arrive(edge_sem, edges)
    for r in range(ring):
        for at in range(x):
            msg0[r, at] = turned[at, r * zb : (r + 1) * zb].astype(jnp.bfloat16)
            before, after = around(turned, edges, r, at)
            msg0[r, x + at] = jnp.concatenate([after, before], axis=0).astype(jnp.bfloat16)
    to_owners(msg0, got0.at[me], field_sem)

    half = 0.125
    decay = float(np.exp(np.float32(-0.25)))
    kick = float(np.sqrt(np.float32(1.0) - np.exp(np.float32(-0.25)) ** 2))
    push = half * (1.0 + decay)
    loads[3].wait()
    loads[4].wait()
    loads[5].wait()
    q = pos_ref[...]
    known = q.astype(jnp.bfloat16).astype(jnp.float32)
    p = mom_ref[...] - half * q
    total = x * y * c
    for k in range(steps):
        noise = noise_ref[k * total : (k + 1) * total].astype(jnp.float32)
        q = q + push * p + (half * kick) * noise
        drift = (q - known).astype(jnp.bfloat16).astype(jnp.float32)
        known = known + drift
        last = k == steps - 1
        p = decay * p + kick * noise - (half if last else 2 * half) * q
        loose[k] = drift
        for at in range(x):
            flat = turn(loose.at[k], at)
            if k == 0:
                turned_d[at] = flat
                for r in range(ring):
                    msge[r, at] = flat[r * zb : (r + 1) * zb].astype(jnp.bfloat16)
            else:
                flat = flat.astype(jnp.bfloat16)
                for r in range(ring):
                    msgd[k - 1, r, at] = flat[r * zb : (r + 1) * zb]
        if k == 0:
            start(turned_d.at[:, z - ROWS : z], edges_d.at[0], drift_edge_sem, {"gz": (iz + 1) % nz})
            start(turned_d.at[:, 0:ROWS], edges_d.at[1], drift_edge_sem, {"gz": (iz + nz - 1) % nz})
    fixed[0] = q
    fixed[1] = p

    def send_drift(k):
        if k == 0:
            to_owners(msge, gote.at[me], drift_sem[0])
        else:
            to_owners(msgd.at[k - 1], gotd.at[k - 1, me], drift_sem[k])

    @pl.when(outer)
    def _():
        pass_on(0)

    arrive(drift_edge_sem, edges_d)
    for r in range(ring):
        beyond = []
        for at in range(x):
            before, after = around(turned_d, edges_d, r, at)
            beyond.append(jnp.where(upper, after, before))
        msge[r, x] = jnp.concatenate(beyond, axis=0).astype(jnp.bfloat16)
    send_drift(0)

    def swap(which):
        arrive(across_sem[which], all_w.at[which, 0:nx])
        start(all_w.at[which], all_w.at[which], swap_sem[which], other)

    @pl.when(outer)
    def _():
        swap(0)
        pass_on(1)

    for later in range(1, steps):
        send_drift(later)

    def swapped(which):
        @pl.when(jnp.logical_not(outer))
        def _():
            arrive(swap_sem[which], all_w.at[which])

    at_lane = lax.broadcasted_iota(jnp.int32, (co, lane), 1)

    def build(which):
        def place(gx, carry):
            row = pl.multiple_of(gx * co, co)
            for a in range(3):
                for cz in range(3):
                    moved = {}
                    for b in range(3):
                        t = a * 9 + b * 3 + cz
                        tile, spot = t // per, t % per
                        for side in range(2):
                            pieces = []
                            for gy in range(ny):
                                r = gy * nx + gx + (gy % 2) * (nx - 1 - 2 * gx)
                                piece = all_w[which, r, tile].astype(jnp.float32)
                                shift = (side * ny + gy - spot) % per
                                pieces.append(pltpu.roll(piece, shift * ci, 1) if shift else piece)
                            moved[b, side] = pieces
                    pairs = []
                    for b in range(yy):
                        value = jnp.zeros((co, lane), jnp.float32)
                        for side in range(y):
                            near = (b + side) % yy
                            if near > 2:
                                continue
                            for gy in range(ny):
                                spot = (side * ny + gy) * ci
                                inside = (at_lane >= spot) & (at_lane < spot + ci)
                                value = jnp.where(inside, moved[near, side][gy], value)
                        pairs.append(value.astype(jnp.bfloat16))
                    for yo in range(yy):
                        for h in range(yy // y):
                            mats[which, a * 3 + cz, pl.ds(yo * c + row, co), h * lane : (h + 1) * lane] = (
                                pairs[(h * y + 1 - yo) % yy]
                            )
            return carry

        lax.fori_loop(0, nx, place, 0)

    def turn_over(which):
        for tap in range(9):
            flipped[which, tap] = mats[which, tap].T

    def scatter(target, zs, value, r, at):
        gx, gy = ring_place(r, nx)
        target[gy, pl.ds(zs * xx + gx * x + at, value.shape[0], stride=xx), :] = value

    def whole(ref, rows_from, rows_to):
        return jnp.concatenate([ref[gy, rows_from:rows_to] for gy in range(ny)], axis=1)

    swapped(0)
    build(0)

    @pl.when(outer)
    def _():
        swap(1)

    turn_over(0)
    arrive(field_sem, got0)
    for r in range(ring):
        for at in range(x):
            scatter(stage, 0, got0[r, at].astype(jnp.float32), r, at)
            scatter(stage, zb, got0[r, x + at].astype(jnp.float32), r, at)

    def spread(value):
        n = value.shape[0]
        cube = value.reshape(n // xx, xx, wide)
        for a in range(3):
            moved = cube if a == 1 else pltpu.roll(cube, (1 - a) % xx, 1)
            moved = moved.reshape(n, wide)
            lhs[a, 0, 0:n] = moved.astype(jnp.bfloat16)
            lhs[a, 1, 0 : n - 2 * xx] = moved[xx : n - xx].astype(jnp.bfloat16)

    def conv(height, which, adjoint, flip=False):
        source = mats if adjoint or flip else flipped
        low, high = split_rows(height)
        sums = [[banks[unit, low, 0], banks[unit, high, int(low == high)]] for unit in range(2)]
        plans = (
            [(0, True, True), (1, True, True), (2, True, True), (3, True, True), (4, True, False)],
            [(8, True, True), (7, True, True), (6, True, True), (5, True, True), (4, False, True)],
        )
        for at in range(5):
            for unit in range(2):
                tap, use_low, use_high = plans[unit][at]
                a, cz = tap // 3, tap % 3
                pltpu.matmul_push_rhs(
                    source[which, 8 - tap if adjoint else tap],
                    staging_register=at % 2,
                    mxu_index=unit,
                    transpose=flip,
                )
                copy, first_row = (1, 0) if cz == 1 else (0, cz * xx)
                fresh = at % 2
                if use_low:
                    left = lhs[a, copy, first_row : first_row + low]
                    pltpu.matmul_acc_lhs(sums[unit][0], left, load_staged_rhs=fresh)
                    fresh = None
                if use_high:
                    left = lhs[a, copy, first_row + low : first_row + low + high]
                    pltpu.matmul_acc_lhs(sums[unit][1], left, load_staged_rhs=fresh)
        halves = [pltpu.matmul_pop(sums[0][part]) + pltpu.matmul_pop(sums[1][part]) for part in range(2)]
        return jnp.concatenate(halves, axis=0)

    row = jnp.concatenate([bias_ref[...]] * yy, axis=1)

    def gradient(extent, between=lambda: None, flip=False):
        n = [rows + 2 * (extent + 3 - i) * xx for i in range(4)]
        t = jnp.tanh(conv(n[0], 0, False) + row)
        t_ref[0 : n[0]] = t
        spread(t)
        between()
        spread(conv(n[1], 1, False, flip))
        gu = conv(n[2], 1, True)
        t = t_ref[2 * xx : 2 * xx + n[2]]
        spread(gu * (1.0 - t * t))
        return conv(n[3], 0, True)

    def take_drift(k):
        arrive(drift_sem[k], gotd.at[k - 1])
        for r in range(ring):
            for at in range(x):
                scatter(extra, 0, gotd[k - 1, r, at].astype(jnp.float32), r, at)
        base[...] = base[...] + whole(extra, 0, rows)

    def second_filters():
        swapped(1)
        build(1)

    def collect(ref, r, at):
        gx, gy = ring_place(r, nx)
        return ref[gy, pl.ds(gx * x + at, zb, stride=xx), :]

    def put(ref, value):
        for gy in range(ny):
            ref[gy] = value[:, gy * lane : (gy + 1) * lane]

    edge = reach * xx
    full = rows + 4 * edge
    ends = [whole(stage, full - 2 * edge, full), whole(stage, 0, full - 2 * edge)]
    spread(jnp.concatenate(ends, axis=0))
    g = gradient(reach, second_filters, True)

    arrive(drift_sem[0], gote)
    for r in range(ring):
        beyond = gote[r, x].astype(jnp.float32)
        for at in range(x):
            scatter(extra, 0, gote[r, at].astype(jnp.float32), r, at)
            scatter(extra, zb, beyond[at * ROWS : (at + 1) * ROWS], r, at)
    now = whole(stage, 0, rows) + whole(extra, 0, rows)
    base[...] = now
    above = whole(stage, rows, rows + edge) + whole(extra, rows, rows + edge)
    below = whole(stage, full - edge, full) + whole(extra, rows + edge, rows + 2 * edge)
    force = g[edge : edge + rows]
    put(dp, -half * force)
    put(dq, (-half * push) * force)
    spread(jnp.concatenate([below, now, above], axis=0) + (-half * push) * g)

    left = device((me + ring - 1 + iz) % ring, 1 - iz)
    right = device((me + iz) % ring, 1 - iz)
    mine = pl.ds(pl.multiple_of(filed * zb, zb), zb)

    def kicked(g):
        shift = whole(dq, 0, rows)
        now = decay * whole(dp, 0, rows) - (2 * half) * (g + shift)
        put(dp, now)
        put(dq, shift + push * now)

    for pair in range(pairs):
        kicked(gradient(0, flip=pair == 0))
        k = 2 * pair + 2
        take_drift(k - 1)
        q = base[...] + whole(dq, 0, rows)
        qb[pair] = q.astype(jnp.bfloat16)
        start(qb.at[pair, rows - 2 * edge : rows], halo.at[pair, 0], halo_sem[pair], right)
        start(qb.at[pair, 0 : 2 * edge], halo.at[pair, 1], halo_sem[pair], left)
        if pair == 0:
            turn_over(1)
        take_drift(k)
        shift = whole(dq, 0, rows)
        v = base[...] + shift + push * (decay * whole(dp, 0, rows) - (2 * half) * shift)
        vb[pair] = v.astype(jnp.bfloat16)
        start(vb.at[pair, rows - edge : rows], ring_v.at[pair, 0], v_sem[pair], right)
        start(vb.at[pair, 0:edge], ring_v.at[pair, 1], v_sem[pair], left)
        arrive(halo_sem[pair], halo.at[pair])
        ends = [halo[pair, side].astype(jnp.float32) for side in range(2)]
        spread(jnp.concatenate([ends[0], q, ends[1]], axis=0))
        g = gradient(reach)
        kicked(g[edge : edge + rows])
        q = base[...] + whole(dq, 0, rows)
        arrive(v_sem[pair], ring_v.at[pair])
        ends = [
            ring_v[pair, side].astype(jnp.float32) - (2 * half * push) * g[at : at + edge]
            for side, at in enumerate((0, edge + rows))
        ]
        spread(jnp.concatenate([ends[0], q, ends[1]], axis=0))

    put(dp, decay * whole(dp, 0, rows) - half * whole(dq, 0, rows))
    for r in range(ring):
        for at in range(x):
            back_q[r, at] = collect(dq, r, at).astype(jnp.bfloat16)
            back_p[0, r, at] = collect(dp, r, at).astype(jnp.bfloat16)
    to_sources(back_q, got_q.at[:, mine], q_sem)
    to_sources(back_p.at[0], got_p.at[0, :, mine], p_sem[0])
    g = gradient(0)
    left_over = whole(dp, 0, rows)
    left_over = left_over - left_over.astype(jnp.bfloat16).astype(jnp.float32)
    put(dp, left_over - half * g)
    for r in range(ring):
        for at in range(x):
            back_p[1, r, at] = collect(dp, r, at).astype(jnp.bfloat16)
    to_sources(back_p.at[1], got_p.at[1, :, mine], p_sem[1])

    def untie(value, which, out, at):
        flat = value.T
        for j in range(y):
            part = pl.ds(at * y + j, c, stride=x * y)
            out[part, :] = fixed[which, part, :] + flat[j * c : (j + 1) * c]

    arrive(q_sem, got_q)
    for at in range(x):
        untie(got_q[at].astype(jnp.float32), 0, q_out, at)
    arrive(p_sem[0], got_p.at[0])
    arrive(p_sem[1], got_p.at[1])
    for at in range(x):
        untie(got_p[0, at].astype(jnp.float32) + got_p[1, at].astype(jnp.float32), 1, p_out, at)

    @pl.when(outer)
    def _():
        for which in range(2):
            for number in column_sems[which]:
                leave(number, own_w.at[which])
            leave(across_sem[which], all_w.at[which, 0:nx])
            leave(swap_sem[which], all_w.at[which])

    leave(edge_sem, edges)
    leave(drift_edge_sem, edges_d)
    left_ring(field_sem, msg0)
    left_ring(drift_sem[0], msge)
    for k in range(1, steps):
        left_ring(drift_sem[k], msgd.at[k - 1])
    for pair in range(pairs):
        leave(halo_sem[pair], halo.at[pair])
        leave(v_sem[pair], ring_v.at[pair])
    left_ring(q_sem, back_q)
    for part in range(2):
        left_ring(p_sem[part], back_p.at[part])


def fits_ring(steps, sizes, position, filter_in):
    nx, ny, nz = sizes
    c, x, y, z = position.shape
    co, ci = filter_in.shape[:2]
    ring = nx * ny
    return (
        steps % 2 == 1 and steps > 2 and nz == 2 and ny == 2 and nx > 1 and y * c == LANES and x * nx == ROWS and y * ny > 2
        and z % (ring * EDGE) == 0 and z // ring == EDGE and co % EDGE == 0 and LANES % ci == 0
        and y * ny * ci == LANES
    )


def on_ring(sizes, position, momentum, noise, filter_in, filter_out, bias):
    nx, ny, nz = sizes
    c, x, y, z = position.shape
    steps = noise.shape[0]
    co, ci = filter_in.shape[:2]
    ring = nx * ny
    zb = z // ring
    xx, yy = x * nx, y * ny
    wide = yy * c
    rows = zb * xx
    lane = LANES
    tiles = -(-27 * ci // lane)
    flat = jax.ShapeDtypeStruct((c * x * y, z), jnp.float32)
    reach, pairs = 4, (steps - 1) // 2
    copies = 2 * nx + 8 + steps + 2 * pairs
    edge = reach * xx
    heights = [(zb + 2 * beyond) * xx for beyond in range(2 * reach)]
    vmem = pl.BlockSpec(memory_space=pltpu.VMEM)
    bf16, f32 = jnp.bfloat16, jnp.float32
    q, p = pl.pallas_call(
        functools.partial(ring_kernel, steps, sizes, heights),
        out_shape=(flat, flat),
        in_specs=[pl.BlockSpec(memory_space=pl.ANY)] * 6,
        out_specs=(vmem, vmem),
        scratch_shapes=[
            pltpu.VMEM((c * x * y, z), f32),
            pltpu.VMEM((c * x * y, z), f32),
            pltpu.VMEM((steps * c * x * y, z), bf16),
            pltpu.VMEM((27, co, ci), bf16),
            pltpu.VMEM((27, co, ci), bf16),
            pltpu.VMEM((1, c), f32),
            pltpu.VMEM((2, tiles, co, lane), bf16),
            pltpu.VMEM((2, ring, tiles, co, lane), bf16),
            pltpu.VMEM((2, 9, wide, wide), bf16),
            pltpu.VMEM((2, 9, wide, wide), bf16),
            pltpu.VMEM((x, z, lane), f32),
            pltpu.VMEM((x, z, lane), f32),
            pltpu.VMEM((2, x, ROWS, lane), f32),
            pltpu.VMEM((ring, 2 * x, zb, lane), bf16),
            pltpu.VMEM((ring, 2 * x, zb, lane), bf16),
            pltpu.VMEM((steps - 1, ring, x, zb, lane), bf16),
            pltpu.VMEM((steps - 1, ring, x, zb, lane), bf16),
            pltpu.VMEM((ny, rows + 4 * edge, lane), f32),
            pltpu.VMEM((3, 2, rows + 4 * edge, wide), bf16),
            pltpu.VMEM((rows + 4 * edge - 2 * xx, wide), f32),
            pltpu.VMEM((rows, wide), f32),
            pltpu.VMEM((ny, rows + 2 * edge, lane), f32),
            pltpu.VMEM((ny, rows, lane), f32),
            pltpu.VMEM((ny, rows, lane), f32),
            pltpu.VMEM((pairs, rows, wide), bf16),
            pltpu.VMEM((pairs, 2, 2 * edge, wide), bf16),
            pltpu.VMEM((pairs, rows, wide), bf16),
            pltpu.VMEM((pairs, 2, edge, wide), bf16),
            pltpu.VMEM((ring, x, zb, lane), bf16),
            pltpu.VMEM((x, z, lane), bf16),
            pltpu.VMEM((2, ring, x, zb, lane), bf16),
            pltpu.VMEM((2, x, z, lane), bf16),
            pltpu.VMEM((2, c * x * y, z), f32),
            pltpu.VMEM((steps, c * x * y, z), f32),
            pltpu.VMEM((2, x, ROWS, lane), f32),
            pltpu.VMEM((ring, x + 1, zb, lane), bf16),
            pltpu.VMEM((ring, x + 1, zb, lane), bf16),
            pltpu.SemaphoreType.DMA((copies,)),
            pltpu.SemaphoreType.DMA((copies,)),
            pltpu.SemaphoreType.DMA((6,)),
        ],
        compiler_params=pltpu.CompilerParams(
            collective_id=0, has_side_effects=True, vmem_limit_bytes=24 * 2**20
        ),
    )(
        *(
            pltpu.with_memory_space_constraint(each, pltpu.HBM)
            for each in (
                position.reshape(-1, z),
                momentum.reshape(-1, z),
                noise.reshape(-1, z),
                filter_in.transpose(2, 3, 4, 0, 1).reshape(27, co, ci),
                filter_out.transpose(2, 3, 4, 0, 1).reshape(27, co, ci),
                bias[None],
            )
        )
    )
    return q.reshape(position.shape), p.reshape(momentum.shape)


def on_device(sizes, position, momentum, noise, filter_in, filter_out, bias):
    if fits_ring(noise.shape[0], sizes, position, filter_in):
        return on_ring(sizes, position, momentum, noise, filter_in, filter_out, bias)
    nx, ny, nz = sizes
    c, x, y, z = position.shape
    steps = noise.shape[0]
    assert x >= 2 and y == 2 and z % EDGE == 0 and nx > 2 and ny > 1
    both = jnp.stack([filter_in, filter_out])
    co, ci = both.shape[1], both.shape[2]
    gather = []
    if co % EDGE == 0:
        both = both.transpose(0, 1, 3, 5, 4, 2).reshape(2, co, 27 * ci)
        gather = [
            pltpu.VMEM((ny, nx, 2, co, 27 * ci), jnp.bfloat16),
            pltpu.VMEM((2, 9, 3, c, c), jnp.bfloat16),
            pltpu.SemaphoreType.DMA((nx * ny - 1,)),
            pltpu.SemaphoreType.DMA((nx * ny - 1,)),
        ]
    else:
        both = both.reshape(2 * co, ci * 27)
        both = lax.all_gather(both, ("gx", "gy"), axis=0, tiled=True)
        both = both.reshape(nx, ny, 2, co, ci, 3, 3, 3)
        both = both.transpose(2, 5, 7, 6, 0, 3, 1, 4).reshape(2, 9, 3, c, c)
    lanes = y * c
    slots = 2 * y if ny == 2 else 3 * y
    full = z + 2 * EDGE
    wide = (y + 2) * c
    flat = jax.ShapeDtypeStruct((c, x * y * z), jnp.float32)
    copies = 15 if ny == 2 else 24
    vmem = pl.BlockSpec(memory_space=pltpu.VMEM)
    q, p = pl.pallas_call(
        functools.partial(kernel, steps, sizes),
        out_shape=(flat, flat),
        in_specs=[vmem] * 5,
        out_specs=(vmem, vmem),
        scratch_shapes=[
            pltpu.VMEM((9, wide, slots * c), jnp.bfloat16),
            pltpu.VMEM((9, lanes, wide), jnp.bfloat16),
            pltpu.VMEM((9, wide, lanes), jnp.bfloat16),
            pltpu.VMEM((9, slots * c, wide), jnp.bfloat16),
            pltpu.VMEM((x + 4, full, slots * c), jnp.bfloat16),
            pltpu.VMEM((x + 4, full, slots * c), jnp.bfloat16),
            pltpu.VMEM((x + 2, full, wide), jnp.float32),
            pltpu.VMEM((x, z, lanes), jnp.float32),
            pltpu.VMEM((x, z, lanes), jnp.float32),
            pltpu.SemaphoreType.DMA((2, copies)),
            pltpu.SemaphoreType.DMA((2, copies)),
            *gather,
        ],
        compiler_params=pltpu.CompilerParams(
            collective_id=0, has_side_effects=True, vmem_limit_bytes=56 * 2**20
        ),
    )(
        position.reshape(c, -1),
        momentum.reshape(c, -1),
        noise.reshape(steps, c, -1),
        both,
        jnp.tile(bias, y + 2)[None],
    )
    return q.reshape(position.shape), p.reshape(momentum.shape)


def solution(mesh):
    field = P(None, ("grp", "gx"), "gy", "gz")
    filters = P("gx", "gy", None, None, None)
    sizes = tuple(mesh.shape[name] for name in ("gx", "gy", "gz"))
    return jax.shard_map(
        functools.partial(on_device, sizes),
        mesh=mesh,
        in_specs=(field, field, P(None, None, ("grp", "gx"), "gy", "gz"), filters, filters, P()),
        out_specs=(field, field),
        check_vma=False,
    )
```

```python
import functools

import jax
import jax.numpy as jnp
import numpy as np
from jax import lax
from jax.experimental import pallas as pl
from jax.experimental.pallas import tpu as pltpu
from jax.sharding import PartitionSpec as P

EDGE = 16
MESH = pl.DeviceIdType.MESH


def kernel(steps, sizes, pos_ref, mom_ref, noise_ref, w_ref, bias_ref,
           q_out, p_out, a1, a2, b1, b2, eq, eh, t_ref, q_ref, p_ref, send, recv, *gather):
    nx, ny, nz = sizes
    c = pos_ref.shape[0]
    inside = len(gather) > 0
    if inside:
        wg, wf, wsend, wrecv = gather
    x, z, lanes = q_ref.shape
    y = lanes // c
    full = eq.shape[1]
    wrap = ny == 2
    slots = eq.shape[2] // c
    own = slice(EDGE, EDGE + z)
    mine = slice(lanes, 2 * lanes)

    ix, iy, iz = lax.axis_index("gx"), lax.axis_index("gy"), lax.axis_index("gz")
    up = {"gx": lax.rem(ix + 1, nx), "gy": lax.rem(iy + 1, ny), "gz": lax.rem(iz + 1, nz)}
    down = {
        "gx": lax.rem(ix + nx - 1, nx),
        "gy": lax.rem(iy + ny - 1, ny),
        "gz": lax.rem(iz + nz - 1, nz),
    }

    def at_side(**which):
        return {axis: which[axis][axis] for axis in which}

    def early(buf):
        core = slice(2, 2 + x)
        low, high = slice(0, EDGE), slice(z + EDGE, full)
        block = buf.at[core, own, mine]
        edges = (
            (up, buf.at[core, z : z + EDGE, mine], low),
            (down, buf.at[core, EDGE : 2 * EDGE, mine], high),
        )
        out = []
        for side, source, rows in edges:
            out.append((at_side(gz=side), source, buf.at[core, rows, mine], True))
        for beside, part in others:
            out.append((at_side(gy=beside), block, buf.at[core, own, part], True))
            for side, source, rows in edges:
                target = buf.at[core, rows, part]
                out.append((at_side(gy=beside, gz=side), source, target, True))
        out.append(
            (at_side(gx=down), buf.at[2:4, own, mine], buf.at[2 + x : 4 + x, own, mine], False)
        )
        out.append((at_side(gx=up), buf.at[x : 2 + x, own, mine], buf.at[0:2, own, mine], False))
        return out

    def late(buf):
        low, high = slice(0, EDGE), slice(z + EDGE, full)
        from_low = (up, slice(x, 2 + x), slice(0, 2))
        from_high = (down, slice(2, 4), slice(2 + x, 4 + x))
        plan = []
        for _, part in others:
            plan.append((from_low, slice(0, full), part))
            plan += [(from_high, low, part), (from_high, high, part)]
        for side in (from_low, from_high):
            plan += [(side, low, mine), (side, high, mine)]
        return [
            (at_side(gx=side), buf.at[source, rows, part], buf.at[target, rows, part])
            for (side, source, target), rows, part in plan
        ]

    def forward(buf):
        planes = slice(2 + x, 4 + x)
        return [
            (at_side(gy=beside), buf.at[planes, own, mine], buf.at[planes, own, part])
            for beside, part in others
        ]

    others = [(up, slice(0, lanes))]
    if not wrap:
        others.append((down, slice(2 * lanes, 3 * lanes)))

    def remote(source, target, sems, number, device):
        return pltpu.make_async_remote_copy(
            src_ref=source,
            dst_ref=target,
            send_sem=sems[0].at[number],
            recv_sem=sems[1].at[number],
            device_id=device,
            device_id_type=MESH,
        )

    peers = []
    if inside:
        for dx in range(nx):
            for dy in range(ny):
                if dx or dy:
                    peers.append({"gx": lax.rem(ix + dx, nx), "gy": lax.rem(iy + dy, ny)})
    barrier = pltpu.get_barrier_semaphore()
    greeted = peers + [device for device, _, _, _ in early(eq)]
    for device in greeted:
        pl.semaphore_signal(barrier, inc=1, device_id=device, device_id_type=MESH)
    pl.semaphore_wait(barrier, len(greeted))

    if inside:
        copies = []
        for number, device in enumerate(peers):
            copy = remote(w_ref, wg.at[iy, ix], (wsend, wrecv), number, device)
            copy.start()
            copies.append(copy)
        wg[iy, ix] = w_ref[...]
        for copy in copies:
            copy.wait()
        ci = c // ny
        for which in range(2):
            for at in range(27):
                columns = []
                for j in range(ny):
                    pieces = [wg[j, i, which, :, at * ci : (at + 1) * ci] for i in range(nx)]
                    columns.append(jnp.concatenate(pieces, axis=0))
                wf[which, at // 3, at % 3] = jnp.concatenate(columns, axis=1)
        filters = wf
    else:
        filters = w_ref

    def exchange(buf, bank):
        sems = (send.at[bank], recv.at[bank])
        first, own_x = [], []
        number = 0
        for device, source, target, passed in early(buf):
            copy = remote(source, target, sems, number, device)
            number += 1
            copy.start()
            (first if passed else own_x).append(copy)
        for copy in first:
            copy.wait_recv()
        second = []
        for device, source, target in late(buf):
            copy = remote(source, target, sems, number, device)
            number += 1
            copy.start()
            second.append(copy)
        own_x[0].wait_recv()
        for device, source, target in forward(buf):
            copy = remote(source, target, sems, number, device)
            number += 1
            copy.start()
            second.append(copy)
        for copy in own_x[1:] + second:
            copy.wait_recv()
        for copy in first + own_x + second:
            copy.wait_send()

    def slot(at):
        return at % slots

    def unfold(tap, carry):
        blank = jnp.zeros((c, c), jnp.bfloat16)

        def rows(out, which, at, flip, cols, pick):
            line = [blank] * cols
            for col, b in pick:
                line[col] = filters[which, at, 2 - b if flip else b]
            return jnp.concatenate(line, axis=1)

        back = 8 - tap
        for yo in range(y + 2):
            a1[tap, yo * c : (yo + 1) * c, :] = rows(
                a1, 0, tap, False, slots, [(slot(yo + b), b) for b in range(3)]
            )
        for yo in range(y):
            a2[tap, yo * c : (yo + 1) * c, :] = rows(
                a2, 1, tap, False, y + 2, [(yo + b, b) for b in range(3)]
            )
        for s in range(slots):
            pick = [(yo, b) for yo in range(y + 2) for b in range(3) if slot(yo + b) == s]
            b2[tap, s * c : (s + 1) * c, :] = rows(b2, 1, back, True, y + 2, pick)
        for yi in range(y + 2):
            pick = [(yo, yi - yo) for yo in range(y) if 0 <= yi - yo <= 2]
            b1[tap, yi * c : (yi + 1) * c, :] = rows(b1, 0, back, True, y, pick)
        return carry

    lax.fori_loop(0, 9, unfold, 0)

    def load(ref2d, at):
        span = [ref2d[:, (at * y + j) * z : (at * y + j + 1) * z] for j in range(y)]
        return jnp.concatenate(span, axis=0).astype(jnp.float32).T

    for at in range(x):
        q_ref[at] = load(pos_ref, at)
        p_ref[at] = load(mom_ref, at)

    def conv(source, weights, out_x, transposed):
        width = source.shape[2]
        total = None
        for tz in range(3):
            part = None
            for tx in range(3):
                left = source[tx : tx + out_x].reshape(out_x * full, width)
                term = lax.dot_general(
                    left,
                    weights[tx * 3 + tz],
                    (((1,), (1 if transposed else 0,)), ((), ())),
                    preferred_element_type=jnp.float32,
                )
                part = term if part is None else part + term
            if tz != 1:
                part = pltpu.roll(part, 1 if tz == 0 else out_x * full - 1, 0)
            total = part if total is None else total + part
        return total.reshape(out_x, full, total.shape[-1])

    step = 0.25
    decay = jnp.exp(jnp.float32(-0.25))
    kick = jnp.sqrt(1.0 - decay * decay)

    def body(k, carry):
        eq[2 : 2 + x, own, mine] = q_ref[...].astype(jnp.bfloat16)
        exchange(eq, 0)
        t_ref[...] = jnp.tanh(conv(eq, a1, x + 2, True) + bias_ref[...][None])
        h2 = conv(t_ref[...].astype(jnp.bfloat16), a2, x, True)
        eh[2 : 2 + x, own, mine] = h2[:, own].astype(jnp.bfloat16)
        exchange(eh, 1)
        gu = conv(eh, b2, x + 2, False)
        t = t_ref[...]
        gh = (gu * (1.0 - t * t)).astype(jnp.bfloat16)
        force = conv(gh, b1, x, False)[:, own] + q_ref[...]
        half = 0.5 * step

        @pl.when(k > 0)
        def _():
            p_ref[...] = p_ref[...] - half * force

        @pl.when(k < steps)
        def _():
            p = p_ref[...] - half * force
            q = q_ref[...] + half * p
            now = noise_ref.at[k]
            drawn = jnp.stack([load(now, at) for at in range(x)])
            p = decay * p + kick * drawn
            q_ref[...] = q + half * p
            p_ref[...] = p

        return carry

    lax.fori_loop(0, steps + 1, body, 0)

    for ref, out in ((q_ref, q_out), (p_ref, p_out)):
        for at in range(x):
            flat = ref[at].T
            for j in range(y):
                out[:, (at * y + j) * z : (at * y + j + 1) * z] = flat[j * c : (j + 1) * c]


LANES = 128
ROWS = 8


def ring_place(r, nx):
    row, step = r // nx, r % nx
    return step + (row % 2) * (nx - 1 - 2 * step), row


def split_rows(height):
    low = -(-height // (2 * EDGE)) * EDGE
    return low, height - low


def ring_kernel(steps, sizes, heights, *refs):
    pool = {}
    for height in heights:
        parts = split_rows(height)
        for part in parts:
            pool[part] = max(pool.get(part, 0), parts.count(part))
    order = [(unit, part, i) for unit in range(2) for part in sorted(pool) for i in range(pool[part])]
    spaces = [pltpu.ACC(unit)((part, 2 * LANES), jnp.float32) for unit, part, _ in order]
    pl.run_scoped(functools.partial(ring_body, steps, sizes, order, refs), *spaces)


def ring_body(steps, sizes, order, refs, *sums):
    nx, ny, nz = sizes
    banks = dict(zip(order, sums))
    inputs, refs = refs[:6], refs[6:]
    (q_out, p_out, pos_ref, mom_ref, noise_ref, fin_ref, fout_ref, bias_ref, own_w, all_w, mats,
     flipped, turned_d, msg0, got0, msgd, gotd, stage, lhs, t_ref, base, extra, dq, dp, qb,
     halo, vb, ring_v, back_q, got_q, back_p, got_p, fixed, loose, edges_d, msge, gote, send, recv,
     load) = refs
    ring = nx * ny
    x, zb = msg0.shape[1], msg0.shape[2]
    lane = LANES
    z = ring * zb
    taps, co, ci = fin_ref.shape
    c = ny * ci
    y = lane // c
    xx, yy = x * nx, y * ny
    per = lane // ci
    tiles = own_w.shape[1]
    wide = yy * c
    reach = 4
    rows = zb * xx

    ix, iy, iz = lax.axis_index("gx"), lax.axis_index("gy"), lax.axis_index("gz")
    me = iy * nx + ix + (iy % 2) * (nx - 1 - 2 * ix)
    block = nz * me + iz
    home = block // ring == iz
    filed = block % ring

    def device(r, core):
        gx, gy = ring_place(r, nx)
        return {"gx": gx, "gy": gy, "gz": core}

    barrier = pltpu.get_barrier_semaphore()
    everyone = 0
    for dx in range(nx):
        for dy in range(ny):
            for dz in range(nz):
                if dx or dy or dz:
                    everyone += 1
                    pl.semaphore_signal(
                        barrier,
                        inc=1,
                        device_id={"gx": (ix + dx) % nx, "gy": (iy + dy) % ny, "gz": (iz + dz) % nz},
                        device_id_type=MESH,
                    )

    loads = []
    held = (pos_ref, mom_ref, noise_ref, fin_ref, fout_ref, bias_ref)
    for number in (3, 4, 0, 1, 2, 5):
        copy = pltpu.make_async_copy(inputs[number], held[number], load.at[number])
        copy.start()
        loads.append(copy)

    def copy_of(source, target, number, where):
        return pltpu.make_async_remote_copy(
            src_ref=source,
            dst_ref=target,
            send_sem=send.at[number],
            recv_sem=recv.at[number],
            device_id=where,
            device_id_type=MESH,
        )

    across = {"gy": (iy + 1) % ny}
    other = {"gz": (iz + 1) % nz}

    def start(source, target, number, where):
        copy_of(source, target, number, where).start()

    def arrive(number, like):
        copy_of(like, like, number, other).wait_recv()

    def leave(number, like):
        copy_of(like, like, number, other).wait_send()

    def start_or_keep(source, target, number, where):
        @pl.when(home)
        def _():
            pltpu.make_async_copy(source, target, recv.at[number]).start()

        @pl.when(jnp.logical_not(home))
        def _():
            start(source, target, number, where)

    def to_owners(buf, target, number):
        for j in range(1, ring + 1):
            at = (filed + j) % ring
            owner = iz * ring + at
            go = start if j < ring else start_or_keep
            go(buf.at[at], target, number, device(owner // nz, owner % nz))

    def to_sources(buf, target, number):
        for j in range(1, ring + 1):
            r = (me + j) % ring
            go = start if j < ring else start_or_keep
            go(buf.at[r], target, number, device(r, block // ring))

    def left_ring(number, buf):
        @pl.when(home)
        def _():
            leave(number, buf.at[0 : ring - 1])

        @pl.when(jnp.logical_not(home))
        def _():
            leave(number, buf)

    column_sems = [[which * (nx - 1) + dx for dx in range(nx - 1)] for which in range(2)]
    across_sem = [2 * (nx - 1), 2 * (nx - 1) + 1]
    swap_sem = [2 * nx, 2 * nx + 1]
    field_sem = 2 * nx + 2
    drift_sem = [2 * nx + 3 + k for k in range(steps)]
    pairs = (steps - 1) // 2
    q_sem = 2 * nx + 3 + steps
    p_sem, drift_edge_sem = q_sem + 1, q_sem + 2
    halo_sem = [q_sem + 3 + k for k in range(pairs + 1)]
    v_sem = [q_sem + 4 + pairs + k for k in range(pairs)]

    outer = iz == nz - 1
    loads[0].wait()
    loads[1].wait()

    @pl.when(outer)
    def _():
        for which, ref in enumerate((fin_ref, fout_ref)):
            for tile in range(tiles):
                span = range(tile * per, min(taps, (tile + 1) * per))
                parts = [ref[t].astype(jnp.float32) for t in span]
                parts += [jnp.zeros((co, ci), jnp.float32)] * (per - len(parts))
                own_w[which, tile] = jnp.concatenate(parts, axis=1).astype(jnp.bfloat16)

    def turn(ref, at):
        parts = [ref[pl.ds(at * y + j, c, stride=x * y), :] for j in range(y)]
        return jnp.concatenate(parts, axis=0).T

    loads[2].wait()
    for at in range(x):
        flat = turn(pos_ref, at).astype(jnp.bfloat16)
        for r in range(ring):
            msg0[r, at] = flat[r * zb : (r + 1) * zb]

    for each in sums:
        pltpu.matmul_pop(each)

    pl.semaphore_wait(barrier, everyone)

    def to_column(which):
        for dx in range(1, nx):
            there = {"gx": (ix + dx) % nx}
            start(own_w.at[which], all_w.at[which, me], column_sems[which][dx - 1], there)
        start(own_w.at[which], all_w.at[which, me], across_sem[which], across)

    def pass_on(which):
        for dx in range(1, nx):
            arrive(column_sems[which][dx - 1], own_w.at[which])
            gx = (ix + nx - dx) % nx
            r = iy * nx + gx + (iy % 2) * (nx - 1 - 2 * gx)
            start(all_w.at[which, r], all_w.at[which, r], across_sem[which], across)

    @pl.when(outer)
    def _():
        to_column(0)

    @pl.when(outer)
    def _():
        to_column(1)
        all_w[:, me] = own_w[...]

    upper = lax.broadcasted_iota(jnp.int32, (ROWS, lane), 0) < reach

    def around(ref, beyond, r, at):
        before = ref[at, r * zb - ROWS : r * zb] if r else beyond[0, at]
        after = ref[at, (r + 1) * zb : (r + 1) * zb + ROWS] if r < ring - 1 else beyond[1, at]
        return before, after

    to_owners(msg0, got0.at[me], field_sem)

    half = 0.125
    decay = float(np.exp(np.float32(-0.25)))
    kick = float(np.sqrt(np.float32(1.0) - np.exp(np.float32(-0.25)) ** 2))
    push = half * (1.0 + decay)
    loads[3].wait()
    loads[4].wait()
    loads[5].wait()
    q = pos_ref[...]
    known = q.astype(jnp.bfloat16).astype(jnp.float32)
    p = mom_ref[...] - half * q
    total = x * y * c
    for k in range(steps):
        noise = noise_ref[k * total : (k + 1) * total].astype(jnp.float32)
        q = q + push * p + (half * kick) * noise
        drift = (q - known).astype(jnp.bfloat16).astype(jnp.float32)
        known = known + drift
        last = k == steps - 1
        p = decay * p + kick * noise - (half if last else 2 * half) * q
        loose[k] = drift
        for at in range(x):
            flat = turn(loose.at[k], at)
            if k == 0:
                turned_d[at] = flat
                for r in range(ring):
                    msge[r, at] = flat[r * zb : (r + 1) * zb].astype(jnp.bfloat16)
            else:
                flat = flat.astype(jnp.bfloat16)
                for r in range(ring):
                    msgd[k - 1, r, at] = flat[r * zb : (r + 1) * zb]
        if k == 0:
            start(turned_d.at[:, z - ROWS : z], edges_d.at[0], drift_edge_sem, {"gz": (iz + 1) % nz})
            start(turned_d.at[:, 0:ROWS], edges_d.at[1], drift_edge_sem, {"gz": (iz + nz - 1) % nz})
    fixed[0] = q
    fixed[1] = p

    def send_drift(k):
        if k == 0:
            to_owners(msge, gote.at[me], drift_sem[0])
        else:
            to_owners(msgd.at[k - 1], gotd.at[k - 1, me], drift_sem[k])

    @pl.when(outer)
    def _():
        pass_on(0)

    arrive(drift_edge_sem, edges_d)
    for r in range(ring):
        beyond = []
        for at in range(x):
            before, after = around(turned_d, edges_d, r, at)
            beyond.append(jnp.where(upper, after, before))
        msge[r, x] = jnp.concatenate(beyond, axis=0).astype(jnp.bfloat16)
    send_drift(0)

    def swap(which):
        arrive(across_sem[which], all_w.at[which, 0:nx])
        start(all_w.at[which], all_w.at[which], swap_sem[which], other)

    @pl.when(outer)
    def _():
        swap(0)
        pass_on(1)

    def swapped(which):
        @pl.when(jnp.logical_not(outer))
        def _():
            arrive(swap_sem[which], all_w.at[which])

    at_lane = lax.broadcasted_iota(jnp.int32, (co, lane), 1)

    def build(which):
        def place(gx, carry):
            row = pl.multiple_of(gx * co, co)
            for a in range(3):
                for cz in range(3):
                    moved = {}
                    for b in range(3):
                        t = a * 9 + b * 3 + cz
                        tile, spot = t // per, t % per
                        for side in range(2):
                            pieces = []
                            for gy in range(ny):
                                r = gy * nx + gx + (gy % 2) * (nx - 1 - 2 * gx)
                                piece = all_w[which, r, tile].astype(jnp.float32)
                                shift = (side * ny + gy - spot) % per
                                pieces.append(pltpu.roll(piece, shift * ci, 1) if shift else piece)
                            moved[b, side] = pieces
                    pairs = []
                    for b in range(yy):
                        value = jnp.zeros((co, lane), jnp.float32)
                        for side in range(y):
                            near = (b + side) % yy
                            if near > 2:
                                continue
                            for gy in range(ny):
                                spot = (side * ny + gy) * ci
                                inside = (at_lane >= spot) & (at_lane < spot + ci)
                                value = jnp.where(inside, moved[near, side][gy], value)
                        pairs.append(value.astype(jnp.bfloat16))
                    for yo in range(yy):
                        for h in range(yy // y):
                            mats[which, a * 3 + cz, pl.ds(yo * c + row, co), h * lane : (h + 1) * lane] = (
                                pairs[(h * y + 1 - yo) % yy]
                            )
            return carry

        lax.fori_loop(0, nx, place, 0)

    def turn_over(which):
        for tap in range(9):
            flipped[which, tap] = mats[which, tap].T

    def scatter(target, zs, value, r, at):
        gx, gy = ring_place(r, nx)
        target[gy, pl.ds(zs * xx + gx * x + at, value.shape[0], stride=xx), :] = value

    def whole(ref, rows_from, rows_to):
        return jnp.concatenate([ref[gy, rows_from:rows_to] for gy in range(ny)], axis=1)

    left = device((me + ring - 1 + iz) % ring, 1 - iz)
    right = device((me + iz) % ring, 1 - iz)
    edge = reach * xx

    def send_halo(slot, value):
        qb[slot] = value.astype(jnp.bfloat16)
        start(qb.at[slot, rows - 2 * edge : rows], halo.at[slot, 0], halo_sem[slot], right)
        start(qb.at[slot, 0 : 2 * edge], halo.at[slot, 1], halo_sem[slot], left)

    def with_halo(slot, value):
        arrive(halo_sem[slot], halo.at[slot])
        ends = [halo[slot, side].astype(jnp.float32) for side in range(2)]
        return jnp.concatenate([ends[0], value, ends[1]], axis=0)

    arrive(field_sem, got0)
    for r in range(ring):
        for at in range(x):
            scatter(stage, 0, got0[r, at].astype(jnp.float32), r, at)
    send_halo(0, whole(stage, 0, rows))
    send_drift(1)
    swapped(0)
    build(0)
    turn_over(0)

    def spread(value):
        n = value.shape[0]
        cube = value.reshape(n // xx, xx, wide)
        for a in range(3):
            moved = cube if a == 1 else pltpu.roll(cube, (1 - a) % xx, 1)
            moved = moved.reshape(n, wide)
            lhs[a, 0, 0:n] = moved.astype(jnp.bfloat16)
            lhs[a, 1, 0 : n - 2 * xx] = moved[xx : n - xx].astype(jnp.bfloat16)

    def conv(height, which, adjoint, flip=False):
        source = mats if adjoint or flip else flipped
        low, high = split_rows(height)
        sums = [[banks[unit, low, 0], banks[unit, high, int(low == high)]] for unit in range(2)]
        plans = (
            [(0, True, True), (1, True, True), (2, True, True), (3, True, True), (4, True, False)],
            [(8, True, True), (7, True, True), (6, True, True), (5, True, True), (4, False, True)],
        )
        for at in range(5):
            for unit in range(2):
                tap, use_low, use_high = plans[unit][at]
                a, cz = tap // 3, tap % 3
                pltpu.matmul_push_rhs(
                    source[which, 8 - tap if adjoint else tap],
                    staging_register=at % 2,
                    mxu_index=unit,
                    transpose=flip,
                )
                copy, first_row = (1, 0) if cz == 1 else (0, cz * xx)
                fresh = at % 2
                if use_low:
                    left = lhs[a, copy, first_row : first_row + low]
                    pltpu.matmul_acc_lhs(sums[unit][0], left, load_staged_rhs=fresh)
                    fresh = None
                if use_high:
                    left = lhs[a, copy, first_row + low : first_row + low + high]
                    pltpu.matmul_acc_lhs(sums[unit][1], left, load_staged_rhs=fresh)
        halves = [pltpu.matmul_pop(sums[0][part]) + pltpu.matmul_pop(sums[1][part]) for part in range(2)]
        return jnp.concatenate(halves, axis=0)

    row = jnp.concatenate([bias_ref[...]] * yy, axis=1)

    def gradient(extent, between=lambda: None, flip=False):
        n = [rows + 2 * (extent + 3 - i) * xx for i in range(4)]
        t = jnp.tanh(conv(n[0], 0, False) + row)
        t_ref[0 : n[0]] = t
        spread(t)
        between()
        spread(conv(n[1], 1, False, flip))
        gu = conv(n[2], 1, True)
        t = t_ref[2 * xx : 2 * xx + n[2]]
        spread(gu * (1.0 - t * t))
        return conv(n[3], 0, True)

    def take_drift(k):
        arrive(drift_sem[k], gotd.at[k - 1])
        for r in range(ring):
            for at in range(x):
                scatter(extra, 0, gotd[k - 1, r, at].astype(jnp.float32), r, at)
        base[...] = base[...] + whole(extra, 0, rows)

    def second_filters():
        @pl.when(outer)
        def _():
            swap(1)

        swapped(1)
        for later in range(2, steps):
            send_drift(later)
        build(1)

    def collect(ref, r, at):
        gx, gy = ring_place(r, nx)
        return ref[gy, pl.ds(gx * x + at, zb, stride=xx), :]

    def put(ref, value):
        for gy in range(ny):
            ref[gy] = value[:, gy * lane : (gy + 1) * lane]

    base[...] = whole(stage, 0, rows)
    spread(with_halo(0, base[...]))
    g = gradient(reach, second_filters, True)

    arrive(drift_sem[0], gote)
    for r in range(ring):
        beyond = gote[r, x].astype(jnp.float32)
        for at in range(x):
            scatter(extra, 0, gote[r, at].astype(jnp.float32), r, at)
            scatter(extra, zb, beyond[at * ROWS : (at + 1) * ROWS], r, at)
    now = base[...] + whole(extra, 0, rows)
    base[...] = now
    below = halo[0, 0, edge : 2 * edge].astype(jnp.float32) + whole(extra, rows + edge, rows + 2 * edge)
    above = halo[0, 1, 0:edge].astype(jnp.float32) + whole(extra, rows, rows + edge)
    force = g[edge : edge + rows]
    put(dp, -half * force)
    put(dq, (-half * push) * force)
    spread(jnp.concatenate([below, now, above], axis=0) + (-half * push) * g)

    mine = pl.ds(pl.multiple_of(filed * zb, zb), zb)

    def kicked(g):
        shift = whole(dq, 0, rows)
        now = decay * whole(dp, 0, rows) - (2 * half) * (g + shift)
        put(dp, now)
        put(dq, shift + push * now)

    for pair in range(pairs):
        kicked(gradient(0, flip=pair == 0))
        k = 2 * pair + 2
        take_drift(k - 1)
        q = base[...] + whole(dq, 0, rows)
        send_halo(pair + 1, q)
        if pair == 0:
            turn_over(1)
        take_drift(k)
        shift = whole(dq, 0, rows)
        v = base[...] + shift + push * (decay * whole(dp, 0, rows) - (2 * half) * shift)
        vb[pair] = v.astype(jnp.bfloat16)
        start(vb.at[pair, rows - edge : rows], ring_v.at[pair, 0], v_sem[pair], right)
        start(vb.at[pair, 0:edge], ring_v.at[pair, 1], v_sem[pair], left)
        spread(with_halo(pair + 1, q))
        g = gradient(reach)
        kicked(g[edge : edge + rows])
        q = base[...] + whole(dq, 0, rows)
        arrive(v_sem[pair], ring_v.at[pair])
        ends = [
            ring_v[pair, side].astype(jnp.float32) - (2 * half * push) * g[at : at + edge]
            for side, at in enumerate((0, edge + rows))
        ]
        spread(jnp.concatenate([ends[0], q, ends[1]], axis=0))

    put(dp, decay * whole(dp, 0, rows) - half * whole(dq, 0, rows))
    for r in range(ring):
        for at in range(x):
            back_q[r, at] = collect(dq, r, at).astype(jnp.bfloat16)
    to_sources(back_q, got_q.at[:, mine], q_sem)
    g = gradient(0)
    put(dp, whole(dp, 0, rows) - half * g)
    for r in range(ring):
        for at in range(x):
            back_p[r, at] = collect(dp, r, at).astype(jnp.bfloat16)
    to_sources(back_p, got_p.at[:, mine], p_sem)

    def untie(value, which, out, at):
        flat = value.T
        for j in range(y):
            part = pl.ds(at * y + j, c, stride=x * y)
            out[part, :] = fixed[which, part, :] + flat[j * c : (j + 1) * c]

    arrive(q_sem, got_q)
    for at in range(x):
        untie(got_q[at].astype(jnp.float32), 0, q_out, at)
    arrive(p_sem, got_p)
    for at in range(x):
        untie(got_p[at].astype(jnp.float32), 1, p_out, at)

    @pl.when(outer)
    def _():
        for which in range(2):
            for number in column_sems[which]:
                leave(number, own_w.at[which])
            leave(across_sem[which], all_w.at[which, 0:nx])
            leave(swap_sem[which], all_w.at[which])

    leave(drift_edge_sem, edges_d)
    left_ring(field_sem, msg0)
    left_ring(drift_sem[0], msge)
    for k in range(1, steps):
        left_ring(drift_sem[k], msgd.at[k - 1])
    for slot in range(pairs + 1):
        leave(halo_sem[slot], halo.at[slot])
    for pair in range(pairs):
        leave(v_sem[pair], ring_v.at[pair])
    left_ring(q_sem, back_q)
    left_ring(p_sem, back_p)


def fits_ring(steps, sizes, position, filter_in):
    nx, ny, nz = sizes
    c, x, y, z = position.shape
    co, ci = filter_in.shape[:2]
    ring = nx * ny
    return (
        steps % 2 == 1 and steps > 2 and nz == 2 and ny == 2 and nx > 1 and y * c == LANES and x * nx == ROWS and y * ny > 2
        and z % (ring * EDGE) == 0 and z // ring == EDGE and co % EDGE == 0 and LANES % ci == 0
        and y * ny * ci == LANES
    )


def on_ring(sizes, position, momentum, noise, filter_in, filter_out, bias):
    nx, ny, nz = sizes
    c, x, y, z = position.shape
    steps = noise.shape[0]
    co, ci = filter_in.shape[:2]
    ring = nx * ny
    zb = z // ring
    xx, yy = x * nx, y * ny
    wide = yy * c
    rows = zb * xx
    lane = LANES
    tiles = -(-27 * ci // lane)
    flat = jax.ShapeDtypeStruct((c * x * y, z), jnp.float32)
    reach, pairs = 4, (steps - 1) // 2
    copies = 2 * nx + 7 + steps + 2 * pairs
    edge = reach * xx
    heights = [(zb + 2 * beyond) * xx for beyond in range(2 * reach)]
    vmem = pl.BlockSpec(memory_space=pltpu.VMEM)
    bf16, f32 = jnp.bfloat16, jnp.float32
    q, p = pl.pallas_call(
        functools.partial(ring_kernel, steps, sizes, heights),
        out_shape=(flat, flat),
        in_specs=[pl.BlockSpec(memory_space=pl.ANY)] * 6,
        out_specs=(vmem, vmem),
        scratch_shapes=[
            pltpu.VMEM((c * x * y, z), f32),
            pltpu.VMEM((c * x * y, z), f32),
            pltpu.VMEM((steps * c * x * y, z), bf16),
            pltpu.VMEM((27, co, ci), bf16),
            pltpu.VMEM((27, co, ci), bf16),
            pltpu.VMEM((1, c), f32),
            pltpu.VMEM((2, tiles, co, lane), bf16),
            pltpu.VMEM((2, ring, tiles, co, lane), bf16),
            pltpu.VMEM((2, 9, wide, wide), bf16),
            pltpu.VMEM((2, 9, wide, wide), bf16),
            pltpu.VMEM((x, z, lane), f32),
            pltpu.VMEM((ring, x, zb, lane), bf16),
            pltpu.VMEM((ring, x, zb, lane), bf16),
            pltpu.VMEM((steps - 1, ring, x, zb, lane), bf16),
            pltpu.VMEM((steps - 1, ring, x, zb, lane), bf16),
            pltpu.VMEM((ny, rows, lane), f32),
            pltpu.VMEM((3, 2, rows + 4 * edge, wide), bf16),
            pltpu.VMEM((rows + 4 * edge - 2 * xx, wide), f32),
            pltpu.VMEM((rows, wide), f32),
            pltpu.VMEM((ny, rows + 2 * edge, lane), f32),
            pltpu.VMEM((ny, rows, lane), f32),
            pltpu.VMEM((ny, rows, lane), f32),
            pltpu.VMEM((pairs + 1, rows, wide), bf16),
            pltpu.VMEM((pairs + 1, 2, 2 * edge, wide), bf16),
            pltpu.VMEM((pairs, rows, wide), bf16),
            pltpu.VMEM((pairs, 2, edge, wide), bf16),
            pltpu.VMEM((ring, x, zb, lane), bf16),
            pltpu.VMEM((x, z, lane), bf16),
            pltpu.VMEM((ring, x, zb, lane), bf16),
            pltpu.VMEM((x, z, lane), bf16),
            pltpu.VMEM((2, c * x * y, z), f32),
            pltpu.VMEM((steps, c * x * y, z), f32),
            pltpu.VMEM((2, x, ROWS, lane), f32),
            pltpu.VMEM((ring, x + 1, zb, lane), bf16),
            pltpu.VMEM((ring, x + 1, zb, lane), bf16),
            pltpu.SemaphoreType.DMA((copies,)),
            pltpu.SemaphoreType.DMA((copies,)),
            pltpu.SemaphoreType.DMA((6,)),
        ],
        compiler_params=pltpu.CompilerParams(
            collective_id=0, has_side_effects=True, vmem_limit_bytes=24 * 2**20
        ),
    )(
        *(
            pltpu.with_memory_space_constraint(each, pltpu.HBM)
            for each in (
                position.reshape(-1, z),
                momentum.reshape(-1, z),
                noise.reshape(-1, z),
                filter_in.transpose(2, 3, 4, 0, 1).reshape(27, co, ci),
                filter_out.transpose(2, 3, 4, 0, 1).reshape(27, co, ci),
                bias[None],
            )
        )
    )
    return q.reshape(position.shape), p.reshape(momentum.shape)


def on_device(sizes, position, momentum, noise, filter_in, filter_out, bias):
    if fits_ring(noise.shape[0], sizes, position, filter_in):
        return on_ring(sizes, position, momentum, noise, filter_in, filter_out, bias)
    nx, ny, nz = sizes
    c, x, y, z = position.shape
    steps = noise.shape[0]
    assert x >= 2 and y == 2 and z % EDGE == 0 and nx > 2 and ny > 1
    both = jnp.stack([filter_in, filter_out])
    co, ci = both.shape[1], both.shape[2]
    gather = []
    if co % EDGE == 0:
        both = both.transpose(0, 1, 3, 5, 4, 2).reshape(2, co, 27 * ci)
        gather = [
            pltpu.VMEM((ny, nx, 2, co, 27 * ci), jnp.bfloat16),
            pltpu.VMEM((2, 9, 3, c, c), jnp.bfloat16),
            pltpu.SemaphoreType.DMA((nx * ny - 1,)),
            pltpu.SemaphoreType.DMA((nx * ny - 1,)),
        ]
    else:
        both = both.reshape(2 * co, ci * 27)
        both = lax.all_gather(both, ("gx", "gy"), axis=0, tiled=True)
        both = both.reshape(nx, ny, 2, co, ci, 3, 3, 3)
        both = both.transpose(2, 5, 7, 6, 0, 3, 1, 4).reshape(2, 9, 3, c, c)
    lanes = y * c
    slots = 2 * y if ny == 2 else 3 * y
    full = z + 2 * EDGE
    wide = (y + 2) * c
    flat = jax.ShapeDtypeStruct((c, x * y * z), jnp.float32)
    copies = 15 if ny == 2 else 24
    vmem = pl.BlockSpec(memory_space=pltpu.VMEM)
    q, p = pl.pallas_call(
        functools.partial(kernel, steps, sizes),
        out_shape=(flat, flat),
        in_specs=[vmem] * 5,
        out_specs=(vmem, vmem),
        scratch_shapes=[
            pltpu.VMEM((9, wide, slots * c), jnp.bfloat16),
            pltpu.VMEM((9, lanes, wide), jnp.bfloat16),
            pltpu.VMEM((9, wide, lanes), jnp.bfloat16),
            pltpu.VMEM((9, slots * c, wide), jnp.bfloat16),
            pltpu.VMEM((x + 4, full, slots * c), jnp.bfloat16),
            pltpu.VMEM((x + 4, full, slots * c), jnp.bfloat16),
            pltpu.VMEM((x + 2, full, wide), jnp.float32),
            pltpu.VMEM((x, z, lanes), jnp.float32),
            pltpu.VMEM((x, z, lanes), jnp.float32),
            pltpu.SemaphoreType.DMA((2, copies)),
            pltpu.SemaphoreType.DMA((2, copies)),
            *gather,
        ],
        compiler_params=pltpu.CompilerParams(
            collective_id=0, has_side_effects=True, vmem_limit_bytes=56 * 2**20
        ),
    )(
        position.reshape(c, -1),
        momentum.reshape(c, -1),
        noise.reshape(steps, c, -1),
        both,
        jnp.tile(bias, y + 2)[None],
    )
    return q.reshape(position.shape), p.reshape(momentum.shape)


def solution(mesh):
    field = P(None, ("grp", "gx"), "gy", "gz")
    filters = P("gx", "gy", None, None, None)
    sizes = tuple(mesh.shape[name] for name in ("gx", "gy", "gz"))
    return jax.shard_map(
        functools.partial(on_device, sizes),
        mesh=mesh,
        in_specs=(field, field, P(None, None, ("grp", "gx"), "gy", "gz"), filters, filters, P()),
        out_specs=(field, field),
        check_vma=False,
    )
```

```python
import functools

import jax
import jax.numpy as jnp
import numpy as np
from jax import lax
from jax.experimental import pallas as pl
from jax.experimental.pallas import tpu as pltpu
from jax.sharding import PartitionSpec as P

EDGE = 16
MESH = pl.DeviceIdType.MESH


def kernel(steps, sizes, pos_ref, mom_ref, noise_ref, w_ref, bias_ref,
           q_out, p_out, a1, a2, b1, b2, eq, eh, t_ref, q_ref, p_ref, send, recv, *gather):
    nx, ny, nz = sizes
    c = pos_ref.shape[0]
    inside = len(gather) > 0
    if inside:
        wg, wf, wsend, wrecv = gather
    x, z, lanes = q_ref.shape
    y = lanes // c
    full = eq.shape[1]
    wrap = ny == 2
    slots = eq.shape[2] // c
    own = slice(EDGE, EDGE + z)
    mine = slice(lanes, 2 * lanes)

    ix, iy, iz = lax.axis_index("gx"), lax.axis_index("gy"), lax.axis_index("gz")
    up = {"gx": lax.rem(ix + 1, nx), "gy": lax.rem(iy + 1, ny), "gz": lax.rem(iz + 1, nz)}
    down = {
        "gx": lax.rem(ix + nx - 1, nx),
        "gy": lax.rem(iy + ny - 1, ny),
        "gz": lax.rem(iz + nz - 1, nz),
    }

    def at_side(**which):
        return {axis: which[axis][axis] for axis in which}

    def early(buf):
        core = slice(2, 2 + x)
        low, high = slice(0, EDGE), slice(z + EDGE, full)
        block = buf.at[core, own, mine]
        edges = (
            (up, buf.at[core, z : z + EDGE, mine], low),
            (down, buf.at[core, EDGE : 2 * EDGE, mine], high),
        )
        out = []
        for side, source, rows in edges:
            out.append((at_side(gz=side), source, buf.at[core, rows, mine], True))
        for beside, part in others:
            out.append((at_side(gy=beside), block, buf.at[core, own, part], True))
            for side, source, rows in edges:
                target = buf.at[core, rows, part]
                out.append((at_side(gy=beside, gz=side), source, target, True))
        out.append(
            (at_side(gx=down), buf.at[2:4, own, mine], buf.at[2 + x : 4 + x, own, mine], False)
        )
        out.append((at_side(gx=up), buf.at[x : 2 + x, own, mine], buf.at[0:2, own, mine], False))
        return out

    def late(buf):
        low, high = slice(0, EDGE), slice(z + EDGE, full)
        from_low = (up, slice(x, 2 + x), slice(0, 2))
        from_high = (down, slice(2, 4), slice(2 + x, 4 + x))
        plan = []
        for _, part in others:
            plan.append((from_low, slice(0, full), part))
            plan += [(from_high, low, part), (from_high, high, part)]
        for side in (from_low, from_high):
            plan += [(side, low, mine), (side, high, mine)]
        return [
            (at_side(gx=side), buf.at[source, rows, part], buf.at[target, rows, part])
            for (side, source, target), rows, part in plan
        ]

    def forward(buf):
        planes = slice(2 + x, 4 + x)
        return [
            (at_side(gy=beside), buf.at[planes, own, mine], buf.at[planes, own, part])
            for beside, part in others
        ]

    others = [(up, slice(0, lanes))]
    if not wrap:
        others.append((down, slice(2 * lanes, 3 * lanes)))

    def remote(source, target, sems, number, device):
        return pltpu.make_async_remote_copy(
            src_ref=source,
            dst_ref=target,
            send_sem=sems[0].at[number],
            recv_sem=sems[1].at[number],
            device_id=device,
            device_id_type=MESH,
        )

    peers = []
    if inside:
        for dx in range(nx):
            for dy in range(ny):
                if dx or dy:
                    peers.append({"gx": lax.rem(ix + dx, nx), "gy": lax.rem(iy + dy, ny)})
    barrier = pltpu.get_barrier_semaphore()
    greeted = peers + [device for device, _, _, _ in early(eq)]
    for device in greeted:
        pl.semaphore_signal(barrier, inc=1, device_id=device, device_id_type=MESH)
    pl.semaphore_wait(barrier, len(greeted))

    if inside:
        copies = []
        for number, device in enumerate(peers):
            copy = remote(w_ref, wg.at[iy, ix], (wsend, wrecv), number, device)
            copy.start()
            copies.append(copy)
        wg[iy, ix] = w_ref[...]
        for copy in copies:
            copy.wait()
        ci = c // ny
        for which in range(2):
            for at in range(27):
                columns = []
                for j in range(ny):
                    pieces = [wg[j, i, which, :, at * ci : (at + 1) * ci] for i in range(nx)]
                    columns.append(jnp.concatenate(pieces, axis=0))
                wf[which, at // 3, at % 3] = jnp.concatenate(columns, axis=1)
        filters = wf
    else:
        filters = w_ref

    def exchange(buf, bank):
        sems = (send.at[bank], recv.at[bank])
        first, own_x = [], []
        number = 0
        for device, source, target, passed in early(buf):
            copy = remote(source, target, sems, number, device)
            number += 1
            copy.start()
            (first if passed else own_x).append(copy)
        for copy in first:
            copy.wait_recv()
        second = []
        for device, source, target in late(buf):
            copy = remote(source, target, sems, number, device)
            number += 1
            copy.start()
            second.append(copy)
        own_x[0].wait_recv()
        for device, source, target in forward(buf):
            copy = remote(source, target, sems, number, device)
            number += 1
            copy.start()
            second.append(copy)
        for copy in own_x[1:] + second:
            copy.wait_recv()
        for copy in first + own_x + second:
            copy.wait_send()

    def slot(at):
        return at % slots

    def unfold(tap, carry):
        blank = jnp.zeros((c, c), jnp.bfloat16)

        def rows(out, which, at, flip, cols, pick):
            line = [blank] * cols
            for col, b in pick:
                line[col] = filters[which, at, 2 - b if flip else b]
            return jnp.concatenate(line, axis=1)

        back = 8 - tap
        for yo in range(y + 2):
            a1[tap, yo * c : (yo + 1) * c, :] = rows(
                a1, 0, tap, False, slots, [(slot(yo + b), b) for b in range(3)]
            )
        for yo in range(y):
            a2[tap, yo * c : (yo + 1) * c, :] = rows(
                a2, 1, tap, False, y + 2, [(yo + b, b) for b in range(3)]
            )
        for s in range(slots):
            pick = [(yo, b) for yo in range(y + 2) for b in range(3) if slot(yo + b) == s]
            b2[tap, s * c : (s + 1) * c, :] = rows(b2, 1, back, True, y + 2, pick)
        for yi in range(y + 2):
            pick = [(yo, yi - yo) for yo in range(y) if 0 <= yi - yo <= 2]
            b1[tap, yi * c : (yi + 1) * c, :] = rows(b1, 0, back, True, y, pick)
        return carry

    lax.fori_loop(0, 9, unfold, 0)

    def load(ref2d, at):
        span = [ref2d[:, (at * y + j) * z : (at * y + j + 1) * z] for j in range(y)]
        return jnp.concatenate(span, axis=0).astype(jnp.float32).T

    for at in range(x):
        q_ref[at] = load(pos_ref, at)
        p_ref[at] = load(mom_ref, at)

    def conv(source, weights, out_x, transposed):
        width = source.shape[2]
        total = None
        for tz in range(3):
            part = None
            for tx in range(3):
                left = source[tx : tx + out_x].reshape(out_x * full, width)
                term = lax.dot_general(
                    left,
                    weights[tx * 3 + tz],
                    (((1,), (1 if transposed else 0,)), ((), ())),
                    preferred_element_type=jnp.float32,
                )
                part = term if part is None else part + term
            if tz != 1:
                part = pltpu.roll(part, 1 if tz == 0 else out_x * full - 1, 0)
            total = part if total is None else total + part
        return total.reshape(out_x, full, total.shape[-1])

    step = 0.25
    decay = jnp.exp(jnp.float32(-0.25))
    kick = jnp.sqrt(1.0 - decay * decay)

    def body(k, carry):
        eq[2 : 2 + x, own, mine] = q_ref[...].astype(jnp.bfloat16)
        exchange(eq, 0)
        t_ref[...] = jnp.tanh(conv(eq, a1, x + 2, True) + bias_ref[...][None])
        h2 = conv(t_ref[...].astype(jnp.bfloat16), a2, x, True)
        eh[2 : 2 + x, own, mine] = h2[:, own].astype(jnp.bfloat16)
        exchange(eh, 1)
        gu = conv(eh, b2, x + 2, False)
        t = t_ref[...]
        gh = (gu * (1.0 - t * t)).astype(jnp.bfloat16)
        force = conv(gh, b1, x, False)[:, own] + q_ref[...]
        half = 0.5 * step

        @pl.when(k > 0)
        def _():
            p_ref[...] = p_ref[...] - half * force

        @pl.when(k < steps)
        def _():
            p = p_ref[...] - half * force
            q = q_ref[...] + half * p
            now = noise_ref.at[k]
            drawn = jnp.stack([load(now, at) for at in range(x)])
            p = decay * p + kick * drawn
            q_ref[...] = q + half * p
            p_ref[...] = p

        return carry

    lax.fori_loop(0, steps + 1, body, 0)

    for ref, out in ((q_ref, q_out), (p_ref, p_out)):
        for at in range(x):
            flat = ref[at].T
            for j in range(y):
                out[:, (at * y + j) * z : (at * y + j + 1) * z] = flat[j * c : (j + 1) * c]


LANES = 128
ROWS = 8


def ring_place(r, nx):
    row, step = r // nx, r % nx
    return step + (row % 2) * (nx - 1 - 2 * step), row


def split_rows(height):
    low = -(-height // (2 * EDGE)) * EDGE
    return low, height - low


def ring_kernel(steps, sizes, heights, *refs):
    pool = {}
    for height in heights:
        parts = split_rows(height)
        for part in parts:
            pool[part] = max(pool.get(part, 0), parts.count(part))
    order = [(unit, part, i) for unit in range(2) for part in sorted(pool) for i in range(pool[part])]
    spaces = [pltpu.ACC(unit)((part, 2 * LANES), jnp.float32) for unit, part, _ in order]
    pl.run_scoped(functools.partial(ring_body, steps, sizes, order, refs), *spaces)


def ring_body(steps, sizes, order, refs, *sums):
    nx, ny, nz = sizes
    banks = dict(zip(order, sums))
    inputs, refs = refs[:6], refs[6:]
    (q_out, p_out, pos_ref, mom_ref, noise_ref, fin_ref, fout_ref, bias_ref, own_w, all_w, mats,
     flipped, turned_d, msg0, got0, msgd, gotd, stage, lhs, t_ref, base, extra, dq, dp, qb,
     halo, vb, ring_v, back_q, got_q, back_p, got_p, fixed, loose, edges_d, msge, gote, send, recv,
     load) = refs
    ring = nx * ny
    x, zb = msg0.shape[1], msg0.shape[2]
    lane = LANES
    z = ring * zb
    taps, co, ci = fin_ref.shape
    c = ny * ci
    y = lane // c
    xx, yy = x * nx, y * ny
    per = lane // ci
    half_tiles = own_w.shape[2]
    wide = yy * c
    reach = 4
    rows = zb * xx

    ix, iy, iz = lax.axis_index("gx"), lax.axis_index("gy"), lax.axis_index("gz")
    ig = lax.axis_index("grp")
    me = iy * nx + ix + (iy % 2) * (nx - 1 - 2 * ix)
    block = nz * me + iz
    home = block // ring == iz
    filed = block % ring

    def device(r, core):
        gx, gy = ring_place(r, nx)
        return {"gx": gx, "gy": gy, "gz": core}

    barrier = pltpu.get_barrier_semaphore()
    everyone = 0
    for dx in range(nx):
        for dy in range(ny):
            for dz in range(nz):
                if dx or dy or dz:
                    everyone += 1
                    pl.semaphore_signal(
                        barrier,
                        inc=1,
                        device_id={"gx": (ix + dx) % nx, "gy": (iy + dy) % ny, "gz": (iz + dz) % nz},
                        device_id_type=MESH,
                    )

    across = [{"gy": 1 - iy}, {"grp": 1 - ig}, {"grp": 1 - ig, "gy": 1 - iy}]
    for where in across[1:]:
        everyone += 1
        pl.semaphore_signal(barrier, inc=1, device_id=where, device_id_type=MESH)

    loads = []
    held = (pos_ref, mom_ref, noise_ref, fin_ref, fout_ref, bias_ref)
    for number in (3, 4, 0, 1, 2, 5):
        copy = pltpu.make_async_copy(inputs[number], held[number], load.at[number])
        copy.start()
        loads.append(copy)

    def copy_of(source, target, number, where):
        return pltpu.make_async_remote_copy(
            src_ref=source,
            dst_ref=target,
            send_sem=send.at[number],
            recv_sem=recv.at[number],
            device_id=where,
            device_id_type=MESH,
        )

    other = {"gz": (iz + 1) % nz}

    def start(source, target, number, where):
        copy_of(source, target, number, where).start()

    def arrive(number, like):
        copy_of(like, like, number, other).wait_recv()

    def leave(number, like):
        copy_of(like, like, number, other).wait_send()

    def start_or_keep(source, target, number, where):
        @pl.when(home)
        def _():
            pltpu.make_async_copy(source, target, recv.at[number]).start()

        @pl.when(jnp.logical_not(home))
        def _():
            start(source, target, number, where)

    def to_owners(buf, target, number):
        for j in range(1, ring + 1):
            at = (filed + j) % ring
            owner = iz * ring + at
            go = start if j < ring else start_or_keep
            go(buf.at[at], target, number, device(owner // nz, owner % nz))

    def to_sources(buf, target, number):
        for j in range(1, ring + 1):
            r = (me + j) % ring
            go = start if j < ring else start_or_keep
            go(buf.at[r], target, number, device(r, block // ring))

    def left_ring(number, buf):
        @pl.when(home)
        def _():
            leave(number, buf.at[0 : ring - 1])

        @pl.when(jnp.logical_not(home))
        def _():
            leave(number, buf)

    column_sems = [[which * (nx - 1) + dx for dx in range(nx - 1)] for which in range(2)]
    across_sems = [[2 * (nx - 1) + 3 * which + i for i in range(3)] for which in range(2)]
    swap_sem = [2 * nx + 4, 2 * nx + 5]
    field_sem = 2 * nx + 6
    drift_sem = [field_sem + 1 + k for k in range(steps)]
    pairs = (steps - 1) // 2
    q_sem = field_sem + 1 + steps
    p_sem, drift_edge_sem = q_sem + 1, q_sem + 2
    halo_sem = [q_sem + 3 + k for k in range(pairs + 1)]
    v_sem = [q_sem + 4 + pairs + k for k in range(pairs)]

    outer = iz == nz - 1
    loads[0].wait()
    loads[1].wait()

    @pl.when(outer)
    def _():
        for which, ref in enumerate((fin_ref, fout_ref)):
            for tile in range(2 * half_tiles):
                span = range(tile * per, min(taps, (tile + 1) * per))
                parts = [ref[t].astype(jnp.float32) for t in span]
                parts += [jnp.zeros((co, ci), jnp.float32)] * (per - len(parts))
                own_w[which, tile // half_tiles, tile % half_tiles] = jnp.concatenate(parts, axis=1).astype(jnp.bfloat16)

    def turn(ref, at):
        parts = [ref[pl.ds(at * y + j, c, stride=x * y), :] for j in range(y)]
        return jnp.concatenate(parts, axis=0).T

    loads[2].wait()
    for at in range(x):
        flat = turn(pos_ref, at).astype(jnp.bfloat16)
        for r in range(ring):
            msg0[r, at] = flat[r * zb : (r + 1) * zb]

    for each in sums:
        pltpu.matmul_pop(each)

    pl.semaphore_wait(barrier, everyone)

    def to_column(which):
        for dx in range(1, nx):
            there = {"gx": (ix + dx) % nx}
            start(own_w.at[which, ig], all_w.at[which, me, ig], column_sems[which][dx - 1], there)
        for where, number in zip(across, across_sems[which]):
            start(own_w.at[which, ig], all_w.at[which, me, ig], number, where)

    def hand_over(which, gy, part):
        piece = all_w.at[which, pl.ds(gy * nx, nx), part]
        start(piece, piece, swap_sem[which], other)

    def pass_on(which):
        for dx in range(1, nx):
            arrive(column_sems[which][dx - 1], own_w.at[which, 0])
            gx = (ix + nx - dx) % nx
            piece = all_w.at[which, iy * nx + gx + (iy % 2) * (nx - 1 - 2 * gx), ig]
            for where, number in zip(across, across_sems[which]):
                start(piece, piece, number, where)
        hand_over(which, iy, ig)

    def take_across(which):
        for number, gy, part in zip(across_sems[which], (1 - iy, iy, 1 - iy), (ig, 1 - ig, 1 - ig)):
            arrive(number, all_w.at[which, 0:nx, 0])
            hand_over(which, gy, part)

    @pl.when(outer)
    def _():
        to_column(0)
        to_column(1)
        for which in range(2):
            all_w[which, me, ig] = own_w[which, ig]

    upper = lax.broadcasted_iota(jnp.int32, (ROWS, lane), 0) < reach

    def around(ref, beyond, r, at):
        before = ref[at, r * zb - ROWS : r * zb] if r else beyond[0, at]
        after = ref[at, (r + 1) * zb : (r + 1) * zb + ROWS] if r < ring - 1 else beyond[1, at]
        return before, after

    to_owners(msg0, got0.at[me], field_sem)

    half = 0.125
    decay = float(np.exp(np.float32(-0.25)))
    kick = float(np.sqrt(np.float32(1.0) - np.exp(np.float32(-0.25)) ** 2))
    push = half * (1.0 + decay)
    loads[3].wait()
    loads[4].wait()
    loads[5].wait()
    q = pos_ref[...]
    known = q.astype(jnp.bfloat16).astype(jnp.float32)
    p = mom_ref[...] - half * q
    total = x * y * c
    for k in range(steps):
        noise = noise_ref[k * total : (k + 1) * total].astype(jnp.float32)
        q = q + push * p + (half * kick) * noise
        drift = (q - known).astype(jnp.bfloat16).astype(jnp.float32)
        known = known + drift
        last = k == steps - 1
        p = decay * p + kick * noise - (half if last else 2 * half) * q
        loose[k] = drift
        for at in range(x):
            flat = turn(loose.at[k], at)
            if k == 0:
                turned_d[at] = flat
                for r in range(ring):
                    msge[r, at] = flat[r * zb : (r + 1) * zb].astype(jnp.bfloat16)
            else:
                flat = flat.astype(jnp.bfloat16)
                for r in range(ring):
                    msgd[k - 1, r, at] = flat[r * zb : (r + 1) * zb]
        if k == 0:
            start(turned_d.at[:, z - ROWS : z], edges_d.at[0], drift_edge_sem, {"gz": (iz + 1) % nz})
            start(turned_d.at[:, 0:ROWS], edges_d.at[1], drift_edge_sem, {"gz": (iz + nz - 1) % nz})
    fixed[0] = q
    fixed[1] = p

    def send_drift(k):
        if k == 0:
            to_owners(msge, gote.at[me], drift_sem[0])
        else:
            to_owners(msgd.at[k - 1], gotd.at[k - 1, me], drift_sem[k])

    @pl.when(outer)
    def _():
        pass_on(0)
        pass_on(1)

    arrive(drift_edge_sem, edges_d)
    for r in range(ring):
        beyond = []
        for at in range(x):
            before, after = around(turned_d, edges_d, r, at)
            beyond.append(jnp.where(upper, after, before))
        msge[r, x] = jnp.concatenate(beyond, axis=0).astype(jnp.bfloat16)
    send_drift(0)

    @pl.when(outer)
    def _():
        take_across(0)

    def swapped(which):
        @pl.when(jnp.logical_not(outer))
        def _():
            arrive(swap_sem[which], all_w.at[which])

    at_lane = lax.broadcasted_iota(jnp.int32, (co, lane), 1)

    def build(which):
        def place(gx, carry):
            row = pl.multiple_of(gx * co, co)
            for a in range(3):
                for cz in range(3):
                    moved = {}
                    for b in range(3):
                        t = a * 9 + b * 3 + cz
                        tile, spot = t // per, t % per
                        held_at = tile // half_tiles, tile % half_tiles
                        for side in range(2):
                            pieces = []
                            for gy in range(ny):
                                r = gy * nx + gx + (gy % 2) * (nx - 1 - 2 * gx)
                                piece = all_w[which, r, held_at[0], held_at[1]].astype(jnp.float32)
                                shift = (side * ny + gy - spot) % per
                                pieces.append(pltpu.roll(piece, shift * ci, 1) if shift else piece)
                            moved[b, side] = pieces
                    pairs = []
                    for b in range(yy):
                        value = jnp.zeros((co, lane), jnp.float32)
                        for side in range(y):
                            near = (b + side) % yy
                            if near > 2:
                                continue
                            for gy in range(ny):
                                spot = (side * ny + gy) * ci
                                inside = (at_lane >= spot) & (at_lane < spot + ci)
                                value = jnp.where(inside, moved[near, side][gy], value)
                        pairs.append(value.astype(jnp.bfloat16))
                    for yo in range(yy):
                        for h in range(yy // y):
                            mats[which, a * 3 + cz, pl.ds(yo * c + row, co), h * lane : (h + 1) * lane] = (
                                pairs[(h * y + 1 - yo) % yy]
                            )
            return carry

        lax.fori_loop(0, nx, place, 0)

    def turn_over(which):
        for tap in range(9):
            flipped[which, tap] = mats[which, tap].T

    def scatter(target, zs, value, r, at):
        gx, gy = ring_place(r, nx)
        target[gy, pl.ds(zs * xx + gx * x + at, value.shape[0], stride=xx), :] = value

    def whole(ref, rows_from, rows_to):
        return jnp.concatenate([ref[gy, rows_from:rows_to] for gy in range(ny)], axis=1)

    left = device((me + ring - 1 + iz) % ring, 1 - iz)
    right = device((me + iz) % ring, 1 - iz)
    edge = reach * xx

    def send_halo(slot, value):
        qb[slot] = value.astype(jnp.bfloat16)
        start(qb.at[slot, rows - 2 * edge : rows], halo.at[slot, 0], halo_sem[slot], right)
        start(qb.at[slot, 0 : 2 * edge], halo.at[slot, 1], halo_sem[slot], left)

    def with_halo(slot, value):
        arrive(halo_sem[slot], halo.at[slot])
        ends = [halo[slot, side].astype(jnp.float32) for side in range(2)]
        return jnp.concatenate([ends[0], value, ends[1]], axis=0)

    arrive(field_sem, got0)
    for r in range(ring):
        for at in range(x):
            scatter(stage, 0, got0[r, at].astype(jnp.float32), r, at)
    send_halo(0, whole(stage, 0, rows))
    for later in range(1, steps):
        send_drift(later)
    swapped(0)
    build(0)
    turn_over(0)

    def spread(value):
        n = value.shape[0]
        cube = value.reshape(n // xx, xx, wide)
        for a in range(3):
            moved = cube if a == 1 else pltpu.roll(cube, (1 - a) % xx, 1)
            moved = moved.reshape(n, wide)
            lhs[a, 0, 0:n] = moved.astype(jnp.bfloat16)
            lhs[a, 1, 0 : n - 2 * xx] = moved[xx : n - xx].astype(jnp.bfloat16)

    def conv(height, which, adjoint, flip=False):
        source = mats if adjoint or flip else flipped
        low, high = split_rows(height)
        sums = [[banks[unit, low, 0], banks[unit, high, int(low == high)]] for unit in range(2)]
        plans = (
            [(0, True, True), (1, True, True), (2, True, True), (3, True, True), (4, True, False)],
            [(8, True, True), (7, True, True), (6, True, True), (5, True, True), (4, False, True)],
        )
        for at in range(5):
            for unit in range(2):
                tap, use_low, use_high = plans[unit][at]
                a, cz = tap // 3, tap % 3
                pltpu.matmul_push_rhs(
                    source[which, 8 - tap if adjoint else tap],
                    staging_register=at % 2,
                    mxu_index=unit,
                    transpose=flip,
                )
                copy, first_row = (1, 0) if cz == 1 else (0, cz * xx)
                fresh = at % 2
                if use_low:
                    left = lhs[a, copy, first_row : first_row + low]
                    pltpu.matmul_acc_lhs(sums[unit][0], left, load_staged_rhs=fresh)
                    fresh = None
                if use_high:
                    left = lhs[a, copy, first_row + low : first_row + low + high]
                    pltpu.matmul_acc_lhs(sums[unit][1], left, load_staged_rhs=fresh)
        halves = [pltpu.matmul_pop(sums[0][part]) + pltpu.matmul_pop(sums[1][part]) for part in range(2)]
        return jnp.concatenate(halves, axis=0)

    row = jnp.concatenate([bias_ref[...]] * yy, axis=1)

    def gradient(extent, between=lambda: None, flip=False):
        n = [rows + 2 * (extent + 3 - i) * xx for i in range(4)]
        t = jnp.tanh(conv(n[0], 0, False) + row)
        t_ref[0 : n[0]] = t
        spread(t)
        between()
        spread(conv(n[1], 1, False, flip))
        gu = conv(n[2], 1, True)
        t = t_ref[2 * xx : 2 * xx + n[2]]
        spread(gu * (1.0 - t * t))
        return conv(n[3], 0, True)

    def take_drift(k):
        arrive(drift_sem[k], gotd.at[k - 1])
        for r in range(ring):
            for at in range(x):
                scatter(extra, 0, gotd[k - 1, r, at].astype(jnp.float32), r, at)
        base[...] = base[...] + whole(extra, 0, rows)

    def second_filters():
        @pl.when(outer)
        def _():
            take_across(1)

        swapped(1)
        build(1)

    def collect(ref, r, at):
        gx, gy = ring_place(r, nx)
        return ref[gy, pl.ds(gx * x + at, zb, stride=xx), :]

    def put(ref, value):
        for gy in range(ny):
            ref[gy] = value[:, gy * lane : (gy + 1) * lane]

    base[...] = whole(stage, 0, rows)
    spread(with_halo(0, base[...]))
    g = gradient(reach, second_filters, True)

    arrive(drift_sem[0], gote)
    for r in range(ring):
        beyond = gote[r, x].astype(jnp.float32)
        for at in range(x):
            scatter(extra, 0, gote[r, at].astype(jnp.float32), r, at)
            scatter(extra, zb, beyond[at * ROWS : (at + 1) * ROWS], r, at)
    now = base[...] + whole(extra, 0, rows)
    base[...] = now
    below = halo[0, 0, edge : 2 * edge].astype(jnp.float32) + whole(extra, rows + edge, rows + 2 * edge)
    above = halo[0, 1, 0:edge].astype(jnp.float32) + whole(extra, rows, rows + edge)
    force = g[edge : edge + rows]
    put(dp, -half * force)
    put(dq, (-half * push) * force)
    spread(jnp.concatenate([below, now, above], axis=0) + (-half * push) * g)

    mine = pl.ds(pl.multiple_of(filed * zb, zb), zb)

    def kicked(g):
        shift = whole(dq, 0, rows)
        now = decay * whole(dp, 0, rows) - (2 * half) * (g + shift)
        put(dp, now)
        put(dq, shift + push * now)

    for pair in range(pairs):
        kicked(gradient(0, flip=pair == 0))
        k = 2 * pair + 2
        take_drift(k - 1)
        q = base[...] + whole(dq, 0, rows)
        send_halo(pair + 1, q)
        if pair == 0:
            turn_over(1)
        take_drift(k)
        shift = whole(dq, 0, rows)
        v = base[...] + shift + push * (decay * whole(dp, 0, rows) - (2 * half) * shift)
        vb[pair] = v.astype(jnp.bfloat16)
        start(vb.at[pair, rows - edge : rows], ring_v.at[pair, 0], v_sem[pair], right)
        start(vb.at[pair, 0:edge], ring_v.at[pair, 1], v_sem[pair], left)
        spread(with_halo(pair + 1, q))
        g = gradient(reach)
        kicked(g[edge : edge + rows])
        q = base[...] + whole(dq, 0, rows)
        arrive(v_sem[pair], ring_v.at[pair])
        ends = [
            ring_v[pair, side].astype(jnp.float32) - (2 * half * push) * g[at : at + edge]
            for side, at in enumerate((0, edge + rows))
        ]
        spread(jnp.concatenate([ends[0], q, ends[1]], axis=0))

    put(dp, decay * whole(dp, 0, rows) - half * whole(dq, 0, rows))
    for r in range(ring):
        for at in range(x):
            back_q[r, at] = collect(dq, r, at).astype(jnp.bfloat16)
    to_sources(back_q, got_q.at[:, mine], q_sem)
    g = gradient(0)
    put(dp, whole(dp, 0, rows) - half * g)
    for r in range(ring):
        for at in range(x):
            back_p[r, at] = collect(dp, r, at).astype(jnp.bfloat16)
    to_sources(back_p, got_p.at[:, mine], p_sem)

    def untie(value, which, out, at):
        flat = value.T
        for j in range(y):
            part = pl.ds(at * y + j, c, stride=x * y)
            out[part, :] = fixed[which, part, :] + flat[j * c : (j + 1) * c]

    arrive(q_sem, got_q)
    for at in range(x):
        untie(got_q[at].astype(jnp.float32), 0, q_out, at)
    arrive(p_sem, got_p)
    for at in range(x):
        untie(got_p[at].astype(jnp.float32), 1, p_out, at)

    @pl.when(outer)
    def _():
        for which in range(2):
            for number in column_sems[which]:
                leave(number, own_w.at[which, 0])
            for number in across_sems[which]:
                leave(number, all_w.at[which, 0:nx, 0])
            leave(swap_sem[which], all_w.at[which])

    leave(drift_edge_sem, edges_d)
    left_ring(field_sem, msg0)
    left_ring(drift_sem[0], msge)
    for k in range(1, steps):
        left_ring(drift_sem[k], msgd.at[k - 1])
    for slot in range(pairs + 1):
        leave(halo_sem[slot], halo.at[slot])
    for pair in range(pairs):
        leave(v_sem[pair], ring_v.at[pair])
    left_ring(q_sem, back_q)
    left_ring(p_sem, back_p)


def fits_ring(steps, sizes, position, filter_in):
    nx, ny, nz = sizes
    c, x, y, z = position.shape
    co, ci = filter_in.shape[:2]
    ring = nx * ny
    return (
        steps % 2 == 1 and steps > 2 and nz == 2 and ny == 2 and nx > 1 and y * c == LANES and x * nx == ROWS and y * ny > 2
        and z % (ring * EDGE) == 0 and z // ring == EDGE and co % EDGE == 0 and LANES % ci == 0
        and y * ny * ci == LANES
    )


def on_ring(sizes, position, momentum, noise, filter_in, filter_out, bias):
    nx, ny, nz = sizes
    c, x, y, z = position.shape
    steps = noise.shape[0]
    co, ci = filter_in.shape[:2]
    ring = nx * ny
    zb = z // ring
    xx, yy = x * nx, y * ny
    wide = yy * c
    rows = zb * xx
    lane = LANES
    half_tiles = -(-27 * ci // (2 * lane))
    flat = jax.ShapeDtypeStruct((c * x * y, z), jnp.float32)
    reach, pairs = 4, (steps - 1) // 2
    copies = 2 * nx + 11 + steps + 2 * pairs
    edge = reach * xx
    heights = [(zb + 2 * beyond) * xx for beyond in range(2 * reach)]
    vmem = pl.BlockSpec(memory_space=pltpu.VMEM)
    bf16, f32 = jnp.bfloat16, jnp.float32
    q, p = pl.pallas_call(
        functools.partial(ring_kernel, steps, sizes, heights),
        out_shape=(flat, flat),
        in_specs=[pl.BlockSpec(memory_space=pl.ANY)] * 6,
        out_specs=(vmem, vmem),
        scratch_shapes=[
            pltpu.VMEM((c * x * y, z), f32),
            pltpu.VMEM((c * x * y, z), f32),
            pltpu.VMEM((steps * c * x * y, z), bf16),
            pltpu.VMEM((27, co, ci), bf16),
            pltpu.VMEM((27, co, ci), bf16),
            pltpu.VMEM((1, c), f32),
            pltpu.VMEM((2, 2, half_tiles, co, lane), bf16),
            pltpu.VMEM((2, ring, 2, half_tiles, co, lane), bf16),
            pltpu.VMEM((2, 9, wide, wide), bf16),
            pltpu.VMEM((2, 9, wide, wide), bf16),
            pltpu.VMEM((x, z, lane), f32),
            pltpu.VMEM((ring, x, zb, lane), bf16),
            pltpu.VMEM((ring, x, zb, lane), bf16),
            pltpu.VMEM((steps - 1, ring, x, zb, lane), bf16),
            pltpu.VMEM((steps - 1, ring, x, zb, lane), bf16),
            pltpu.VMEM((ny, rows, lane), f32),
            pltpu.VMEM((3, 2, rows + 4 * edge, wide), bf16),
            pltpu.VMEM((rows + 4 * edge - 2 * xx, wide), f32),
            pltpu.VMEM((rows, wide), f32),
            pltpu.VMEM((ny, rows + 2 * edge, lane), f32),
            pltpu.VMEM((ny, rows, lane), f32),
            pltpu.VMEM((ny, rows, lane), f32),
            pltpu.VMEM((pairs + 1, rows, wide), bf16),
            pltpu.VMEM((pairs + 1, 2, 2 * edge, wide), bf16),
            pltpu.VMEM((pairs, rows, wide), bf16),
            pltpu.VMEM((pairs, 2, edge, wide), bf16),
            pltpu.VMEM((ring, x, zb, lane), bf16),
            pltpu.VMEM((x, z, lane), bf16),
            pltpu.VMEM((ring, x, zb, lane), bf16),
            pltpu.VMEM((x, z, lane), bf16),
            pltpu.VMEM((2, c * x * y, z), f32),
            pltpu.VMEM((steps, c * x * y, z), f32),
            pltpu.VMEM((2, x, ROWS, lane), f32),
            pltpu.VMEM((ring, x + 1, zb, lane), bf16),
            pltpu.VMEM((ring, x + 1, zb, lane), bf16),
            pltpu.SemaphoreType.DMA((copies,)),
            pltpu.SemaphoreType.DMA((copies,)),
            pltpu.SemaphoreType.DMA((6,)),
        ],
        compiler_params=pltpu.CompilerParams(
            collective_id=0, has_side_effects=True, vmem_limit_bytes=24 * 2**20
        ),
    )(
        *(
            pltpu.with_memory_space_constraint(each, pltpu.HBM)
            for each in (
                position.reshape(-1, z),
                momentum.reshape(-1, z),
                noise.reshape(-1, z),
                filter_in.transpose(2, 3, 4, 0, 1).reshape(27, co, ci),
                filter_out.transpose(2, 3, 4, 0, 1).reshape(27, co, ci),
                bias[None],
            )
        )
    )
    return q.reshape(position.shape), p.reshape(momentum.shape)


def on_device(groups, sizes, position, momentum, noise, filter_in, filter_out, bias):
    if groups == 2 and fits_ring(noise.shape[0], sizes, position, filter_in):
        return on_ring(sizes, position, momentum, noise, filter_in, filter_out, bias)
    nx, ny, nz = sizes
    c, x, y, z = position.shape
    steps = noise.shape[0]
    assert x >= 2 and y == 2 and z % EDGE == 0 and nx > 2 and ny > 1
    both = jnp.stack([filter_in, filter_out])
    co, ci = both.shape[1], both.shape[2]
    gather = []
    if co % EDGE == 0:
        both = both.transpose(0, 1, 3, 5, 4, 2).reshape(2, co, 27 * ci)
        gather = [
            pltpu.VMEM((ny, nx, 2, co, 27 * ci), jnp.bfloat16),
            pltpu.VMEM((2, 9, 3, c, c), jnp.bfloat16),
            pltpu.SemaphoreType.DMA((nx * ny - 1,)),
            pltpu.SemaphoreType.DMA((nx * ny - 1,)),
        ]
    else:
        both = both.reshape(2 * co, ci * 27)
        both = lax.all_gather(both, ("gx", "gy"), axis=0, tiled=True)
        both = both.reshape(nx, ny, 2, co, ci, 3, 3, 3)
        both = both.transpose(2, 5, 7, 6, 0, 3, 1, 4).reshape(2, 9, 3, c, c)
    lanes = y * c
    slots = 2 * y if ny == 2 else 3 * y
    full = z + 2 * EDGE
    wide = (y + 2) * c
    flat = jax.ShapeDtypeStruct((c, x * y * z), jnp.float32)
    copies = 15 if ny == 2 else 24
    vmem = pl.BlockSpec(memory_space=pltpu.VMEM)
    q, p = pl.pallas_call(
        functools.partial(kernel, steps, sizes),
        out_shape=(flat, flat),
        in_specs=[vmem] * 5,
        out_specs=(vmem, vmem),
        scratch_shapes=[
            pltpu.VMEM((9, wide, slots * c), jnp.bfloat16),
            pltpu.VMEM((9, lanes, wide), jnp.bfloat16),
            pltpu.VMEM((9, wide, lanes), jnp.bfloat16),
            pltpu.VMEM((9, slots * c, wide), jnp.bfloat16),
            pltpu.VMEM((x + 4, full, slots * c), jnp.bfloat16),
            pltpu.VMEM((x + 4, full, slots * c), jnp.bfloat16),
            pltpu.VMEM((x + 2, full, wide), jnp.float32),
            pltpu.VMEM((x, z, lanes), jnp.float32),
            pltpu.VMEM((x, z, lanes), jnp.float32),
            pltpu.SemaphoreType.DMA((2, copies)),
            pltpu.SemaphoreType.DMA((2, copies)),
            *gather,
        ],
        compiler_params=pltpu.CompilerParams(
            collective_id=0, has_side_effects=True, vmem_limit_bytes=56 * 2**20
        ),
    )(
        position.reshape(c, -1),
        momentum.reshape(c, -1),
        noise.reshape(steps, c, -1),
        both,
        jnp.tile(bias, y + 2)[None],
    )
    return q.reshape(position.shape), p.reshape(momentum.shape)


def solution(mesh):
    field = P(None, ("grp", "gx"), "gy", "gz")
    filters = P("gx", "gy", None, None, None)
    sizes = tuple(mesh.shape[name] for name in ("gx", "gy", "gz"))
    groups = mesh.shape["grp"]
    return jax.shard_map(
        functools.partial(on_device, groups, sizes),
        mesh=mesh,
        in_specs=(field, field, P(None, None, ("grp", "gx"), "gy", "gz"), filters, filters, P()),
        out_specs=(field, field),
        check_vma=False,
    )
```

```python
import functools

import jax
import jax.numpy as jnp
import numpy as np
from jax import lax
from jax.experimental import pallas as pl
from jax.experimental.pallas import tpu as pltpu
from jax.sharding import PartitionSpec as P

EDGE = 16
MESH = pl.DeviceIdType.MESH


def kernel(steps, sizes, pos_ref, mom_ref, noise_ref, w_ref, bias_ref,
           q_out, p_out, a1, a2, b1, b2, eq, eh, t_ref, q_ref, p_ref, send, recv, *gather):
    nx, ny, nz = sizes
    c = pos_ref.shape[0]
    inside = len(gather) > 0
    if inside:
        wg, wf, wsend, wrecv = gather
    x, z, lanes = q_ref.shape
    y = lanes // c
    full = eq.shape[1]
    wrap = ny == 2
    slots = eq.shape[2] // c
    own = slice(EDGE, EDGE + z)
    mine = slice(lanes, 2 * lanes)

    ix, iy, iz = lax.axis_index("gx"), lax.axis_index("gy"), lax.axis_index("gz")
    up = {"gx": lax.rem(ix + 1, nx), "gy": lax.rem(iy + 1, ny), "gz": lax.rem(iz + 1, nz)}
    down = {
        "gx": lax.rem(ix + nx - 1, nx),
        "gy": lax.rem(iy + ny - 1, ny),
        "gz": lax.rem(iz + nz - 1, nz),
    }

    def at_side(**which):
        return {axis: which[axis][axis] for axis in which}

    def early(buf):
        core = slice(2, 2 + x)
        low, high = slice(0, EDGE), slice(z + EDGE, full)
        block = buf.at[core, own, mine]
        edges = (
            (up, buf.at[core, z : z + EDGE, mine], low),
            (down, buf.at[core, EDGE : 2 * EDGE, mine], high),
        )
        out = []
        for side, source, rows in edges:
            out.append((at_side(gz=side), source, buf.at[core, rows, mine], True))
        for beside, part in others:
            out.append((at_side(gy=beside), block, buf.at[core, own, part], True))
            for side, source, rows in edges:
                target = buf.at[core, rows, part]
                out.append((at_side(gy=beside, gz=side), source, target, True))
        out.append(
            (at_side(gx=down), buf.at[2:4, own, mine], buf.at[2 + x : 4 + x, own, mine], False)
        )
        out.append((at_side(gx=up), buf.at[x : 2 + x, own, mine], buf.at[0:2, own, mine], False))
        return out

    def late(buf):
        low, high = slice(0, EDGE), slice(z + EDGE, full)
        from_low = (up, slice(x, 2 + x), slice(0, 2))
        from_high = (down, slice(2, 4), slice(2 + x, 4 + x))
        plan = []
        for _, part in others:
            plan.append((from_low, slice(0, full), part))
            plan += [(from_high, low, part), (from_high, high, part)]
        for side in (from_low, from_high):
            plan += [(side, low, mine), (side, high, mine)]
        return [
            (at_side(gx=side), buf.at[source, rows, part], buf.at[target, rows, part])
            for (side, source, target), rows, part in plan
        ]

    def forward(buf):
        planes = slice(2 + x, 4 + x)
        return [
            (at_side(gy=beside), buf.at[planes, own, mine], buf.at[planes, own, part])
            for beside, part in others
        ]

    others = [(up, slice(0, lanes))]
    if not wrap:
        others.append((down, slice(2 * lanes, 3 * lanes)))

    def remote(source, target, sems, number, device):
        return pltpu.make_async_remote_copy(
            src_ref=source,
            dst_ref=target,
            send_sem=sems[0].at[number],
            recv_sem=sems[1].at[number],
            device_id=device,
            device_id_type=MESH,
        )

    peers = []
    if inside:
        for dx in range(nx):
            for dy in range(ny):
                if dx or dy:
                    peers.append({"gx": lax.rem(ix + dx, nx), "gy": lax.rem(iy + dy, ny)})
    barrier = pltpu.get_barrier_semaphore()
    greeted = peers + [device for device, _, _, _ in early(eq)]
    for device in greeted:
        pl.semaphore_signal(barrier, inc=1, device_id=device, device_id_type=MESH)
    pl.semaphore_wait(barrier, len(greeted))

    if inside:
        copies = []
        for number, device in enumerate(peers):
            copy = remote(w_ref, wg.at[iy, ix], (wsend, wrecv), number, device)
            copy.start()
            copies.append(copy)
        wg[iy, ix] = w_ref[...]
        for copy in copies:
            copy.wait()
        ci = c // ny
        for which in range(2):
            for at in range(27):
                columns = []
                for j in range(ny):
                    pieces = [wg[j, i, which, :, at * ci : (at + 1) * ci] for i in range(nx)]
                    columns.append(jnp.concatenate(pieces, axis=0))
                wf[which, at // 3, at % 3] = jnp.concatenate(columns, axis=1)
        filters = wf
    else:
        filters = w_ref

    def exchange(buf, bank):
        sems = (send.at[bank], recv.at[bank])
        first, own_x = [], []
        number = 0
        for device, source, target, passed in early(buf):
            copy = remote(source, target, sems, number, device)
            number += 1
            copy.start()
            (first if passed else own_x).append(copy)
        for copy in first:
            copy.wait_recv()
        second = []
        for device, source, target in late(buf):
            copy = remote(source, target, sems, number, device)
            number += 1
            copy.start()
            second.append(copy)
        own_x[0].wait_recv()
        for device, source, target in forward(buf):
            copy = remote(source, target, sems, number, device)
            number += 1
            copy.start()
            second.append(copy)
        for copy in own_x[1:] + second:
            copy.wait_recv()
        for copy in first + own_x + second:
            copy.wait_send()

    def slot(at):
        return at % slots

    def unfold(tap, carry):
        blank = jnp.zeros((c, c), jnp.bfloat16)

        def rows(out, which, at, flip, cols, pick):
            line = [blank] * cols
            for col, b in pick:
                line[col] = filters[which, at, 2 - b if flip else b]
            return jnp.concatenate(line, axis=1)

        back = 8 - tap
        for yo in range(y + 2):
            a1[tap, yo * c : (yo + 1) * c, :] = rows(
                a1, 0, tap, False, slots, [(slot(yo + b), b) for b in range(3)]
            )
        for yo in range(y):
            a2[tap, yo * c : (yo + 1) * c, :] = rows(
                a2, 1, tap, False, y + 2, [(yo + b, b) for b in range(3)]
            )
        for s in range(slots):
            pick = [(yo, b) for yo in range(y + 2) for b in range(3) if slot(yo + b) == s]
            b2[tap, s * c : (s + 1) * c, :] = rows(b2, 1, back, True, y + 2, pick)
        for yi in range(y + 2):
            pick = [(yo, yi - yo) for yo in range(y) if 0 <= yi - yo <= 2]
            b1[tap, yi * c : (yi + 1) * c, :] = rows(b1, 0, back, True, y, pick)
        return carry

    lax.fori_loop(0, 9, unfold, 0)

    def load(ref2d, at):
        span = [ref2d[:, (at * y + j) * z : (at * y + j + 1) * z] for j in range(y)]
        return jnp.concatenate(span, axis=0).astype(jnp.float32).T

    for at in range(x):
        q_ref[at] = load(pos_ref, at)
        p_ref[at] = load(mom_ref, at)

    def conv(source, weights, out_x, transposed):
        width = source.shape[2]
        total = None
        for tz in range(3):
            part = None
            for tx in range(3):
                left = source[tx : tx + out_x].reshape(out_x * full, width)
                term = lax.dot_general(
                    left,
                    weights[tx * 3 + tz],
                    (((1,), (1 if transposed else 0,)), ((), ())),
                    preferred_element_type=jnp.float32,
                )
                part = term if part is None else part + term
            if tz != 1:
                part = pltpu.roll(part, 1 if tz == 0 else out_x * full - 1, 0)
            total = part if total is None else total + part
        return total.reshape(out_x, full, total.shape[-1])

    step = 0.25
    decay = jnp.exp(jnp.float32(-0.25))
    kick = jnp.sqrt(1.0 - decay * decay)

    def body(k, carry):
        eq[2 : 2 + x, own, mine] = q_ref[...].astype(jnp.bfloat16)
        exchange(eq, 0)
        t_ref[...] = jnp.tanh(conv(eq, a1, x + 2, True) + bias_ref[...][None])
        h2 = conv(t_ref[...].astype(jnp.bfloat16), a2, x, True)
        eh[2 : 2 + x, own, mine] = h2[:, own].astype(jnp.bfloat16)
        exchange(eh, 1)
        gu = conv(eh, b2, x + 2, False)
        t = t_ref[...]
        gh = (gu * (1.0 - t * t)).astype(jnp.bfloat16)
        force = conv(gh, b1, x, False)[:, own] + q_ref[...]
        half = 0.5 * step

        @pl.when(k > 0)
        def _():
            p_ref[...] = p_ref[...] - half * force

        @pl.when(k < steps)
        def _():
            p = p_ref[...] - half * force
            q = q_ref[...] + half * p
            now = noise_ref.at[k]
            drawn = jnp.stack([load(now, at) for at in range(x)])
            p = decay * p + kick * drawn
            q_ref[...] = q + half * p
            p_ref[...] = p

        return carry

    lax.fori_loop(0, steps + 1, body, 0)

    for ref, out in ((q_ref, q_out), (p_ref, p_out)):
        for at in range(x):
            flat = ref[at].T
            for j in range(y):
                out[:, (at * y + j) * z : (at * y + j + 1) * z] = flat[j * c : (j + 1) * c]


LANES = 128
ROWS = 8


def ring_place(r, nx):
    row, step = r // nx, r % nx
    return step + (row % 2) * (nx - 1 - 2 * step), row


def split_rows(height):
    low = -(-height // (2 * EDGE)) * EDGE
    return low, height - low


def ring_kernel(steps, sizes, heights, *refs):
    pool = {}
    for height in heights:
        parts = split_rows(height)
        for part in parts:
            pool[part] = max(pool.get(part, 0), parts.count(part))
    order = [(unit, part, i) for unit in range(2) for part in sorted(pool) for i in range(pool[part])]
    spaces = [pltpu.ACC(unit)((part, 2 * LANES), jnp.float32) for unit, part, _ in order]
    pl.run_scoped(functools.partial(ring_body, steps, sizes, order, refs), *spaces)


def ring_body(steps, sizes, order, refs, *sums):
    nx, ny, nz = sizes
    banks = dict(zip(order, sums))
    inputs, refs = refs[:6], refs[6:]
    (q_out, p_out, pos_ref, mom_ref, noise_ref, fin_ref, fout_ref, bias_ref, own_w, all_w, mats,
     flipped, turned_d, msg0, got0, msgd, gotd, stage, lhs, t_ref, base, extra, dq, dp, qb,
     halo, vb, ring_v, back_q, got_q, back_p, got_p, fixed, loose, edges_d, msge, gote, send, recv,
     load) = refs
    ring = nx * ny
    x, zb = msg0.shape[1], msg0.shape[2]
    lane = LANES
    z = ring * zb
    taps, co, ci = fin_ref.shape
    c = ny * ci
    y = lane // c
    xx, yy = x * nx, y * ny
    per = lane // ci
    half_tiles = own_w.shape[2]
    wide = yy * c
    reach = 4
    rows = zb * xx

    ix, iy, iz = lax.axis_index("gx"), lax.axis_index("gy"), lax.axis_index("gz")
    ig = lax.axis_index("grp")
    me = iy * nx + ix + (iy % 2) * (nx - 1 - 2 * ix)
    block = nz * me + iz
    home = block // ring == iz
    filed = block % ring

    def device(r, core):
        gx, gy = ring_place(r, nx)
        return {"gx": gx, "gy": gy, "gz": core}

    barrier = pltpu.get_barrier_semaphore()
    everyone = 0
    for dx in range(nx):
        for dy in range(ny):
            for dz in range(nz):
                if dx or dy or dz:
                    everyone += 1
                    pl.semaphore_signal(
                        barrier,
                        inc=1,
                        device_id={"gx": (ix + dx) % nx, "gy": (iy + dy) % ny, "gz": (iz + dz) % nz},
                        device_id_type=MESH,
                    )

    across = [{"gy": 1 - iy}, {"grp": 1 - ig}, {"grp": 1 - ig, "gy": 1 - iy}]
    for where in across[1:]:
        everyone += 1
        pl.semaphore_signal(barrier, inc=1, device_id=where, device_id_type=MESH)

    loads = []
    held = (pos_ref, mom_ref, noise_ref, fin_ref, fout_ref, bias_ref)
    for number in (3, 4, 0, 1, 2, 5):
        copy = pltpu.make_async_copy(inputs[number], held[number], load.at[number])
        copy.start()
        loads.append(copy)

    def copy_of(source, target, number, where):
        return pltpu.make_async_remote_copy(
            src_ref=source,
            dst_ref=target,
            send_sem=send.at[number],
            recv_sem=recv.at[number],
            device_id=where,
            device_id_type=MESH,
        )

    other = {"gz": (iz + 1) % nz}

    def start(source, target, number, where):
        copy_of(source, target, number, where).start()

    def arrive(number, like):
        copy_of(like, like, number, other).wait_recv()

    def leave(number, like):
        copy_of(like, like, number, other).wait_send()

    def start_or_keep(source, target, number, where):
        @pl.when(home)
        def _():
            pltpu.make_async_copy(source, target, recv.at[number]).start()

        @pl.when(jnp.logical_not(home))
        def _():
            start(source, target, number, where)

    def to_owners(buf, target, number):
        for j in range(1, ring + 1):
            at = (filed + j) % ring
            owner = iz * ring + at
            go = start if j < ring else start_or_keep
            go(buf.at[at], target, number, device(owner // nz, owner % nz))

    def to_sources(buf, target, number):
        for j in range(1, ring + 1):
            r = (me + j) % ring
            go = start if j < ring else start_or_keep
            go(buf.at[r], target, number, device(r, block // ring))

    def left_ring(number, buf):
        @pl.when(home)
        def _():
            leave(number, buf.at[0 : ring - 1])

        @pl.when(jnp.logical_not(home))
        def _():
            leave(number, buf)

    column_sems = [[which * (nx - 1) + dx for dx in range(nx - 1)] for which in range(2)]
    across_sems = [[2 * (nx - 1) + 3 * which + i for i in range(3)] for which in range(2)]
    swap_sem = [2 * nx + 4, 2 * nx + 5]
    field_sem = 2 * nx + 6
    drift_sem = [field_sem + 1 + k for k in range(steps)]
    pairs = (steps - 1) // 2
    q_sem = field_sem + 1 + steps
    p_sem, drift_edge_sem = q_sem + 1, q_sem + 2
    halo_sem = [q_sem + 3 + k for k in range(pairs + 1)]
    v_sem = [q_sem + 4 + pairs + k for k in range(pairs)]

    outer = iz == nz - 1

    def pack(which, ref):
        for tile in range(2 * half_tiles):
            span = range(tile * per, min(taps, (tile + 1) * per))
            parts = [ref[t].astype(jnp.float32) for t in span]
            parts += [jnp.zeros((co, ci), jnp.float32)] * (per - len(parts))
            row = jnp.concatenate(parts, axis=1).astype(jnp.bfloat16)
            own_w[which, tile // half_tiles, tile % half_tiles] = row

    loads[0].wait()

    @pl.when(outer)
    def _():
        pack(0, fin_ref)

    def turn(ref, at):
        parts = [ref[pl.ds(at * y + j, c, stride=x * y), :] for j in range(y)]
        return jnp.concatenate(parts, axis=0).T

    pl.semaphore_wait(barrier, everyone)

    def to_column(which):
        for dx in range(1, nx):
            there = {"gx": (ix + dx) % nx}
            start(own_w.at[which, ig], all_w.at[which, me, ig], column_sems[which][dx - 1], there)
        for where, number in zip(across, across_sems[which]):
            start(own_w.at[which, ig], all_w.at[which, me, ig], number, where)

    def hand_over(which, gy, part):
        piece = all_w.at[which, pl.ds(gy * nx, nx), part]
        start(piece, piece, swap_sem[which], other)

    def pass_on(which):
        for dx in range(1, nx):
            arrive(column_sems[which][dx - 1], own_w.at[which, 0])
            gx = (ix + nx - dx) % nx
            piece = all_w.at[which, iy * nx + gx + (iy % 2) * (nx - 1 - 2 * gx), ig]
            for where, number in zip(across, across_sems[which]):
                start(piece, piece, number, where)
        hand_over(which, iy, ig)

    def take_across(which):
        for number, gy, part in zip(across_sems[which], (1 - iy, iy, 1 - iy), (ig, 1 - ig, 1 - ig)):
            arrive(number, all_w.at[which, 0:nx, 0])
            hand_over(which, gy, part)

    @pl.when(outer)
    def _():
        to_column(0)

    loads[1].wait()

    @pl.when(outer)
    def _():
        pack(1, fout_ref)
        to_column(1)
        for which in range(2):
            all_w[which, me, ig] = own_w[which, ig]

    upper = lax.broadcasted_iota(jnp.int32, (ROWS, lane), 0) < reach

    def around(ref, beyond, r, at):
        before = ref[at, r * zb - ROWS : r * zb] if r else beyond[0, at]
        after = ref[at, (r + 1) * zb : (r + 1) * zb + ROWS] if r < ring - 1 else beyond[1, at]
        return before, after

    loads[2].wait()
    for at in range(x):
        flat = turn(pos_ref, at).astype(jnp.bfloat16)
        for r in range(ring):
            msg0[r, at] = flat[r * zb : (r + 1) * zb]
    to_owners(msg0, got0.at[me], field_sem)
    for each in sums:
        pltpu.matmul_pop(each)

    half = 0.125
    decay = float(np.exp(np.float32(-0.25)))
    kick = float(np.sqrt(np.float32(1.0) - np.exp(np.float32(-0.25)) ** 2))
    push = half * (1.0 + decay)
    loads[3].wait()
    loads[4].wait()
    loads[5].wait()
    q = pos_ref[...]
    known = q.astype(jnp.bfloat16).astype(jnp.float32)
    p = mom_ref[...] - half * q
    total = x * y * c
    for k in range(steps):
        noise = noise_ref[k * total : (k + 1) * total].astype(jnp.float32)
        q = q + push * p + (half * kick) * noise
        drift = (q - known).astype(jnp.bfloat16).astype(jnp.float32)
        known = known + drift
        last = k == steps - 1
        p = decay * p + kick * noise - (half if last else 2 * half) * q
        loose[k] = drift
        for at in range(x):
            flat = turn(loose.at[k], at)
            if k == 0:
                turned_d[at] = flat
                for r in range(ring):
                    msge[r, at] = flat[r * zb : (r + 1) * zb].astype(jnp.bfloat16)
            else:
                flat = flat.astype(jnp.bfloat16)
                for r in range(ring):
                    msgd[k - 1, r, at] = flat[r * zb : (r + 1) * zb]
        if k == 0:
            start(turned_d.at[:, z - ROWS : z], edges_d.at[0], drift_edge_sem, {"gz": (iz + 1) % nz})
            start(turned_d.at[:, 0:ROWS], edges_d.at[1], drift_edge_sem, {"gz": (iz + nz - 1) % nz})
    fixed[0] = q
    fixed[1] = p

    def send_drift(k):
        if k == 0:
            to_owners(msge, gote.at[me], drift_sem[0])
        else:
            to_owners(msgd.at[k - 1], gotd.at[k - 1, me], drift_sem[k])

    @pl.when(outer)
    def _():
        pass_on(0)
        pass_on(1)

    arrive(drift_edge_sem, edges_d)
    for r in range(ring):
        beyond = []
        for at in range(x):
            before, after = around(turned_d, edges_d, r, at)
            beyond.append(jnp.where(upper, after, before))
        msge[r, x] = jnp.concatenate(beyond, axis=0).astype(jnp.bfloat16)

    def swapped(which):
        @pl.when(jnp.logical_not(outer))
        def _():
            arrive(swap_sem[which], all_w.at[which])

    at_lane = lax.broadcasted_iota(jnp.int32, (co, lane), 1)

    def build(which):
        def place(gx, carry):
            row = pl.multiple_of(gx * co, co)
            for a in range(3):
                for cz in range(3):
                    moved = {}
                    for b in range(3):
                        t = a * 9 + b * 3 + cz
                        tile, spot = t // per, t % per
                        held_at = tile // half_tiles, tile % half_tiles
                        for side in range(2):
                            pieces = []
                            for gy in range(ny):
                                r = gy * nx + gx + (gy % 2) * (nx - 1 - 2 * gx)
                                piece = all_w[which, r, held_at[0], held_at[1]]
                                shift = (side * ny + gy - spot) % per
                                pieces.append(pltpu.roll(piece, shift * ci, 1) if shift else piece)
                            moved[b, side] = pieces
                    pairs = []
                    for b in range(yy):
                        value = jnp.zeros((co, lane), jnp.bfloat16)
                        for side in range(y):
                            near = (b + side) % yy
                            if near > 2:
                                continue
                            for gy in range(ny):
                                spot = (side * ny + gy) * ci
                                inside = (at_lane >= spot) & (at_lane < spot + ci)
                                value = jnp.where(inside, moved[near, side][gy], value)
                        pairs.append(value)
                    for yo in range(yy):
                        for h in range(yy // y):
                            mats[which, a * 3 + cz, pl.ds(yo * c + row, co), h * lane : (h + 1) * lane] = (
                                pairs[(h * y + 1 - yo) % yy]
                            )
            return carry

        lax.fori_loop(0, nx, place, 0)

    def turn_over(which):
        for tap in range(9):
            flipped[which, tap] = mats[which, tap].T

    def scatter(target, zs, value, r, at):
        gx, gy = ring_place(r, nx)
        target[gy, pl.ds(zs * xx + gx * x + at, value.shape[0], stride=xx), :] = value

    def whole(ref, rows_from, rows_to):
        return jnp.concatenate([ref[gy, rows_from:rows_to] for gy in range(ny)], axis=1)

    left = device((me + ring - 1 + iz) % ring, 1 - iz)
    right = device((me + iz) % ring, 1 - iz)
    edge = reach * xx

    def send_halo(slot, value):
        qb[slot] = value.astype(jnp.bfloat16)
        start(qb.at[slot, rows - 2 * edge : rows], halo.at[slot, 0], halo_sem[slot], right)
        start(qb.at[slot, 0 : 2 * edge], halo.at[slot, 1], halo_sem[slot], left)

    def with_halo(slot, value):
        arrive(halo_sem[slot], halo.at[slot])
        ends = [halo[slot, side].astype(jnp.float32) for side in range(2)]
        return jnp.concatenate([ends[0], value, ends[1]], axis=0)

    arrive(field_sem, got0)
    for r in range(ring):
        for at in range(x):
            scatter(stage, 0, got0[r, at].astype(jnp.float32), r, at)
    send_halo(0, whole(stage, 0, rows))
    send_drift(0)

    @pl.when(outer)
    def _():
        take_across(0)

    swapped(0)
    for later in range(1, steps):
        send_drift(later)
    build(0)

    def spread(value):
        n = value.shape[0]
        cube = value.reshape(n // xx, xx, wide)
        for a in range(3):
            moved = cube if a == 1 else pltpu.roll(cube, (1 - a) % xx, 1)
            moved = moved.reshape(n, wide)
            lhs[a, 0, 0:n] = moved.astype(jnp.bfloat16)
            lhs[a, 1, 0 : n - 2 * xx] = moved[xx : n - xx].astype(jnp.bfloat16)

    def conv(height, which, adjoint, flip=False):
        source = mats if adjoint or flip else flipped
        low, high = split_rows(height)
        sums = [[banks[unit, low, 0], banks[unit, high, int(low == high)]] for unit in range(2)]
        plans = (
            [(3, True, True), (0, True, True), (1, True, True), (2, True, True), (4, True, False)],
            [(5, True, True), (8, True, True), (7, True, True), (6, True, True), (4, False, True)],
        )
        for at in range(5):
            for unit in range(2):
                tap, use_low, use_high = plans[unit][at]
                a, cz = tap // 3, tap % 3
                pltpu.matmul_push_rhs(
                    source[which, 8 - tap if adjoint else tap],
                    staging_register=at % 2,
                    mxu_index=unit,
                    transpose=flip,
                )
                copy, first_row = (1, 0) if cz == 1 else (0, cz * xx)
                fresh = at % 2
                if use_low:
                    left = lhs[a, copy, first_row : first_row + low]
                    pltpu.matmul_acc_lhs(sums[unit][0], left, load_staged_rhs=fresh)
                    fresh = None
                if use_high:
                    left = lhs[a, copy, first_row + low : first_row + low + high]
                    pltpu.matmul_acc_lhs(sums[unit][1], left, load_staged_rhs=fresh)
        halves = [pltpu.matmul_pop(sums[0][part]) + pltpu.matmul_pop(sums[1][part]) for part in range(2)]
        return jnp.concatenate(halves, axis=0)

    row = jnp.concatenate([bias_ref[...]] * yy, axis=1)

    def gradient(extent, between=lambda: None, flip=False):
        n = [rows + 2 * (extent + 3 - i) * xx for i in range(4)]
        t = jnp.tanh(conv(n[0], 0, False, flip) + row)
        if flip:
            turn_over(0)
        t_ref[0 : n[0]] = t
        spread(t)
        between()
        out = conv(n[1], 1, False, flip)
        if flip:
            turn_over(1)
        spread(out)
        gu = conv(n[2], 1, True)
        t = t_ref[2 * xx : 2 * xx + n[2]]
        spread(gu * (1.0 - t * t))
        return conv(n[3], 0, True)

    def take_drift(k):
        arrive(drift_sem[k], gotd.at[k - 1])
        for r in range(ring):
            for at in range(x):
                scatter(extra, 0, gotd[k - 1, r, at].astype(jnp.float32), r, at)
        base[...] = base[...] + whole(extra, 0, rows)

    def second_filters():
        swapped(1)
        build(1)

    def collect(ref, r, at):
        gx, gy = ring_place(r, nx)
        return ref[gy, pl.ds(gx * x + at, zb, stride=xx), :]

    def put(ref, value):
        for gy in range(ny):
            ref[gy] = value[:, gy * lane : (gy + 1) * lane]

    @pl.when(outer)
    def _():
        take_across(1)

    base[...] = whole(stage, 0, rows)
    spread(with_halo(0, base[...]))
    g = gradient(reach, second_filters, True)

    arrive(drift_sem[0], gote)
    for r in range(ring):
        beyond = gote[r, x].astype(jnp.float32)
        for at in range(x):
            scatter(extra, 0, gote[r, at].astype(jnp.float32), r, at)
            scatter(extra, zb, beyond[at * ROWS : (at + 1) * ROWS], r, at)
    now = base[...] + whole(extra, 0, rows)
    base[...] = now
    below = halo[0, 0, edge : 2 * edge].astype(jnp.float32) + whole(extra, rows + edge, rows + 2 * edge)
    above = halo[0, 1, 0:edge].astype(jnp.float32) + whole(extra, rows, rows + edge)
    force = g[edge : edge + rows]
    put(dp, -half * force)
    put(dq, (-half * push) * force)
    spread(jnp.concatenate([below, now, above], axis=0) + (-half * push) * g)

    mine = pl.ds(pl.multiple_of(filed * zb, zb), zb)

    def kicked(g):
        shift = whole(dq, 0, rows)
        now = decay * whole(dp, 0, rows) - (2 * half) * (g + shift)
        put(dp, now)
        put(dq, shift + push * now)

    for pair in range(pairs):
        kicked(gradient(0))
        k = 2 * pair + 2
        take_drift(k - 1)
        q = base[...] + whole(dq, 0, rows)
        send_halo(pair + 1, q)
        take_drift(k)
        shift = whole(dq, 0, rows)
        v = base[...] + shift + push * (decay * whole(dp, 0, rows) - (2 * half) * shift)
        vb[pair] = v.astype(jnp.bfloat16)
        start(vb.at[pair, rows - edge : rows], ring_v.at[pair, 0], v_sem[pair], right)
        start(vb.at[pair, 0:edge], ring_v.at[pair, 1], v_sem[pair], left)
        spread(with_halo(pair + 1, q))
        g = gradient(reach)
        kicked(g[edge : edge + rows])
        q = base[...] + whole(dq, 0, rows)
        arrive(v_sem[pair], ring_v.at[pair])
        ends = [
            ring_v[pair, side].astype(jnp.float32) - (2 * half * push) * g[at : at + edge]
            for side, at in enumerate((0, edge + rows))
        ]
        spread(jnp.concatenate([ends[0], q, ends[1]], axis=0))

    put(dp, decay * whole(dp, 0, rows) - half * whole(dq, 0, rows))

    def return_q():
        for r in range(ring):
            for at in range(x):
                back_q[r, at] = collect(dq, r, at).astype(jnp.bfloat16)
        to_sources(back_q, got_q.at[:, mine], q_sem)

    g = gradient(0, return_q)
    put(dp, whole(dp, 0, rows) - half * g)
    for r in range(ring):
        for at in range(x):
            back_p[r, at] = collect(dp, r, at).astype(jnp.bfloat16)
    to_sources(back_p, got_p.at[:, mine], p_sem)

    def untie(value, which, out, at):
        flat = value.T
        for j in range(y):
            part = pl.ds(at * y + j, c, stride=x * y)
            out[part, :] = fixed[which, part, :] + flat[j * c : (j + 1) * c]

    arrive(q_sem, got_q)
    for at in range(x):
        untie(got_q[at].astype(jnp.float32), 0, q_out, at)
    arrive(p_sem, got_p)
    for at in range(x):
        untie(got_p[at].astype(jnp.float32), 1, p_out, at)

    @pl.when(outer)
    def _():
        for which in range(2):
            for number in column_sems[which]:
                leave(number, own_w.at[which, 0])
            for number in across_sems[which]:
                leave(number, all_w.at[which, 0:nx, 0])
            leave(swap_sem[which], all_w.at[which])

    leave(drift_edge_sem, edges_d)
    left_ring(field_sem, msg0)
    left_ring(drift_sem[0], msge)
    for k in range(1, steps):
        left_ring(drift_sem[k], msgd.at[k - 1])
    for slot in range(pairs + 1):
        leave(halo_sem[slot], halo.at[slot])
    for pair in range(pairs):
        leave(v_sem[pair], ring_v.at[pair])
    left_ring(q_sem, back_q)
    left_ring(p_sem, back_p)


def fits_ring(steps, sizes, position, filter_in):
    nx, ny, nz = sizes
    c, x, y, z = position.shape
    co, ci = filter_in.shape[:2]
    ring = nx * ny
    return (
        steps % 2 == 1 and steps > 2 and nz == 2 and ny == 2 and nx > 1 and y * c == LANES and x * nx == ROWS and y * ny > 2
        and z % (ring * EDGE) == 0 and z // ring == EDGE and co % EDGE == 0 and LANES % ci == 0
        and y * ny * ci == LANES
    )


def on_ring(sizes, position, momentum, noise, filter_in, filter_out, bias):
    nx, ny, nz = sizes
    c, x, y, z = position.shape
    steps = noise.shape[0]
    co, ci = filter_in.shape[:2]
    ring = nx * ny
    zb = z // ring
    xx, yy = x * nx, y * ny
    wide = yy * c
    rows = zb * xx
    lane = LANES
    half_tiles = -(-27 * ci // (2 * lane))
    flat = jax.ShapeDtypeStruct((c * x * y, z), jnp.float32)
    reach, pairs = 4, (steps - 1) // 2
    copies = 2 * nx + 11 + steps + 2 * pairs
    edge = reach * xx
    heights = [(zb + 2 * beyond) * xx for beyond in range(2 * reach)]
    vmem = pl.BlockSpec(memory_space=pltpu.VMEM)
    bf16, f32 = jnp.bfloat16, jnp.float32
    q, p = pl.pallas_call(
        functools.partial(ring_kernel, steps, sizes, heights),
        out_shape=(flat, flat),
        in_specs=[pl.BlockSpec(memory_space=pl.ANY)] * 6,
        out_specs=(vmem, vmem),
        scratch_shapes=[
            pltpu.VMEM((c * x * y, z), f32),
            pltpu.VMEM((c * x * y, z), f32),
            pltpu.VMEM((steps * c * x * y, z), bf16),
            pltpu.VMEM((27, co, ci), bf16),
            pltpu.VMEM((27, co, ci), bf16),
            pltpu.VMEM((1, c), f32),
            pltpu.VMEM((2, 2, half_tiles, co, lane), bf16),
            pltpu.VMEM((2, ring, 2, half_tiles, co, lane), bf16),
            pltpu.VMEM((2, 9, wide, wide), bf16),
            pltpu.VMEM((2, 9, wide, wide), bf16),
            pltpu.VMEM((x, z, lane), f32),
            pltpu.VMEM((ring, x, zb, lane), bf16),
            pltpu.VMEM((ring, x, zb, lane), bf16),
            pltpu.VMEM((steps - 1, ring, x, zb, lane), bf16),
            pltpu.VMEM((steps - 1, ring, x, zb, lane), bf16),
            pltpu.VMEM((ny, rows, lane), f32),
            pltpu.VMEM((3, 2, rows + 4 * edge, wide), bf16),
            pltpu.VMEM((rows + 4 * edge - 2 * xx, wide), f32),
            pltpu.VMEM((rows, wide), f32),
            pltpu.VMEM((ny, rows + 2 * edge, lane), f32),
            pltpu.VMEM((ny, rows, lane), f32),
            pltpu.VMEM((ny, rows, lane), f32),
            pltpu.VMEM((pairs + 1, rows, wide), bf16),
            pltpu.VMEM((pairs + 1, 2, 2 * edge, wide), bf16),
            pltpu.VMEM((pairs, rows, wide), bf16),
            pltpu.VMEM((pairs, 2, edge, wide), bf16),
            pltpu.VMEM((ring, x, zb, lane), bf16),
            pltpu.VMEM((x, z, lane), bf16),
            pltpu.VMEM((ring, x, zb, lane), bf16),
            pltpu.VMEM((x, z, lane), bf16),
            pltpu.VMEM((2, c * x * y, z), f32),
            pltpu.VMEM((steps, c * x * y, z), f32),
            pltpu.VMEM((2, x, ROWS, lane), f32),
            pltpu.VMEM((ring, x + 1, zb, lane), bf16),
            pltpu.VMEM((ring, x + 1, zb, lane), bf16),
            pltpu.SemaphoreType.DMA((copies,)),
            pltpu.SemaphoreType.DMA((copies,)),
            pltpu.SemaphoreType.DMA((6,)),
        ],
        compiler_params=pltpu.CompilerParams(
            collective_id=0, has_side_effects=True, vmem_limit_bytes=24 * 2**20
        ),
    )(
        *(
            pltpu.with_memory_space_constraint(each, pltpu.HBM)
            for each in (
                position.reshape(-1, z),
                momentum.reshape(-1, z),
                noise.reshape(-1, z),
                filter_in.transpose(2, 3, 4, 0, 1).reshape(27, co, ci),
                filter_out.transpose(2, 3, 4, 0, 1).reshape(27, co, ci),
                bias[None],
            )
        )
    )
    return q.reshape(position.shape), p.reshape(momentum.shape)


def on_device(groups, sizes, position, momentum, noise, filter_in, filter_out, bias):
    if groups == 2 and fits_ring(noise.shape[0], sizes, position, filter_in):
        return on_ring(sizes, position, momentum, noise, filter_in, filter_out, bias)
    nx, ny, nz = sizes
    c, x, y, z = position.shape
    steps = noise.shape[0]
    assert x >= 2 and y == 2 and z % EDGE == 0 and nx > 2 and ny > 1
    both = jnp.stack([filter_in, filter_out])
    co, ci = both.shape[1], both.shape[2]
    gather = []
    if co % EDGE == 0:
        both = both.transpose(0, 1, 3, 5, 4, 2).reshape(2, co, 27 * ci)
        gather = [
            pltpu.VMEM((ny, nx, 2, co, 27 * ci), jnp.bfloat16),
            pltpu.VMEM((2, 9, 3, c, c), jnp.bfloat16),
            pltpu.SemaphoreType.DMA((nx * ny - 1,)),
            pltpu.SemaphoreType.DMA((nx * ny - 1,)),
        ]
    else:
        both = both.reshape(2 * co, ci * 27)
        both = lax.all_gather(both, ("gx", "gy"), axis=0, tiled=True)
        both = both.reshape(nx, ny, 2, co, ci, 3, 3, 3)
        both = both.transpose(2, 5, 7, 6, 0, 3, 1, 4).reshape(2, 9, 3, c, c)
    lanes = y * c
    slots = 2 * y if ny == 2 else 3 * y
    full = z + 2 * EDGE
    wide = (y + 2) * c
    flat = jax.ShapeDtypeStruct((c, x * y * z), jnp.float32)
    copies = 15 if ny == 2 else 24
    vmem = pl.BlockSpec(memory_space=pltpu.VMEM)
    q, p = pl.pallas_call(
        functools.partial(kernel, steps, sizes),
        out_shape=(flat, flat),
        in_specs=[vmem] * 5,
        out_specs=(vmem, vmem),
        scratch_shapes=[
            pltpu.VMEM((9, wide, slots * c), jnp.bfloat16),
            pltpu.VMEM((9, lanes, wide), jnp.bfloat16),
            pltpu.VMEM((9, wide, lanes), jnp.bfloat16),
            pltpu.VMEM((9, slots * c, wide), jnp.bfloat16),
            pltpu.VMEM((x + 4, full, slots * c), jnp.bfloat16),
            pltpu.VMEM((x + 4, full, slots * c), jnp.bfloat16),
            pltpu.VMEM((x + 2, full, wide), jnp.float32),
            pltpu.VMEM((x, z, lanes), jnp.float32),
            pltpu.VMEM((x, z, lanes), jnp.float32),
            pltpu.SemaphoreType.DMA((2, copies)),
            pltpu.SemaphoreType.DMA((2, copies)),
            *gather,
        ],
        compiler_params=pltpu.CompilerParams(
            collective_id=0, has_side_effects=True, vmem_limit_bytes=56 * 2**20
        ),
    )(
        position.reshape(c, -1),
        momentum.reshape(c, -1),
        noise.reshape(steps, c, -1),
        both,
        jnp.tile(bias, y + 2)[None],
    )
    return q.reshape(position.shape), p.reshape(momentum.shape)


def solution(mesh):
    field = P(None, ("grp", "gx"), "gy", "gz")
    filters = P("gx", "gy", None, None, None)
    sizes = tuple(mesh.shape[name] for name in ("gx", "gy", "gz"))
    groups = mesh.shape["grp"]
    return jax.shard_map(
        functools.partial(on_device, groups, sizes),
        mesh=mesh,
        in_specs=(field, field, P(None, None, ("grp", "gx"), "gy", "gz"), filters, filters, P()),
        out_specs=(field, field),
        check_vma=False,
    )
```

```python
import functools

import jax
import jax.numpy as jnp
import numpy as np
from jax import lax
from jax.experimental import pallas as pl
from jax.experimental.pallas import tpu as pltpu
from jax.sharding import PartitionSpec as P

EDGE = 16
MESH = pl.DeviceIdType.MESH


def kernel(steps, sizes, pos_ref, mom_ref, noise_ref, w_ref, bias_ref,
           q_out, p_out, a1, a2, b1, b2, eq, eh, t_ref, q_ref, p_ref, send, recv, *gather):
    nx, ny, nz = sizes
    c = pos_ref.shape[0]
    inside = len(gather) > 0
    if inside:
        wg, wf, wsend, wrecv = gather
    x, z, lanes = q_ref.shape
    y = lanes // c
    full = eq.shape[1]
    wrap = ny == 2
    slots = eq.shape[2] // c
    own = slice(EDGE, EDGE + z)
    mine = slice(lanes, 2 * lanes)

    ix, iy, iz = lax.axis_index("gx"), lax.axis_index("gy"), lax.axis_index("gz")
    up = {"gx": lax.rem(ix + 1, nx), "gy": lax.rem(iy + 1, ny), "gz": lax.rem(iz + 1, nz)}
    down = {
        "gx": lax.rem(ix + nx - 1, nx),
        "gy": lax.rem(iy + ny - 1, ny),
        "gz": lax.rem(iz + nz - 1, nz),
    }

    def at_side(**which):
        return {axis: which[axis][axis] for axis in which}

    def early(buf):
        core = slice(2, 2 + x)
        low, high = slice(0, EDGE), slice(z + EDGE, full)
        block = buf.at[core, own, mine]
        edges = (
            (up, buf.at[core, z : z + EDGE, mine], low),
            (down, buf.at[core, EDGE : 2 * EDGE, mine], high),
        )
        out = []
        for side, source, rows in edges:
            out.append((at_side(gz=side), source, buf.at[core, rows, mine], True))
        for beside, part in others:
            out.append((at_side(gy=beside), block, buf.at[core, own, part], True))
            for side, source, rows in edges:
                target = buf.at[core, rows, part]
                out.append((at_side(gy=beside, gz=side), source, target, True))
        out.append(
            (at_side(gx=down), buf.at[2:4, own, mine], buf.at[2 + x : 4 + x, own, mine], False)
        )
        out.append((at_side(gx=up), buf.at[x : 2 + x, own, mine], buf.at[0:2, own, mine], False))
        return out

    def late(buf):
        low, high = slice(0, EDGE), slice(z + EDGE, full)
        from_low = (up, slice(x, 2 + x), slice(0, 2))
        from_high = (down, slice(2, 4), slice(2 + x, 4 + x))
        plan = []
        for _, part in others:
            plan.append((from_low, slice(0, full), part))
            plan += [(from_high, low, part), (from_high, high, part)]
        for side in (from_low, from_high):
            plan += [(side, low, mine), (side, high, mine)]
        return [
            (at_side(gx=side), buf.at[source, rows, part], buf.at[target, rows, part])
            for (side, source, target), rows, part in plan
        ]

    def forward(buf):
        planes = slice(2 + x, 4 + x)
        return [
            (at_side(gy=beside), buf.at[planes, own, mine], buf.at[planes, own, part])
            for beside, part in others
        ]

    others = [(up, slice(0, lanes))]
    if not wrap:
        others.append((down, slice(2 * lanes, 3 * lanes)))

    def remote(source, target, sems, number, device):
        return pltpu.make_async_remote_copy(
            src_ref=source,
            dst_ref=target,
            send_sem=sems[0].at[number],
            recv_sem=sems[1].at[number],
            device_id=device,
            device_id_type=MESH,
        )

    peers = []
    if inside:
        for dx in range(nx):
            for dy in range(ny):
                if dx or dy:
                    peers.append({"gx": lax.rem(ix + dx, nx), "gy": lax.rem(iy + dy, ny)})
    barrier = pltpu.get_barrier_semaphore()
    greeted = peers + [device for device, _, _, _ in early(eq)]
    for device in greeted:
        pl.semaphore_signal(barrier, inc=1, device_id=device, device_id_type=MESH)
    pl.semaphore_wait(barrier, len(greeted))

    if inside:
        copies = []
        for number, device in enumerate(peers):
            copy = remote(w_ref, wg.at[iy, ix], (wsend, wrecv), number, device)
            copy.start()
            copies.append(copy)
        wg[iy, ix] = w_ref[...]
        for copy in copies:
            copy.wait()
        ci = c // ny
        for which in range(2):
            for at in range(27):
                columns = []
                for j in range(ny):
                    pieces = [wg[j, i, which, :, at * ci : (at + 1) * ci] for i in range(nx)]
                    columns.append(jnp.concatenate(pieces, axis=0))
                wf[which, at // 3, at % 3] = jnp.concatenate(columns, axis=1)
        filters = wf
    else:
        filters = w_ref

    def exchange(buf, bank):
        sems = (send.at[bank], recv.at[bank])
        first, own_x = [], []
        number = 0
        for device, source, target, passed in early(buf):
            copy = remote(source, target, sems, number, device)
            number += 1
            copy.start()
            (first if passed else own_x).append(copy)
        for copy in first:
            copy.wait_recv()
        second = []
        for device, source, target in late(buf):
            copy = remote(source, target, sems, number, device)
            number += 1
            copy.start()
            second.append(copy)
        own_x[0].wait_recv()
        for device, source, target in forward(buf):
            copy = remote(source, target, sems, number, device)
            number += 1
            copy.start()
            second.append(copy)
        for copy in own_x[1:] + second:
            copy.wait_recv()
        for copy in first + own_x + second:
            copy.wait_send()

    def slot(at):
        return at % slots

    def unfold(tap, carry):
        blank = jnp.zeros((c, c), jnp.bfloat16)

        def rows(out, which, at, flip, cols, pick):
            line = [blank] * cols
            for col, b in pick:
                line[col] = filters[which, at, 2 - b if flip else b]
            return jnp.concatenate(line, axis=1)

        back = 8 - tap
        for yo in range(y + 2):
            a1[tap, yo * c : (yo + 1) * c, :] = rows(
                a1, 0, tap, False, slots, [(slot(yo + b), b) for b in range(3)]
            )
        for yo in range(y):
            a2[tap, yo * c : (yo + 1) * c, :] = rows(
                a2, 1, tap, False, y + 2, [(yo + b, b) for b in range(3)]
            )
        for s in range(slots):
            pick = [(yo, b) for yo in range(y + 2) for b in range(3) if slot(yo + b) == s]
            b2[tap, s * c : (s + 1) * c, :] = rows(b2, 1, back, True, y + 2, pick)
        for yi in range(y + 2):
            pick = [(yo, yi - yo) for yo in range(y) if 0 <= yi - yo <= 2]
            b1[tap, yi * c : (yi + 1) * c, :] = rows(b1, 0, back, True, y, pick)
        return carry

    lax.fori_loop(0, 9, unfold, 0)

    def load(ref2d, at):
        span = [ref2d[:, (at * y + j) * z : (at * y + j + 1) * z] for j in range(y)]
        return jnp.concatenate(span, axis=0).astype(jnp.float32).T

    for at in range(x):
        q_ref[at] = load(pos_ref, at)
        p_ref[at] = load(mom_ref, at)

    def conv(source, weights, out_x, transposed):
        width = source.shape[2]
        total = None
        for tz in range(3):
            part = None
            for tx in range(3):
                left = source[tx : tx + out_x].reshape(out_x * full, width)
                term = lax.dot_general(
                    left,
                    weights[tx * 3 + tz],
                    (((1,), (1 if transposed else 0,)), ((), ())),
                    preferred_element_type=jnp.float32,
                )
                part = term if part is None else part + term
            if tz != 1:
                part = pltpu.roll(part, 1 if tz == 0 else out_x * full - 1, 0)
            total = part if total is None else total + part
        return total.reshape(out_x, full, total.shape[-1])

    step = 0.25
    decay = jnp.exp(jnp.float32(-0.25))
    kick = jnp.sqrt(1.0 - decay * decay)

    def body(k, carry):
        eq[2 : 2 + x, own, mine] = q_ref[...].astype(jnp.bfloat16)
        exchange(eq, 0)
        t_ref[...] = jnp.tanh(conv(eq, a1, x + 2, True) + bias_ref[...][None])
        h2 = conv(t_ref[...].astype(jnp.bfloat16), a2, x, True)
        eh[2 : 2 + x, own, mine] = h2[:, own].astype(jnp.bfloat16)
        exchange(eh, 1)
        gu = conv(eh, b2, x + 2, False)
        t = t_ref[...]
        gh = (gu * (1.0 - t * t)).astype(jnp.bfloat16)
        force = conv(gh, b1, x, False)[:, own] + q_ref[...]
        half = 0.5 * step

        @pl.when(k > 0)
        def _():
            p_ref[...] = p_ref[...] - half * force

        @pl.when(k < steps)
        def _():
            p = p_ref[...] - half * force
            q = q_ref[...] + half * p
            now = noise_ref.at[k]
            drawn = jnp.stack([load(now, at) for at in range(x)])
            p = decay * p + kick * drawn
            q_ref[...] = q + half * p
            p_ref[...] = p

        return carry

    lax.fori_loop(0, steps + 1, body, 0)

    for ref, out in ((q_ref, q_out), (p_ref, p_out)):
        for at in range(x):
            flat = ref[at].T
            for j in range(y):
                out[:, (at * y + j) * z : (at * y + j + 1) * z] = flat[j * c : (j + 1) * c]


LANES = 128
ROWS = 8


def ring_place(r, nx):
    row, step = r // nx, r % nx
    return step + (row % 2) * (nx - 1 - 2 * step), row


def split_rows(height):
    low = -(-height // (2 * EDGE)) * EDGE
    return low, height - low


def ring_kernel(steps, sizes, heights, *refs):
    pool = {}
    for height in heights:
        parts = split_rows(height)
        for part in parts:
            pool[part] = max(pool.get(part, 0), parts.count(part))
    order = [(unit, part, i) for unit in range(2) for part in sorted(pool) for i in range(pool[part])]
    spaces = [pltpu.ACC(unit)((part, 2 * LANES), jnp.float32) for unit, part, _ in order]
    pl.run_scoped(functools.partial(ring_body, steps, sizes, order, refs), *spaces)


def ring_body(steps, sizes, order, refs, *sums):
    nx, ny, nz = sizes
    banks = dict(zip(order, sums))
    inputs, refs = refs[:6], refs[6:]
    (q_out, p_out, pos_ref, mom_ref, noise_ref, fin_ref, fout_ref, bias_ref, own_w, all_w, mats,
     flipped, turned_d, msg0, got0, msgd, gotd, stage, lhs, t_ref, base, extra, dq, dp, qb,
     halo, vb, ring_v, back_q, got_q, back_p, got_p, fixed, loose, edges_d, msge, gote, send, recv,
     load) = refs
    ring = nx * ny
    x, zb = msg0.shape[1], msg0.shape[2]
    lane = LANES
    z = ring * zb
    taps, co, ci = fin_ref.shape
    c = ny * ci
    y = lane // c
    xx, yy = x * nx, y * ny
    per = lane // ci
    half_tiles = own_w.shape[2]
    wide = yy * c
    reach = 4
    rows = zb * xx

    ix, iy, iz = lax.axis_index("gx"), lax.axis_index("gy"), lax.axis_index("gz")
    ig = lax.axis_index("grp")
    me = iy * nx + ix + (iy % 2) * (nx - 1 - 2 * ix)
    block = nz * me + iz
    home = block // ring == iz
    filed = block % ring

    def device(r, core):
        gx, gy = ring_place(r, nx)
        return {"gx": gx, "gy": gy, "gz": core}

    barrier = pltpu.get_barrier_semaphore()
    everyone = 0
    for dx in range(nx):
        for dy in range(ny):
            for dz in range(nz):
                if dx or dy or dz:
                    everyone += 1
                    pl.semaphore_signal(
                        barrier,
                        inc=1,
                        device_id={"gx": (ix + dx) % nx, "gy": (iy + dy) % ny, "gz": (iz + dz) % nz},
                        device_id_type=MESH,
                    )

    across = [{"gy": 1 - iy}, {"grp": 1 - ig}, {"grp": 1 - ig, "gy": 1 - iy}]
    for where in across[1:]:
        everyone += 1
        pl.semaphore_signal(barrier, inc=1, device_id=where, device_id_type=MESH)

    loads = []
    held = (pos_ref, mom_ref, noise_ref, fin_ref, fout_ref, bias_ref)
    for number in (3, 4, 0, 1, 2, 5):
        copy = pltpu.make_async_copy(inputs[number], held[number], load.at[number])
        copy.start()
        loads.append(copy)

    def copy_of(source, target, number, where):
        return pltpu.make_async_remote_copy(
            src_ref=source,
            dst_ref=target,
            send_sem=send.at[number],
            recv_sem=recv.at[number],
            device_id=where,
            device_id_type=MESH,
        )

    other = {"gz": (iz + 1) % nz}

    def start(source, target, number, where):
        copy_of(source, target, number, where).start()

    def arrive(number, like):
        copy_of(like, like, number, other).wait_recv()

    def leave(number, like):
        copy_of(like, like, number, other).wait_send()

    def start_or_keep(source, target, number, where):
        @pl.when(home)
        def _():
            pltpu.make_async_copy(source, target, recv.at[number]).start()

        @pl.when(jnp.logical_not(home))
        def _():
            start(source, target, number, where)

    def to_owners(buf, target, number):
        for j in range(1, ring + 1):
            at = (filed + j) % ring
            owner = iz * ring + at
            go = start if j < ring else start_or_keep
            go(buf.at[at], target, number, device(owner // nz, owner % nz))

    turns = sorted(range(1, ring), key=lambda j: (abs(j - ring // 2), j)) + [ring]

    def to_sources(buf, target, number):
        for j in turns:
            r = (me + j) % ring
            go = start if j < ring else start_or_keep
            go(buf.at[r], target, number, device(r, block // ring))

    def left_ring(number, buf):
        @pl.when(home)
        def _():
            leave(number, buf.at[0 : ring - 1])

        @pl.when(jnp.logical_not(home))
        def _():
            leave(number, buf)

    column_sems = [[which * (nx - 1) + dx for dx in range(nx - 1)] for which in range(2)]
    across_sems = [[2 * (nx - 1) + 3 * which + i for i in range(3)] for which in range(2)]
    swap_sem = [2 * nx + 4, 2 * nx + 5]
    field_sem = 2 * nx + 6
    drift_sem = [field_sem + 1 + k for k in range(steps)]
    pairs = (steps - 1) // 2
    q_sem = field_sem + 1 + steps
    p_sem, drift_edge_sem = q_sem + 1, q_sem + 2
    halo_sem = [q_sem + 3 + k for k in range(pairs + 1)]
    v_sem = [q_sem + 4 + pairs + k for k in range(pairs)]

    outer = iz == nz - 1

    def pack(which, ref):
        for tile in range(2 * half_tiles):
            span = range(tile * per, min(taps, (tile + 1) * per))
            parts = [ref[t].astype(jnp.float32) for t in span]
            parts += [jnp.zeros((co, ci), jnp.float32)] * (per - len(parts))
            row = jnp.concatenate(parts, axis=1).astype(jnp.bfloat16)
            own_w[which, tile // half_tiles, tile % half_tiles] = row

    loads[0].wait()

    @pl.when(outer)
    def _():
        pack(0, fin_ref)

    def turn(ref, at):
        parts = [ref[pl.ds(at * y + j, c, stride=x * y), :] for j in range(y)]
        return jnp.concatenate(parts, axis=0).T

    pl.semaphore_wait(barrier, everyone)

    def to_column(which):
        for dx in range(1, nx):
            there = {"gx": (ix + dx) % nx}
            start(own_w.at[which, ig], all_w.at[which, me, ig], column_sems[which][dx - 1], there)
        for where, number in zip(across, across_sems[which]):
            start(own_w.at[which, ig], all_w.at[which, me, ig], number, where)

    def hand_over(which, gy, part):
        piece = all_w.at[which, pl.ds(gy * nx, nx), part]
        start(piece, piece, swap_sem[which], other)

    def pass_on(which):
        for dx in range(1, nx):
            arrive(column_sems[which][dx - 1], own_w.at[which, 0])
            gx = (ix + nx - dx) % nx
            piece = all_w.at[which, iy * nx + gx + (iy % 2) * (nx - 1 - 2 * gx), ig]
            for where, number in zip(across, across_sems[which]):
                start(piece, piece, number, where)
        hand_over(which, iy, ig)

    def take_across(which):
        for number, gy, part in zip(across_sems[which], (1 - iy, iy, 1 - iy), (ig, 1 - ig, 1 - ig)):
            arrive(number, all_w.at[which, 0:nx, 0])
            hand_over(which, gy, part)

    @pl.when(outer)
    def _():
        to_column(0)

    loads[1].wait()

    @pl.when(outer)
    def _():
        pack(1, fout_ref)
        to_column(1)
        for which in range(2):
            all_w[which, me, ig] = own_w[which, ig]

    upper = lax.broadcasted_iota(jnp.int32, (ROWS, lane), 0) < reach

    def around(ref, beyond, r, at):
        before = ref[at, r * zb - ROWS : r * zb] if r else beyond[0, at]
        after = ref[at, (r + 1) * zb : (r + 1) * zb + ROWS] if r < ring - 1 else beyond[1, at]
        return before, after

    loads[2].wait()
    for at in range(x):
        flat = turn(pos_ref, at).astype(jnp.bfloat16)
        for r in range(ring):
            msg0[r, at] = flat[r * zb : (r + 1) * zb]
    to_owners(msg0, got0.at[me], field_sem)
    for each in sums:
        pltpu.matmul_pop(each)

    half = 0.125
    decay = float(np.exp(np.float32(-0.25)))
    kick = float(np.sqrt(np.float32(1.0) - np.exp(np.float32(-0.25)) ** 2))
    push = half * (1.0 + decay)
    loads[3].wait()
    loads[4].wait()
    loads[5].wait()
    q = pos_ref[...]
    known = q.astype(jnp.bfloat16).astype(jnp.float32)
    p = mom_ref[...] - half * q
    total = x * y * c
    for k in range(steps):
        noise = noise_ref[k * total : (k + 1) * total].astype(jnp.float32)
        q = q + push * p + (half * kick) * noise
        drift = (q - known).astype(jnp.bfloat16).astype(jnp.float32)
        known = known + drift
        last = k == steps - 1
        p = decay * p + kick * noise - (half if last else 2 * half) * q
        loose[k] = drift
        for at in range(x):
            flat = turn(loose.at[k], at)
            if k == 0:
                turned_d[at] = flat
                for r in range(ring):
                    msge[r, at] = flat[r * zb : (r + 1) * zb].astype(jnp.bfloat16)
            else:
                flat = flat.astype(jnp.bfloat16)
                for r in range(ring):
                    msgd[k - 1, r, at] = flat[r * zb : (r + 1) * zb]
        if k == 0:
            start(turned_d.at[:, z - ROWS : z], edges_d.at[0], drift_edge_sem, {"gz": (iz + 1) % nz})
            start(turned_d.at[:, 0:ROWS], edges_d.at[1], drift_edge_sem, {"gz": (iz + nz - 1) % nz})
    fixed[0] = q
    fixed[1] = p

    def send_drift(k):
        if k == 0:
            to_owners(msge, gote.at[me], drift_sem[0])
        else:
            to_owners(msgd.at[k - 1], gotd.at[k - 1, me], drift_sem[k])

    @pl.when(outer)
    def _():
        pass_on(0)
        pass_on(1)

    arrive(drift_edge_sem, edges_d)
    for r in range(ring):
        beyond = []
        for at in range(x):
            before, after = around(turned_d, edges_d, r, at)
            beyond.append(jnp.where(upper, after, before))
        msge[r, x] = jnp.concatenate(beyond, axis=0).astype(jnp.bfloat16)

    def swapped(which):
        @pl.when(jnp.logical_not(outer))
        def _():
            arrive(swap_sem[which], all_w.at[which])

    at_lane = lax.broadcasted_iota(jnp.int32, (co, lane), 1)

    def build(which):
        def place(gx, carry):
            row = pl.multiple_of(gx * co, co)
            for a in range(3):
                for cz in range(3):
                    moved = {}
                    for b in range(3):
                        t = a * 9 + b * 3 + cz
                        tile, spot = t // per, t % per
                        held_at = tile // half_tiles, tile % half_tiles
                        for side in range(2):
                            pieces = []
                            for gy in range(ny):
                                r = gy * nx + gx + (gy % 2) * (nx - 1 - 2 * gx)
                                piece = all_w[which, r, held_at[0], held_at[1]]
                                shift = (side * ny + gy - spot) % per
                                pieces.append(pltpu.roll(piece, shift * ci, 1) if shift else piece)
                            moved[b, side] = pieces
                    pairs = []
                    for b in range(yy):
                        value = jnp.zeros((co, lane), jnp.bfloat16)
                        for side in range(y):
                            near = (b + side) % yy
                            if near > 2:
                                continue
                            for gy in range(ny):
                                spot = (side * ny + gy) * ci
                                inside = (at_lane >= spot) & (at_lane < spot + ci)
                                value = jnp.where(inside, moved[near, side][gy], value)
                        pairs.append(value)
                    for yo in range(yy):
                        for h in range(yy // y):
                            mats[which, a * 3 + cz, pl.ds(yo * c + row, co), h * lane : (h + 1) * lane] = (
                                pairs[(h * y + 1 - yo) % yy]
                            )
            return carry

        lax.fori_loop(0, nx, place, 0)

    def turn_over(which):
        for tap in range(9):
            flipped[which, tap] = mats[which, tap].T

    def scatter(target, zs, value, r, at):
        gx, gy = ring_place(r, nx)
        target[gy, pl.ds(zs * xx + gx * x + at, value.shape[0], stride=xx), :] = value

    def whole(ref, rows_from, rows_to):
        return jnp.concatenate([ref[gy, rows_from:rows_to] for gy in range(ny)], axis=1)

    left = device((me + ring - 1 + iz) % ring, 1 - iz)
    right = device((me + iz) % ring, 1 - iz)
    edge = reach * xx

    def send_halo(slot, value):
        qb[slot] = value.astype(jnp.bfloat16)
        start(qb.at[slot, rows - 2 * edge : rows], halo.at[slot, 0], halo_sem[slot], right)
        start(qb.at[slot, 0 : 2 * edge], halo.at[slot, 1], halo_sem[slot], left)

    def with_halo(slot, value):
        arrive(halo_sem[slot], halo.at[slot])
        ends = [halo[slot, side].astype(jnp.float32) for side in range(2)]
        return jnp.concatenate([ends[0], value, ends[1]], axis=0)

    arrive(field_sem, got0)
    for r in range(ring):
        for at in range(x):
            scatter(stage, 0, got0[r, at].astype(jnp.float32), r, at)
    send_halo(0, whole(stage, 0, rows))
    send_drift(0)

    @pl.when(outer)
    def _():
        take_across(0)

    swapped(0)
    for later in range(1, steps):
        send_drift(later)
    build(0)

    def spread(value):
        n = value.shape[0]
        cube = value.reshape(n // xx, xx, wide)
        for a in range(3):
            moved = cube if a == 1 else pltpu.roll(cube, (1 - a) % xx, 1)
            moved = moved.reshape(n, wide)
            lhs[a, 0, 0:n] = moved.astype(jnp.bfloat16)
            lhs[a, 1, 0 : n - 2 * xx] = moved[xx : n - xx].astype(jnp.bfloat16)

    def conv(height, which, adjoint, flip=False):
        source = mats if adjoint or flip else flipped
        low, high = split_rows(height)
        sums = [[banks[unit, low, 0], banks[unit, high, int(low == high)]] for unit in range(2)]
        plans = (
            [(3, True, True), (0, True, True), (1, True, True), (2, True, True), (4, True, False)],
            [(5, True, True), (8, True, True), (7, True, True), (6, True, True), (4, False, True)],
        )
        for at in range(5):
            for unit in range(2):
                tap, use_low, use_high = plans[unit][at]
                a, cz = tap // 3, tap % 3
                pltpu.matmul_push_rhs(
                    source[which, 8 - tap if adjoint else tap],
                    staging_register=at % 2,
                    mxu_index=unit,
                    transpose=flip,
                )
                copy, first_row = (1, 0) if cz == 1 else (0, cz * xx)
                fresh = at % 2
                if use_low:
                    left = lhs[a, copy, first_row : first_row + low]
                    pltpu.matmul_acc_lhs(sums[unit][0], left, load_staged_rhs=fresh)
                    fresh = None
                if use_high:
                    left = lhs[a, copy, first_row + low : first_row + low + high]
                    pltpu.matmul_acc_lhs(sums[unit][1], left, load_staged_rhs=fresh)
        halves = [pltpu.matmul_pop(sums[0][part]) + pltpu.matmul_pop(sums[1][part]) for part in range(2)]
        return jnp.concatenate(halves, axis=0)

    row = jnp.concatenate([bias_ref[...]] * yy, axis=1)

    def gradient(extent, between=lambda: None, flip=False):
        n = [rows + 2 * (extent + 3 - i) * xx for i in range(4)]
        t = jnp.tanh(conv(n[0], 0, False, flip) + row)
        if flip:
            turn_over(0)
        t_ref[0 : n[0]] = t
        spread(t)
        between()
        out = conv(n[1], 1, False, flip)
        if flip:
            turn_over(1)
        spread(out)
        gu = conv(n[2], 1, True)
        t = t_ref[2 * xx : 2 * xx + n[2]]
        spread(gu * (1.0 - t * t))
        return conv(n[3], 0, True)

    def take_drift(k):
        arrive(drift_sem[k], gotd.at[k - 1])
        for r in range(ring):
            for at in range(x):
                scatter(extra, 0, gotd[k - 1, r, at].astype(jnp.float32), r, at)
        base[...] = base[...] + whole(extra, 0, rows)

    def second_filters():
        swapped(1)
        build(1)

    def collect(ref, r, at):
        gx, gy = ring_place(r, nx)
        return ref[gy, pl.ds(gx * x + at, zb, stride=xx), :]

    def put(ref, value):
        for gy in range(ny):
            ref[gy] = value[:, gy * lane : (gy + 1) * lane]

    @pl.when(outer)
    def _():
        take_across(1)

    base[...] = whole(stage, 0, rows)
    spread(with_halo(0, base[...]))
    g = gradient(reach, second_filters, True)

    arrive(drift_sem[0], gote)
    for r in range(ring):
        beyond = gote[r, x].astype(jnp.float32)
        for at in range(x):
            scatter(extra, 0, gote[r, at].astype(jnp.float32), r, at)
            scatter(extra, zb, beyond[at * ROWS : (at + 1) * ROWS], r, at)
    now = base[...] + whole(extra, 0, rows)
    base[...] = now
    below = halo[0, 0, edge : 2 * edge].astype(jnp.float32) + whole(extra, rows + edge, rows + 2 * edge)
    above = halo[0, 1, 0:edge].astype(jnp.float32) + whole(extra, rows, rows + edge)
    force = g[edge : edge + rows]
    put(dp, -half * force)
    put(dq, (-half * push) * force)
    spread(jnp.concatenate([below, now, above], axis=0) + (-half * push) * g)

    mine = pl.ds(pl.multiple_of(filed * zb, zb), zb)

    def kicked(g):
        shift = whole(dq, 0, rows)
        now = decay * whole(dp, 0, rows) - (2 * half) * (g + shift)
        put(dp, now)
        put(dq, shift + push * now)

    for pair in range(pairs):
        kicked(gradient(0))
        k = 2 * pair + 2
        take_drift(k - 1)
        q = base[...] + whole(dq, 0, rows)
        send_halo(pair + 1, q)
        take_drift(k)
        shift = whole(dq, 0, rows)
        v = base[...] + shift + push * (decay * whole(dp, 0, rows) - (2 * half) * shift)
        vb[pair] = v.astype(jnp.bfloat16)
        start(vb.at[pair, rows - edge : rows], ring_v.at[pair, 0], v_sem[pair], right)
        start(vb.at[pair, 0:edge], ring_v.at[pair, 1], v_sem[pair], left)
        spread(with_halo(pair + 1, q))
        g = gradient(reach)
        kicked(g[edge : edge + rows])
        q = base[...] + whole(dq, 0, rows)
        arrive(v_sem[pair], ring_v.at[pair])
        ends = [
            ring_v[pair, side].astype(jnp.float32) - (2 * half * push) * g[at : at + edge]
            for side, at in enumerate((0, edge + rows))
        ]
        spread(jnp.concatenate([ends[0], q, ends[1]], axis=0))

    put(dp, decay * whole(dp, 0, rows) - half * whole(dq, 0, rows))

    def return_q():
        for r in range(ring):
            for at in range(x):
                back_q[r, at] = collect(dq, r, at).astype(jnp.bfloat16)
        to_sources(back_q, got_q.at[:, mine], q_sem)

    g = gradient(0, return_q)
    put(dp, whole(dp, 0, rows) - half * g)
    for r in range(ring):
        for at in range(x):
            back_p[r, at] = collect(dp, r, at).astype(jnp.bfloat16)
    to_sources(back_p, got_p.at[:, mine], p_sem)

    def untie(value, which, out, at):
        flat = value.T
        for j in range(y):
            part = pl.ds(at * y + j, c, stride=x * y)
            out[part, :] = fixed[which, part, :] + flat[j * c : (j + 1) * c]

    arrive(q_sem, got_q)
    for at in range(x):
        untie(got_q[at].astype(jnp.float32), 0, q_out, at)
    arrive(p_sem, got_p)
    for at in range(x):
        untie(got_p[at].astype(jnp.float32), 1, p_out, at)

    @pl.when(outer)
    def _():
        for which in range(2):
            for number in column_sems[which]:
                leave(number, own_w.at[which, 0])
            for number in across_sems[which]:
                leave(number, all_w.at[which, 0:nx, 0])
            leave(swap_sem[which], all_w.at[which])

    leave(drift_edge_sem, edges_d)
    left_ring(field_sem, msg0)
    left_ring(drift_sem[0], msge)
    for k in range(1, steps):
        left_ring(drift_sem[k], msgd.at[k - 1])
    for slot in range(pairs + 1):
        leave(halo_sem[slot], halo.at[slot])
    for pair in range(pairs):
        leave(v_sem[pair], ring_v.at[pair])
    left_ring(q_sem, back_q)
    left_ring(p_sem, back_p)


def copy_out(q_ref, p_ref, q_out, p_out, sems):
    copies = [
        pltpu.make_async_copy(q_ref, q_out, sems.at[0]),
        pltpu.make_async_copy(p_ref, p_out, sems.at[1]),
    ]
    for copy in copies:
        copy.start()
    for copy in copies:
        copy.wait()


def fits_ring(steps, sizes, position, filter_in):
    nx, ny, nz = sizes
    c, x, y, z = position.shape
    co, ci = filter_in.shape[:2]
    ring = nx * ny
    return (
        steps % 2 == 1 and steps > 2 and nz == 2 and ny == 2 and nx > 1 and y * c == LANES and x * nx == ROWS and y * ny > 2
        and z % (ring * EDGE) == 0 and z // ring == EDGE and co % EDGE == 0 and LANES % ci == 0
        and y * ny * ci == LANES
    )


def on_ring(sizes, position, momentum, noise, filter_in, filter_out, bias):
    nx, ny, nz = sizes
    c, x, y, z = position.shape
    steps = noise.shape[0]
    co, ci = filter_in.shape[:2]
    ring = nx * ny
    zb = z // ring
    xx, yy = x * nx, y * ny
    wide = yy * c
    rows = zb * xx
    lane = LANES
    half_tiles = -(-27 * ci // (2 * lane))
    flat = jax.ShapeDtypeStruct((c * x * y, z), jnp.float32)
    reach, pairs = 4, (steps - 1) // 2
    copies = 2 * nx + 11 + steps + 2 * pairs
    edge = reach * xx
    heights = [(zb + 2 * beyond) * xx for beyond in range(2 * reach)]
    vmem = pl.BlockSpec(memory_space=pltpu.VMEM)
    bf16, f32 = jnp.bfloat16, jnp.float32
    q, p = pl.pallas_call(
        functools.partial(ring_kernel, steps, sizes, heights),
        out_shape=(flat, flat),
        in_specs=[pl.BlockSpec(memory_space=pl.ANY)] * 6,
        out_specs=(vmem, vmem),
        scratch_shapes=[
            pltpu.VMEM((c * x * y, z), f32),
            pltpu.VMEM((c * x * y, z), f32),
            pltpu.VMEM((steps * c * x * y, z), bf16),
            pltpu.VMEM((27, co, ci), bf16),
            pltpu.VMEM((27, co, ci), bf16),
            pltpu.VMEM((1, c), f32),
            pltpu.VMEM((2, 2, half_tiles, co, lane), bf16),
            pltpu.VMEM((2, ring, 2, half_tiles, co, lane), bf16),
            pltpu.VMEM((2, 9, wide, wide), bf16),
            pltpu.VMEM((2, 9, wide, wide), bf16),
            pltpu.VMEM((x, z, lane), f32),
            pltpu.VMEM((ring, x, zb, lane), bf16),
            pltpu.VMEM((ring, x, zb, lane), bf16),
            pltpu.VMEM((steps - 1, ring, x, zb, lane), bf16),
            pltpu.VMEM((steps - 1, ring, x, zb, lane), bf16),
            pltpu.VMEM((ny, rows, lane), f32),
            pltpu.VMEM((3, 2, rows + 4 * edge, wide), bf16),
            pltpu.VMEM((rows + 4 * edge - 2 * xx, wide), f32),
            pltpu.VMEM((rows, wide), f32),
            pltpu.VMEM((ny, rows + 2 * edge, lane), f32),
            pltpu.VMEM((ny, rows, lane), f32),
            pltpu.VMEM((ny, rows, lane), f32),
            pltpu.VMEM((pairs + 1, rows, wide), bf16),
            pltpu.VMEM((pairs + 1, 2, 2 * edge, wide), bf16),
            pltpu.VMEM((pairs, rows, wide), bf16),
            pltpu.VMEM((pairs, 2, edge, wide), bf16),
            pltpu.VMEM((ring, x, zb, lane), bf16),
            pltpu.VMEM((x, z, lane), bf16),
            pltpu.VMEM((ring, x, zb, lane), bf16),
            pltpu.VMEM((x, z, lane), bf16),
            pltpu.VMEM((2, c * x * y, z), f32),
            pltpu.VMEM((steps, c * x * y, z), f32),
            pltpu.VMEM((2, x, ROWS, lane), f32),
            pltpu.VMEM((ring, x + 1, zb, lane), bf16),
            pltpu.VMEM((ring, x + 1, zb, lane), bf16),
            pltpu.SemaphoreType.DMA((copies,)),
            pltpu.SemaphoreType.DMA((copies,)),
            pltpu.SemaphoreType.DMA((6,)),
        ],
        compiler_params=pltpu.CompilerParams(
            collective_id=0, has_side_effects=True, vmem_limit_bytes=24 * 2**20
        ),
    )(
        *(
            pltpu.with_memory_space_constraint(each, pltpu.HBM)
            for each in (
                position.reshape(-1, z),
                momentum.reshape(-1, z),
                noise.reshape(-1, z),
                filter_in.transpose(2, 3, 4, 0, 1).reshape(27, co, ci),
                filter_out.transpose(2, 3, 4, 0, 1).reshape(27, co, ci),
                bias[None],
            )
        )
    )
    q, p = pl.pallas_call(
        copy_out,
        out_shape=(flat, flat),
        in_specs=[pl.BlockSpec(memory_space=pl.ANY)] * 2,
        out_specs=[pl.BlockSpec(memory_space=pl.ANY)] * 2,
        scratch_shapes=[pltpu.SemaphoreType.DMA((2,))],
        compiler_params=pltpu.CompilerParams(vmem_limit_bytes=2**20),
    )(q, p)
    return q.reshape(position.shape), p.reshape(momentum.shape)


def on_device(groups, sizes, position, momentum, noise, filter_in, filter_out, bias):
    if groups == 2 and fits_ring(noise.shape[0], sizes, position, filter_in):
        return on_ring(sizes, position, momentum, noise, filter_in, filter_out, bias)
    nx, ny, nz = sizes
    c, x, y, z = position.shape
    steps = noise.shape[0]
    assert x >= 2 and y == 2 and z % EDGE == 0 and nx > 2 and ny > 1
    both = jnp.stack([filter_in, filter_out])
    co, ci = both.shape[1], both.shape[2]
    gather = []
    if co % EDGE == 0:
        both = both.transpose(0, 1, 3, 5, 4, 2).reshape(2, co, 27 * ci)
        gather = [
            pltpu.VMEM((ny, nx, 2, co, 27 * ci), jnp.bfloat16),
            pltpu.VMEM((2, 9, 3, c, c), jnp.bfloat16),
            pltpu.SemaphoreType.DMA((nx * ny - 1,)),
            pltpu.SemaphoreType.DMA((nx * ny - 1,)),
        ]
    else:
        both = both.reshape(2 * co, ci * 27)
        both = lax.all_gather(both, ("gx", "gy"), axis=0, tiled=True)
        both = both.reshape(nx, ny, 2, co, ci, 3, 3, 3)
        both = both.transpose(2, 5, 7, 6, 0, 3, 1, 4).reshape(2, 9, 3, c, c)
    lanes = y * c
    slots = 2 * y if ny == 2 else 3 * y
    full = z + 2 * EDGE
    wide = (y + 2) * c
    flat = jax.ShapeDtypeStruct((c, x * y * z), jnp.float32)
    copies = 15 if ny == 2 else 24
    vmem = pl.BlockSpec(memory_space=pltpu.VMEM)
    q, p = pl.pallas_call(
        functools.partial(kernel, steps, sizes),
        out_shape=(flat, flat),
        in_specs=[vmem] * 5,
        out_specs=(vmem, vmem),
        scratch_shapes=[
            pltpu.VMEM((9, wide, slots * c), jnp.bfloat16),
            pltpu.VMEM((9, lanes, wide), jnp.bfloat16),
            pltpu.VMEM((9, wide, lanes), jnp.bfloat16),
            pltpu.VMEM((9, slots * c, wide), jnp.bfloat16),
            pltpu.VMEM((x + 4, full, slots * c), jnp.bfloat16),
            pltpu.VMEM((x + 4, full, slots * c), jnp.bfloat16),
            pltpu.VMEM((x + 2, full, wide), jnp.float32),
            pltpu.VMEM((x, z, lanes), jnp.float32),
            pltpu.VMEM((x, z, lanes), jnp.float32),
            pltpu.SemaphoreType.DMA((2, copies)),
            pltpu.SemaphoreType.DMA((2, copies)),
            *gather,
        ],
        compiler_params=pltpu.CompilerParams(
            collective_id=0, has_side_effects=True, vmem_limit_bytes=56 * 2**20
        ),
    )(
        position.reshape(c, -1),
        momentum.reshape(c, -1),
        noise.reshape(steps, c, -1),
        both,
        jnp.tile(bias, y + 2)[None],
    )
    return q.reshape(position.shape), p.reshape(momentum.shape)


def solution(mesh):
    field = P(None, ("grp", "gx"), "gy", "gz")
    filters = P("gx", "gy", None, None, None)
    sizes = tuple(mesh.shape[name] for name in ("gx", "gy", "gz"))
    groups = mesh.shape["grp"]
    return jax.shard_map(
        functools.partial(on_device, groups, sizes),
        mesh=mesh,
        in_specs=(field, field, P(None, None, ("grp", "gx"), "gy", "gz"), filters, filters, P()),
        out_specs=(field, field),
        check_vma=False,
    )
```

```python
import functools

import jax
import jax.numpy as jnp
import numpy as np
from jax import lax
from jax.experimental import pallas as pl
from jax.experimental.pallas import tpu as pltpu
from jax.sharding import PartitionSpec as P

EDGE = 16
MESH = pl.DeviceIdType.MESH


def kernel(steps, sizes, pos_ref, mom_ref, noise_ref, w_ref, bias_ref,
           q_out, p_out, a1, a2, b1, b2, eq, eh, t_ref, q_ref, p_ref, send, recv, *gather):
    nx, ny, nz = sizes
    c = pos_ref.shape[0]
    inside = len(gather) > 0
    if inside:
        wg, wf, wsend, wrecv = gather
    x, z, lanes = q_ref.shape
    y = lanes // c
    full = eq.shape[1]
    wrap = ny == 2
    slots = eq.shape[2] // c
    own = slice(EDGE, EDGE + z)
    mine = slice(lanes, 2 * lanes)

    ix, iy, iz = lax.axis_index("gx"), lax.axis_index("gy"), lax.axis_index("gz")
    up = {"gx": lax.rem(ix + 1, nx), "gy": lax.rem(iy + 1, ny), "gz": lax.rem(iz + 1, nz)}
    down = {
        "gx": lax.rem(ix + nx - 1, nx),
        "gy": lax.rem(iy + ny - 1, ny),
        "gz": lax.rem(iz + nz - 1, nz),
    }

    def at_side(**which):
        return {axis: which[axis][axis] for axis in which}

    def early(buf):
        core = slice(2, 2 + x)
        low, high = slice(0, EDGE), slice(z + EDGE, full)
        block = buf.at[core, own, mine]
        edges = (
            (up, buf.at[core, z : z + EDGE, mine], low),
            (down, buf.at[core, EDGE : 2 * EDGE, mine], high),
        )
        out = []
        for side, source, rows in edges:
            out.append((at_side(gz=side), source, buf.at[core, rows, mine], True))
        for beside, part in others:
            out.append((at_side(gy=beside), block, buf.at[core, own, part], True))
            for side, source, rows in edges:
                target = buf.at[core, rows, part]
                out.append((at_side(gy=beside, gz=side), source, target, True))
        out.append(
            (at_side(gx=down), buf.at[2:4, own, mine], buf.at[2 + x : 4 + x, own, mine], False)
        )
        out.append((at_side(gx=up), buf.at[x : 2 + x, own, mine], buf.at[0:2, own, mine], False))
        return out

    def late(buf):
        low, high = slice(0, EDGE), slice(z + EDGE, full)
        from_low = (up, slice(x, 2 + x), slice(0, 2))
        from_high = (down, slice(2, 4), slice(2 + x, 4 + x))
        plan = []
        for _, part in others:
            plan.append((from_low, slice(0, full), part))
            plan += [(from_high, low, part), (from_high, high, part)]
        for side in (from_low, from_high):
            plan += [(side, low, mine), (side, high, mine)]
        return [
            (at_side(gx=side), buf.at[source, rows, part], buf.at[target, rows, part])
            for (side, source, target), rows, part in plan
        ]

    def forward(buf):
        planes = slice(2 + x, 4 + x)
        return [
            (at_side(gy=beside), buf.at[planes, own, mine], buf.at[planes, own, part])
            for beside, part in others
        ]

    others = [(up, slice(0, lanes))]
    if not wrap:
        others.append((down, slice(2 * lanes, 3 * lanes)))

    def remote(source, target, sems, number, device):
        return pltpu.make_async_remote_copy(
            src_ref=source,
            dst_ref=target,
            send_sem=sems[0].at[number],
            recv_sem=sems[1].at[number],
            device_id=device,
            device_id_type=MESH,
        )

    peers = []
    if inside:
        for dx in range(nx):
            for dy in range(ny):
                if dx or dy:
                    peers.append({"gx": lax.rem(ix + dx, nx), "gy": lax.rem(iy + dy, ny)})
    barrier = pltpu.get_barrier_semaphore()
    greeted = peers + [device for device, _, _, _ in early(eq)]
    for device in greeted:
        pl.semaphore_signal(barrier, inc=1, device_id=device, device_id_type=MESH)
    pl.semaphore_wait(barrier, len(greeted))

    if inside:
        copies = []
        for number, device in enumerate(peers):
            copy = remote(w_ref, wg.at[iy, ix], (wsend, wrecv), number, device)
            copy.start()
            copies.append(copy)
        wg[iy, ix] = w_ref[...]
        for copy in copies:
            copy.wait()
        ci = c // ny
        for which in range(2):
            for at in range(27):
                columns = []
                for j in range(ny):
                    pieces = [wg[j, i, which, :, at * ci : (at + 1) * ci] for i in range(nx)]
                    columns.append(jnp.concatenate(pieces, axis=0))
                wf[which, at // 3, at % 3] = jnp.concatenate(columns, axis=1)
        filters = wf
    else:
        filters = w_ref

    def exchange(buf, bank):
        sems = (send.at[bank], recv.at[bank])
        first, own_x = [], []
        number = 0
        for device, source, target, passed in early(buf):
            copy = remote(source, target, sems, number, device)
            number += 1
            copy.start()
            (first if passed else own_x).append(copy)
        for copy in first:
            copy.wait_recv()
        second = []
        for device, source, target in late(buf):
            copy = remote(source, target, sems, number, device)
            number += 1
            copy.start()
            second.append(copy)
        own_x[0].wait_recv()
        for device, source, target in forward(buf):
            copy = remote(source, target, sems, number, device)
            number += 1
            copy.start()
            second.append(copy)
        for copy in own_x[1:] + second:
            copy.wait_recv()
        for copy in first + own_x + second:
            copy.wait_send()

    def slot(at):
        return at % slots

    def unfold(tap, carry):
        blank = jnp.zeros((c, c), jnp.bfloat16)

        def rows(out, which, at, flip, cols, pick):
            line = [blank] * cols
            for col, b in pick:
                line[col] = filters[which, at, 2 - b if flip else b]
            return jnp.concatenate(line, axis=1)

        back = 8 - tap
        for yo in range(y + 2):
            a1[tap, yo * c : (yo + 1) * c, :] = rows(
                a1, 0, tap, False, slots, [(slot(yo + b), b) for b in range(3)]
            )
        for yo in range(y):
            a2[tap, yo * c : (yo + 1) * c, :] = rows(
                a2, 1, tap, False, y + 2, [(yo + b, b) for b in range(3)]
            )
        for s in range(slots):
            pick = [(yo, b) for yo in range(y + 2) for b in range(3) if slot(yo + b) == s]
            b2[tap, s * c : (s + 1) * c, :] = rows(b2, 1, back, True, y + 2, pick)
        for yi in range(y + 2):
            pick = [(yo, yi - yo) for yo in range(y) if 0 <= yi - yo <= 2]
            b1[tap, yi * c : (yi + 1) * c, :] = rows(b1, 0, back, True, y, pick)
        return carry

    lax.fori_loop(0, 9, unfold, 0)

    def load(ref2d, at):
        span = [ref2d[:, (at * y + j) * z : (at * y + j + 1) * z] for j in range(y)]
        return jnp.concatenate(span, axis=0).astype(jnp.float32).T

    for at in range(x):
        q_ref[at] = load(pos_ref, at)
        p_ref[at] = load(mom_ref, at)

    def conv(source, weights, out_x, transposed):
        width = source.shape[2]
        total = None
        for tz in range(3):
            part = None
            for tx in range(3):
                left = source[tx : tx + out_x].reshape(out_x * full, width)
                term = lax.dot_general(
                    left,
                    weights[tx * 3 + tz],
                    (((1,), (1 if transposed else 0,)), ((), ())),
                    preferred_element_type=jnp.float32,
                )
                part = term if part is None else part + term
            if tz != 1:
                part = pltpu.roll(part, 1 if tz == 0 else out_x * full - 1, 0)
            total = part if total is None else total + part
        return total.reshape(out_x, full, total.shape[-1])

    step = 0.25
    decay = jnp.exp(jnp.float32(-0.25))
    kick = jnp.sqrt(1.0 - decay * decay)

    def body(k, carry):
        eq[2 : 2 + x, own, mine] = q_ref[...].astype(jnp.bfloat16)
        exchange(eq, 0)
        t_ref[...] = jnp.tanh(conv(eq, a1, x + 2, True) + bias_ref[...][None])
        h2 = conv(t_ref[...].astype(jnp.bfloat16), a2, x, True)
        eh[2 : 2 + x, own, mine] = h2[:, own].astype(jnp.bfloat16)
        exchange(eh, 1)
        gu = conv(eh, b2, x + 2, False)
        t = t_ref[...]
        gh = (gu * (1.0 - t * t)).astype(jnp.bfloat16)
        force = conv(gh, b1, x, False)[:, own] + q_ref[...]
        half = 0.5 * step

        @pl.when(k > 0)
        def _():
            p_ref[...] = p_ref[...] - half * force

        @pl.when(k < steps)
        def _():
            p = p_ref[...] - half * force
            q = q_ref[...] + half * p
            now = noise_ref.at[k]
            drawn = jnp.stack([load(now, at) for at in range(x)])
            p = decay * p + kick * drawn
            q_ref[...] = q + half * p
            p_ref[...] = p

        return carry

    lax.fori_loop(0, steps + 1, body, 0)

    for ref, out in ((q_ref, q_out), (p_ref, p_out)):
        for at in range(x):
            flat = ref[at].T
            for j in range(y):
                out[:, (at * y + j) * z : (at * y + j + 1) * z] = flat[j * c : (j + 1) * c]


LANES = 128
ROWS = 8


def ring_place(r, nx):
    row, step = r // nx, r % nx
    return step + (row % 2) * (nx - 1 - 2 * step), row


def split_rows(height):
    low = -(-height // (2 * EDGE)) * EDGE
    return low, height - low


def ring_kernel(steps, sizes, heights, *refs):
    pool = {}
    for height in heights:
        parts = split_rows(height)
        for part in parts:
            pool[part] = max(pool.get(part, 0), parts.count(part))
    order = [(unit, part, i) for unit in range(2) for part in sorted(pool) for i in range(pool[part])]
    spaces = [pltpu.ACC(unit)((part, 2 * LANES), jnp.float32) for unit, part, _ in order]
    pl.run_scoped(functools.partial(ring_body, steps, sizes, order, refs), *spaces)


def ring_body(steps, sizes, order, refs, *sums):
    nx, ny, nz = sizes
    banks = dict(zip(order, sums))
    inputs, refs = refs[:6], refs[6:]
    (q_out, p_out, pos_ref, mom_ref, noise_ref, fin_ref, fout_ref, bias_ref, own_w, all_w, mats,
     flipped, turned_d, msg0, got0, msgd, gotd, stage, lhs, t_ref, base, extra, dq, dp, qb,
     halo, vb, ring_v, back_q, got_q, back_p, got_p, fixed, loose, edges_d, msge, gote, mid, send, recv,
     load) = refs
    ring = nx * ny
    x, zb = msg0.shape[1], msg0.shape[2]
    lane = LANES
    z = ring * zb
    taps, co, ci = fin_ref.shape
    c = ny * ci
    y = lane // c
    xx, yy = x * nx, y * ny
    per = lane // ci
    half_tiles = own_w.shape[2]
    wide = yy * c
    reach = 4
    rows = zb * xx

    ix, iy, iz = lax.axis_index("gx"), lax.axis_index("gy"), lax.axis_index("gz")
    ig = lax.axis_index("grp")
    me = iy * nx + ix + (iy % 2) * (nx - 1 - 2 * ix)
    block = nz * me + iz
    home = block // ring == iz
    filed = block % ring

    def device(r, core):
        gx, gy = ring_place(r, nx)
        return {"gx": gx, "gy": gy, "gz": core}

    barrier = pltpu.get_barrier_semaphore()
    everyone = 0
    for dx in range(nx):
        for dy in range(ny):
            for dz in range(nz):
                if dx or dy or dz:
                    everyone += 1
                    pl.semaphore_signal(
                        barrier,
                        inc=1,
                        device_id={"gx": (ix + dx) % nx, "gy": (iy + dy) % ny, "gz": (iz + dz) % nz},
                        device_id_type=MESH,
                    )

    across = [{"gy": 1 - iy}, {"grp": 1 - ig}, {"grp": 1 - ig, "gy": 1 - iy}]
    for where in across[1:]:
        everyone += 1
        pl.semaphore_signal(barrier, inc=1, device_id=where, device_id_type=MESH)

    loads = []
    held = (pos_ref, mom_ref, noise_ref, fin_ref, fout_ref, bias_ref)
    for number in (3, 4, 0, 1, 2, 5):
        copy = pltpu.make_async_copy(inputs[number], held[number], load.at[number])
        copy.start()
        loads.append(copy)

    def copy_of(source, target, number, where):
        return pltpu.make_async_remote_copy(
            src_ref=source,
            dst_ref=target,
            send_sem=send.at[number],
            recv_sem=recv.at[number],
            device_id=where,
            device_id_type=MESH,
        )

    other = {"gz": (iz + 1) % nz}

    def start(source, target, number, where):
        copy_of(source, target, number, where).start()

    def arrive(number, like):
        copy_of(like, like, number, other).wait_recv()

    def leave(number, like):
        copy_of(like, like, number, other).wait_send()

    def start_or_keep(source, target, number, where):
        @pl.when(home)
        def _():
            pltpu.make_async_copy(source, target, recv.at[number]).start()

        @pl.when(jnp.logical_not(home))
        def _():
            start(source, target, number, where)

    def to_owners(buf, target, number):
        for j in range(1, ring + 1):
            at = (filed + j) % ring
            owner = iz * ring + at
            go = start if j < ring else start_or_keep
            go(buf.at[at], target, number, device(owner // nz, owner % nz))

    turns = sorted(range(1, ring), key=lambda j: (abs(j - ring // 2), j)) + [ring]

    def to_sources(buf, target, number):
        for j in turns:
            r = (me + j) % ring
            go = start if j < ring else start_or_keep
            go(buf.at[r], target, number, device(r, block // ring))

    def left_ring(number, buf):
        @pl.when(home)
        def _():
            leave(number, buf.at[0 : ring - 1])

        @pl.when(jnp.logical_not(home))
        def _():
            leave(number, buf)

    column_sems = [[which * (nx - 1) + dx for dx in range(nx - 1)] for which in range(2)]
    across_sems = [[2 * (nx - 1) + 3 * which + i for i in range(3)] for which in range(2)]
    swap_sem = [2 * nx + 4, 2 * nx + 5]
    field_sem = 2 * nx + 6
    drift_sem = [field_sem + 1 + k for k in range(steps)]
    pairs = (steps - 1) // 2
    q_sem = field_sem + 1 + steps
    p_sem, drift_edge_sem = q_sem + 1, q_sem + 2
    halo_sem = [q_sem + 3 + k for k in range(pairs + 1)]
    v_sem = [q_sem + 4 + pairs + k for k in range(pairs)]

    outer = iz == nz - 1

    def pack(which, ref):
        for tile in range(2 * half_tiles):
            span = range(tile * per, min(taps, (tile + 1) * per))
            parts = [ref[t].astype(jnp.float32) for t in span]
            parts += [jnp.zeros((co, ci), jnp.float32)] * (per - len(parts))
            row = jnp.concatenate(parts, axis=1).astype(jnp.bfloat16)
            own_w[which, tile // half_tiles, tile % half_tiles] = row

    loads[0].wait()

    @pl.when(outer)
    def _():
        pack(0, fin_ref)

    def turn(ref, at):
        parts = [ref[pl.ds(at * y + j, c, stride=x * y), :] for j in range(y)]
        return jnp.concatenate(parts, axis=0).T

    pl.semaphore_wait(barrier, everyone)

    def to_column(which):
        for dx in range(1, nx):
            there = {"gx": (ix + dx) % nx}
            start(own_w.at[which, ig], all_w.at[which, me, ig], column_sems[which][dx - 1], there)
        for where, number in zip(across, across_sems[which]):
            start(own_w.at[which, ig], all_w.at[which, me, ig], number, where)

    def hand_over(which, gy, part):
        piece = all_w.at[which, pl.ds(gy * nx, nx), part]
        start(piece, piece, swap_sem[which], other)

    def pass_on(which):
        for dx in range(1, nx):
            arrive(column_sems[which][dx - 1], own_w.at[which, 0])
            gx = (ix + nx - dx) % nx
            piece = all_w.at[which, iy * nx + gx + (iy % 2) * (nx - 1 - 2 * gx), ig]
            for where, number in zip(across, across_sems[which]):
                start(piece, piece, number, where)
        hand_over(which, iy, ig)

    def take_across(which):
        for number, gy, part in zip(across_sems[which], (1 - iy, iy, 1 - iy), (ig, 1 - ig, 1 - ig)):
            arrive(number, all_w.at[which, 0:nx, 0])
            hand_over(which, gy, part)

    @pl.when(outer)
    def _():
        to_column(0)

    loads[1].wait()

    @pl.when(outer)
    def _():
        pack(1, fout_ref)
        to_column(1)
        for which in range(2):
            all_w[which, me, ig] = own_w[which, ig]

    upper = lax.broadcasted_iota(jnp.int32, (ROWS, lane), 0) < reach

    def around(ref, beyond, r, at):
        before = ref[at, r * zb - ROWS : r * zb] if r else beyond[0, at]
        after = ref[at, (r + 1) * zb : (r + 1) * zb + ROWS] if r < ring - 1 else beyond[1, at]
        return before, after

    loads[2].wait()
    for at in range(x):
        flat = turn(pos_ref, at).astype(jnp.bfloat16)
        for r in range(ring):
            msg0[r, at] = flat[r * zb : (r + 1) * zb]
    to_owners(msg0, got0.at[me], field_sem)
    for each in sums:
        pltpu.matmul_pop(each)

    half = 0.125
    decay = float(np.exp(np.float32(-0.25)))
    kick = float(np.sqrt(np.float32(1.0) - np.exp(np.float32(-0.25)) ** 2))
    push = half * (1.0 + decay)
    loads[3].wait()
    loads[4].wait()
    loads[5].wait()
    q = pos_ref[...]
    known = q.astype(jnp.bfloat16).astype(jnp.float32)
    p = mom_ref[...] - half * q
    total = x * y * c
    for k in range(steps):
        noise = noise_ref[k * total : (k + 1) * total].astype(jnp.float32)
        q = q + push * p + (half * kick) * noise
        drift = (q - known).astype(jnp.bfloat16).astype(jnp.float32)
        known = known + drift
        last = k == steps - 1
        p = decay * p + kick * noise - (half if last else 2 * half) * q
        loose[k] = drift
        for at in range(x):
            flat = turn(loose.at[k], at)
            if k == 0:
                turned_d[at] = flat
                for r in range(ring):
                    msge[r, at] = flat[r * zb : (r + 1) * zb].astype(jnp.bfloat16)
            else:
                flat = flat.astype(jnp.bfloat16)
                for r in range(ring):
                    msgd[k - 1, r, at] = flat[r * zb : (r + 1) * zb]
        if k == 0:
            start(turned_d.at[:, z - ROWS : z], edges_d.at[0], drift_edge_sem, {"gz": (iz + 1) % nz})
            start(turned_d.at[:, 0:ROWS], edges_d.at[1], drift_edge_sem, {"gz": (iz + nz - 1) % nz})
    fixed[0] = q
    fixed[1] = p

    def send_drift(k):
        if k == 0:
            to_owners(msge, gote.at[me], drift_sem[0])
        else:
            to_owners(msgd.at[k - 1], gotd.at[k - 1, me], drift_sem[k])

    @pl.when(outer)
    def _():
        pass_on(0)
        pass_on(1)

    arrive(drift_edge_sem, edges_d)
    for r in range(ring):
        beyond = []
        for at in range(x):
            before, after = around(turned_d, edges_d, r, at)
            beyond.append(jnp.where(upper, after, before))
        msge[r, x] = jnp.concatenate(beyond, axis=0).astype(jnp.bfloat16)

    def swapped(which):
        @pl.when(jnp.logical_not(outer))
        def _():
            arrive(swap_sem[which], all_w.at[which])

    at_lane = lax.broadcasted_iota(jnp.int32, (co, lane), 1)

    def build(which):
        def place(gx, carry):
            row = pl.multiple_of(gx * co, co)
            for a in range(3):
                for cz in range(3):
                    moved = {}
                    for b in range(3):
                        t = a * 9 + b * 3 + cz
                        tile, spot = t // per, t % per
                        held_at = tile // half_tiles, tile % half_tiles
                        for side in range(2):
                            pieces = []
                            for gy in range(ny):
                                r = gy * nx + gx + (gy % 2) * (nx - 1 - 2 * gx)
                                piece = all_w[which, r, held_at[0], held_at[1]]
                                shift = (side * ny + gy - spot) % per
                                pieces.append(pltpu.roll(piece, shift * ci, 1) if shift else piece)
                            moved[b, side] = pieces
                    pairs = []
                    for b in range(yy):
                        value = jnp.zeros((co, lane), jnp.bfloat16)
                        for side in range(y):
                            near = (b + side) % yy
                            if near > 2:
                                continue
                            for gy in range(ny):
                                spot = (side * ny + gy) * ci
                                inside = (at_lane >= spot) & (at_lane < spot + ci)
                                value = jnp.where(inside, moved[near, side][gy], value)
                        pairs.append(value)
                    for yo in range(yy):
                        for h in range(yy // y):
                            mats[which, a * 3 + cz, pl.ds(yo * c + row, co), h * lane : (h + 1) * lane] = (
                                pairs[(h * y + 1 - yo) % yy]
                            )
            return carry

        lax.fori_loop(0, nx, place, 0)

    def turn_over(which):
        for tap in range(9):
            flipped[which, tap] = mats[which, tap].T

    def scatter(target, zs, value, r, at):
        gx, gy = ring_place(r, nx)
        target[gy, pl.ds(zs * xx + gx * x + at, value.shape[0], stride=xx), :] = value

    def whole(ref, rows_from, rows_to):
        return jnp.concatenate([ref[gy, rows_from:rows_to] for gy in range(ny)], axis=1)

    left = device((me + ring - 1 + iz) % ring, 1 - iz)
    right = device((me + iz) % ring, 1 - iz)
    edge = reach * xx

    def send_halo(slot, value):
        qb[slot] = value.astype(jnp.bfloat16)
        start(qb.at[slot, rows - 2 * edge : rows], halo.at[slot, 0], halo_sem[slot], right)
        start(qb.at[slot, 0 : 2 * edge], halo.at[slot, 1], halo_sem[slot], left)

    def with_halo(slot, value):
        arrive(halo_sem[slot], halo.at[slot])
        ends = [halo[slot, side].astype(jnp.float32) for side in range(2)]
        return jnp.concatenate([ends[0], value, ends[1]], axis=0)

    arrive(field_sem, got0)
    for r in range(ring):
        for at in range(x):
            scatter(stage, 0, got0[r, at].astype(jnp.float32), r, at)
    send_halo(0, whole(stage, 0, rows))
    send_drift(0)

    @pl.when(outer)
    def _():
        take_across(0)

    swapped(0)
    for later in range(1, steps):
        send_drift(later)
    build(0)

    def spread(value):
        n = value.shape[0]
        cube = value.reshape(n // xx, xx, wide)
        for a in range(3):
            moved = cube if a == 1 else pltpu.roll(cube, (1 - a) % xx, 1)
            moved = moved.reshape(n, wide)
            lhs[a, 0, 0:n] = moved.astype(jnp.bfloat16)
            lhs[a, 1, 0 : n - 2 * xx] = moved[xx : n - xx].astype(jnp.bfloat16)

    def conv(height, which, adjoint, flip=False):
        low, high = split_rows(height)
        return jnp.concatenate(conv_at((0, low), low, high, which, adjoint, flip), axis=0)

    def conv_at(spots, low, high, which, adjoint, flip=False):
        source = mats if adjoint or flip else flipped
        sums = [[banks[unit, low, 0], banks[unit, high, int(low == high)]] for unit in range(2)]
        plans = (
            [(3, True, True), (0, True, True), (1, True, True), (2, True, True), (4, True, False)],
            [(5, True, True), (8, True, True), (7, True, True), (6, True, True), (4, False, True)],
        )
        for at in range(5):
            for unit in range(2):
                tap, use_low, use_high = plans[unit][at]
                a, cz = tap // 3, tap % 3
                pltpu.matmul_push_rhs(
                    source[which, 8 - tap if adjoint else tap],
                    staging_register=at % 2,
                    mxu_index=unit,
                    transpose=flip,
                )
                copy, first_row = (1, 0) if cz == 1 else (0, cz * xx)
                fresh = at % 2
                if use_low:
                    begin = first_row + spots[0]
                    left = lhs[a, copy, begin : begin + low]
                    pltpu.matmul_acc_lhs(sums[unit][0], left, load_staged_rhs=fresh)
                    fresh = None
                if use_high:
                    begin = first_row + spots[1]
                    left = lhs[a, copy, begin : begin + high]
                    pltpu.matmul_acc_lhs(sums[unit][1], left, load_staged_rhs=fresh)
        return [pltpu.matmul_pop(sums[0][part]) + pltpu.matmul_pop(sums[1][part]) for part in range(2)]

    row = jnp.concatenate([bias_ref[...]] * yy, axis=1)

    def gradient(extent, between=lambda: None, flip=False):
        n = [rows + 2 * (extent + 3 - i) * xx for i in range(4)]
        t = jnp.tanh(conv(n[0], 0, False, flip) + row)
        if flip:
            turn_over(0)
        t_ref[0 : n[0]] = t
        spread(t)
        between()
        out = conv(n[1], 1, False, flip)
        if flip:
            turn_over(1)
        spread(out)
        gu = conv(n[2], 1, True)
        t = t_ref[2 * xx : 2 * xx + n[2]]
        spread(gu * (1.0 - t * t))
        return conv(n[3], 0, True)

    def inner(q):
        n = [rows - 2 * (i + 1) * xx for i in range(4)]
        spread(q)
        t = jnp.tanh(conv(n[0], 0, False) + row)
        mid[0, 0 : n[0]] = t
        spread(t)
        out = conv(n[1], 1, False)
        mid[1, 0 : n[1]] = out
        spread(out)
        gu = conv(n[2], 1, True)
        t = t[2 * xx : 2 * xx + n[2]]
        out = gu * (1.0 - t * t)
        mid[2, 0 : n[2]] = out
        spread(out)
        mid[3, 0 : n[3]] = conv(n[3], 0, True)

    def outside(slot, q):
        n = [rows - 2 * (i + 1) * xx for i in range(4)]
        side = 2 * edge
        two = 2 * xx

        def both(which, adjoint):
            return conv_at((0, side + two), side, side, which, adjoint)

        arrive(halo_sem[slot], halo.at[slot])
        ends = [halo[slot, at].astype(jnp.float32) for at in range(2)]
        spread(jnp.concatenate([ends[0], q[0:two], q[rows - two :], ends[1]], axis=0))
        ends = [jnp.tanh(each + row) for each in both(0, False)]
        t = [
            jnp.concatenate([ends[0], mid[0, 0:two]], axis=0),
            jnp.concatenate([mid[0, n[0] - two : n[0]], ends[1]], axis=0),
        ]
        spread(jnp.concatenate(t, axis=0))
        ends = both(1, False)
        spread(jnp.concatenate([ends[0], mid[1, 0:two], mid[1, n[1] - two : n[1]], ends[1]], axis=0))
        gu = both(1, True)
        near = t[0][two:], t[1][0:side]
        ends = [each * (1.0 - at * at) for each, at in zip(gu, near)]
        spread(jnp.concatenate([ends[0], mid[2, 0:two], mid[2, n[2] - two : n[2]], ends[1]], axis=0))
        ends = both(0, True)
        return jnp.concatenate([ends[0], mid[3, 0 : n[3]], ends[1]], axis=0)

    def take_drift(k):
        arrive(drift_sem[k], gotd.at[k - 1])
        for r in range(ring):
            for at in range(x):
                scatter(extra, 0, gotd[k - 1, r, at].astype(jnp.float32), r, at)
        base[...] = base[...] + whole(extra, 0, rows)

    def second_filters():
        swapped(1)
        build(1)

    def collect(ref, r, at):
        gx, gy = ring_place(r, nx)
        return ref[gy, pl.ds(gx * x + at, zb, stride=xx), :]

    def put(ref, value):
        for gy in range(ny):
            ref[gy] = value[:, gy * lane : (gy + 1) * lane]

    @pl.when(outer)
    def _():
        take_across(1)

    base[...] = whole(stage, 0, rows)
    spread(with_halo(0, base[...]))
    g = gradient(reach, second_filters, True)

    arrive(drift_sem[0], gote)
    for r in range(ring):
        beyond = gote[r, x].astype(jnp.float32)
        for at in range(x):
            scatter(extra, 0, gote[r, at].astype(jnp.float32), r, at)
            scatter(extra, zb, beyond[at * ROWS : (at + 1) * ROWS], r, at)
    now = base[...] + whole(extra, 0, rows)
    base[...] = now
    below = halo[0, 0, edge : 2 * edge].astype(jnp.float32) + whole(extra, rows + edge, rows + 2 * edge)
    above = halo[0, 1, 0:edge].astype(jnp.float32) + whole(extra, rows, rows + edge)
    force = g[edge : edge + rows]
    put(dp, -half * force)
    put(dq, (-half * push) * force)
    spread(jnp.concatenate([below, now, above], axis=0) + (-half * push) * g)

    mine = pl.ds(pl.multiple_of(filed * zb, zb), zb)

    def kicked(g):
        shift = whole(dq, 0, rows)
        now = decay * whole(dp, 0, rows) - (2 * half) * (g + shift)
        put(dp, now)
        put(dq, shift + push * now)

    for pair in range(pairs):
        kicked(gradient(0))
        k = 2 * pair + 2
        take_drift(k - 1)
        q = base[...] + whole(dq, 0, rows)
        send_halo(pair + 1, q)
        take_drift(k)
        shift = whole(dq, 0, rows)
        v = base[...] + shift + push * (decay * whole(dp, 0, rows) - (2 * half) * shift)
        vb[pair] = v.astype(jnp.bfloat16)
        start(vb.at[pair, rows - edge : rows], ring_v.at[pair, 0], v_sem[pair], right)
        start(vb.at[pair, 0:edge], ring_v.at[pair, 1], v_sem[pair], left)
        inner(q)
        g = outside(pair + 1, q)
        kicked(g[edge : edge + rows])
        q = base[...] + whole(dq, 0, rows)
        arrive(v_sem[pair], ring_v.at[pair])
        ends = [
            ring_v[pair, side].astype(jnp.float32) - (2 * half * push) * g[at : at + edge]
            for side, at in enumerate((0, edge + rows))
        ]
        spread(jnp.concatenate([ends[0], q, ends[1]], axis=0))

    put(dp, decay * whole(dp, 0, rows) - half * whole(dq, 0, rows))

    def return_q():
        for r in range(ring):
            for at in range(x):
                back_q[r, at] = collect(dq, r, at).astype(jnp.bfloat16)
        to_sources(back_q, got_q.at[:, mine], q_sem)

    g = gradient(0, return_q)
    put(dp, whole(dp, 0, rows) - half * g)
    for r in range(ring):
        for at in range(x):
            back_p[r, at] = collect(dp, r, at).astype(jnp.bfloat16)
    to_sources(back_p, got_p.at[:, mine], p_sem)

    def untie(value, which, out, at):
        flat = value.T
        for j in range(y):
            part = pl.ds(at * y + j, c, stride=x * y)
            out[part, :] = fixed[which, part, :] + flat[j * c : (j + 1) * c]

    arrive(q_sem, got_q)
    for at in range(x):
        untie(got_q[at].astype(jnp.float32), 0, q_out, at)
    arrive(p_sem, got_p)
    for at in range(x):
        untie(got_p[at].astype(jnp.float32), 1, p_out, at)

    @pl.when(outer)
    def _():
        for which in range(2):
            for number in column_sems[which]:
                leave(number, own_w.at[which, 0])
            for number in across_sems[which]:
                leave(number, all_w.at[which, 0:nx, 0])
            leave(swap_sem[which], all_w.at[which])

    leave(drift_edge_sem, edges_d)
    left_ring(field_sem, msg0)
    left_ring(drift_sem[0], msge)
    for k in range(1, steps):
        left_ring(drift_sem[k], msgd.at[k - 1])
    for slot in range(pairs + 1):
        leave(halo_sem[slot], halo.at[slot])
    for pair in range(pairs):
        leave(v_sem[pair], ring_v.at[pair])
    left_ring(q_sem, back_q)
    left_ring(p_sem, back_p)


def copy_out(q_ref, p_ref, q_out, p_out, sems):
    copies = [
        pltpu.make_async_copy(q_ref, q_out, sems.at[0]),
        pltpu.make_async_copy(p_ref, p_out, sems.at[1]),
    ]
    for copy in copies:
        copy.start()
    for copy in copies:
        copy.wait()


def fits_ring(steps, sizes, position, filter_in):
    nx, ny, nz = sizes
    c, x, y, z = position.shape
    co, ci = filter_in.shape[:2]
    ring = nx * ny
    return (
        steps % 2 == 1 and steps > 2 and nz == 2 and ny == 2 and nx > 1 and y * c == LANES and x * nx == ROWS and y * ny > 2
        and z % (ring * EDGE) == 0 and z // ring == EDGE and co % EDGE == 0 and LANES % ci == 0
        and y * ny * ci == LANES
    )


def on_ring(sizes, position, momentum, noise, filter_in, filter_out, bias):
    nx, ny, nz = sizes
    c, x, y, z = position.shape
    steps = noise.shape[0]
    co, ci = filter_in.shape[:2]
    ring = nx * ny
    zb = z // ring
    xx, yy = x * nx, y * ny
    wide = yy * c
    rows = zb * xx
    lane = LANES
    half_tiles = -(-27 * ci // (2 * lane))
    flat = jax.ShapeDtypeStruct((c * x * y, z), jnp.float32)
    reach, pairs = 4, (steps - 1) // 2
    copies = 2 * nx + 11 + steps + 2 * pairs
    edge = reach * xx
    heights = [(zb + 2 * beyond) * xx for beyond in range(-reach, 2 * reach)]
    vmem = pl.BlockSpec(memory_space=pltpu.VMEM)
    bf16, f32 = jnp.bfloat16, jnp.float32
    q, p = pl.pallas_call(
        functools.partial(ring_kernel, steps, sizes, heights),
        out_shape=(flat, flat),
        in_specs=[pl.BlockSpec(memory_space=pl.ANY)] * 6,
        out_specs=(vmem, vmem),
        scratch_shapes=[
            pltpu.VMEM((c * x * y, z), f32),
            pltpu.VMEM((c * x * y, z), f32),
            pltpu.VMEM((steps * c * x * y, z), bf16),
            pltpu.VMEM((27, co, ci), bf16),
            pltpu.VMEM((27, co, ci), bf16),
            pltpu.VMEM((1, c), f32),
            pltpu.VMEM((2, 2, half_tiles, co, lane), bf16),
            pltpu.VMEM((2, ring, 2, half_tiles, co, lane), bf16),
            pltpu.VMEM((2, 9, wide, wide), bf16),
            pltpu.VMEM((2, 9, wide, wide), bf16),
            pltpu.VMEM((x, z, lane), f32),
            pltpu.VMEM((ring, x, zb, lane), bf16),
            pltpu.VMEM((ring, x, zb, lane), bf16),
            pltpu.VMEM((steps - 1, ring, x, zb, lane), bf16),
            pltpu.VMEM((steps - 1, ring, x, zb, lane), bf16),
            pltpu.VMEM((ny, rows, lane), f32),
            pltpu.VMEM((3, 2, rows + 4 * edge, wide), bf16),
            pltpu.VMEM((rows + 4 * edge - 2 * xx, wide), f32),
            pltpu.VMEM((rows, wide), f32),
            pltpu.VMEM((ny, rows + 2 * edge, lane), f32),
            pltpu.VMEM((ny, rows, lane), f32),
            pltpu.VMEM((ny, rows, lane), f32),
            pltpu.VMEM((pairs + 1, rows, wide), bf16),
            pltpu.VMEM((pairs + 1, 2, 2 * edge, wide), bf16),
            pltpu.VMEM((pairs, rows, wide), bf16),
            pltpu.VMEM((pairs, 2, edge, wide), bf16),
            pltpu.VMEM((ring, x, zb, lane), bf16),
            pltpu.VMEM((x, z, lane), bf16),
            pltpu.VMEM((ring, x, zb, lane), bf16),
            pltpu.VMEM((x, z, lane), bf16),
            pltpu.VMEM((2, c * x * y, z), f32),
            pltpu.VMEM((steps, c * x * y, z), f32),
            pltpu.VMEM((2, x, ROWS, lane), f32),
            pltpu.VMEM((ring, x + 1, zb, lane), bf16),
            pltpu.VMEM((ring, x + 1, zb, lane), bf16),
            pltpu.VMEM((4, rows - 2 * xx, wide), f32),
            pltpu.SemaphoreType.DMA((copies,)),
            pltpu.SemaphoreType.DMA((copies,)),
            pltpu.SemaphoreType.DMA((6,)),
        ],
        compiler_params=pltpu.CompilerParams(
            collective_id=0, has_side_effects=True, vmem_limit_bytes=24 * 2**20
        ),
    )(
        *(
            pltpu.with_memory_space_constraint(each, pltpu.HBM)
            for each in (
                position.reshape(-1, z),
                momentum.reshape(-1, z),
                noise.reshape(-1, z),
                filter_in.transpose(2, 3, 4, 0, 1).reshape(27, co, ci),
                filter_out.transpose(2, 3, 4, 0, 1).reshape(27, co, ci),
                bias[None],
            )
        )
    )
    q, p = pl.pallas_call(
        copy_out,
        out_shape=(flat, flat),
        in_specs=[pl.BlockSpec(memory_space=pl.ANY)] * 2,
        out_specs=[pl.BlockSpec(memory_space=pl.ANY)] * 2,
        scratch_shapes=[pltpu.SemaphoreType.DMA((2,))],
        compiler_params=pltpu.CompilerParams(vmem_limit_bytes=2**20),
    )(q, p)
    return q.reshape(position.shape), p.reshape(momentum.shape)


def on_device(groups, sizes, position, momentum, noise, filter_in, filter_out, bias):
    if groups == 2 and fits_ring(noise.shape[0], sizes, position, filter_in):
        return on_ring(sizes, position, momentum, noise, filter_in, filter_out, bias)
    nx, ny, nz = sizes
    c, x, y, z = position.shape
    steps = noise.shape[0]
    assert x >= 2 and y == 2 and z % EDGE == 0 and nx > 2 and ny > 1
    both = jnp.stack([filter_in, filter_out])
    co, ci = both.shape[1], both.shape[2]
    gather = []
    if co % EDGE == 0:
        both = both.transpose(0, 1, 3, 5, 4, 2).reshape(2, co, 27 * ci)
        gather = [
            pltpu.VMEM((ny, nx, 2, co, 27 * ci), jnp.bfloat16),
            pltpu.VMEM((2, 9, 3, c, c), jnp.bfloat16),
            pltpu.SemaphoreType.DMA((nx * ny - 1,)),
            pltpu.SemaphoreType.DMA((nx * ny - 1,)),
        ]
    else:
        both = both.reshape(2 * co, ci * 27)
        both = lax.all_gather(both, ("gx", "gy"), axis=0, tiled=True)
        both = both.reshape(nx, ny, 2, co, ci, 3, 3, 3)
        both = both.transpose(2, 5, 7, 6, 0, 3, 1, 4).reshape(2, 9, 3, c, c)
    lanes = y * c
    slots = 2 * y if ny == 2 else 3 * y
    full = z + 2 * EDGE
    wide = (y + 2) * c
    flat = jax.ShapeDtypeStruct((c, x * y * z), jnp.float32)
    copies = 15 if ny == 2 else 24
    vmem = pl.BlockSpec(memory_space=pltpu.VMEM)
    q, p = pl.pallas_call(
        functools.partial(kernel, steps, sizes),
        out_shape=(flat, flat),
        in_specs=[vmem] * 5,
        out_specs=(vmem, vmem),
        scratch_shapes=[
            pltpu.VMEM((9, wide, slots * c), jnp.bfloat16),
            pltpu.VMEM((9, lanes, wide), jnp.bfloat16),
            pltpu.VMEM((9, wide, lanes), jnp.bfloat16),
            pltpu.VMEM((9, slots * c, wide), jnp.bfloat16),
            pltpu.VMEM((x + 4, full, slots * c), jnp.bfloat16),
            pltpu.VMEM((x + 4, full, slots * c), jnp.bfloat16),
            pltpu.VMEM((x + 2, full, wide), jnp.float32),
            pltpu.VMEM((x, z, lanes), jnp.float32),
            pltpu.VMEM((x, z, lanes), jnp.float32),
            pltpu.SemaphoreType.DMA((2, copies)),
            pltpu.SemaphoreType.DMA((2, copies)),
            *gather,
        ],
        compiler_params=pltpu.CompilerParams(
            collective_id=0, has_side_effects=True, vmem_limit_bytes=56 * 2**20
        ),
    )(
        position.reshape(c, -1),
        momentum.reshape(c, -1),
        noise.reshape(steps, c, -1),
        both,
        jnp.tile(bias, y + 2)[None],
    )
    return q.reshape(position.shape), p.reshape(momentum.shape)


def solution(mesh):
    field = P(None, ("grp", "gx"), "gy", "gz")
    filters = P("gx", "gy", None, None, None)
    sizes = tuple(mesh.shape[name] for name in ("gx", "gy", "gz"))
    groups = mesh.shape["grp"]
    return jax.shard_map(
        functools.partial(on_device, groups, sizes),
        mesh=mesh,
        in_specs=(field, field, P(None, None, ("grp", "gx"), "gy", "gz"), filters, filters, P()),
        out_specs=(field, field),
        check_vma=False,
    )
```

```python
import functools

import jax
import jax.numpy as jnp
import numpy as np
from jax import lax
from jax.experimental import pallas as pl
from jax.experimental.pallas import tpu as pltpu
from jax.sharding import PartitionSpec as P

EDGE = 16
MESH = pl.DeviceIdType.MESH


def kernel(steps, sizes, pos_ref, mom_ref, noise_ref, w_ref, bias_ref,
           q_out, p_out, a1, a2, b1, b2, eq, eh, t_ref, q_ref, p_ref, send, recv, *gather):
    nx, ny, nz = sizes
    c = pos_ref.shape[0]
    inside = len(gather) > 0
    if inside:
        wg, wf, wsend, wrecv = gather
    x, z, lanes = q_ref.shape
    y = lanes // c
    full = eq.shape[1]
    wrap = ny == 2
    slots = eq.shape[2] // c
    own = slice(EDGE, EDGE + z)
    mine = slice(lanes, 2 * lanes)

    ix, iy, iz = lax.axis_index("gx"), lax.axis_index("gy"), lax.axis_index("gz")
    up = {"gx": lax.rem(ix + 1, nx), "gy": lax.rem(iy + 1, ny), "gz": lax.rem(iz + 1, nz)}
    down = {
        "gx": lax.rem(ix + nx - 1, nx),
        "gy": lax.rem(iy + ny - 1, ny),
        "gz": lax.rem(iz + nz - 1, nz),
    }

    def at_side(**which):
        return {axis: which[axis][axis] for axis in which}

    def early(buf):
        core = slice(2, 2 + x)
        low, high = slice(0, EDGE), slice(z + EDGE, full)
        block = buf.at[core, own, mine]
        edges = (
            (up, buf.at[core, z : z + EDGE, mine], low),
            (down, buf.at[core, EDGE : 2 * EDGE, mine], high),
        )
        out = []
        for side, source, rows in edges:
            out.append((at_side(gz=side), source, buf.at[core, rows, mine], True))
        for beside, part in others:
            out.append((at_side(gy=beside), block, buf.at[core, own, part], True))
            for side, source, rows in edges:
                target = buf.at[core, rows, part]
                out.append((at_side(gy=beside, gz=side), source, target, True))
        out.append(
            (at_side(gx=down), buf.at[2:4, own, mine], buf.at[2 + x : 4 + x, own, mine], False)
        )
        out.append((at_side(gx=up), buf.at[x : 2 + x, own, mine], buf.at[0:2, own, mine], False))
        return out

    def late(buf):
        low, high = slice(0, EDGE), slice(z + EDGE, full)
        from_low = (up, slice(x, 2 + x), slice(0, 2))
        from_high = (down, slice(2, 4), slice(2 + x, 4 + x))
        plan = []
        for _, part in others:
            plan.append((from_low, slice(0, full), part))
            plan += [(from_high, low, part), (from_high, high, part)]
        for side in (from_low, from_high):
            plan += [(side, low, mine), (side, high, mine)]
        return [
            (at_side(gx=side), buf.at[source, rows, part], buf.at[target, rows, part])
            for (side, source, target), rows, part in plan
        ]

    def forward(buf):
        planes = slice(2 + x, 4 + x)
        return [
            (at_side(gy=beside), buf.at[planes, own, mine], buf.at[planes, own, part])
            for beside, part in others
        ]

    others = [(up, slice(0, lanes))]
    if not wrap:
        others.append((down, slice(2 * lanes, 3 * lanes)))

    def remote(source, target, sems, number, device):
        return pltpu.make_async_remote_copy(
            src_ref=source,
            dst_ref=target,
            send_sem=sems[0].at[number],
            recv_sem=sems[1].at[number],
            device_id=device,
            device_id_type=MESH,
        )

    peers = []
    if inside:
        for dx in range(nx):
            for dy in range(ny):
                if dx or dy:
                    peers.append({"gx": lax.rem(ix + dx, nx), "gy": lax.rem(iy + dy, ny)})
    barrier = pltpu.get_barrier_semaphore()
    greeted = peers + [device for device, _, _, _ in early(eq)]
    for device in greeted:
        pl.semaphore_signal(barrier, inc=1, device_id=device, device_id_type=MESH)
    pl.semaphore_wait(barrier, len(greeted))

    if inside:
        copies = []
        for number, device in enumerate(peers):
            copy = remote(w_ref, wg.at[iy, ix], (wsend, wrecv), number, device)
            copy.start()
            copies.append(copy)
        wg[iy, ix] = w_ref[...]
        for copy in copies:
            copy.wait()
        ci = c // ny
        for which in range(2):
            for at in range(27):
                columns = []
                for j in range(ny):
                    pieces = [wg[j, i, which, :, at * ci : (at + 1) * ci] for i in range(nx)]
                    columns.append(jnp.concatenate(pieces, axis=0))
                wf[which, at // 3, at % 3] = jnp.concatenate(columns, axis=1)
        filters = wf
    else:
        filters = w_ref

    def exchange(buf, bank):
        sems = (send.at[bank], recv.at[bank])
        first, own_x = [], []
        number = 0
        for device, source, target, passed in early(buf):
            copy = remote(source, target, sems, number, device)
            number += 1
            copy.start()
            (first if passed else own_x).append(copy)
        for copy in first:
            copy.wait_recv()
        second = []
        for device, source, target in late(buf):
            copy = remote(source, target, sems, number, device)
            number += 1
            copy.start()
            second.append(copy)
        own_x[0].wait_recv()
        for device, source, target in forward(buf):
            copy = remote(source, target, sems, number, device)
            number += 1
            copy.start()
            second.append(copy)
        for copy in own_x[1:] + second:
            copy.wait_recv()
        for copy in first + own_x + second:
            copy.wait_send()

    def slot(at):
        return at % slots

    def unfold(tap, carry):
        blank = jnp.zeros((c, c), jnp.bfloat16)

        def rows(out, which, at, flip, cols, pick):
            line = [blank] * cols
            for col, b in pick:
                line[col] = filters[which, at, 2 - b if flip else b]
            return jnp.concatenate(line, axis=1)

        back = 8 - tap
        for yo in range(y + 2):
            a1[tap, yo * c : (yo + 1) * c, :] = rows(
                a1, 0, tap, False, slots, [(slot(yo + b), b) for b in range(3)]
            )
        for yo in range(y):
            a2[tap, yo * c : (yo + 1) * c, :] = rows(
                a2, 1, tap, False, y + 2, [(yo + b, b) for b in range(3)]
            )
        for s in range(slots):
            pick = [(yo, b) for yo in range(y + 2) for b in range(3) if slot(yo + b) == s]
            b2[tap, s * c : (s + 1) * c, :] = rows(b2, 1, back, True, y + 2, pick)
        for yi in range(y + 2):
            pick = [(yo, yi - yo) for yo in range(y) if 0 <= yi - yo <= 2]
            b1[tap, yi * c : (yi + 1) * c, :] = rows(b1, 0, back, True, y, pick)
        return carry

    lax.fori_loop(0, 9, unfold, 0)

    def load(ref2d, at):
        span = [ref2d[:, (at * y + j) * z : (at * y + j + 1) * z] for j in range(y)]
        return jnp.concatenate(span, axis=0).astype(jnp.float32).T

    for at in range(x):
        q_ref[at] = load(pos_ref, at)
        p_ref[at] = load(mom_ref, at)

    def conv(source, weights, out_x, transposed):
        width = source.shape[2]
        total = None
        for tz in range(3):
            part = None
            for tx in range(3):
                left = source[tx : tx + out_x].reshape(out_x * full, width)
                term = lax.dot_general(
                    left,
                    weights[tx * 3 + tz],
                    (((1,), (1 if transposed else 0,)), ((), ())),
                    preferred_element_type=jnp.float32,
                )
                part = term if part is None else part + term
            if tz != 1:
                part = pltpu.roll(part, 1 if tz == 0 else out_x * full - 1, 0)
            total = part if total is None else total + part
        return total.reshape(out_x, full, total.shape[-1])

    step = 0.25
    decay = jnp.exp(jnp.float32(-0.25))
    kick = jnp.sqrt(1.0 - decay * decay)

    def body(k, carry):
        eq[2 : 2 + x, own, mine] = q_ref[...].astype(jnp.bfloat16)
        exchange(eq, 0)
        t_ref[...] = jnp.tanh(conv(eq, a1, x + 2, True) + bias_ref[...][None])
        h2 = conv(t_ref[...].astype(jnp.bfloat16), a2, x, True)
        eh[2 : 2 + x, own, mine] = h2[:, own].astype(jnp.bfloat16)
        exchange(eh, 1)
        gu = conv(eh, b2, x + 2, False)
        t = t_ref[...]
        gh = (gu * (1.0 - t * t)).astype(jnp.bfloat16)
        force = conv(gh, b1, x, False)[:, own] + q_ref[...]
        half = 0.5 * step

        @pl.when(k > 0)
        def _():
            p_ref[...] = p_ref[...] - half * force

        @pl.when(k < steps)
        def _():
            p = p_ref[...] - half * force
            q = q_ref[...] + half * p
            now = noise_ref.at[k]
            drawn = jnp.stack([load(now, at) for at in range(x)])
            p = decay * p + kick * drawn
            q_ref[...] = q + half * p
            p_ref[...] = p

        return carry

    lax.fori_loop(0, steps + 1, body, 0)

    for ref, out in ((q_ref, q_out), (p_ref, p_out)):
        for at in range(x):
            flat = ref[at].T
            for j in range(y):
                out[:, (at * y + j) * z : (at * y + j + 1) * z] = flat[j * c : (j + 1) * c]


LANES = 128
ROWS = 8


def ring_place(r, nx):
    row, step = r // nx, r % nx
    return step + (row % 2) * (nx - 1 - 2 * step), row


def split_rows(height):
    low = -(-height // (2 * EDGE)) * EDGE
    return low, height - low


def ring_kernel(steps, sizes, heights, *refs):
    pool = {}
    for height in heights:
        parts = split_rows(height)
        for part in parts:
            pool[part] = max(pool.get(part, 0), parts.count(part))
    order = [(unit, part, i) for unit in range(2) for part in sorted(pool) for i in range(pool[part])]
    spaces = [pltpu.ACC(unit)((part, 2 * LANES), jnp.float32) for unit, part, _ in order]
    pl.run_scoped(functools.partial(ring_body, steps, sizes, order, refs), *spaces)


def ring_body(steps, sizes, order, refs, *sums):
    nx, ny, nz = sizes
    banks = dict(zip(order, sums))
    inputs, refs = refs[:6], refs[6:]
    (q_out, p_out, pos_ref, mom_ref, noise_ref, fin_ref, fout_ref, bias_ref, own_w, all_w, mats,
     flipped, turned_d, msg0, got0, msgd, gotd, stage, lhs, t_ref, base, extra, dq, dp, qb,
     halo, vb, ring_v, back_q, got_q, back_p, got_p, fixed, loose, edges_d, msge, gote, mid, send, recv,
     load) = refs
    ring = nx * ny
    x, zb = msg0.shape[1], msg0.shape[2]
    lane = LANES
    z = ring * zb
    taps, co, ci = fin_ref.shape
    c = ny * ci
    y = lane // c
    xx, yy = x * nx, y * ny
    per = lane // ci
    half_tiles = own_w.shape[2]
    wide = yy * c
    reach = 4
    rows = zb * xx

    ix, iy, iz = lax.axis_index("gx"), lax.axis_index("gy"), lax.axis_index("gz")
    ig = lax.axis_index("grp")
    me = iy * nx + ix + (iy % 2) * (nx - 1 - 2 * ix)
    block = nz * me + iz
    home = block // ring == iz
    filed = block % ring

    def device(r, core):
        gx, gy = ring_place(r, nx)
        return {"gx": gx, "gy": gy, "gz": core}

    barrier = pltpu.get_barrier_semaphore()
    everyone = 0
    for dx in range(nx):
        for dy in range(ny):
            for dz in range(nz):
                if dx or dy or dz:
                    everyone += 1
                    pl.semaphore_signal(
                        barrier,
                        inc=1,
                        device_id={"gx": (ix + dx) % nx, "gy": (iy + dy) % ny, "gz": (iz + dz) % nz},
                        device_id_type=MESH,
                    )

    across = [{"gy": 1 - iy}, {"grp": 1 - ig}, {"grp": 1 - ig, "gy": 1 - iy}]
    for where in across[1:]:
        everyone += 1
        pl.semaphore_signal(barrier, inc=1, device_id=where, device_id_type=MESH)

    loads = []
    held = (pos_ref, mom_ref, noise_ref, fin_ref, fout_ref, bias_ref)
    for number in (3, 4, 0, 1, 2, 5):
        copy = pltpu.make_async_copy(inputs[number], held[number], load.at[number])
        copy.start()
        loads.append(copy)

    def copy_of(source, target, number, where):
        return pltpu.make_async_remote_copy(
            src_ref=source,
            dst_ref=target,
            send_sem=send.at[number],
            recv_sem=recv.at[number],
            device_id=where,
            device_id_type=MESH,
        )

    other = {"gz": (iz + 1) % nz}

    def start(source, target, number, where):
        copy_of(source, target, number, where).start()

    def arrive(number, like):
        copy_of(like, like, number, other).wait_recv()

    def leave(number, like):
        copy_of(like, like, number, other).wait_send()

    def start_or_keep(source, target, number, where):
        @pl.when(home)
        def _():
            pltpu.make_async_copy(source, target, recv.at[number]).start()

        @pl.when(jnp.logical_not(home))
        def _():
            start(source, target, number, where)

    def to_owners(buf, target, number):
        for j in range(1, ring + 1):
            at = (filed + j) % ring
            owner = iz * ring + at
            go = start if j < ring else start_or_keep
            go(buf.at[at], target, number, device(owner // nz, owner % nz))

    turns = [0] + sorted(range(1, ring), key=lambda r: (-ring_place(r, nx)[0], r))

    def to_sources(buf, target, number):
        for r in turns:
            kept = jnp.logical_and(home, me == r)

            @pl.when(kept)
            def _():
                pltpu.make_async_copy(buf.at[r], target, recv.at[number]).start()

            @pl.when(jnp.logical_not(kept))
            def _():
                start(buf.at[r], target, number, device(r, block // ring))

    def left_ring(number, buf):
        @pl.when(home)
        def _():
            leave(number, buf.at[0 : ring - 1])

        @pl.when(jnp.logical_not(home))
        def _():
            leave(number, buf)

    column_sems = [[which * (nx - 1) + dx for dx in range(nx - 1)] for which in range(2)]
    across_sems = [[2 * (nx - 1) + 3 * which + i for i in range(3)] for which in range(2)]
    swap_sem = [2 * nx + 4, 2 * nx + 5]
    field_sem = 2 * nx + 6
    drift_sem = [field_sem + 1 + k for k in range(steps)]
    pairs = (steps - 1) // 2
    q_sem = field_sem + 1 + steps
    p_sem, drift_edge_sem = q_sem + 1, q_sem + 2
    halo_sem = [q_sem + 3 + k for k in range(pairs + 1)]
    v_sem = [q_sem + 4 + pairs + k for k in range(pairs)]

    outer = iz == nz - 1

    def pack(which, ref):
        for tile in range(2 * half_tiles):
            span = range(tile * per, min(taps, (tile + 1) * per))
            parts = [ref[t].astype(jnp.float32) for t in span]
            parts += [jnp.zeros((co, ci), jnp.float32)] * (per - len(parts))
            row = jnp.concatenate(parts, axis=1).astype(jnp.bfloat16)
            own_w[which, tile // half_tiles, tile % half_tiles] = row

    loads[0].wait()

    @pl.when(outer)
    def _():
        pack(0, fin_ref)

    def turn(ref, at):
        parts = [ref[pl.ds(at * y + j, c, stride=x * y), :] for j in range(y)]
        return jnp.concatenate(parts, axis=0).T

    pl.semaphore_wait(barrier, everyone)

    def to_column(which):
        for dx in range(1, nx):
            there = {"gx": (ix + dx) % nx}
            start(own_w.at[which, ig], all_w.at[which, me, ig], column_sems[which][dx - 1], there)
        for where, number in zip(across, across_sems[which]):
            start(own_w.at[which, ig], all_w.at[which, me, ig], number, where)

    def hand_over(which, gy, part):
        piece = all_w.at[which, pl.ds(gy * nx, nx), part]
        start(piece, piece, swap_sem[which], other)

    def pass_on(which):
        for dx in range(1, nx):
            arrive(column_sems[which][dx - 1], own_w.at[which, 0])
            gx = (ix + nx - dx) % nx
            piece = all_w.at[which, iy * nx + gx + (iy % 2) * (nx - 1 - 2 * gx), ig]
            for where, number in zip(across, across_sems[which]):
                start(piece, piece, number, where)
        hand_over(which, iy, ig)

    def take_across(which):
        for number, gy, part in zip(across_sems[which], (1 - iy, iy, 1 - iy), (ig, 1 - ig, 1 - ig)):
            arrive(number, all_w.at[which, 0:nx, 0])
            hand_over(which, gy, part)

    @pl.when(outer)
    def _():
        to_column(0)

    loads[1].wait()

    @pl.when(outer)
    def _():
        pack(1, fout_ref)
        to_column(1)
        for which in range(2):
            all_w[which, me, ig] = own_w[which, ig]

    upper = lax.broadcasted_iota(jnp.int32, (ROWS, lane), 0) < reach

    def around(ref, beyond, r, at):
        before = ref[at, r * zb - ROWS : r * zb] if r else beyond[0, at]
        after = ref[at, (r + 1) * zb : (r + 1) * zb + ROWS] if r < ring - 1 else beyond[1, at]
        return before, after

    loads[2].wait()
    for at in range(x):
        flat = turn(pos_ref, at).astype(jnp.bfloat16)
        for r in range(ring):
            msg0[r, at] = flat[r * zb : (r + 1) * zb]
    to_owners(msg0, got0.at[me], field_sem)
    for each in sums:
        pltpu.matmul_pop(each)

    half = 0.125
    decay = float(np.exp(np.float32(-0.25)))
    kick = float(np.sqrt(np.float32(1.0) - np.exp(np.float32(-0.25)) ** 2))
    push = half * (1.0 + decay)
    loads[3].wait()
    loads[4].wait()
    loads[5].wait()
    q = pos_ref[...]
    known = q.astype(jnp.bfloat16).astype(jnp.float32)
    p = mom_ref[...] - half * q
    total = x * y * c
    for k in range(steps):
        noise = noise_ref[k * total : (k + 1) * total].astype(jnp.float32)
        q = q + push * p + (half * kick) * noise
        drift = (q - known).astype(jnp.bfloat16).astype(jnp.float32)
        known = known + drift
        last = k == steps - 1
        p = decay * p + kick * noise - (half if last else 2 * half) * q
        loose[k] = drift
        for at in range(x):
            flat = turn(loose.at[k], at)
            if k == 0:
                turned_d[at] = flat
                for r in range(ring):
                    msge[r, at] = flat[r * zb : (r + 1) * zb].astype(jnp.bfloat16)
            else:
                flat = flat.astype(jnp.bfloat16)
                for r in range(ring):
                    msgd[k - 1, r, at] = flat[r * zb : (r + 1) * zb]
        if k == 0:
            start(turned_d.at[:, z - ROWS : z], edges_d.at[0], drift_edge_sem, {"gz": (iz + 1) % nz})
            start(turned_d.at[:, 0:ROWS], edges_d.at[1], drift_edge_sem, {"gz": (iz + nz - 1) % nz})
    fixed[0] = q
    fixed[1] = p

    def send_drift(k):
        if k == 0:
            to_owners(msge, gote.at[me], drift_sem[0])
        else:
            to_owners(msgd.at[k - 1], gotd.at[k - 1, me], drift_sem[k])

    @pl.when(outer)
    def _():
        pass_on(0)
        pass_on(1)

    arrive(drift_edge_sem, edges_d)
    for r in range(ring):
        beyond = []
        for at in range(x):
            before, after = around(turned_d, edges_d, r, at)
            beyond.append(jnp.where(upper, after, before))
        msge[r, x] = jnp.concatenate(beyond, axis=0).astype(jnp.bfloat16)

    def swapped(which):
        @pl.when(jnp.logical_not(outer))
        def _():
            arrive(swap_sem[which], all_w.at[which])

    at_lane = lax.broadcasted_iota(jnp.int32, (co, lane), 1)

    def build(which):
        def place(gx, carry):
            row = pl.multiple_of(gx * co, co)
            for a in range(3):
                for cz in range(3):
                    moved = {}
                    for b in range(3):
                        t = a * 9 + b * 3 + cz
                        tile, spot = t // per, t % per
                        held_at = tile // half_tiles, tile % half_tiles
                        for side in range(2):
                            pieces = []
                            for gy in range(ny):
                                r = gy * nx + gx + (gy % 2) * (nx - 1 - 2 * gx)
                                piece = all_w[which, r, held_at[0], held_at[1]]
                                shift = (side * ny + gy - spot) % per
                                pieces.append(pltpu.roll(piece, shift * ci, 1) if shift else piece)
                            moved[b, side] = pieces
                    pairs = []
                    for b in range(yy):
                        value = jnp.zeros((co, lane), jnp.bfloat16)
                        for side in range(y):
                            near = (b + side) % yy
                            if near > 2:
                                continue
                            for gy in range(ny):
                                spot = (side * ny + gy) * ci
                                inside = (at_lane >= spot) & (at_lane < spot + ci)
                                value = jnp.where(inside, moved[near, side][gy], value)
                        pairs.append(value)
                    for yo in range(yy):
                        for h in range(yy // y):
                            mats[which, a * 3 + cz, pl.ds(yo * c + row, co), h * lane : (h + 1) * lane] = (
                                pairs[(h * y + 1 - yo) % yy]
                            )
            return carry

        lax.fori_loop(0, nx, place, 0)

    def turn_over(which):
        for tap in range(9):
            flipped[which, tap] = mats[which, tap].T

    def scatter(target, zs, value, r, at):
        gx, gy = ring_place(r, nx)
        target[gy, pl.ds(zs * xx + gx * x + at, value.shape[0], stride=xx), :] = value

    def whole(ref, rows_from, rows_to):
        return jnp.concatenate([ref[gy, rows_from:rows_to] for gy in range(ny)], axis=1)

    left = device((me + ring - 1 + iz) % ring, 1 - iz)
    right = device((me + iz) % ring, 1 - iz)
    edge = reach * xx

    def send_halo(slot, value):
        qb[slot] = value.astype(jnp.bfloat16)
        start(qb.at[slot, rows - 2 * edge : rows], halo.at[slot, 0], halo_sem[slot], right)
        start(qb.at[slot, 0 : 2 * edge], halo.at[slot, 1], halo_sem[slot], left)

    def with_halo(slot, value):
        arrive(halo_sem[slot], halo.at[slot])
        ends = [halo[slot, side].astype(jnp.float32) for side in range(2)]
        return jnp.concatenate([ends[0], value, ends[1]], axis=0)

    arrive(field_sem, got0)
    for r in range(ring):
        for at in range(x):
            scatter(stage, 0, got0[r, at].astype(jnp.float32), r, at)
    send_halo(0, whole(stage, 0, rows))
    send_drift(0)

    @pl.when(outer)
    def _():
        take_across(0)

    swapped(0)
    for later in range(1, steps):
        send_drift(later)
    build(0)

    def spread(value):
        n = value.shape[0]
        cube = value.reshape(n // xx, xx, wide)
        for a in range(3):
            moved = cube if a == 1 else pltpu.roll(cube, (1 - a) % xx, 1)
            moved = moved.reshape(n, wide)
            lhs[a, 0, 0:n] = moved.astype(jnp.bfloat16)
            lhs[a, 1, 0 : n - 2 * xx] = moved[xx : n - xx].astype(jnp.bfloat16)

    def conv(height, which, adjoint, flip=False):
        low, high = split_rows(height)
        return jnp.concatenate(conv_at((0, low), low, high, which, adjoint, flip), axis=0)

    def conv_at(spots, low, high, which, adjoint, flip=False):
        source = mats if adjoint or flip else flipped
        sums = [[banks[unit, low, 0], banks[unit, high, int(low == high)]] for unit in range(2)]
        plans = (
            [(4, True, False), (3, True, True), (0, True, True), (1, True, True), (2, True, True)],
            [(4, False, True), (5, True, True), (8, True, True), (7, True, True), (6, True, True)],
        )
        for at in range(5):
            for unit in range(2):
                tap, use_low, use_high = plans[unit][at]
                a, cz = tap // 3, tap % 3
                pltpu.matmul_push_rhs(
                    source[which, 8 - tap if adjoint else tap],
                    staging_register=at % 2,
                    mxu_index=unit,
                    transpose=flip,
                )
                copy, first_row = (1, 0) if cz == 1 else (0, cz * xx)
                fresh = at % 2
                if use_low:
                    begin = first_row + spots[0]
                    left = lhs[a, copy, begin : begin + low]
                    pltpu.matmul_acc_lhs(sums[unit][0], left, load_staged_rhs=fresh)
                    fresh = None
                if use_high:
                    begin = first_row + spots[1]
                    left = lhs[a, copy, begin : begin + high]
                    pltpu.matmul_acc_lhs(sums[unit][1], left, load_staged_rhs=fresh)
        return [pltpu.matmul_pop(sums[0][part]) + pltpu.matmul_pop(sums[1][part]) for part in range(2)]

    row = jnp.concatenate([bias_ref[...]] * yy, axis=1)

    def gradient(extent, between=lambda: None, flip=False):
        n = [rows + 2 * (extent + 3 - i) * xx for i in range(4)]
        t = jnp.tanh(conv(n[0], 0, False, flip) + row)
        if flip:
            turn_over(0)
        t_ref[0 : n[0]] = t
        spread(t)
        between()
        out = conv(n[1], 1, False, flip)
        if flip:
            turn_over(1)
        spread(out)
        gu = conv(n[2], 1, True)
        t = t_ref[2 * xx : 2 * xx + n[2]]
        spread(gu * (1.0 - t * t))
        return conv(n[3], 0, True)

    def inner(q):
        n = [rows - 2 * (i + 1) * xx for i in range(4)]
        spread(q)
        t = jnp.tanh(conv(n[0], 0, False) + row)
        mid[0, 0 : n[0]] = t
        spread(t)
        out = conv(n[1], 1, False)
        mid[1, 0 : n[1]] = out
        spread(out)
        gu = conv(n[2], 1, True)
        t = t[2 * xx : 2 * xx + n[2]]
        out = gu * (1.0 - t * t)
        mid[2, 0 : n[2]] = out
        spread(out)
        mid[3, 0 : n[3]] = conv(n[3], 0, True)

    def outside(slot, q):
        n = [rows - 2 * (i + 1) * xx for i in range(4)]
        side = 2 * edge
        two = 2 * xx

        def both(which, adjoint):
            return conv_at((0, side + two), side, side, which, adjoint)

        arrive(halo_sem[slot], halo.at[slot])
        ends = [halo[slot, at].astype(jnp.float32) for at in range(2)]
        spread(jnp.concatenate([ends[0], q[0:two], q[rows - two :], ends[1]], axis=0))
        ends = [jnp.tanh(each + row) for each in both(0, False)]
        t = [
            jnp.concatenate([ends[0], mid[0, 0:two]], axis=0),
            jnp.concatenate([mid[0, n[0] - two : n[0]], ends[1]], axis=0),
        ]
        spread(jnp.concatenate(t, axis=0))
        ends = both(1, False)
        spread(jnp.concatenate([ends[0], mid[1, 0:two], mid[1, n[1] - two : n[1]], ends[1]], axis=0))
        gu = both(1, True)
        near = t[0][two:], t[1][0:side]
        ends = [each * (1.0 - at * at) for each, at in zip(gu, near)]
        spread(jnp.concatenate([ends[0], mid[2, 0:two], mid[2, n[2] - two : n[2]], ends[1]], axis=0))
        ends = both(0, True)
        return jnp.concatenate([ends[0], mid[3, 0 : n[3]], ends[1]], axis=0)

    def take_drift(k):
        arrive(drift_sem[k], gotd.at[k - 1])
        for r in range(ring):
            for at in range(x):
                scatter(extra, 0, gotd[k - 1, r, at].astype(jnp.float32), r, at)
        base[...] = base[...] + whole(extra, 0, rows)

    def second_filters():
        swapped(1)
        build(1)

    def collect(ref, r, at):
        gx, gy = ring_place(r, nx)
        return ref[gy, pl.ds(gx * x + at, zb, stride=xx), :]

    def put(ref, value):
        for gy in range(ny):
            ref[gy] = value[:, gy * lane : (gy + 1) * lane]

    @pl.when(outer)
    def _():
        take_across(1)

    base[...] = whole(stage, 0, rows)
    spread(with_halo(0, base[...]))
    g = gradient(reach, second_filters, True)

    arrive(drift_sem[0], gote)
    for r in range(ring):
        beyond = gote[r, x].astype(jnp.float32)
        for at in range(x):
            scatter(extra, 0, gote[r, at].astype(jnp.float32), r, at)
            scatter(extra, zb, beyond[at * ROWS : (at + 1) * ROWS], r, at)
    now = base[...] + whole(extra, 0, rows)
    base[...] = now
    below = halo[0, 0, edge : 2 * edge].astype(jnp.float32) + whole(extra, rows + edge, rows + 2 * edge)
    above = halo[0, 1, 0:edge].astype(jnp.float32) + whole(extra, rows, rows + edge)
    force = g[edge : edge + rows]
    put(dp, -half * force)
    put(dq, (-half * push) * force)
    spread(jnp.concatenate([below, now, above], axis=0) + (-half * push) * g)

    mine = pl.ds(pl.multiple_of(filed * zb, zb), zb)

    def kicked(g):
        shift = whole(dq, 0, rows)
        now = decay * whole(dp, 0, rows) - (2 * half) * (g + shift)
        put(dp, now)
        put(dq, shift + push * now)

    for pair in range(pairs):
        kicked(gradient(0))
        k = 2 * pair + 2
        take_drift(k - 1)
        q = base[...] + whole(dq, 0, rows)
        send_halo(pair + 1, q)
        take_drift(k)
        shift = whole(dq, 0, rows)
        v = base[...] + shift + push * (decay * whole(dp, 0, rows) - (2 * half) * shift)
        vb[pair] = v.astype(jnp.bfloat16)
        start(vb.at[pair, rows - edge : rows], ring_v.at[pair, 0], v_sem[pair], right)
        start(vb.at[pair, 0:edge], ring_v.at[pair, 1], v_sem[pair], left)
        inner(q)
        g = outside(pair + 1, q)
        kicked(g[edge : edge + rows])
        q = base[...] + whole(dq, 0, rows)
        arrive(v_sem[pair], ring_v.at[pair])
        ends = [
            ring_v[pair, side].astype(jnp.float32) - (2 * half * push) * g[at : at + edge]
            for side, at in enumerate((0, edge + rows))
        ]
        spread(jnp.concatenate([ends[0], q, ends[1]], axis=0))

    put(dp, decay * whole(dp, 0, rows) - half * whole(dq, 0, rows))

    def return_q():
        for r in range(ring):
            for at in range(x):
                back_q[r, at] = collect(dq, r, at).astype(jnp.bfloat16)
        to_sources(back_q, got_q.at[:, mine], q_sem)

    return_q()
    g = gradient(0)
    put(dp, whole(dp, 0, rows) - half * g)
    for r in range(ring):
        for at in range(x):
            back_p[r, at] = collect(dp, r, at).astype(jnp.bfloat16)
    to_sources(back_p, got_p.at[:, mine], p_sem)

    def untie(value, which, out, at):
        flat = value.T
        for j in range(y):
            part = pl.ds(at * y + j, c, stride=x * y)
            out[part, :] = fixed[which, part, :] + flat[j * c : (j + 1) * c]

    arrive(q_sem, got_q)
    for at in range(x):
        untie(got_q[at].astype(jnp.float32), 0, q_out, at)
    arrive(p_sem, got_p)
    for at in range(x):
        untie(got_p[at].astype(jnp.float32), 1, p_out, at)

    @pl.when(outer)
    def _():
        for which in range(2):
            for number in column_sems[which]:
                leave(number, own_w.at[which, 0])
            for number in across_sems[which]:
                leave(number, all_w.at[which, 0:nx, 0])
            leave(swap_sem[which], all_w.at[which])

    leave(drift_edge_sem, edges_d)
    left_ring(field_sem, msg0)
    left_ring(drift_sem[0], msge)
    for k in range(1, steps):
        left_ring(drift_sem[k], msgd.at[k - 1])
    for slot in range(pairs + 1):
        leave(halo_sem[slot], halo.at[slot])
    for pair in range(pairs):
        leave(v_sem[pair], ring_v.at[pair])
    left_ring(q_sem, back_q)
    left_ring(p_sem, back_p)


def copy_out(q_ref, p_ref, q_out, p_out, sems):
    copies = [
        pltpu.make_async_copy(q_ref, q_out, sems.at[0]),
        pltpu.make_async_copy(p_ref, p_out, sems.at[1]),
    ]
    for copy in copies:
        copy.start()
    for copy in copies:
        copy.wait()


def fits_ring(steps, sizes, position, filter_in):
    nx, ny, nz = sizes
    c, x, y, z = position.shape
    co, ci = filter_in.shape[:2]
    ring = nx * ny
    return (
        steps % 2 == 1 and steps > 2 and nz == 2 and ny == 2 and nx > 1 and y * c == LANES and x * nx == ROWS and y * ny > 2
        and z % (ring * EDGE) == 0 and z // ring == EDGE and co % EDGE == 0 and LANES % ci == 0
        and y * ny * ci == LANES
    )


def on_ring(sizes, position, momentum, noise, filter_in, filter_out, bias):
    nx, ny, nz = sizes
    c, x, y, z = position.shape
    steps = noise.shape[0]
    co, ci = filter_in.shape[:2]
    ring = nx * ny
    zb = z // ring
    xx, yy = x * nx, y * ny
    wide = yy * c
    rows = zb * xx
    lane = LANES
    half_tiles = -(-27 * ci // (2 * lane))
    flat = jax.ShapeDtypeStruct((c * x * y, z), jnp.float32)
    reach, pairs = 4, (steps - 1) // 2
    copies = 2 * nx + 11 + steps + 2 * pairs
    edge = reach * xx
    heights = [(zb + 2 * beyond) * xx for beyond in range(-reach, 2 * reach)]
    vmem = pl.BlockSpec(memory_space=pltpu.VMEM)
    bf16, f32 = jnp.bfloat16, jnp.float32
    q, p = pl.pallas_call(
        functools.partial(ring_kernel, steps, sizes, heights),
        out_shape=(flat, flat),
        in_specs=[pl.BlockSpec(memory_space=pl.ANY)] * 6,
        out_specs=(vmem, vmem),
        scratch_shapes=[
            pltpu.VMEM((c * x * y, z), f32),
            pltpu.VMEM((c * x * y, z), f32),
            pltpu.VMEM((steps * c * x * y, z), bf16),
            pltpu.VMEM((27, co, ci), bf16),
            pltpu.VMEM((27, co, ci), bf16),
            pltpu.VMEM((1, c), f32),
            pltpu.VMEM((2, 2, half_tiles, co, lane), bf16),
            pltpu.VMEM((2, ring, 2, half_tiles, co, lane), bf16),
            pltpu.VMEM((2, 9, wide, wide), bf16),
            pltpu.VMEM((2, 9, wide, wide), bf16),
            pltpu.VMEM((x, z, lane), f32),
            pltpu.VMEM((ring, x, zb, lane), bf16),
            pltpu.VMEM((ring, x, zb, lane), bf16),
            pltpu.VMEM((steps - 1, ring, x, zb, lane), bf16),
            pltpu.VMEM((steps - 1, ring, x, zb, lane), bf16),
            pltpu.VMEM((ny, rows, lane), f32),
            pltpu.VMEM((3, 2, rows + 4 * edge, wide), bf16),
            pltpu.VMEM((rows + 4 * edge - 2 * xx, wide), f32),
            pltpu.VMEM((rows, wide), f32),
            pltpu.VMEM((ny, rows + 2 * edge, lane), f32),
            pltpu.VMEM((ny, rows, lane), f32),
            pltpu.VMEM((ny, rows, lane), f32),
            pltpu.VMEM((pairs + 1, rows, wide), bf16),
            pltpu.VMEM((pairs + 1, 2, 2 * edge, wide), bf16),
            pltpu.VMEM((pairs, rows, wide), bf16),
            pltpu.VMEM((pairs, 2, edge, wide), bf16),
            pltpu.VMEM((ring, x, zb, lane), bf16),
            pltpu.VMEM((x, z, lane), bf16),
            pltpu.VMEM((ring, x, zb, lane), bf16),
            pltpu.VMEM((x, z, lane), bf16),
            pltpu.VMEM((2, c * x * y, z), f32),
            pltpu.VMEM((steps, c * x * y, z), f32),
            pltpu.VMEM((2, x, ROWS, lane), f32),
            pltpu.VMEM((ring, x + 1, zb, lane), bf16),
            pltpu.VMEM((ring, x + 1, zb, lane), bf16),
            pltpu.VMEM((4, rows - 2 * xx, wide), f32),
            pltpu.SemaphoreType.DMA((copies,)),
            pltpu.SemaphoreType.DMA((copies,)),
            pltpu.SemaphoreType.DMA((6,)),
        ],
        compiler_params=pltpu.CompilerParams(
            collective_id=0, has_side_effects=True, vmem_limit_bytes=24 * 2**20
        ),
    )(
        *(
            pltpu.with_memory_space_constraint(each, pltpu.HBM)
            for each in (
                position.reshape(-1, z),
                momentum.reshape(-1, z),
                noise.reshape(-1, z),
                filter_in.transpose(2, 3, 4, 0, 1).reshape(27, co, ci),
                filter_out.transpose(2, 3, 4, 0, 1).reshape(27, co, ci),
                bias[None],
            )
        )
    )
    q, p = pl.pallas_call(
        copy_out,
        out_shape=(flat, flat),
        in_specs=[pl.BlockSpec(memory_space=pl.ANY)] * 2,
        out_specs=[pl.BlockSpec(memory_space=pl.ANY)] * 2,
        scratch_shapes=[pltpu.SemaphoreType.DMA((2,))],
        compiler_params=pltpu.CompilerParams(vmem_limit_bytes=2**20),
    )(q, p)
    return q.reshape(position.shape), p.reshape(momentum.shape)


def on_device(groups, sizes, position, momentum, noise, filter_in, filter_out, bias):
    if groups == 2 and fits_ring(noise.shape[0], sizes, position, filter_in):
        return on_ring(sizes, position, momentum, noise, filter_in, filter_out, bias)
    nx, ny, nz = sizes
    c, x, y, z = position.shape
    steps = noise.shape[0]
    assert x >= 2 and y == 2 and z % EDGE == 0 and nx > 2 and ny > 1
    both = jnp.stack([filter_in, filter_out])
    co, ci = both.shape[1], both.shape[2]
    gather = []
    if co % EDGE == 0:
        both = both.transpose(0, 1, 3, 5, 4, 2).reshape(2, co, 27 * ci)
        gather = [
            pltpu.VMEM((ny, nx, 2, co, 27 * ci), jnp.bfloat16),
            pltpu.VMEM((2, 9, 3, c, c), jnp.bfloat16),
            pltpu.SemaphoreType.DMA((nx * ny - 1,)),
            pltpu.SemaphoreType.DMA((nx * ny - 1,)),
        ]
    else:
        both = both.reshape(2 * co, ci * 27)
        both = lax.all_gather(both, ("gx", "gy"), axis=0, tiled=True)
        both = both.reshape(nx, ny, 2, co, ci, 3, 3, 3)
        both = both.transpose(2, 5, 7, 6, 0, 3, 1, 4).reshape(2, 9, 3, c, c)
    lanes = y * c
    slots = 2 * y if ny == 2 else 3 * y
    full = z + 2 * EDGE
    wide = (y + 2) * c
    flat = jax.ShapeDtypeStruct((c, x * y * z), jnp.float32)
    copies = 15 if ny == 2 else 24
    vmem = pl.BlockSpec(memory_space=pltpu.VMEM)
    q, p = pl.pallas_call(
        functools.partial(kernel, steps, sizes),
        out_shape=(flat, flat),
        in_specs=[vmem] * 5,
        out_specs=(vmem, vmem),
        scratch_shapes=[
            pltpu.VMEM((9, wide, slots * c), jnp.bfloat16),
            pltpu.VMEM((9, lanes, wide), jnp.bfloat16),
            pltpu.VMEM((9, wide, lanes), jnp.bfloat16),
            pltpu.VMEM((9, slots * c, wide), jnp.bfloat16),
            pltpu.VMEM((x + 4, full, slots * c), jnp.bfloat16),
            pltpu.VMEM((x + 4, full, slots * c), jnp.bfloat16),
            pltpu.VMEM((x + 2, full, wide), jnp.float32),
            pltpu.VMEM((x, z, lanes), jnp.float32),
            pltpu.VMEM((x, z, lanes), jnp.float32),
            pltpu.SemaphoreType.DMA((2, copies)),
            pltpu.SemaphoreType.DMA((2, copies)),
            *gather,
        ],
        compiler_params=pltpu.CompilerParams(
            collective_id=0, has_side_effects=True, vmem_limit_bytes=56 * 2**20
        ),
    )(
        position.reshape(c, -1),
        momentum.reshape(c, -1),
        noise.reshape(steps, c, -1),
        both,
        jnp.tile(bias, y + 2)[None],
    )
    return q.reshape(position.shape), p.reshape(momentum.shape)


def solution(mesh):
    field = P(None, ("grp", "gx"), "gy", "gz")
    filters = P("gx", "gy", None, None, None)
    sizes = tuple(mesh.shape[name] for name in ("gx", "gy", "gz"))
    groups = mesh.shape["grp"]
    return jax.shard_map(
        functools.partial(on_device, groups, sizes),
        mesh=mesh,
        in_specs=(field, field, P(None, None, ("grp", "gx"), "gy", "gz"), filters, filters, P()),
        out_specs=(field, field),
        check_vma=False,
    )
```

```python
import functools

import jax
import jax.numpy as jnp
import numpy as np
from jax import lax
from jax.experimental import pallas as pl
from jax.experimental.pallas import tpu as pltpu
from jax.sharding import PartitionSpec as P

EDGE = 16
MESH = pl.DeviceIdType.MESH


def kernel(steps, sizes, pos_ref, mom_ref, noise_ref, w_ref, bias_ref,
           q_out, p_out, a1, a2, b1, b2, eq, eh, t_ref, q_ref, p_ref, send, recv, *gather):
    nx, ny, nz = sizes
    c = pos_ref.shape[0]
    inside = len(gather) > 0
    if inside:
        wg, wf, wsend, wrecv = gather
    x, z, lanes = q_ref.shape
    y = lanes // c
    full = eq.shape[1]
    wrap = ny == 2
    slots = eq.shape[2] // c
    own = slice(EDGE, EDGE + z)
    mine = slice(lanes, 2 * lanes)

    ix, iy, iz = lax.axis_index("gx"), lax.axis_index("gy"), lax.axis_index("gz")
    up = {"gx": lax.rem(ix + 1, nx), "gy": lax.rem(iy + 1, ny), "gz": lax.rem(iz + 1, nz)}
    down = {
        "gx": lax.rem(ix + nx - 1, nx),
        "gy": lax.rem(iy + ny - 1, ny),
        "gz": lax.rem(iz + nz - 1, nz),
    }

    def at_side(**which):
        return {axis: which[axis][axis] for axis in which}

    def early(buf):
        core = slice(2, 2 + x)
        low, high = slice(0, EDGE), slice(z + EDGE, full)
        block = buf.at[core, own, mine]
        edges = (
            (up, buf.at[core, z : z + EDGE, mine], low),
            (down, buf.at[core, EDGE : 2 * EDGE, mine], high),
        )
        out = []
        for side, source, rows in edges:
            out.append((at_side(gz=side), source, buf.at[core, rows, mine], True))
        for beside, part in others:
            out.append((at_side(gy=beside), block, buf.at[core, own, part], True))
            for side, source, rows in edges:
                target = buf.at[core, rows, part]
                out.append((at_side(gy=beside, gz=side), source, target, True))
        out.append(
            (at_side(gx=down), buf.at[2:4, own, mine], buf.at[2 + x : 4 + x, own, mine], False)
        )
        out.append((at_side(gx=up), buf.at[x : 2 + x, own, mine], buf.at[0:2, own, mine], False))
        return out

    def late(buf):
        low, high = slice(0, EDGE), slice(z + EDGE, full)
        from_low = (up, slice(x, 2 + x), slice(0, 2))
        from_high = (down, slice(2, 4), slice(2 + x, 4 + x))
        plan = []
        for _, part in others:
            plan.append((from_low, slice(0, full), part))
            plan += [(from_high, low, part), (from_high, high, part)]
        for side in (from_low, from_high):
            plan += [(side, low, mine), (side, high, mine)]
        return [
            (at_side(gx=side), buf.at[source, rows, part], buf.at[target, rows, part])
            for (side, source, target), rows, part in plan
        ]

    def forward(buf):
        planes = slice(2 + x, 4 + x)
        return [
            (at_side(gy=beside), buf.at[planes, own, mine], buf.at[planes, own, part])
            for beside, part in others
        ]

    others = [(up, slice(0, lanes))]
    if not wrap:
        others.append((down, slice(2 * lanes, 3 * lanes)))

    def remote(source, target, sems, number, device):
        return pltpu.make_async_remote_copy(
            src_ref=source,
            dst_ref=target,
            send_sem=sems[0].at[number],
            recv_sem=sems[1].at[number],
            device_id=device,
            device_id_type=MESH,
        )

    peers = []
    if inside:
        for dx in range(nx):
            for dy in range(ny):
                if dx or dy:
                    peers.append({"gx": lax.rem(ix + dx, nx), "gy": lax.rem(iy + dy, ny)})
    barrier = pltpu.get_barrier_semaphore()
    greeted = peers + [device for device, _, _, _ in early(eq)]
    for device in greeted:
        pl.semaphore_signal(barrier, inc=1, device_id=device, device_id_type=MESH)
    pl.semaphore_wait(barrier, len(greeted))

    if inside:
        copies = []
        for number, device in enumerate(peers):
            copy = remote(w_ref, wg.at[iy, ix], (wsend, wrecv), number, device)
            copy.start()
            copies.append(copy)
        wg[iy, ix] = w_ref[...]
        for copy in copies:
            copy.wait()
        ci = c // ny
        for which in range(2):
            for at in range(27):
                columns = []
                for j in range(ny):
                    pieces = [wg[j, i, which, :, at * ci : (at + 1) * ci] for i in range(nx)]
                    columns.append(jnp.concatenate(pieces, axis=0))
                wf[which, at // 3, at % 3] = jnp.concatenate(columns, axis=1)
        filters = wf
    else:
        filters = w_ref

    def exchange(buf, bank):
        sems = (send.at[bank], recv.at[bank])
        first, own_x = [], []
        number = 0
        for device, source, target, passed in early(buf):
            copy = remote(source, target, sems, number, device)
            number += 1
            copy.start()
            (first if passed else own_x).append(copy)
        for copy in first:
            copy.wait_recv()
        second = []
        for device, source, target in late(buf):
            copy = remote(source, target, sems, number, device)
            number += 1
            copy.start()
            second.append(copy)
        own_x[0].wait_recv()
        for device, source, target in forward(buf):
            copy = remote(source, target, sems, number, device)
            number += 1
            copy.start()
            second.append(copy)
        for copy in own_x[1:] + second:
            copy.wait_recv()
        for copy in first + own_x + second:
            copy.wait_send()

    def slot(at):
        return at % slots

    def unfold(tap, carry):
        blank = jnp.zeros((c, c), jnp.bfloat16)

        def rows(out, which, at, flip, cols, pick):
            line = [blank] * cols
            for col, b in pick:
                line[col] = filters[which, at, 2 - b if flip else b]
            return jnp.concatenate(line, axis=1)

        back = 8 - tap
        for yo in range(y + 2):
            a1[tap, yo * c : (yo + 1) * c, :] = rows(
                a1, 0, tap, False, slots, [(slot(yo + b), b) for b in range(3)]
            )
        for yo in range(y):
            a2[tap, yo * c : (yo + 1) * c, :] = rows(
                a2, 1, tap, False, y + 2, [(yo + b, b) for b in range(3)]
            )
        for s in range(slots):
            pick = [(yo, b) for yo in range(y + 2) for b in range(3) if slot(yo + b) == s]
            b2[tap, s * c : (s + 1) * c, :] = rows(b2, 1, back, True, y + 2, pick)
        for yi in range(y + 2):
            pick = [(yo, yi - yo) for yo in range(y) if 0 <= yi - yo <= 2]
            b1[tap, yi * c : (yi + 1) * c, :] = rows(b1, 0, back, True, y, pick)
        return carry

    lax.fori_loop(0, 9, unfold, 0)

    def load(ref2d, at):
        span = [ref2d[:, (at * y + j) * z : (at * y + j + 1) * z] for j in range(y)]
        return jnp.concatenate(span, axis=0).astype(jnp.float32).T

    for at in range(x):
        q_ref[at] = load(pos_ref, at)
        p_ref[at] = load(mom_ref, at)

    def conv(source, weights, out_x, transposed):
        width = source.shape[2]
        total = None
        for tz in range(3):
            part = None
            for tx in range(3):
                left = source[tx : tx + out_x].reshape(out_x * full, width)
                term = lax.dot_general(
                    left,
                    weights[tx * 3 + tz],
                    (((1,), (1 if transposed else 0,)), ((), ())),
                    preferred_element_type=jnp.float32,
                )
                part = term if part is None else part + term
            if tz != 1:
                part = pltpu.roll(part, 1 if tz == 0 else out_x * full - 1, 0)
            total = part if total is None else total + part
        return total.reshape(out_x, full, total.shape[-1])

    step = 0.25
    decay = jnp.exp(jnp.float32(-0.25))
    kick = jnp.sqrt(1.0 - decay * decay)

    def body(k, carry):
        eq[2 : 2 + x, own, mine] = q_ref[...].astype(jnp.bfloat16)
        exchange(eq, 0)
        t_ref[...] = jnp.tanh(conv(eq, a1, x + 2, True) + bias_ref[...][None])
        h2 = conv(t_ref[...].astype(jnp.bfloat16), a2, x, True)
        eh[2 : 2 + x, own, mine] = h2[:, own].astype(jnp.bfloat16)
        exchange(eh, 1)
        gu = conv(eh, b2, x + 2, False)
        t = t_ref[...]
        gh = (gu * (1.0 - t * t)).astype(jnp.bfloat16)
        force = conv(gh, b1, x, False)[:, own] + q_ref[...]
        half = 0.5 * step

        @pl.when(k > 0)
        def _():
            p_ref[...] = p_ref[...] - half * force

        @pl.when(k < steps)
        def _():
            p = p_ref[...] - half * force
            q = q_ref[...] + half * p
            now = noise_ref.at[k]
            drawn = jnp.stack([load(now, at) for at in range(x)])
            p = decay * p + kick * drawn
            q_ref[...] = q + half * p
            p_ref[...] = p

        return carry

    lax.fori_loop(0, steps + 1, body, 0)

    for ref, out in ((q_ref, q_out), (p_ref, p_out)):
        for at in range(x):
            flat = ref[at].T
            for j in range(y):
                out[:, (at * y + j) * z : (at * y + j + 1) * z] = flat[j * c : (j + 1) * c]


LANES = 128
ROWS = 8


def ring_place(r, nx):
    row, step = r // nx, r % nx
    return step + (row % 2) * (nx - 1 - 2 * step), row


def split_rows(height):
    low = -(-height // (2 * EDGE)) * EDGE
    return low, height - low


def ring_kernel(steps, sizes, heights, *refs):
    pool = {}
    for height in heights:
        parts = split_rows(height)
        for part in parts:
            pool[part] = max(pool.get(part, 0), parts.count(part))
    order = [(unit, part, i) for unit in range(2) for part in sorted(pool) for i in range(pool[part])]
    spaces = [pltpu.ACC(unit)((part, 2 * LANES), jnp.float32) for unit, part, _ in order]
    pl.run_scoped(functools.partial(ring_body, steps, sizes, order, refs), *spaces)


def ring_body(steps, sizes, order, refs, *sums):
    nx, ny, nz = sizes
    banks = dict(zip(order, sums))
    inputs, refs = refs[:6], refs[6:]
    (q_out, p_out, pos_ref, mom_ref, noise_ref, fin_ref, fout_ref, bias_ref, own_w, all_w, mats,
     flipped, turned_d, msg0, got0, msgd, gotd, stage, lhs, t_ref, base, extra, dq, dp, qb,
     halo, vb, ring_v, back_q, got_q, back_p, got_p, fixed, loose, edges_d, msge, gote, mid, send, recv,
     load) = refs
    ring = nx * ny
    x, zb = msg0.shape[1], msg0.shape[2]
    lane = LANES
    z = ring * zb
    taps, co, ci = fin_ref.shape
    c = ny * ci
    y = lane // c
    xx, yy = x * nx, y * ny
    per = lane // ci
    half_tiles = own_w.shape[2]
    wide = yy * c
    reach = 4
    rows = zb * xx

    ix, iy, iz = lax.axis_index("gx"), lax.axis_index("gy"), lax.axis_index("gz")
    ig = lax.axis_index("grp")
    me = iy * nx + ix + (iy % 2) * (nx - 1 - 2 * ix)
    block = nz * me + iz
    home = block // ring == iz
    filed = block % ring

    def device(r, core):
        gx, gy = ring_place(r, nx)
        return {"gx": gx, "gy": gy, "gz": core}

    barrier = pltpu.get_barrier_semaphore()
    everyone = 0
    for dx in range(nx):
        for dy in range(ny):
            for dz in range(nz):
                if dx or dy or dz:
                    everyone += 1
                    pl.semaphore_signal(
                        barrier,
                        inc=1,
                        device_id={"gx": (ix + dx) % nx, "gy": (iy + dy) % ny, "gz": (iz + dz) % nz},
                        device_id_type=MESH,
                    )

    across = [{"gy": 1 - iy}, {"grp": 1 - ig}, {"grp": 1 - ig, "gy": 1 - iy}]
    for where in across[1:]:
        everyone += 1
        pl.semaphore_signal(barrier, inc=1, device_id=where, device_id_type=MESH)

    loads = []
    held = (pos_ref, mom_ref, noise_ref, fin_ref, fout_ref, bias_ref)
    for number in (3, 4, 0, 1, 2, 5):
        copy = pltpu.make_async_copy(inputs[number], held[number], load.at[number])
        copy.start()
        loads.append(copy)

    def copy_of(source, target, number, where):
        return pltpu.make_async_remote_copy(
            src_ref=source,
            dst_ref=target,
            send_sem=send.at[number],
            recv_sem=recv.at[number],
            device_id=where,
            device_id_type=MESH,
        )

    other = {"gz": (iz + 1) % nz}

    def start(source, target, number, where):
        copy_of(source, target, number, where).start()

    def arrive(number, like):
        copy_of(like, like, number, other).wait_recv()

    def leave(number, like):
        copy_of(like, like, number, other).wait_send()

    def start_or_keep(source, target, number, where):
        @pl.when(home)
        def _():
            pltpu.make_async_copy(source, target, recv.at[number]).start()

        @pl.when(jnp.logical_not(home))
        def _():
            start(source, target, number, where)

    def to_owners(buf, target, number):
        for j in range(1, ring + 1):
            at = (filed + j) % ring
            owner = iz * ring + at
            go = start if j < ring else start_or_keep
            go(buf.at[at], target, number, device(owner // nz, owner % nz))

    turns = [0] + sorted(range(1, ring), key=lambda r: (-ring_place(r, nx)[0], r))

    def to_sources(buf, target, number):
        for r in turns:
            kept = jnp.logical_and(home, me == r)

            @pl.when(kept)
            def _():
                pltpu.make_async_copy(buf.at[r], target, recv.at[number]).start()

            @pl.when(jnp.logical_not(kept))
            def _():
                start(buf.at[r], target, number, device(r, block // ring))

    def left_ring(number, buf):
        @pl.when(home)
        def _():
            leave(number, buf.at[0 : ring - 1])

        @pl.when(jnp.logical_not(home))
        def _():
            leave(number, buf)

    column_sems = [[which * (nx - 1) + dx for dx in range(nx - 1)] for which in range(2)]
    across_sems = [[2 * (nx - 1) + 3 * which + i for i in range(3)] for which in range(2)]
    swap_sem = [2 * nx + 4, 2 * nx + 5]
    field_sem = 2 * nx + 6
    drift_sem = [field_sem + 1 + k for k in range(steps)]
    pairs = (steps - 1) // 2
    q_sem = field_sem + 1 + steps
    p_sem, drift_edge_sem = q_sem + 1, q_sem + 2
    halo_sem = [q_sem + 3 + k for k in range(pairs + 1)]
    v_sem = [q_sem + 4 + pairs + k for k in range(pairs)]

    outer = iz == nz - 1

    def pack(which, ref):
        for tile in range(2 * half_tiles):
            span = range(tile * per, min(taps, (tile + 1) * per))
            parts = [ref[t].astype(jnp.float32) for t in span]
            parts += [jnp.zeros((co, ci), jnp.float32)] * (per - len(parts))
            row = jnp.concatenate(parts, axis=1).astype(jnp.bfloat16)
            own_w[which, tile // half_tiles, tile % half_tiles] = row

    loads[0].wait()

    @pl.when(outer)
    def _():
        pack(0, fin_ref)

    def turn(ref, at):
        parts = [ref[pl.ds(at * y + j, c, stride=x * y), :] for j in range(y)]
        return jnp.concatenate(parts, axis=0).T

    pl.semaphore_wait(barrier, everyone)

    def to_column(which):
        for dx in range(1, nx):
            there = {"gx": (ix + dx) % nx}
            start(own_w.at[which, ig], all_w.at[which, me, ig], column_sems[which][dx - 1], there)
        for where, number in zip(across, across_sems[which]):
            start(own_w.at[which, ig], all_w.at[which, me, ig], number, where)

    def hand_over(which, gy, part):
        piece = all_w.at[which, pl.ds(gy * nx, nx), part]
        start(piece, piece, swap_sem[which], other)

    def pass_on(which):
        for dx in range(1, nx):
            arrive(column_sems[which][dx - 1], own_w.at[which, 0])
            gx = (ix + nx - dx) % nx
            piece = all_w.at[which, iy * nx + gx + (iy % 2) * (nx - 1 - 2 * gx), ig]
            for where, number in zip(across, across_sems[which]):
                start(piece, piece, number, where)
        hand_over(which, iy, ig)

    def take_across(which):
        for number, gy, part in zip(across_sems[which], (1 - iy, iy, 1 - iy), (ig, 1 - ig, 1 - ig)):
            arrive(number, all_w.at[which, 0:nx, 0])
            hand_over(which, gy, part)

    @pl.when(outer)
    def _():
        to_column(0)

    loads[1].wait()

    @pl.when(outer)
    def _():
        pack(1, fout_ref)
        to_column(1)
        for which in range(2):
            all_w[which, me, ig] = own_w[which, ig]

    upper = lax.broadcasted_iota(jnp.int32, (ROWS, lane), 0) < reach

    def around(ref, beyond, r, at):
        before = ref[at, r * zb - ROWS : r * zb] if r else beyond[0, at]
        after = ref[at, (r + 1) * zb : (r + 1) * zb + ROWS] if r < ring - 1 else beyond[1, at]
        return before, after

    loads[2].wait()
    for at in range(x):
        flat = turn(pos_ref, at).astype(jnp.bfloat16)
        for r in range(ring):
            msg0[r, at] = flat[r * zb : (r + 1) * zb]
    to_owners(msg0, got0.at[me], field_sem)
    for each in sums:
        pltpu.matmul_pop(each)

    half = 0.125
    decay = float(np.exp(np.float32(-0.25)))
    kick = float(np.sqrt(np.float32(1.0) - np.exp(np.float32(-0.25)) ** 2))
    push = half * (1.0 + decay)
    loads[3].wait()
    loads[4].wait()
    loads[5].wait()
    q = pos_ref[...]
    known = q.astype(jnp.bfloat16).astype(jnp.float32)
    p = mom_ref[...] - half * q
    total = x * y * c
    for k in range(steps):
        noise = noise_ref[k * total : (k + 1) * total].astype(jnp.float32)
        q = q + push * p + (half * kick) * noise
        drift = (q - known).astype(jnp.bfloat16).astype(jnp.float32)
        known = known + drift
        last = k == steps - 1
        p = decay * p + kick * noise - (half if last else 2 * half) * q
        loose[k] = drift
        for at in range(x):
            flat = turn(loose.at[k], at)
            if k == 0:
                turned_d[at] = flat
                for r in range(ring):
                    msge[r, at] = flat[r * zb : (r + 1) * zb].astype(jnp.bfloat16)
            else:
                flat = flat.astype(jnp.bfloat16)
                for r in range(ring):
                    msgd[k - 1, r, at] = flat[r * zb : (r + 1) * zb]
        if k == 0:
            start(turned_d.at[:, z - ROWS : z], edges_d.at[0], drift_edge_sem, {"gz": (iz + 1) % nz})
            start(turned_d.at[:, 0:ROWS], edges_d.at[1], drift_edge_sem, {"gz": (iz + nz - 1) % nz})
    fixed[0] = q
    fixed[1] = p

    def send_drift(k):
        if k == 0:
            to_owners(msge, gote.at[me], drift_sem[0])
        else:
            to_owners(msgd.at[k - 1], gotd.at[k - 1, me], drift_sem[k])

    @pl.when(outer)
    def _():
        pass_on(0)
        pass_on(1)

    arrive(drift_edge_sem, edges_d)
    for r in range(ring):
        beyond = []
        for at in range(x):
            before, after = around(turned_d, edges_d, r, at)
            beyond.append(jnp.where(upper, after, before))
        msge[r, x] = jnp.concatenate(beyond, axis=0).astype(jnp.bfloat16)

    def swapped(which):
        @pl.when(jnp.logical_not(outer))
        def _():
            arrive(swap_sem[which], all_w.at[which])

    at_lane = lax.broadcasted_iota(jnp.int32, (co, lane), 1)

    def build(which):
        def place(gx, carry):
            row = pl.multiple_of(gx * co, co)
            for a in range(3):
                for cz in range(3):
                    moved = {}
                    for b in range(3):
                        t = a * 9 + b * 3 + cz
                        tile, spot = t // per, t % per
                        held_at = tile // half_tiles, tile % half_tiles
                        for side in range(2):
                            pieces = []
                            for gy in range(ny):
                                r = gy * nx + gx + (gy % 2) * (nx - 1 - 2 * gx)
                                piece = all_w[which, r, held_at[0], held_at[1]]
                                shift = (side * ny + gy - spot) % per
                                pieces.append(pltpu.roll(piece, shift * ci, 1) if shift else piece)
                            moved[b, side] = pieces
                    pairs = []
                    for b in range(yy):
                        value = jnp.zeros((co, lane), jnp.bfloat16)
                        for side in range(y):
                            near = (b + side) % yy
                            if near > 2:
                                continue
                            for gy in range(ny):
                                spot = (side * ny + gy) * ci
                                inside = (at_lane >= spot) & (at_lane < spot + ci)
                                value = jnp.where(inside, moved[near, side][gy], value)
                        pairs.append(value)
                    for yo in range(yy):
                        for h in range(yy // y):
                            mats[which, a * 3 + cz, pl.ds(yo * c + row, co), h * lane : (h + 1) * lane] = (
                                pairs[(h * y + 1 - yo) % yy]
                            )
            return carry

        lax.fori_loop(0, nx, place, 0)

    def turn_over(which):
        for tap in range(9):
            flipped[which, tap] = mats[which, tap].T

    def scatter(target, zs, value, r, at):
        gx, gy = ring_place(r, nx)
        target[gy, pl.ds(zs * xx + gx * x + at, value.shape[0], stride=xx), :] = value

    def whole(ref, rows_from, rows_to):
        return jnp.concatenate([ref[gy, rows_from:rows_to] for gy in range(ny)], axis=1)

    left = device((me + ring - 1 + iz) % ring, 1 - iz)
    right = device((me + iz) % ring, 1 - iz)
    edge = reach * xx

    def send_halo(slot, value):
        qb[slot] = value.astype(jnp.bfloat16)
        start(qb.at[slot, rows - 2 * edge : rows], halo.at[slot, 0], halo_sem[slot], right)
        start(qb.at[slot, 0 : 2 * edge], halo.at[slot, 1], halo_sem[slot], left)

    def with_halo(slot, value):
        arrive(halo_sem[slot], halo.at[slot])
        ends = [halo[slot, side].astype(jnp.float32) for side in range(2)]
        return jnp.concatenate([ends[0], value, ends[1]], axis=0)

    arrive(field_sem, got0)
    for r in range(ring):
        for at in range(x):
            scatter(stage, 0, got0[r, at].astype(jnp.float32), r, at)
    send_halo(0, whole(stage, 0, rows))
    send_drift(0)

    @pl.when(outer)
    def _():
        take_across(0)

    swapped(0)
    for later in range(1, steps):
        send_drift(later)
    build(0)

    def spread(value):
        n = value.shape[0]
        cube = value.reshape(n // xx, xx, wide)
        for a in range(3):
            moved = cube if a == 1 else pltpu.roll(cube, (1 - a) % xx, 1)
            moved = moved.reshape(n, wide)
            lhs[a, 0, 0:n] = moved.astype(jnp.bfloat16)
            lhs[a, 1, 0 : n - 2 * xx] = moved[xx : n - xx].astype(jnp.bfloat16)

    def conv(height, which, adjoint, flip=False):
        low, high = split_rows(height)
        return jnp.concatenate(conv_at((0, low), low, high, which, adjoint, flip), axis=0)

    def conv_at(spots, low, high, which, adjoint, flip=False):
        source = mats if adjoint or flip else flipped
        sums = [[banks[unit, low, 0], banks[unit, high, int(low == high)]] for unit in range(2)]
        plans = (
            [(4, True, False), (3, True, True), (0, True, True), (1, True, True), (2, True, True)],
            [(4, False, True), (5, True, True), (8, True, True), (7, True, True), (6, True, True)],
        )
        for at in range(5):
            for unit in range(2):
                tap, use_low, use_high = plans[unit][at]
                a, cz = tap // 3, tap % 3
                pltpu.matmul_push_rhs(
                    source[which, 8 - tap if adjoint else tap],
                    staging_register=at % 2,
                    mxu_index=unit,
                    transpose=flip,
                )
                copy, first_row = (1, 0) if cz == 1 else (0, cz * xx)
                fresh = at % 2
                if use_low:
                    begin = first_row + spots[0]
                    left = lhs[a, copy, begin : begin + low]
                    pltpu.matmul_acc_lhs(sums[unit][0], left, load_staged_rhs=fresh)
                    fresh = None
                if use_high:
                    begin = first_row + spots[1]
                    left = lhs[a, copy, begin : begin + high]
                    pltpu.matmul_acc_lhs(sums[unit][1], left, load_staged_rhs=fresh)
        return [pltpu.matmul_pop(sums[0][part]) + pltpu.matmul_pop(sums[1][part]) for part in range(2)]

    row = jnp.concatenate([bias_ref[...]] * yy, axis=1)

    def gradient(extent, between=lambda: None, flip=False):
        n = [rows + 2 * (extent + 3 - i) * xx for i in range(4)]
        t = jnp.tanh(conv(n[0], 0, False, flip) + row)
        if flip:
            turn_over(0)
        t_ref[0 : n[0]] = t
        spread(t)
        between()
        out = conv(n[1], 1, False, flip)
        if flip:
            turn_over(1)
        spread(out)
        gu = conv(n[2], 1, True)
        t = t_ref[2 * xx : 2 * xx + n[2]]
        spread(gu * (1.0 - t * t))
        return conv(n[3], 0, True)

    def inner(q):
        n = [rows - 2 * (i + 1) * xx for i in range(4)]
        spread(q)
        t = jnp.tanh(conv(n[0], 0, False) + row)
        mid[0, 0 : n[0]] = t
        spread(t)
        out = conv(n[1], 1, False)
        mid[1, 0 : n[1]] = out
        spread(out)
        gu = conv(n[2], 1, True)
        t = t[2 * xx : 2 * xx + n[2]]
        out = gu * (1.0 - t * t)
        mid[2, 0 : n[2]] = out
        spread(out)
        mid[3, 0 : n[3]] = conv(n[3], 0, True)

    def outside(slot, q):
        n = [rows - 2 * (i + 1) * xx for i in range(4)]
        side = 2 * edge
        two = 2 * xx

        def both(which, adjoint):
            return conv_at((0, side + two), side, side, which, adjoint)

        arrive(halo_sem[slot], halo.at[slot])
        ends = [halo[slot, at].astype(jnp.float32) for at in range(2)]
        spread(jnp.concatenate([ends[0], q[0:two], q[rows - two :], ends[1]], axis=0))
        ends = [jnp.tanh(each + row) for each in both(0, False)]
        t = [
            jnp.concatenate([ends[0], mid[0, 0:two]], axis=0),
            jnp.concatenate([mid[0, n[0] - two : n[0]], ends[1]], axis=0),
        ]
        spread(jnp.concatenate(t, axis=0))
        ends = both(1, False)
        spread(jnp.concatenate([ends[0], mid[1, 0:two], mid[1, n[1] - two : n[1]], ends[1]], axis=0))
        gu = both(1, True)
        near = t[0][two:], t[1][0:side]
        ends = [each * (1.0 - at * at) for each, at in zip(gu, near)]
        spread(jnp.concatenate([ends[0], mid[2, 0:two], mid[2, n[2] - two : n[2]], ends[1]], axis=0))
        ends = both(0, True)
        return jnp.concatenate([ends[0], mid[3, 0 : n[3]], ends[1]], axis=0)

    def take_drift(k):
        arrive(drift_sem[k], gotd.at[k - 1])
        for r in range(ring):
            for at in range(x):
                scatter(extra, 0, gotd[k - 1, r, at].astype(jnp.float32), r, at)
        base[...] = base[...] + whole(extra, 0, rows)

    def second_filters():
        swapped(1)
        build(1)

    def collect(ref, r, at):
        gx, gy = ring_place(r, nx)
        return ref[gy, pl.ds(gx * x + at, zb, stride=xx), :]

    def put(ref, value):
        for gy in range(ny):
            ref[gy] = value[:, gy * lane : (gy + 1) * lane]

    @pl.when(outer)
    def _():
        take_across(1)

    base[...] = whole(stage, 0, rows)
    spread(with_halo(0, base[...]))
    g = gradient(reach, second_filters, True)

    arrive(drift_sem[0], gote)
    for r in range(ring):
        beyond = gote[r, x].astype(jnp.float32)
        for at in range(x):
            scatter(extra, 0, gote[r, at].astype(jnp.float32), r, at)
            scatter(extra, zb, beyond[at * ROWS : (at + 1) * ROWS], r, at)
    now = base[...] + whole(extra, 0, rows)
    base[...] = now
    below = halo[0, 0, edge : 2 * edge].astype(jnp.float32) + whole(extra, rows + edge, rows + 2 * edge)
    above = halo[0, 1, 0:edge].astype(jnp.float32) + whole(extra, rows, rows + edge)
    force = g[edge : edge + rows]
    put(dp, -half * force)
    put(dq, (-half * push) * force)
    spread(jnp.concatenate([below, now, above], axis=0) + (-half * push) * g)

    mine = pl.ds(pl.multiple_of(filed * zb, zb), zb)

    def kicked(g):
        shift = whole(dq, 0, rows)
        now = decay * whole(dp, 0, rows) - (2 * half) * (g + shift)
        put(dp, now)
        put(dq, shift + push * now)

    for pair in range(pairs):
        kicked(gradient(0))
        k = 2 * pair + 2
        take_drift(k - 1)
        q = base[...] + whole(dq, 0, rows)
        send_halo(pair + 1, q)
        take_drift(k)
        shift = whole(dq, 0, rows)
        v = base[...] + shift + push * (decay * whole(dp, 0, rows) - (2 * half) * shift)
        vb[pair] = v.astype(jnp.bfloat16)
        start(vb.at[pair, rows - edge : rows], ring_v.at[pair, 0], v_sem[pair], right)
        start(vb.at[pair, 0:edge], ring_v.at[pair, 1], v_sem[pair], left)
        inner(q)
        g = outside(pair + 1, q)
        kicked(g[edge : edge + rows])
        q = base[...] + whole(dq, 0, rows)
        arrive(v_sem[pair], ring_v.at[pair])
        ends = [
            ring_v[pair, side].astype(jnp.float32) - (2 * half * push) * g[at : at + edge]
            for side, at in enumerate((0, edge + rows))
        ]
        spread(jnp.concatenate([ends[0], q, ends[1]], axis=0))

    put(dp, decay * whole(dp, 0, rows) - half * whole(dq, 0, rows))

    def return_q():
        for r in range(ring):
            for at in range(x):
                back_q[r, at] = collect(dq, r, at)
        to_sources(back_q, got_q.at[:, mine], q_sem)

    return_q()
    g = gradient(0)
    put(dp, whole(dp, 0, rows) - half * g)
    for r in range(ring):
        for at in range(x):
            back_p[r, at] = collect(dp, r, at)
    to_sources(back_p, got_p.at[:, mine], p_sem)

    def untie(value, which, out, at):
        flat = value.T
        for j in range(y):
            part = pl.ds(at * y + j, c, stride=x * y)
            out[part, :] = fixed[which, part, :] + flat[j * c : (j + 1) * c]

    arrive(q_sem, got_q)
    for at in range(x):
        untie(got_q[at], 0, q_out, at)
    arrive(p_sem, got_p)
    for at in range(x):
        untie(got_p[at], 1, p_out, at)

    @pl.when(outer)
    def _():
        for which in range(2):
            for number in column_sems[which]:
                leave(number, own_w.at[which, 0])
            for number in across_sems[which]:
                leave(number, all_w.at[which, 0:nx, 0])
            leave(swap_sem[which], all_w.at[which])

    leave(drift_edge_sem, edges_d)
    left_ring(field_sem, msg0)
    left_ring(drift_sem[0], msge)
    for k in range(1, steps):
        left_ring(drift_sem[k], msgd.at[k - 1])
    for slot in range(pairs + 1):
        leave(halo_sem[slot], halo.at[slot])
    for pair in range(pairs):
        leave(v_sem[pair], ring_v.at[pair])
    left_ring(q_sem, back_q)
    left_ring(p_sem, back_p)


def copy_out(q_ref, p_ref, q_out, p_out, sems):
    copies = [
        pltpu.make_async_copy(q_ref, q_out, sems.at[0]),
        pltpu.make_async_copy(p_ref, p_out, sems.at[1]),
    ]
    for copy in copies:
        copy.start()
    for copy in copies:
        copy.wait()


def fits_ring(steps, sizes, position, filter_in):
    nx, ny, nz = sizes
    c, x, y, z = position.shape
    co, ci = filter_in.shape[:2]
    ring = nx * ny
    return (
        steps % 2 == 1 and steps > 2 and nz == 2 and ny == 2 and nx > 1 and y * c == LANES and x * nx == ROWS and y * ny > 2
        and z % (ring * EDGE) == 0 and z // ring == EDGE and co % EDGE == 0 and LANES % ci == 0
        and y * ny * ci == LANES
    )


def on_ring(sizes, position, momentum, noise, filter_in, filter_out, bias):
    nx, ny, nz = sizes
    c, x, y, z = position.shape
    steps = noise.shape[0]
    co, ci = filter_in.shape[:2]
    ring = nx * ny
    zb = z // ring
    xx, yy = x * nx, y * ny
    wide = yy * c
    rows = zb * xx
    lane = LANES
    half_tiles = -(-27 * ci // (2 * lane))
    flat = jax.ShapeDtypeStruct((c * x * y, z), jnp.float32)
    reach, pairs = 4, (steps - 1) // 2
    copies = 2 * nx + 11 + steps + 2 * pairs
    edge = reach * xx
    heights = [(zb + 2 * beyond) * xx for beyond in range(-reach, 2 * reach)]
    vmem = pl.BlockSpec(memory_space=pltpu.VMEM)
    bf16, f32 = jnp.bfloat16, jnp.float32
    q, p = pl.pallas_call(
        functools.partial(ring_kernel, steps, sizes, heights),
        out_shape=(flat, flat),
        in_specs=[pl.BlockSpec(memory_space=pl.ANY)] * 6,
        out_specs=(vmem, vmem),
        scratch_shapes=[
            pltpu.VMEM((c * x * y, z), f32),
            pltpu.VMEM((c * x * y, z), f32),
            pltpu.VMEM((steps * c * x * y, z), bf16),
            pltpu.VMEM((27, co, ci), bf16),
            pltpu.VMEM((27, co, ci), bf16),
            pltpu.VMEM((1, c), f32),
            pltpu.VMEM((2, 2, half_tiles, co, lane), bf16),
            pltpu.VMEM((2, ring, 2, half_tiles, co, lane), bf16),
            pltpu.VMEM((2, 9, wide, wide), bf16),
            pltpu.VMEM((2, 9, wide, wide), bf16),
            pltpu.VMEM((x, z, lane), f32),
            pltpu.VMEM((ring, x, zb, lane), bf16),
            pltpu.VMEM((ring, x, zb, lane), bf16),
            pltpu.VMEM((steps - 1, ring, x, zb, lane), bf16),
            pltpu.VMEM((steps - 1, ring, x, zb, lane), bf16),
            pltpu.VMEM((ny, rows, lane), f32),
            pltpu.VMEM((3, 2, rows + 4 * edge, wide), bf16),
            pltpu.VMEM((rows + 4 * edge - 2 * xx, wide), f32),
            pltpu.VMEM((rows, wide), f32),
            pltpu.VMEM((ny, rows + 2 * edge, lane), f32),
            pltpu.VMEM((ny, rows, lane), f32),
            pltpu.VMEM((ny, rows, lane), f32),
            pltpu.VMEM((pairs + 1, rows, wide), bf16),
            pltpu.VMEM((pairs + 1, 2, 2 * edge, wide), bf16),
            pltpu.VMEM((pairs, rows, wide), bf16),
            pltpu.VMEM((pairs, 2, edge, wide), bf16),
            pltpu.VMEM((ring, x, zb, lane), f32),
            pltpu.VMEM((x, z, lane), f32),
            pltpu.VMEM((ring, x, zb, lane), f32),
            pltpu.VMEM((x, z, lane), f32),
            pltpu.VMEM((2, c * x * y, z), f32),
            pltpu.VMEM((steps, c * x * y, z), f32),
            pltpu.VMEM((2, x, ROWS, lane), f32),
            pltpu.VMEM((ring, x + 1, zb, lane), bf16),
            pltpu.VMEM((ring, x + 1, zb, lane), bf16),
            pltpu.VMEM((4, rows - 2 * xx, wide), f32),
            pltpu.SemaphoreType.DMA((copies,)),
            pltpu.SemaphoreType.DMA((copies,)),
            pltpu.SemaphoreType.DMA((6,)),
        ],
        compiler_params=pltpu.CompilerParams(
            collective_id=0, has_side_effects=True, vmem_limit_bytes=24 * 2**20
        ),
    )(
        *(
            pltpu.with_memory_space_constraint(each, pltpu.HBM)
            for each in (
                position.reshape(-1, z),
                momentum.reshape(-1, z),
                noise.reshape(-1, z),
                filter_in.transpose(2, 3, 4, 0, 1).reshape(27, co, ci),
                filter_out.transpose(2, 3, 4, 0, 1).reshape(27, co, ci),
                bias[None],
            )
        )
    )
    q, p = pl.pallas_call(
        copy_out,
        out_shape=(flat, flat),
        in_specs=[pl.BlockSpec(memory_space=pl.ANY)] * 2,
        out_specs=[pl.BlockSpec(memory_space=pl.ANY)] * 2,
        scratch_shapes=[pltpu.SemaphoreType.DMA((2,))],
        compiler_params=pltpu.CompilerParams(vmem_limit_bytes=2**20),
    )(q, p)
    return q.reshape(position.shape), p.reshape(momentum.shape)


def on_device(groups, sizes, position, momentum, noise, filter_in, filter_out, bias):
    if groups == 2 and fits_ring(noise.shape[0], sizes, position, filter_in):
        return on_ring(sizes, position, momentum, noise, filter_in, filter_out, bias)
    nx, ny, nz = sizes
    c, x, y, z = position.shape
    steps = noise.shape[0]
    assert x >= 2 and y == 2 and z % EDGE == 0 and nx > 2 and ny > 1
    both = jnp.stack([filter_in, filter_out])
    co, ci = both.shape[1], both.shape[2]
    gather = []
    if co % EDGE == 0:
        both = both.transpose(0, 1, 3, 5, 4, 2).reshape(2, co, 27 * ci)
        gather = [
            pltpu.VMEM((ny, nx, 2, co, 27 * ci), jnp.bfloat16),
            pltpu.VMEM((2, 9, 3, c, c), jnp.bfloat16),
            pltpu.SemaphoreType.DMA((nx * ny - 1,)),
            pltpu.SemaphoreType.DMA((nx * ny - 1,)),
        ]
    else:
        both = both.reshape(2 * co, ci * 27)
        both = lax.all_gather(both, ("gx", "gy"), axis=0, tiled=True)
        both = both.reshape(nx, ny, 2, co, ci, 3, 3, 3)
        both = both.transpose(2, 5, 7, 6, 0, 3, 1, 4).reshape(2, 9, 3, c, c)
    lanes = y * c
    slots = 2 * y if ny == 2 else 3 * y
    full = z + 2 * EDGE
    wide = (y + 2) * c
    flat = jax.ShapeDtypeStruct((c, x * y * z), jnp.float32)
    copies = 15 if ny == 2 else 24
    vmem = pl.BlockSpec(memory_space=pltpu.VMEM)
    q, p = pl.pallas_call(
        functools.partial(kernel, steps, sizes),
        out_shape=(flat, flat),
        in_specs=[vmem] * 5,
        out_specs=(vmem, vmem),
        scratch_shapes=[
            pltpu.VMEM((9, wide, slots * c), jnp.bfloat16),
            pltpu.VMEM((9, lanes, wide), jnp.bfloat16),
            pltpu.VMEM((9, wide, lanes), jnp.bfloat16),
            pltpu.VMEM((9, slots * c, wide), jnp.bfloat16),
            pltpu.VMEM((x + 4, full, slots * c), jnp.bfloat16),
            pltpu.VMEM((x + 4, full, slots * c), jnp.bfloat16),
            pltpu.VMEM((x + 2, full, wide), jnp.float32),
            pltpu.VMEM((x, z, lanes), jnp.float32),
            pltpu.VMEM((x, z, lanes), jnp.float32),
            pltpu.SemaphoreType.DMA((2, copies)),
            pltpu.SemaphoreType.DMA((2, copies)),
            *gather,
        ],
        compiler_params=pltpu.CompilerParams(
            collective_id=0, has_side_effects=True, vmem_limit_bytes=56 * 2**20
        ),
    )(
        position.reshape(c, -1),
        momentum.reshape(c, -1),
        noise.reshape(steps, c, -1),
        both,
        jnp.tile(bias, y + 2)[None],
    )
    return q.reshape(position.shape), p.reshape(momentum.shape)


def solution(mesh):
    field = P(None, ("grp", "gx"), "gy", "gz")
    filters = P("gx", "gy", None, None, None)
    sizes = tuple(mesh.shape[name] for name in ("gx", "gy", "gz"))
    groups = mesh.shape["grp"]
    return jax.shard_map(
        functools.partial(on_device, groups, sizes),
        mesh=mesh,
        in_specs=(field, field, P(None, None, ("grp", "gx"), "gy", "gz"), filters, filters, P()),
        out_specs=(field, field),
        check_vma=False,
    )
```
